8 devices in a mesh: col: 4 (over z, y, x), row: 2 (over core).
Axes of the slice: x: 2, y: 2, z: 1, core: 2. Of those that a mesh axis runs over, the one named last changes fastest.
Arguments:
- trans_mat: bfloat16 [24576, 24576], P('row', 'col')
- x_start: float32 [24576, 256], P(('col', 'row'))
- teleport: float32 [24576, 256], P(('col', 'row'))
- dangling: int32 [24576], P(('col', 'row'))
Outputs:
- output: float32 [24576, 256], P(('col', 'row'))
All inputs are finite; a program needn't handle non-finite values.
Results may differ from the reference program's by a relative error of at most 0.001.
Values are sent between devices in bfloat16 or wider.
A program may use at most 1 GiB of HBM per device.

```python
import jax
import jax.numpy as jnp
from jax import lax

VERTICES = 24576
VECS = 256
DEGREE = 19
SWEEPS = 8
DAMPING = 0.85


def draw_graph(key_dang, key_target, key_edge):
    dangling = (jax.random.randint(key_dang, (VERTICES,), 0, 5) == 0).astype(jnp.int32)
    live_cols = (1 - dangling).astype(jnp.bfloat16)
    target = jax.random.randint(key_target, (VERTICES,), 0, VERTICES)
    row_blocks = 16
    block_rows = VERTICES // row_blocks
    block_keys = jax.random.split(key_edge, row_blocks)
    block_starts = jnp.arange(row_blocks, dtype=jnp.int32) * block_rows

    def edge_block(block_args):
        block_key, block_start = block_args
        draw_vals = jax.random.randint(block_key, (block_rows, VERTICES), 0, VERTICES)
        row_ids = block_start + jnp.arange(block_rows, dtype=jnp.int32)[:, None]
        edge_mask = (draw_vals < DEGREE) | (row_ids == target[None, :])
        return edge_mask.astype(jnp.bfloat16) * live_cols[None, :]

    adjacency = lax.map(edge_block, (block_keys, block_starts)).reshape(VERTICES, VERTICES)
    out_degree = jnp.sum(adjacency, axis=0, dtype=jnp.float32)
    inv_degree = (1.0 / jnp.maximum(out_degree, 1.0)).astype(jnp.bfloat16)
    trans_mat = adjacency * inv_degree[None, :]
    return trans_mat, dangling


def setup_inputs(seed: int = 0) -> dict:
    base_key = jax.random.key(seed)
    k_dang, k_target, k_edge, k_start, k_scale, k_center, k_weight = jax.random.split(base_key, 7)
    trans_mat, dangling = draw_graph(k_dang, k_target, k_edge)
    col_scale = 2.0 ** jax.random.uniform(k_scale, (1, VECS), jnp.float32, -2.0, 2.0)
    x_start = jax.random.uniform(k_start, (VERTICES, VECS), jnp.float32, 0.0, 2.0) * col_scale
    centers = jax.random.randint(k_center, (1, VECS), 0, VERTICES)
    offsets = (jnp.arange(VERTICES, dtype=jnp.int32)[:, None] - centers) % VERTICES
    inside = (offsets < VERTICES // 8).astype(jnp.float32)
    raw_tele = inside * jax.random.uniform(k_weight, (VERTICES, VECS), jnp.float32, 0.5, 2.0)
    teleport = raw_tele * (VERTICES / jnp.sum(raw_tele, axis=0, keepdims=True))
    return {'trans_mat': trans_mat, 'x_start': x_start, 'teleport': teleport, 'dangling': dangling}


def reference(trans_mat, x_start, teleport, dangling):
    dang_col = dangling.astype(jnp.float32)[:, None]

    def one_sweep(x_cur, unused):
        dang_mass = jnp.sum(dang_col * x_cur, axis=0) / VERTICES
        spread = jnp.dot(trans_mat, x_cur.astype(jnp.bfloat16), preferred_element_type=jnp.float32)
        x_next = DAMPING * spread + (DAMPING * dang_mass + (1.0 - DAMPING))[None, :] * teleport
        return x_next, None

    x_final, unused_out = lax.scan(one_sweep, x_start, None, length=SWEEPS)
    return x_final
```

```python
import functools

import jax
import jax.numpy as jnp
from jax import lax
from jax.experimental import pallas as pl
from jax.experimental.pallas import tpu as pltpu
from jax.sharding import PartitionSpec as P

SWEEPS = 8
DAMPING = 0.85
MESH = pl.DeviceIdType.MESH

VERTS = 24576
VECS = 256
PIECE = 3072
ROWS = 12288
COLS = 6144
BR = 256
NB = PIECE // BR
CH = 32
RING = 4


def kernel(a_hbm, x_hbm, v_hbm, d_hbm, out_hbm,
           abuf, xbf, ybuf, ra, rgy, rdy, rfx, rfy, vbuf, dbuf, sbuf, s0buf, coef,
           a_sem, in_sem, ina_send, ina_recv,
           a_s, a_r, gy_s, gy_r, dy_s, dy_r, fx_s, fx_r, fy_s, fy_r,
           x_s, x_r, s_s, s_r, s0_s, s0_r, o_l, o_s, o_r,
           cr_hh, cr_hw, cr_gy, cr_ww, cr_x):
    col = lax.axis_index('col')
    row = lax.axis_index('row')
    cx, cy = lax.rem(col, 2), lax.div(col, 2)
    home = row == cy
    xn = (cy * 2 + 1 - cx, row)
    yn = ((1 - cy) * 2 + cx, row)
    mate = (col, 1 - row)
    same = cx * COLS
    other = (1 - cx) * COLS

    barrier = pltpu.get_barrier_semaphore()
    for off in range(4):
        for r in range(2):
            if off == 0 and r == 1:
                continue
            dev = (lax.rem(col + off, 4), row if r == 0 and off else 1 - row)
            pl.semaphore_signal(barrier, inc=1, device_id=dev, device_id_type=MESH)

    def blk(n):
        return pl.ds(pl.multiple_of(n * BR, BR), BR)

    def rows_at(base, t, b):
        return pl.ds(pl.multiple_of(base + t * PIECE + b * BR, BR), BR)

    def remote(src, dst, send, recv, dev):
        return pltpu.make_async_remote_copy(
            src_ref=src, dst_ref=dst, send_sem=send, recv_sem=recv, device_id=dev, device_id_type=MESH)

    def c_a(b):
        return remote(ybuf.at[rows_at(other, 0, b)], ra.at[blk(b)], a_s.at[b], a_r.at[b], xn)

    def c_gy(b):
        return remote(ybuf.at[rows_at(other, 1, b)], rgy.at[blk(b)], gy_s.at[b], gy_r.at[b], yn)

    def c_dy(b):
        return remote(ybuf.at[rows_at(same, 1, b)], rdy.at[blk(b)], dy_s.at[b], dy_r.at[b], yn)

    def c_fx(b):
        return remote(ybuf.at[rows_at(other, 1, b)], rfx.at[blk(b)], fx_s.at[b], fx_r.at[b], xn)

    def c_fy(b):
        return remote(ybuf.at[rows_at(same, 0, b)], rfy.at[blk(b)], fy_s.at[b], fy_r.at[b], yn)

    def c_x(n):
        return remote(xbf.at[blk(n)], xbf.at[blk(n)], x_s.at[n], x_r.at[n], mate)

    def block_of(n):
        m = lax.rem(n, 2 * NB)
        first = n < 2 * NB
        t = jnp.where(first, lax.rem(m, 2), 1 - lax.div(m, NB))
        b = jnp.where(first, lax.div(m, 2), lax.rem(m, NB))
        return jnp.where(first, other, same) + t * PIECE + b * BR

    def a_copy(n):
        slot = lax.rem(n, RING)
        start = pl.multiple_of(block_of(n), BR)
        return pltpu.make_async_copy(a_hbm.at[pl.ds(start, BR)], abuf.at[slot], a_sem.at[slot])

    x_in = pltpu.make_async_copy(x_hbm, ybuf.at[pl.ds(0, PIECE)], in_sem.at[0])
    x_in.start()
    piece = pl.ds(pl.multiple_of(row * PIECE, PIECE), PIECE)
    d_in = pltpu.make_async_copy(d_hbm, dbuf.at[piece], in_sem.at[1])
    d_in.start()
    for n in range(RING):
        a_copy(jnp.int32(n)).start()
    v_in = pltpu.make_async_copy(v_hbm, vbuf.at[piece], in_sem.at[2])

    @pl.when(home)
    def _():
        v_in.start()

    v_out = remote(v_hbm, vbuf.at[piece], ina_send.at[0], ina_recv.at[0], mate)
    d_out = remote(d_hbm, dbuf.at[piece], ina_send.at[1], ina_recv.at[1], mate)

    x_in.wait()
    d_in.wait()

    def convert(c, acc):
        x = ybuf[pl.ds(pl.multiple_of(c * CH, CH), CH), :]
        at = pl.ds(pl.multiple_of(row * PIECE + c * CH, CH), CH)
        d = dbuf[at, :]
        xbf[at, :] = x.astype(jnp.bfloat16)
        w = x * jnp.concatenate([d, d], axis=1)
        return acc + jnp.sum(w.reshape(CH // 8, 8, VECS), axis=0)

    s_own = lax.fori_loop(0, PIECE // CH, convert, jnp.zeros((8, VECS), jnp.float32))
    s0buf[row] = s_own
    pl.semaphore_wait(barrier, 7)

    s0_out = remote(s0buf.at[row], s0buf.at[row], s0_s, s0_r, mate)

    def x0_copy(r):
        at = pl.ds(pl.multiple_of(r * PIECE, PIECE), PIECE)
        return remote(xbf.at[at], xbf.at[at], ina_send.at[2], ina_recv.at[2], mate)

    x0_copy(row).start()

    @pl.when(jnp.logical_not(home))
    def _():
        v_out.start()
        d_out.start()
        s0_out.start()

    x0_copy(row).wait_send()
    x0_copy(1 - row).wait_recv()

    def s_copy(par, off):
        dst_col = lax.rem(col + off, 4)
        return remote(sbuf.at[par, col], sbuf.at[par, col], s_s.at[par, off], s_r.at[par, col],
                      (dst_col, lax.div(dst_col, 2)))

    def s_wait(par, off):
        src_col = lax.rem(col + off, 4)
        return remote(sbuf.at[par, src_col], sbuf.at[par, src_col], s_s.at[par, off], s_r.at[par, src_col],
                      (src_col, lax.div(src_col, 2)))

    def s_publish(par, value):
        sbuf[par, col] = value
        for off in range(1, 4):
            s_copy(par, off).start()

    def sweep(k, carry):
        last = k == SWEEPS - 1

        def multiply(n):
            slot = lax.rem(n, RING)
            a_copy(n).wait()
            start = pl.multiple_of(block_of(n), BR)
            ybuf[pl.ds(start, BR), :] = jnp.dot(abuf[slot], xbf[...], preferred_element_type=jnp.float32)
            after = n + RING

            @pl.when(jnp.logical_not(jnp.logical_and(last, after >= 4 * NB)))
            def _():
                a_copy(lax.rem(after, 4 * NB)).start()

        @pl.when(k > 0)
        def _():
            @pl.when(home)
            def _():
                pl.semaphore_wait(cr_hh, 1)

            @pl.when(jnp.logical_not(home))
            def _():
                pl.semaphore_wait(cr_ww, 1)
                pl.semaphore_wait(cr_gy, 1)

        def part_one(n, c):
            multiply(n)
            b = lax.div(n, 2)

            @pl.when(lax.rem(n, 2) == 0)
            def _():
                c_a(b).start()

            @pl.when(jnp.logical_and(lax.rem(n, 2) == 1, jnp.logical_not(home)))
            def _():
                c_gy(b).start()
            return c

        lax.fori_loop(0, 2 * NB, part_one, 0)

        @pl.when(jnp.logical_and(k > 0, jnp.logical_not(home)))
        def _():
            pl.semaphore_wait(cr_hw, 1)

        def part_two(n, c):
            multiply(n)

            @pl.when(jnp.logical_and(n < 3 * NB, jnp.logical_not(home)))
            def _():
                c_dy(n - 2 * NB).start()
            return c

        lax.fori_loop(2 * NB, 4 * NB, part_two, 0)

        def add_into(base, t, b, src):
            def step(c, z):
                at = pl.ds(pl.multiple_of(base + t * PIECE + b * BR + c * CH, CH), CH)
                ybuf[at, :] = ybuf[at, :] + src[pl.ds(pl.multiple_of(b * BR + c * CH, CH), CH), :]
                return z
            lax.fori_loop(0, BR // CH, step, 0)

        @pl.when(jnp.logical_not(home))
        def _away():
            @pl.when(jnp.logical_not(last))
            def _():
                pl.semaphore_signal(cr_x, inc=1, device_id=mate, device_id_type=MESH)

            def forward(b, c):
                c_a(b).wait()
                add_into(same, 0, b, ra)
                c_fy(b).start()
                return c
            lax.fori_loop(0, NB, forward, 0)

            @pl.when(jnp.logical_not(last))
            def _():
                pl.semaphore_signal(cr_ww, inc=1, device_id=xn, device_id_type=MESH)

            def drain(b, c):
                c_gy(b).wait_send()
                c_dy(b).wait_send()
                c_fy(b).wait_send()
                return c
            lax.fori_loop(0, NB, drain, 0)

            @pl.when(k == 0)
            def _():
                v_out.wait_send()
                d_out.wait_send()
                s0_out.wait_send()

            @pl.when(jnp.logical_not(last))
            def _():
                def take(n, c):
                    c_x(n).wait_recv()
                    return c
                lax.fori_loop(0, 2 * NB, take, 0)

        @pl.when(home)
        def _home():
            par = lax.rem(k, 2)

            @pl.when(k == 0)
            def _():
                v_in.wait()
                far = pl.ds(pl.multiple_of((1 - row) * PIECE, PIECE), PIECE)
                remote(v_hbm, vbuf.at[far], ina_send.at[0], ina_recv.at[0], mate).wait_recv()
                remote(d_hbm, dbuf.at[far], ina_send.at[1], ina_recv.at[1], mate).wait_recv()
                remote(s0buf.at[1 - row], s0buf.at[1 - row], s0_s, s0_r, mate).wait_recv()
                s_publish(0, s0buf[0] + s0buf[1])

            def forward(b, c):
                c_gy(b).wait_recv()
                add_into(other, 1, b, rgy)
                c_fx(b).start()
                return c
            lax.fori_loop(0, NB, forward, 0)

            @pl.when(jnp.logical_not(last))
            def _():
                pl.semaphore_signal(cr_gy, inc=1, device_id=yn, device_id_type=MESH)
                pl.semaphore_wait(cr_x, 1)

            for off in range(1, 4):
                s_wait(par, off).wait_recv()
                s_copy(par, off).wait_send()
            total = (sbuf[par, 0] + sbuf[par, 1]) + (sbuf[par, 2] + sbuf[par, 3])
            mass = jnp.sum(total, axis=0, keepdims=True) / VERTS
            coef[...] = jnp.broadcast_to(DAMPING * mass + (1.0 - DAMPING), (8, VECS))

            def update(t, b, one, two, acc):
                def step(c, acc):
                    at = pl.ds(pl.multiple_of(same + t * PIECE + b * BR + c * CH, CH), CH)
                    mine = pl.ds(pl.multiple_of(t * PIECE + b * BR + c * CH, CH), CH)
                    there = pl.ds(pl.multiple_of(b * BR + c * CH, CH), CH)
                    y = (ybuf[at, :] + one[there, :]) + two[there, :]
                    cf = jnp.concatenate([coef[...]] * (CH // 8), axis=0)
                    x = DAMPING * y + cf * vbuf[mine, :]
                    xbf[mine, :] = x.astype(jnp.bfloat16)
                    ybuf[at, :] = x
                    d = dbuf[mine, :]
                    w = x * jnp.concatenate([d, d], axis=1)
                    return acc + jnp.sum(w.reshape(CH // 8, 8, VECS), axis=0)
                return lax.fori_loop(0, BR // CH, step, acc)

            def finish_t(t, b):
                @pl.when(jnp.logical_not(last))
                def _():
                    c_x(t * NB + b).start()

                @pl.when(jnp.logical_and(last, row == t))
                def _():
                    pltpu.make_async_copy(ybuf.at[rows_at(same, t, b)], out_hbm.at[blk(b)], o_l.at[b]).start()

                @pl.when(jnp.logical_and(last, row != t))
                def _():
                    remote(ybuf.at[rows_at(same, t, b)], out_hbm.at[blk(b)], o_s.at[b], o_r.at[b], mate).start()

            def finish(b, acc):
                c_a(b).wait_recv()
                c_fy(b).wait_recv()
                acc = update(0, b, ra, rfy, acc)
                finish_t(0, b)
                c_dy(b).wait_recv()
                c_fx(b).wait_recv()
                acc = update(1, b, rdy, rfx, acc)
                finish_t(1, b)
                return acc

            s_new = lax.fori_loop(0, NB, finish, jnp.zeros((8, VECS), jnp.float32))

            @pl.when(jnp.logical_not(last))
            def _():
                pl.semaphore_signal(cr_hh, inc=1, device_id=xn, device_id_type=MESH)
                pl.semaphore_signal(cr_hw, inc=1, device_id=yn, device_id_type=MESH)
                s_publish(1 - par, s_new)

            def drain(b, c):
                c_a(b).wait_send()
                c_fx(b).wait_send()

                @pl.when(jnp.logical_not(last))
                def _():
                    c_x(b).wait_send()
                    c_x(NB + b).wait_send()
                return c
            lax.fori_loop(0, NB, drain, 0)

        return carry

    lax.fori_loop(0, SWEEPS, sweep, 0)

    def close(b, c):
        @pl.when(home)
        def _():
            pltpu.make_async_copy(ybuf.at[rows_at(same, row, b)], out_hbm.at[blk(b)], o_l.at[b]).wait()
            remote(ybuf.at[rows_at(same, 1 - row, b)], out_hbm.at[blk(b)], o_s.at[b], o_r.at[b], mate).wait_send()

        @pl.when(jnp.logical_not(home))
        def _():
            remote(ybuf.at[rows_at(same, 1 - row, b)], out_hbm.at[blk(b)], o_s.at[b], o_r.at[b], mate).wait_recv()
        return c

    lax.fori_loop(0, NB, close, 0)


def solution(mesh):
    dma = pltpu.SemaphoreType.DMA
    reg = pltpu.SemaphoreType.REGULAR

    def local_sweeps(mat_tile, x_piece, tele_piece, dang_piece):
        dang = jnp.broadcast_to(dang_piece.astype(jnp.float32)[:, None], (PIECE, 128))
        part = pltpu.VMEM((PIECE, VECS), jnp.float32)
        return pl.pallas_call(
            kernel,
            name="sweeps",
            out_shape=jax.ShapeDtypeStruct((PIECE, VECS), jnp.float32),
            in_specs=[pl.BlockSpec(memory_space=pl.ANY)] * 4,
            out_specs=pl.BlockSpec(memory_space=pl.ANY),
            scratch_shapes=[
                pltpu.VMEM((RING, BR, COLS), jnp.bfloat16),
                pltpu.VMEM((COLS, VECS), jnp.bfloat16),
                pltpu.VMEM((ROWS, VECS), jnp.float32),
                part, part, part, part, part,
                pltpu.VMEM((COLS, VECS), jnp.float32),
                pltpu.VMEM((COLS, 128), jnp.float32),
                pltpu.VMEM((2, 4, 8, VECS), jnp.float32),
                pltpu.VMEM((2, 8, VECS), jnp.float32),
                pltpu.VMEM((8, VECS), jnp.float32),
                dma((RING,)), dma((3,)), dma((3,)), dma((3,)),
                dma((NB,)), dma((NB,)), dma((NB,)), dma((NB,)), dma((NB,)), dma((NB,)),
                dma((NB,)), dma((NB,)), dma((NB,)), dma((NB,)),
                dma((2 * NB,)), dma((2 * NB,)), dma((2, 4)), dma((2, 4)), dma, dma,
                dma((NB,)), dma((NB,)), dma((NB,)),
                reg, reg, reg, reg, reg,
            ],
            compiler_params=pltpu.CompilerParams(
                collective_id=0, has_side_effects=True, vmem_limit_bytes=67_000_000),
            cost_estimate=pl.CostEstimate(
                flops=2 * ROWS * COLS * VECS * SWEEPS, bytes_accessed=2 * ROWS * COLS * SWEEPS, transcendentals=0),
        )(mat_tile, x_piece, tele_piece, dang)

    vec_spec = P(('col', 'row'), None)
    return jax.shard_map(local_sweeps, mesh=mesh,
                         in_specs=(P('row', 'col'), vec_spec, vec_spec, P(('col', 'row'))),
                         out_specs=vec_spec, check_vma=False)
```

```python
import jax
import jax.numpy as jnp
from jax import lax
from jax.experimental import pallas as pl
from jax.experimental.pallas import tpu as pltpu
from jax.sharding import PartitionSpec as P

SWEEPS = 8
DAMPING = 0.85
MESH = pl.DeviceIdType.MESH

VERTS = 24576
VECS = 256
HALF = 128
PIECE = 3072
ROWS = 12288
COLS = 6144
BR = 256
NB = PIECE // BR
G = 4
E = NB - G
CH = 32
RING = 4
X0C = 6
X0R = PIECE // X0C


def kernel(a_hbm, x_hbm, v_hbm, d_hbm, out_hbm,
           abuf, xbf, ybuf, ra, rgy, rdy, rfx, rfy, vbuf, dbuf, dint, sbuf, s0buf, coef, sacc,
           a_sem, xin_sem, in_sem, ina_send, ina_recv, x0_s, x0_r,
           a_s, a_r, gy_s, gy_r, dy_s, dy_r, fx_s, fx_r, fy_s, fy_r,
           x_s, x_r, s_s, s_r, s0_s, s0_r, o_l, o_s, o_r,
           cr_hh1, cr_hh2, cr_hw, cr_gy, cr_ww, cr_x):
    col = lax.axis_index('col')
    row = lax.axis_index('row')
    cx, cy = lax.rem(col, 2), lax.div(col, 2)
    home = row == cy
    away = jnp.logical_not(home)
    xn = (cy * 2 + 1 - cx, row)
    yn = ((1 - cy) * 2 + cx, row)
    mate = (col, 1 - row)
    same = cx * COLS
    other = (1 - cx) * COLS

    barrier = pltpu.get_barrier_semaphore()
    for off in range(4):
        for r in range(2):
            if off == 0 and r == 1:
                continue
            dev = (lax.rem(col + off, 4), row if r == 0 and off else 1 - row)
            pl.semaphore_signal(barrier, inc=1, device_id=dev, device_id_type=MESH)

    def signal(sem, dev):
        pl.semaphore_signal(sem, inc=1, device_id=dev, device_id_type=MESH)

    def rows_of(start, size):
        return pl.ds(pl.multiple_of(start, size), size)

    def blk(n):
        return rows_of(n * BR, BR)

    def cols(h):
        return pl.ds(0, VECS) if h is None else pl.ds(h * HALF, HALF)

    def slot_of(b, h, first):
        return b if h != 1 else NB + b - (0 if first else E)

    def remote(src, dst, send, recv, dev):
        return pltpu.make_async_remote_copy(
            src_ref=src, dst_ref=dst, send_sem=send, recv_sem=recv, device_id=dev, device_id_type=MESH)

    def flow(base, t, b, h, dst, send, recv, dev, first):
        i = slot_of(b, h, first)
        return remote(ybuf.at[rows_of(base + t * PIECE + b * BR, BR), cols(h)], dst.at[blk(b), cols(h)],
                      send.at[i], recv.at[i], dev)

    def c_a(b, h=None):
        return flow(other, 0, b, h, ra, a_s, a_r, xn, True)

    def c_gy(b, h=None):
        return flow(other, 1, b, h, rgy, gy_s, gy_r, yn, True)

    def c_dy(b):
        return flow(same, 1, b, None, rdy, dy_s, dy_r, yn, True)

    def c_fx(b, h=None):
        return flow(other, 1, b, h, rfx, fx_s, fx_r, xn, False)

    def c_fy(b, h=None):
        return flow(same, 0, b, h, rfy, fy_s, fy_r, yn, False)

    def c_x(t, b, h=None):
        at = rows_of(t * PIECE + b * BR, BR)
        i = t * (NB + G) + slot_of(b, h, False)
        return remote(xbf.at[at, cols(h)], xbf.at[at, cols(h)], x_s.at[i], x_r.at[i], mate)

    tf = jnp.where(home, 0, 1)

    def block_of(n):
        lead = n < 2 * G
        m = jnp.where(lead, n, n - 2 * G)
        t0 = jnp.where(lead, lax.div(m, G), lax.rem(m, 2))
        b0 = jnp.where(lead, lax.rem(m, G), G + lax.div(m, 2))
        t0 = jnp.where(t0 == 0, tf, 1 - tf)
        m = n - 2 * NB
        first = n < 2 * NB
        t = jnp.where(first, t0, 1 - lax.div(m, NB))
        b = jnp.where(first, b0, lax.rem(m, NB))
        return jnp.where(first, other, same) + t * PIECE + b * BR

    def a_copy(n):
        slot = lax.rem(n, RING)
        return pltpu.make_async_copy(a_hbm.at[rows_of(block_of(n), BR)], abuf.at[slot], a_sem.at[slot])

    def loop(lo, hi, body):
        def step(i, c):
            body(i)
            return c
        lax.fori_loop(lo, hi, step, 0)

    mine = row * PIECE
    far = (1 - row) * PIECE
    piece = rows_of(mine, PIECE)
    far_piece = rows_of(far, PIECE)

    def x_in(c):
        return pltpu.make_async_copy(x_hbm.at[rows_of(c * X0R, X0R)], vbuf.at[rows_of(mine + c * X0R, X0R)], xin_sem.at[c])

    def x0_copy(base, c):
        at = rows_of(base + c * X0R, X0R)
        return remote(xbf.at[at], xbf.at[at], x0_s.at[c], x0_r.at[c], mate)

    for c in range(X0C):
        x_in(c).start()
    d_in = pltpu.make_async_copy(d_hbm, dint.at[row], in_sem.at[0])
    v_in = pltpu.make_async_copy(v_hbm, vbuf.at[piece], in_sem.at[1])
    v_out = remote(v_hbm, vbuf.at[piece], ina_send.at[0], ina_recv.at[0], mate)
    d_out = remote(d_hbm, dint.at[row], ina_send.at[1], ina_recv.at[1], mate)
    s0_out = remote(s0buf.at[row], s0buf.at[row], s0_s, s0_r, mate)

    for c in range(X0C):
        x_in(c).wait()

        def convert(i, c=c):
            at = rows_of(mine + c * X0R + i * CH, CH)
            xbf[at, :] = vbuf[at, :].astype(jnp.bfloat16)
        loop(0, X0R // CH, convert)
        if c == 0:
            pl.semaphore_wait(barrier, 7)
        x0_copy(mine, c).start()
        if c < RING:
            a_copy(jnp.int32(c)).start()
    d_in.start()

    @pl.when(away)
    def _():
        d_out.start()
        v_out.start()

    for c in range(X0C):
        x0_copy(far, c).wait_recv()

    def s_copy(par, off):
        dst_col = lax.rem(col + off, 4)
        return remote(sbuf.at[par, col], sbuf.at[par, col], s_s.at[par, off], s_r.at[par, col],
                      (dst_col, lax.div(dst_col, 2)))

    def s_wait(par, off):
        src_col = lax.rem(col + off, 4)
        return remote(sbuf.at[par, src_col], sbuf.at[par, src_col], s_s.at[par, off], s_r.at[par, src_col],
                      (src_col, lax.div(src_col, 2)))

    def s_publish(par, value):
        sbuf[par, col] = value
        for off in range(1, 4):
            s_copy(par, off).start()

    def spread(r):
        def group(g):
            flags = dint[r, pl.ds(g, 1), :].astype(jnp.float32)
            dbuf[rows_of(r * PIECE + g * 128, 128), :] = jnp.broadcast_to(flags, (128, 128)).T
        loop(0, PIECE // 128, group)

    def first_mass():
        d_in.wait()
        spread(row)

        def add(c, acc):
            at = rows_of(mine + c * CH, CH)
            d = dbuf[at, :]
            w = vbuf[at, :] * jnp.concatenate([d, d], axis=1)
            return acc + jnp.sum(w.reshape(CH // 8, 8, VECS), axis=0)
        s0buf[row] = lax.fori_loop(0, PIECE // CH, add, jnp.zeros((8, VECS), jnp.float32))

    def update(t, b, h, one, two, acc):
        def step(c, acc):
            at = rows_of(same + t * PIECE + b * BR + c * CH, CH)
            own = rows_of(t * PIECE + b * BR + c * CH, CH)
            there = rows_of(b * BR + c * CH, CH)
            y = (ybuf[at, cols(h)] + one[there, cols(h)]) + two[there, cols(h)]
            cf = jnp.concatenate([coef[:, cols(h)]] * (CH // 8), axis=0)
            x = DAMPING * y + cf * vbuf[own, cols(h)]
            xbf[own, cols(h)] = x.astype(jnp.bfloat16)
            ybuf[at, cols(h)] = x
            d = dbuf[own, :]
            if h is None:
                d = jnp.concatenate([d, d], axis=1)
            return acc + jnp.sum((x * d).reshape(CH // 8, 8, d.shape[1]), axis=0)
        return lax.fori_loop(0, BR // CH, step, acc)

    def o_local(t, b, h):
        i = slot_of(b, h, False)
        return pltpu.make_async_copy(
            ybuf.at[rows_of(same + t * PIECE + b * BR, BR), cols(h)], out_hbm.at[blk(b), cols(h)], o_l.at[i])

    def o_remote(t, b, h):
        i = slot_of(b, h, False)
        return remote(ybuf.at[rows_of(same + t * PIECE + b * BR, BR), cols(h)], out_hbm.at[blk(b), cols(h)],
                      o_s.at[i], o_r.at[i], mate)

    def emit(t, b, h, last):
        @pl.when(jnp.logical_not(last))
        def _():
            c_x(t, b, h).start()

        @pl.when(jnp.logical_and(last, row == t))
        def _():
            o_local(t, b, h).start()

        @pl.when(jnp.logical_and(last, row != t))
        def _():
            o_remote(t, b, h).start()

    def finish(b, h, last, acc):
        acc = update(0, b, h, ra, rfy, acc)
        emit(0, b, h, last)
        acc = update(1, b, h, rdy, rfx, acc)
        emit(1, b, h, last)
        return acc

    def finish_half(h, last):
        def one(b, acc):
            if h == 0:
                c_a(b).wait()
                c_dy(b).wait_recv()
            c_fy(b, h).wait_recv()
            c_fx(b, h).wait_recv()
            return finish(b, h, last, acc)
        part = lax.fori_loop(E, NB, one, jnp.zeros((8, HALF), jnp.float32))
        sacc[:, cols(h)] = sacc[:, cols(h)] + part

    def drain_forward():
        @pl.when(home)
        def _():
            loop(0, E, lambda b: c_fx(b).wait_send())
            for h in range(2):
                loop(E, NB, lambda b: c_fx(b, h).wait_send())

        @pl.when(away)
        def _():
            loop(0, E, lambda b: c_fy(b).wait_send())
            for h in range(2):
                loop(E, NB, lambda b: c_fy(b, h).wait_send())

    def sweep(k, carry):
        last = k == SWEEPS - 1
        par = lax.rem(k, 2)

        def multiply(n, h):
            start = block_of(n)
            ybuf[rows_of(start, BR), cols(h)] = jnp.dot(
                abuf[lax.rem(n, RING)], xbf[:, cols(h)], preferred_element_type=jnp.float32)

        def fetch(n):
            @pl.when(jnp.logical_not(jnp.logical_and(last, n >= 4 * NB)))
            def _():
                a_copy(lax.rem(n, 4 * NB)).start()

        @pl.when(k > 0)
        def _():
            @pl.when(home)
            def _():
                pl.semaphore_wait(cr_hh1, 1)

            @pl.when(away)
            def _():
                pl.semaphore_wait(cr_gy, 1)

        def lead(h):
            def one(n):
                if h == 0:
                    a_copy(n).wait()
                multiply(n, h)
                if h == 1:
                    fetch(n + RING)

                @pl.when(home)
                def _():
                    c_a(n, h).start()

                @pl.when(away)
                def _():
                    c_gy(n, h).start()
            loop(0, G, one)

        lead(0)

        @pl.when(k > 0)
        def _():
            @pl.when(home)
            def _():
                finish_half(1, jnp.bool_(False))
                s_publish(par, sacc[...])
                signal(cr_hh2, xn)
                signal(cr_hw, yn)

            @pl.when(away)
            def _():
                for t in range(2):
                    loop(E, NB, lambda b: c_x(t, b, 1).wait_recv())

        lead(1)

        @pl.when(k > 0)
        def _():
            drain_forward()

            @pl.when(home)
            def _():
                pl.semaphore_wait(cr_hh2, 1)

            @pl.when(away)
            def _():
                pl.semaphore_wait(cr_ww, 1)
                pl.semaphore_wait(cr_hw, 1)

        def rest(n):
            a_copy(n).wait()
            multiply(n, None)
            fetch(n + RING)
            start = block_of(n)
            first = n < 2 * NB
            at = start - jnp.where(first, other, same)
            t, b = lax.div(at, PIECE), lax.div(lax.rem(at, PIECE), BR)

            @pl.when(jnp.logical_and(first, t == 0))
            def _():
                c_a(b).start()

            @pl.when(jnp.logical_and(jnp.logical_and(first, t == 1), away))
            def _():
                c_gy(b).start()

            @pl.when(jnp.logical_and(jnp.logical_and(jnp.logical_not(first), t == 1), away))
            def _():
                c_dy(b).start()

        loop(G, 4 * NB, rest)

        def add_into(base, t, b, src):
            def step(c):
                at = rows_of(base + t * PIECE + b * BR + c * CH, CH)
                ybuf[at, :] = ybuf[at, :] + src[rows_of(b * BR + c * CH, CH), :]
            loop(0, BR // CH, step)

        @pl.when(away)
        def _away():
            @pl.when(k == 0)
            def _():
                for c in range(X0C):
                    x0_copy(mine, c).wait_send()

            @pl.when(jnp.logical_not(last))
            def _():
                signal(cr_x, mate)

            @pl.when(k == 0)
            def _():
                first_mass()
                s0_out.start()

            def forward(b):
                c_a(b).wait()
                add_into(same, 0, b, ra)

            def forward_full(b):
                forward(b)
                c_fy(b).start()

            def forward_half(b):
                forward(b)
                c_fy(b, 0).start()
            loop(0, E, forward_full)
            loop(E, NB, forward_half)
            loop(E, NB, lambda b: c_fy(b, 1).start())

            @pl.when(jnp.logical_not(last))
            def _():
                signal(cr_ww, xn)

            for h in range(2):
                loop(0, G, lambda b: c_gy(b, h).wait_send())
            loop(G, NB, lambda b: c_gy(b).wait_send())
            loop(0, NB, lambda b: c_dy(b).wait_send())

            @pl.when(k == 0)
            def _():
                v_out.wait_send()
                d_out.wait_send()
                s0_out.wait_send()

            @pl.when(jnp.logical_not(last))
            def _():
                for t in range(2):
                    loop(0, E, lambda b: c_x(t, b).wait_recv())
                    loop(E, NB, lambda b: c_x(t, b, 0).wait_recv())

        @pl.when(home)
        def _home():
            def forward(b):
                add_into(other, 1, b, rgy)

            def forward_a(b):
                c_gy(b, 0).wait_recv()
                c_gy(b, 1).wait_recv()
                forward(b)
                c_fx(b).start()

            def forward_b(b):
                c_gy(b).wait_recv()
                forward(b)
                c_fx(b).start()

            def forward_c(b):
                c_gy(b).wait_recv()
                forward(b)
                c_fx(b, 0).start()
            loop(0, G, forward_a)
            loop(G, E, forward_b)
            loop(E, NB, forward_c)
            loop(E, NB, lambda b: c_fx(b, 1).start())

            @pl.when(jnp.logical_not(last))
            def _():
                signal(cr_gy, yn)

            @pl.when(k == 0)
            def _():
                first_mass()
                v_in.start()
                remote(d_hbm, dint.at[1 - row], ina_send.at[1], ina_recv.at[1], mate).wait_recv()
                spread(1 - row)
                remote(s0buf.at[1 - row], s0buf.at[1 - row], s0_s, s0_r, mate).wait_recv()
                s_publish(0, s0buf[0] + s0buf[1])
                for c in range(X0C):
                    x0_copy(mine, c).wait_send()
                remote(v_hbm, vbuf.at[far_piece], ina_send.at[0], ina_recv.at[0], mate).wait_recv()
                v_in.wait()

            @pl.when(k > 0)
            def _():
                for t in range(2):
                    loop(0, E, lambda b: c_x(t, b).wait_send())
                    for h in range(2):
                        loop(E, NB, lambda b: c_x(t, b, h).wait_send())

            for off in range(1, 4):
                s_wait(par, off).wait_recv()
                s_copy(par, off).wait_send()
            total = (sbuf[par, 0] + sbuf[par, 1]) + (sbuf[par, 2] + sbuf[par, 3])
            mass = jnp.sum(total, axis=0, keepdims=True) / VERTS
            coef[...] = jnp.broadcast_to(DAMPING * mass + (1.0 - DAMPING), (8, VECS))

            @pl.when(jnp.logical_not(last))
            def _():
                pl.semaphore_wait(cr_x, 1)

            def full(b, acc, halves):
                if halves:
                    c_a(b, 0).wait()
                    c_a(b, 1).wait()
                else:
                    c_a(b).wait()
                c_fy(b).wait_recv()
                acc = update(0, b, None, ra, rfy, acc)
                emit(0, b, None, last)
                c_dy(b).wait_recv()
                c_fx(b).wait_recv()
                acc = update(1, b, None, rdy, rfx, acc)
                emit(1, b, None, last)
                return acc

            acc = lax.fori_loop(0, G, lambda b, acc: full(b, acc, True), jnp.zeros((8, VECS), jnp.float32))
            acc = lax.fori_loop(G, E, lambda b, acc: full(b, acc, False), acc)
            sacc[...] = acc

            @pl.when(jnp.logical_not(last))
            def _():
                signal(cr_hh1, xn)
            finish_half(0, last)

        return carry

    lax.fori_loop(0, SWEEPS, sweep, 0)

    @pl.when(home)
    def _():
        finish_half(1, jnp.bool_(True))
    drain_forward()

    @pl.when(home)
    def _():
        def close(b, h):
            o_local(row, b, h).wait()
            o_remote(1 - row, b, h).wait_send()
        loop(0, E, lambda b: close(b, None))
        for h in range(2):
            loop(E, NB, lambda b: close(b, h))

    @pl.when(away)
    def _():
        loop(0, E, lambda b: o_remote(1 - row, b, None).wait_recv())
        for h in range(2):
            loop(E, NB, lambda b: o_remote(1 - row, b, h).wait_recv())


def solution(mesh):
    dma = pltpu.SemaphoreType.DMA
    reg = pltpu.SemaphoreType.REGULAR

    def local_sweeps(mat_tile, x_piece, tele_piece, dang_piece):
        part = pltpu.VMEM((PIECE, VECS), jnp.float32)
        return pl.pallas_call(
            kernel,
            name="sweeps",
            out_shape=jax.ShapeDtypeStruct((PIECE, VECS), jnp.float32),
            in_specs=[pl.BlockSpec(memory_space=pl.ANY)] * 4,
            out_specs=pl.BlockSpec(memory_space=pl.ANY),
            scratch_shapes=[
                pltpu.VMEM((RING, BR, COLS), jnp.bfloat16),
                pltpu.VMEM((COLS, VECS), jnp.bfloat16),
                pltpu.VMEM((ROWS, VECS), jnp.float32),
                part, part, part, part, part,
                pltpu.VMEM((COLS, VECS), jnp.float32),
                pltpu.VMEM((COLS, 128), jnp.float32),
                pltpu.VMEM((2, PIECE // 128, 128), jnp.int32),
                pltpu.VMEM((2, 4, 8, VECS), jnp.float32),
                pltpu.VMEM((2, 8, VECS), jnp.float32),
                pltpu.VMEM((8, VECS), jnp.float32),
                pltpu.VMEM((8, VECS), jnp.float32),
                dma((RING,)), dma((X0C,)), dma((2,)), dma((2,)), dma((2,)), dma((X0C,)), dma((X0C,)),
                dma((NB + G,)), dma((NB + G,)), dma((NB + G,)), dma((NB + G,)), dma((NB,)), dma((NB,)),
                dma((NB + G,)), dma((NB + G,)), dma((NB + G,)), dma((NB + G,)),
                dma((2 * (NB + G),)), dma((2 * (NB + G),)), dma((2, 4)), dma((2, 4)), dma, dma,
                dma((NB + G,)), dma((NB + G,)), dma((NB + G,)),
                reg, reg, reg, reg, reg, reg,
            ],
            compiler_params=pltpu.CompilerParams(
                collective_id=0, has_side_effects=True, vmem_limit_bytes=67_000_000),
            cost_estimate=pl.CostEstimate(
                flops=2 * ROWS * COLS * VECS * SWEEPS, bytes_accessed=2 * ROWS * COLS * SWEEPS, transcendentals=0),
        )(mat_tile, x_piece, tele_piece, dang_piece.reshape(PIECE // 128, 128))

    vec_spec = P(('col', 'row'), None)
    return jax.shard_map(local_sweeps, mesh=mesh,
                         in_specs=(P('row', 'col'), vec_spec, vec_spec, P(('col', 'row'))),
                         out_specs=vec_spec, check_vma=False)
```

```python
import jax
import jax.numpy as jnp
from jax import lax
from jax.experimental import pallas as pl
from jax.experimental.pallas import tpu as pltpu
from jax.sharding import PartitionSpec as P

SWEEPS = 8
DAMPING = 0.85
MESH = pl.DeviceIdType.MESH

VERTS = 24576
VECS = 256
HALF = 128
PIECE = 3072
ROWS = 12288
COLS = 6144
BR = 256
NB = PIECE // BR
G = 4
E = NB - G
CH = 32
RING = 4
X0C = 6
X0R = PIECE // X0C


def kernel(a_hbm, x_hbm, v_hbm, d_hbm, out_hbm,
           abuf, xbf, ybuf, ra, rgy, rdy, rfx, rfy, vbuf, dbuf, dint, sbuf, s0buf, coef, sacc,
           a_sem, xin_sem, in_sem, ina_send, ina_recv, x0_s, x0_r,
           a_s, a_r, gy_s, gy_r, dy_s, dy_r, fx_s, fx_r, fy_s, fy_r,
           x_s, x_r, s_s, s_r, s0_s, s0_r, o_l, o_s, o_r,
           cr_hh1, cr_hh2, cr_hw, cr_gy, cr_ww, cr_x):
    col = lax.axis_index('col')
    row = lax.axis_index('row')
    cx, cy = lax.rem(col, 2), lax.div(col, 2)
    home = row == cy
    away = jnp.logical_not(home)
    xn = (cy * 2 + 1 - cx, row)
    yn = ((1 - cy) * 2 + cx, row)
    mate = (col, 1 - row)
    same = cx * COLS
    other = (1 - cx) * COLS

    barrier = pltpu.get_barrier_semaphore()
    for off in range(4):
        for r in range(2):
            if off == 0 and r == 1:
                continue
            dev = (lax.rem(col + off, 4), row if r == 0 and off else 1 - row)
            pl.semaphore_signal(barrier, inc=1, device_id=dev, device_id_type=MESH)

    def signal(sem, dev):
        pl.semaphore_signal(sem, inc=1, device_id=dev, device_id_type=MESH)

    def rows_of(start, size):
        return pl.ds(pl.multiple_of(start, size), size)

    def blk(n):
        return rows_of(n * BR, BR)

    def cols(h):
        return pl.ds(0, VECS) if h is None else pl.ds(h * HALF, HALF)

    def slot_of(b, h, first):
        return b if h != 1 else NB + b - (0 if first else E)

    def remote(src, dst, send, recv, dev):
        return pltpu.make_async_remote_copy(
            src_ref=src, dst_ref=dst, send_sem=send, recv_sem=recv, device_id=dev, device_id_type=MESH)

    def flow(base, t, b, h, dst, send, recv, dev, first):
        i = slot_of(b, h, first)
        return remote(ybuf.at[rows_of(base + t * PIECE + b * BR, BR), cols(h)], dst.at[blk(b), cols(h)],
                      send.at[i], recv.at[i], dev)

    def c_a(b, h=None):
        return flow(other, 0, b, h, ra, a_s, a_r, xn, True)

    def c_gy(b, h=None):
        return flow(other, 1, b, h, rgy, gy_s, gy_r, yn, True)

    def c_dy(b):
        return flow(same, 1, b, None, rdy, dy_s, dy_r, yn, True)

    def c_fx(b, h=None):
        return flow(other, 1, b, h, rfx, fx_s, fx_r, xn, False)

    def c_fy(b, h=None):
        return flow(same, 0, b, h, rfy, fy_s, fy_r, yn, False)

    def c_x(t, b, h=None):
        at = rows_of(t * PIECE + b * BR, BR)
        i = t * (NB + G) + slot_of(b, h, False)
        return remote(xbf.at[at, cols(h)], xbf.at[at, cols(h)], x_s.at[i], x_r.at[i], mate)

    def block_of(n):
        m = n - G
        pair = m < 2 * E
        t0 = jnp.where(pair, lax.rem(m, 2), 1)
        b0 = jnp.where(pair, jnp.where(t0 == 0, G, 0) + lax.div(m, 2), m - E)
        b0 = jnp.where(m < 0, n, b0)
        t0 = jnp.where(jnp.logical_xor(home, jnp.logical_or(m < 0, t0 == 0)), 1, 0)
        m = n - 2 * NB
        first = n < 2 * NB
        t = jnp.where(first, t0, 1 - lax.div(m, NB))
        b = jnp.where(first, b0, lax.rem(m, NB))
        return jnp.where(first, other, same) + t * PIECE + b * BR

    def a_copy(n):
        slot = lax.rem(n, RING)
        return pltpu.make_async_copy(a_hbm.at[rows_of(block_of(n), BR)], abuf.at[slot], a_sem.at[slot])

    def loop(lo, hi, body):
        def step(i, c):
            body(i)
            return c
        lax.fori_loop(lo, hi, step, 0)

    mine = row * PIECE
    far = (1 - row) * PIECE
    piece = rows_of(mine, PIECE)
    far_piece = rows_of(far, PIECE)

    def x_in(c):
        return pltpu.make_async_copy(x_hbm.at[rows_of(c * X0R, X0R)], vbuf.at[rows_of(mine + c * X0R, X0R)], xin_sem.at[c])

    def x0_copy(base, c):
        at = rows_of(base + c * X0R, X0R)
        return remote(xbf.at[at], xbf.at[at], x0_s.at[c], x0_r.at[c], mate)

    for c in range(X0C):
        x_in(c).start()
    d_in = pltpu.make_async_copy(d_hbm, dint.at[row], in_sem.at[0])
    v_in = pltpu.make_async_copy(v_hbm, vbuf.at[piece], in_sem.at[1])
    v_out = remote(v_hbm, vbuf.at[piece], ina_send.at[0], ina_recv.at[0], mate)
    d_out = remote(d_hbm, dint.at[row], ina_send.at[1], ina_recv.at[1], mate)
    s0_out = remote(s0buf.at[row], s0buf.at[row], s0_s, s0_r, mate)

    for c in range(X0C):
        x_in(c).wait()

        def convert(i, c=c):
            at = rows_of(mine + c * X0R + i * CH, CH)
            xbf[at, :] = vbuf[at, :].astype(jnp.bfloat16)
        loop(0, X0R // CH, convert)
        if c == 0:
            pl.semaphore_wait(barrier, 7)
        x0_copy(mine, c).start()
        if c < RING:
            a_copy(jnp.int32(c)).start()
    d_in.start()

    @pl.when(away)
    def _():
        d_out.start()
        v_out.start()

    for c in range(X0C):
        x0_copy(far, c).wait_recv()

    def s_copy(par, off):
        dst_col = lax.rem(col + off, 4)
        return remote(sbuf.at[par, col], sbuf.at[par, col], s_s.at[par, off], s_r.at[par, col],
                      (dst_col, lax.div(dst_col, 2)))

    def s_wait(par, off):
        src_col = lax.rem(col + off, 4)
        return remote(sbuf.at[par, src_col], sbuf.at[par, src_col], s_s.at[par, off], s_r.at[par, src_col],
                      (src_col, lax.div(src_col, 2)))

    def s_publish(par, value):
        sbuf[par, col] = value
        for off in range(1, 4):
            s_copy(par, off).start()

    def spread(r):
        def group(g):
            flags = dint[r, pl.ds(g, 1), :].astype(jnp.float32)
            dbuf[rows_of(r * PIECE + g * 128, 128), :] = jnp.broadcast_to(flags, (128, 128)).T
        loop(0, PIECE // 128, group)

    def first_mass():
        d_in.wait()
        spread(row)

        def add(c, acc):
            at = rows_of(mine + c * CH, CH)
            d = dbuf[at, :]
            w = vbuf[at, :] * jnp.concatenate([d, d], axis=1)
            return acc + jnp.sum(w.reshape(CH // 8, 8, VECS), axis=0)
        s0buf[row] = lax.fori_loop(0, PIECE // CH, add, jnp.zeros((8, VECS), jnp.float32))

    def update(t, b, h, one, two, acc):
        def step(c, acc):
            at = rows_of(same + t * PIECE + b * BR + c * CH, CH)
            own = rows_of(t * PIECE + b * BR + c * CH, CH)
            there = rows_of(b * BR + c * CH, CH)
            y = (ybuf[at, cols(h)] + one[there, cols(h)]) + two[there, cols(h)]
            cf = jnp.concatenate([coef[:, cols(h)]] * (CH // 8), axis=0)
            x = DAMPING * y + cf * vbuf[own, cols(h)]
            xbf[own, cols(h)] = x.astype(jnp.bfloat16)
            ybuf[at, cols(h)] = x
            d = dbuf[own, :]
            if h is None:
                d = jnp.concatenate([d, d], axis=1)
            return acc + jnp.sum((x * d).reshape(CH // 8, 8, d.shape[1]), axis=0)
        return lax.fori_loop(0, BR // CH, step, acc)

    def o_local(t, b, h):
        i = slot_of(b, h, False)
        return pltpu.make_async_copy(
            ybuf.at[rows_of(same + t * PIECE + b * BR, BR), cols(h)], out_hbm.at[blk(b), cols(h)], o_l.at[i])

    def o_remote(t, b, h):
        i = slot_of(b, h, False)
        return remote(ybuf.at[rows_of(same + t * PIECE + b * BR, BR), cols(h)], out_hbm.at[blk(b), cols(h)],
                      o_s.at[i], o_r.at[i], mate)

    def emit(t, b, h, last):
        @pl.when(jnp.logical_not(last))
        def _():
            c_x(t, b, h).start()

        @pl.when(jnp.logical_and(last, row == t))
        def _():
            o_local(t, b, h).start()

        @pl.when(jnp.logical_and(last, row != t))
        def _():
            o_remote(t, b, h).start()

    def finish(b, h, last, acc):
        acc = update(0, b, h, ra, rfy, acc)
        emit(0, b, h, last)
        acc = update(1, b, h, rdy, rfx, acc)
        emit(1, b, h, last)
        return acc

    def finish_half(h, last):
        def one(b, acc):
            if h == 0:
                c_a(b).wait()
                c_dy(b).wait_recv()
            c_fy(b, h).wait_recv()
            c_fx(b, h).wait_recv()
            return finish(b, h, last, acc)
        part = lax.fori_loop(E, NB, one, jnp.zeros((8, HALF), jnp.float32))
        sacc[:, cols(h)] = sacc[:, cols(h)] + part

    def drain_forward():
        @pl.when(home)
        def _():
            loop(0, E, lambda b: c_fx(b).wait_send())
            for h in range(2):
                loop(E, NB, lambda b: c_fx(b, h).wait_send())

        @pl.when(away)
        def _():
            loop(0, E, lambda b: c_fy(b).wait_send())
            for h in range(2):
                loop(E, NB, lambda b: c_fy(b, h).wait_send())

    def sweep(k, carry):
        last = k == SWEEPS - 1
        par = lax.rem(k, 2)

        def multiply(n, h):
            start = block_of(n)
            ybuf[rows_of(start, BR), cols(h)] = jnp.dot(
                abuf[lax.rem(n, RING)], xbf[:, cols(h)], preferred_element_type=jnp.float32)

        def fetch(n):
            @pl.when(jnp.logical_not(jnp.logical_and(last, n >= 4 * NB)))
            def _():
                a_copy(lax.rem(n, 4 * NB)).start()

        @pl.when(k > 0)
        def _():
            @pl.when(home)
            def _():
                pl.semaphore_wait(cr_hh1, 1)

            @pl.when(away)
            def _():
                pl.semaphore_wait(cr_gy, 1)

        def lead(h):
            def one(n):
                if h == 0:
                    a_copy(n).wait()
                multiply(n, h)
                if h == 1:
                    fetch(n + RING)

                @pl.when(home)
                def _():
                    c_a(n, h).start()

                @pl.when(away)
                def _():
                    c_gy(n, h).start()
            loop(0, G, one)

        lead(0)

        @pl.when(k > 0)
        def _():
            @pl.when(home)
            def _():
                finish_half(1, jnp.bool_(False))
                s_publish(par, sacc[...])
                signal(cr_hh2, xn)
                signal(cr_hw, yn)

            @pl.when(away)
            def _():
                for t in range(2):
                    loop(E, NB, lambda b: c_x(t, b, 1).wait_recv())

        lead(1)

        @pl.when(k > 0)
        def _():
            drain_forward()

            @pl.when(home)
            def _():
                pl.semaphore_wait(cr_hh2, 1)

            @pl.when(away)
            def _():
                pl.semaphore_wait(cr_ww, 1)
                pl.semaphore_wait(cr_hw, 1)

        def rest(n):
            a_copy(n).wait()
            multiply(n, None)
            fetch(n + RING)
            start = block_of(n)
            first = n < 2 * NB
            at = start - jnp.where(first, other, same)
            t, b = lax.div(at, PIECE), lax.div(lax.rem(at, PIECE), BR)

            @pl.when(jnp.logical_and(first, t == 0))
            def _():
                c_a(b).start()

            @pl.when(jnp.logical_and(jnp.logical_and(first, t == 1), away))
            def _():
                c_gy(b).start()

            @pl.when(jnp.logical_and(jnp.logical_and(jnp.logical_not(first), t == 1), away))
            def _():
                c_dy(b).start()

        loop(G, 4 * NB, rest)

        def add_into(base, t, b, src):
            def step(c):
                at = rows_of(base + t * PIECE + b * BR + c * CH, CH)
                ybuf[at, :] = ybuf[at, :] + src[rows_of(b * BR + c * CH, CH), :]
            loop(0, BR // CH, step)

        @pl.when(away)
        def _away():
            @pl.when(k == 0)
            def _():
                for c in range(X0C):
                    x0_copy(mine, c).wait_send()

            @pl.when(jnp.logical_not(last))
            def _():
                signal(cr_x, mate)

            @pl.when(k == 0)
            def _():
                first_mass()
                s0_out.start()

            def forward(b):
                c_a(b).wait()
                add_into(same, 0, b, ra)

            def forward_full(b):
                forward(b)
                c_fy(b).start()

            def forward_half(b):
                forward(b)
                c_fy(b, 0).start()
            loop(0, E, forward_full)
            loop(E, NB, forward_half)
            loop(E, NB, lambda b: c_fy(b, 1).start())

            @pl.when(jnp.logical_not(last))
            def _():
                signal(cr_ww, xn)

            for h in range(2):
                loop(0, G, lambda b: c_gy(b, h).wait_send())
            loop(G, NB, lambda b: c_gy(b).wait_send())
            loop(0, NB, lambda b: c_dy(b).wait_send())

            @pl.when(k == 0)
            def _():
                v_out.wait_send()
                d_out.wait_send()
                s0_out.wait_send()

            @pl.when(jnp.logical_not(last))
            def _():
                for t in range(2):
                    loop(0, E, lambda b: c_x(t, b).wait_recv())
                    loop(E, NB, lambda b: c_x(t, b, 0).wait_recv())

        @pl.when(home)
        def _home():
            def forward(b):
                add_into(other, 1, b, rgy)

            def forward_a(b):
                c_gy(b, 0).wait_recv()
                c_gy(b, 1).wait_recv()
                forward(b)
                c_fx(b).start()

            def forward_b(b):
                c_gy(b).wait_recv()
                forward(b)
                c_fx(b).start()

            def forward_c(b):
                c_gy(b).wait_recv()
                forward(b)
                c_fx(b, 0).start()
            loop(0, G, forward_a)
            loop(G, E, forward_b)
            loop(E, NB, forward_c)
            loop(E, NB, lambda b: c_fx(b, 1).start())

            @pl.when(jnp.logical_not(last))
            def _():
                signal(cr_gy, yn)

            @pl.when(k == 0)
            def _():
                first_mass()
                v_in.start()
                remote(d_hbm, dint.at[1 - row], ina_send.at[1], ina_recv.at[1], mate).wait_recv()
                spread(1 - row)
                remote(s0buf.at[1 - row], s0buf.at[1 - row], s0_s, s0_r, mate).wait_recv()
                s_publish(0, s0buf[0] + s0buf[1])
                for c in range(X0C):
                    x0_copy(mine, c).wait_send()
                remote(v_hbm, vbuf.at[far_piece], ina_send.at[0], ina_recv.at[0], mate).wait_recv()
                v_in.wait()

            @pl.when(k > 0)
            def _():
                for t in range(2):
                    loop(0, E, lambda b: c_x(t, b).wait_send())
                    for h in range(2):
                        loop(E, NB, lambda b: c_x(t, b, h).wait_send())

            for off in range(1, 4):
                s_wait(par, off).wait_recv()
                s_copy(par, off).wait_send()
            total = (sbuf[par, 0] + sbuf[par, 1]) + (sbuf[par, 2] + sbuf[par, 3])
            mass = jnp.sum(total, axis=0, keepdims=True) / VERTS
            coef[...] = jnp.broadcast_to(DAMPING * mass + (1.0 - DAMPING), (8, VECS))

            @pl.when(jnp.logical_not(last))
            def _():
                pl.semaphore_wait(cr_x, 1)

            def full(b, acc, halves):
                if halves:
                    c_a(b, 0).wait()
                    c_a(b, 1).wait()
                else:
                    c_a(b).wait()
                c_fy(b).wait_recv()
                acc = update(0, b, None, ra, rfy, acc)
                emit(0, b, None, last)
                c_dy(b).wait_recv()
                c_fx(b).wait_recv()
                acc = update(1, b, None, rdy, rfx, acc)
                emit(1, b, None, last)
                return acc

            acc = lax.fori_loop(0, G, lambda b, acc: full(b, acc, True), jnp.zeros((8, VECS), jnp.float32))
            acc = lax.fori_loop(G, E, lambda b, acc: full(b, acc, False), acc)
            sacc[...] = acc

            @pl.when(jnp.logical_not(last))
            def _():
                signal(cr_hh1, xn)
            finish_half(0, last)

        return carry

    lax.fori_loop(0, SWEEPS, sweep, 0)

    @pl.when(home)
    def _():
        finish_half(1, jnp.bool_(True))
    drain_forward()

    @pl.when(home)
    def _():
        def close(b, h):
            o_local(row, b, h).wait()
            o_remote(1 - row, b, h).wait_send()
        loop(0, E, lambda b: close(b, None))
        for h in range(2):
            loop(E, NB, lambda b: close(b, h))

    @pl.when(away)
    def _():
        loop(0, E, lambda b: o_remote(1 - row, b, None).wait_recv())
        for h in range(2):
            loop(E, NB, lambda b: o_remote(1 - row, b, h).wait_recv())


def solution(mesh):
    dma = pltpu.SemaphoreType.DMA
    reg = pltpu.SemaphoreType.REGULAR

    def local_sweeps(mat_tile, x_piece, tele_piece, dang_piece):
        part = pltpu.VMEM((PIECE, VECS), jnp.float32)
        return pl.pallas_call(
            kernel,
            name="sweeps",
            out_shape=jax.ShapeDtypeStruct((PIECE, VECS), jnp.float32),
            in_specs=[pl.BlockSpec(memory_space=pl.ANY)] * 4,
            out_specs=pl.BlockSpec(memory_space=pl.ANY),
            scratch_shapes=[
                pltpu.VMEM((RING, BR, COLS), jnp.bfloat16),
                pltpu.VMEM((COLS, VECS), jnp.bfloat16),
                pltpu.VMEM((ROWS, VECS), jnp.float32),
                part, part, part, part, part,
                pltpu.VMEM((COLS, VECS), jnp.float32),
                pltpu.VMEM((COLS, 128), jnp.float32),
                pltpu.VMEM((2, PIECE // 128, 128), jnp.int32),
                pltpu.VMEM((2, 4, 8, VECS), jnp.float32),
                pltpu.VMEM((2, 8, VECS), jnp.float32),
                pltpu.VMEM((8, VECS), jnp.float32),
                pltpu.VMEM((8, VECS), jnp.float32),
                dma((RING,)), dma((X0C,)), dma((2,)), dma((2,)), dma((2,)), dma((X0C,)), dma((X0C,)),
                dma((NB + G,)), dma((NB + G,)), dma((NB + G,)), dma((NB + G,)), dma((NB,)), dma((NB,)),
                dma((NB + G,)), dma((NB + G,)), dma((NB + G,)), dma((NB + G,)),
                dma((2 * (NB + G),)), dma((2 * (NB + G),)), dma((2, 4)), dma((2, 4)), dma, dma,
                dma((NB + G,)), dma((NB + G,)), dma((NB + G,)),
                reg, reg, reg, reg, reg, reg,
            ],
            compiler_params=pltpu.CompilerParams(
                collective_id=0, has_side_effects=True, vmem_limit_bytes=67_000_000),
            cost_estimate=pl.CostEstimate(
                flops=2 * ROWS * COLS * VECS * SWEEPS, bytes_accessed=2 * ROWS * COLS * SWEEPS, transcendentals=0),
        )(mat_tile, x_piece, tele_piece, dang_piece.reshape(PIECE // 128, 128))

    vec_spec = P(('col', 'row'), None)
    return jax.shard_map(local_sweeps, mesh=mesh,
                         in_specs=(P('row', 'col'), vec_spec, vec_spec, P(('col', 'row'))),
                         out_specs=vec_spec, check_vma=False)
```

```python
import jax
import jax.numpy as jnp
from jax import lax
from jax.experimental import pallas as pl
from jax.experimental.pallas import tpu as pltpu
from jax.sharding import PartitionSpec as P

SWEEPS = 8
DAMPING = 0.85
MESH = pl.DeviceIdType.MESH

VERTS = 24576
VECS = 256
HALF = 128
PIECE = 3072
ROWS = 12288
COLS = 6144
BR = 256
NB = PIECE // BR
G = 4
E = NB - G
CH = 32
LEAD = (1, 2)
TAIL = (2, 2)
UA_HOME = 4
UA_AWAY = 2
UG = 2
UD = 6
UF = 4
RING = 4
X0C = 6
X0R = PIECE // X0C


def kernel(a_hbm, x_hbm, v_hbm, d_hbm, out_hbm,
           abuf, xbf, ybuf, ra, rgy, rdy, rfx, rfy, vbuf, dbuf, dint, sbuf, s0buf, coef, sacc,
           a_sem, xin_sem, in_sem, ina_send, ina_recv, x0_s, x0_r,
           a_s, a_r, gy_s, gy_r, dy_s, dy_r, fx_s, fx_r, fy_s, fy_r,
           x_s, x_r, s_s, s_r, s0_s, s0_r, o_l, o_s, o_r,
           cr_hh1, cr_hh2, cr_hw, cr_gy, cr_ww, cr_x):
    col = lax.axis_index('col')
    row = lax.axis_index('row')
    cx, cy = lax.rem(col, 2), lax.div(col, 2)
    home = row == cy
    away = jnp.logical_not(home)
    xn = (cy * 2 + 1 - cx, row)
    yn = ((1 - cy) * 2 + cx, row)
    mate = (col, 1 - row)
    same = cx * COLS
    other = (1 - cx) * COLS

    barrier = pltpu.get_barrier_semaphore()
    for off in range(4):
        for r in range(2):
            if off == 0 and r == 1:
                continue
            dev = (lax.rem(col + off, 4), row if r == 0 and off else 1 - row)
            pl.semaphore_signal(barrier, inc=1, device_id=dev, device_id_type=MESH)

    def signal(sem, dev):
        pl.semaphore_signal(sem, inc=1, device_id=dev, device_id_type=MESH)

    def rows_of(start, size):
        return pl.ds(pl.multiple_of(start, size), size)

    def blk(b, n):
        return pl.ds(pl.multiple_of(b * BR, BR), n * BR)

    def cols(h):
        return pl.ds(0, VECS) if h is None else pl.ds(h * HALF, HALF)

    def slot_of(b, h):
        return b if h != 1 else NB + b

    def remote(src, dst, send, recv, dev):
        return pltpu.make_async_remote_copy(
            src_ref=src, dst_ref=dst, send_sem=send, recv_sem=recv, device_id=dev, device_id_type=MESH)

    def y_rows(base, t, b, n):
        return pl.ds(pl.multiple_of(base + t * PIECE + b * BR, BR), n * BR)

    def flow(base, t, b, n, h, dst, send, recv, dev):
        i = slot_of(b, h)
        return remote(ybuf.at[y_rows(base, t, b, n), cols(h)], dst.at[blk(b, n), cols(h)], send.at[i], recv.at[i], dev)

    def c_a(b, n, h=None):
        return flow(other, 0, b, n, h, ra, a_s, a_r, xn)

    def c_gy(b, n, h=None):
        return flow(other, 1, b, n, h, rgy, gy_s, gy_r, yn)

    def c_dy(b):
        return flow(same, 1, b, UD, None, rdy, dy_s, dy_r, yn)

    def c_fx(b, n, h=None):
        return flow(other, 1, b, n, h, rfx, fx_s, fx_r, xn)

    def c_fy(b, n, h=None):
        return flow(same, 0, b, n, h, rfy, fy_s, fy_r, yn)

    def c_x(t, b, n, h=None):
        at = pl.ds(pl.multiple_of(t * PIECE + b * BR, BR), n * BR)
        i = t * 2 * NB + slot_of(b, h)
        return remote(xbf.at[at, cols(h)], xbf.at[at, cols(h)], x_s.at[i], x_r.at[i], mate)

    def block_of(n):
        m = n - G
        pair = m < 2 * E
        t0 = jnp.where(pair, lax.rem(m, 2), 1)
        b0 = jnp.where(pair, jnp.where(t0 == 0, G, 0) + lax.div(m, 2), m - E)
        b0 = jnp.where(m < 0, n, b0)
        t0 = jnp.where(jnp.logical_xor(home, jnp.logical_or(m < 0, t0 == 0)), 1, 0)
        m = n - 2 * NB
        first = n < 2 * NB
        t = jnp.where(first, t0, 1 - lax.div(m, NB))
        b = jnp.where(first, b0, lax.rem(m, NB))
        return jnp.where(first, other, same) + t * PIECE + b * BR

    def a_copy(n):
        slot = lax.rem(n, RING)
        return pltpu.make_async_copy(a_hbm.at[rows_of(block_of(n), BR)], abuf.at[slot], a_sem.at[slot])

    def loop(lo, hi, body):
        def step(i, c):
            body(i)
            return c
        lax.fori_loop(lo, hi, step, 0)

    def units(lo, hi, n, body):
        loop(0, (hi - lo) // n, lambda u: body(lo + u * n))

    def lead_units(h, body):
        units(0, G, LEAD[h], lambda b: body(b, LEAD[h], h))

    def tail_units(h, body):
        units(E, NB, TAIL[h], lambda b: body(b, TAIL[h], h))

    def forward_units(body):
        units(0, E, UF, lambda b: body(b, UF, None))

    mine = row * PIECE
    far = (1 - row) * PIECE
    piece = rows_of(mine, PIECE)
    far_piece = rows_of(far, PIECE)

    def x_in(c):
        return pltpu.make_async_copy(x_hbm.at[rows_of(c * X0R, X0R)], vbuf.at[rows_of(mine + c * X0R, X0R)], xin_sem.at[c])

    def x0_copy(base, c):
        at = rows_of(base + c * X0R, X0R)
        return remote(xbf.at[at], xbf.at[at], x0_s.at[c], x0_r.at[c], mate)

    for c in range(X0C):
        x_in(c).start()
    d_in = pltpu.make_async_copy(d_hbm, dint.at[row], in_sem.at[0])
    v_in = pltpu.make_async_copy(v_hbm, vbuf.at[piece], in_sem.at[1])
    v_out = remote(v_hbm, vbuf.at[piece], ina_send.at[0], ina_recv.at[0], mate)
    d_out = remote(d_hbm, dint.at[row], ina_send.at[1], ina_recv.at[1], mate)
    s0_out = remote(s0buf.at[row], s0buf.at[row], s0_s, s0_r, mate)

    for c in range(X0C):
        x_in(c).wait()

        def convert(i, c=c):
            at = rows_of(mine + c * X0R + i * CH, CH)
            xbf[at, :] = vbuf[at, :].astype(jnp.bfloat16)
        loop(0, X0R // CH, convert)
        if c == 0:
            pl.semaphore_wait(barrier, 7)
        x0_copy(mine, c).start()
        if c < RING:
            a_copy(jnp.int32(c)).start()
    d_in.start()

    @pl.when(away)
    def _():
        d_out.start()
        v_out.start()

    for c in range(X0C):
        x0_copy(far, c).wait_recv()

    def s_copy(par, off):
        dst_col = lax.rem(col + off, 4)
        return remote(sbuf.at[par, col], sbuf.at[par, col], s_s.at[par, off], s_r.at[par, col],
                      (dst_col, lax.div(dst_col, 2)))

    def s_wait(par, off):
        src_col = lax.rem(col + off, 4)
        return remote(sbuf.at[par, src_col], sbuf.at[par, src_col], s_s.at[par, off], s_r.at[par, src_col],
                      (src_col, lax.div(src_col, 2)))

    def s_publish(par, value):
        sbuf[par, col] = value
        for off in range(1, 4):
            s_copy(par, off).start()

    def spread(r):
        def group(g):
            flags = dint[r, pl.ds(g, 1), :].astype(jnp.float32)
            dbuf[rows_of(r * PIECE + g * 128, 128), :] = jnp.broadcast_to(flags, (128, 128)).T
        loop(0, PIECE // 128, group)

    def first_mass():
        d_in.wait()
        spread(row)

        def add(c, acc):
            at = rows_of(mine + c * CH, CH)
            d = dbuf[at, :]
            w = vbuf[at, :] * jnp.concatenate([d, d], axis=1)
            return acc + jnp.sum(w.reshape(CH // 8, 8, VECS), axis=0)
        s0buf[row] = lax.fori_loop(0, PIECE // CH, add, jnp.zeros((8, VECS), jnp.float32))

    def update(t, b, n, h, one, two, acc):
        def step(c, acc):
            at = rows_of(same + t * PIECE + b * BR + c * CH, CH)
            own = rows_of(t * PIECE + b * BR + c * CH, CH)
            there = rows_of(b * BR + c * CH, CH)
            y = (ybuf[at, cols(h)] + one[there, cols(h)]) + two[there, cols(h)]
            cf = jnp.concatenate([coef[:, cols(h)]] * (CH // 8), axis=0)
            x = DAMPING * y + cf * vbuf[own, cols(h)]
            xbf[own, cols(h)] = x.astype(jnp.bfloat16)
            ybuf[at, cols(h)] = x
            d = dbuf[own, :]
            if h is None:
                d = jnp.concatenate([d, d], axis=1)
            return acc + jnp.sum((x * d).reshape(CH // 8, 8, d.shape[1]), axis=0)
        return lax.fori_loop(0, n * BR // CH, step, acc)

    def o_local(t, b, n, h):
        return pltpu.make_async_copy(
            ybuf.at[y_rows(same, t, b, n), cols(h)], out_hbm.at[blk(b, n), cols(h)], o_l.at[slot_of(b, h)])

    def o_remote(t, b, n, h):
        i = slot_of(b, h)
        return remote(ybuf.at[y_rows(same, t, b, n), cols(h)], out_hbm.at[blk(b, n), cols(h)], o_s.at[i], o_r.at[i], mate)

    def emit(t, b, n, h, last):
        @pl.when(jnp.logical_not(last))
        def _():
            c_x(t, b, n, h).start()

        @pl.when(jnp.logical_and(last, row == t))
        def _():
            o_local(t, b, n, h).start()

        @pl.when(jnp.logical_and(last, row != t))
        def _():
            o_remote(t, b, n, h).start()

    def finish(b, n, h, last, acc):
        c_fy(b, n, h).wait_recv()
        acc = update(0, b, n, h, ra, rfy, acc)
        emit(0, b, n, h, last)
        c_fx(b, n, h).wait_recv()
        acc = update(1, b, n, h, rdy, rfx, acc)
        emit(1, b, n, h, last)
        return acc

    def finish_half(h, last):
        n = TAIL[h]
        part = lax.fori_loop(
            0, G // n, lambda u, acc: finish(E + u * n, n, h, last, acc), jnp.zeros((8, HALF), jnp.float32))
        sacc[:, cols(h)] = sacc[:, cols(h)] + part

    def drain_forward():
        @pl.when(home)
        def _():
            forward_units(lambda b, n, h: c_fx(b, n, h).wait_send())
            for half in range(2):
                tail_units(half, lambda b, n, h: c_fx(b, n, h).wait_send())

        @pl.when(away)
        def _():
            forward_units(lambda b, n, h: c_fy(b, n, h).wait_send())
            for half in range(2):
                tail_units(half, lambda b, n, h: c_fy(b, n, h).wait_send())

    def sweep(k, carry):
        last = k == SWEEPS - 1
        par = lax.rem(k, 2)

        def multiply(n, h):
            start = block_of(n)
            ybuf[rows_of(start, BR), cols(h)] = jnp.dot(
                abuf[lax.rem(n, RING)], xbf[:, cols(h)], preferred_element_type=jnp.float32)

        def fetch(n):
            @pl.when(jnp.logical_not(jnp.logical_and(last, n >= 4 * NB)))
            def _():
                a_copy(lax.rem(n, 4 * NB)).start()

        @pl.when(k > 0)
        def _():
            @pl.when(home)
            def _():
                pl.semaphore_wait(cr_hh1, 1)

            @pl.when(away)
            def _():
                pl.semaphore_wait(cr_gy, 1)

        def lead(h):
            def one(n):
                if h == 0:
                    a_copy(n).wait()
                multiply(n, h)
                if h == 1:
                    fetch(n + RING)
                size = LEAD[h]
                whole = lax.rem(n, size) == size - 1
                b = n - (size - 1)

                @pl.when(jnp.logical_and(whole, home))
                def _():
                    c_a(b, size, h).start()

                @pl.when(jnp.logical_and(whole, away))
                def _():
                    c_gy(b, size, h).start()
            loop(0, G, one)

        lead(0)

        @pl.when(k > 0)
        def _():
            @pl.when(home)
            def _():
                finish_half(1, jnp.bool_(False))
                s_publish(par, sacc[...])
                signal(cr_hh2, xn)
                signal(cr_hw, yn)

            @pl.when(away)
            def _():
                for t in range(2):
                    tail_units(1, lambda b, n, h: c_x(t, b, n, h).wait_recv())

        lead(1)

        @pl.when(k > 0)
        def _():
            drain_forward()

            @pl.when(home)
            def _():
                pl.semaphore_wait(cr_hh2, 1)

            @pl.when(away)
            def _():
                pl.semaphore_wait(cr_ww, 1)
                pl.semaphore_wait(cr_hw, 1)

        def rest(n):
            a_copy(n).wait()
            multiply(n, None)
            fetch(n + RING)
            start = block_of(n)
            first = n < 2 * NB
            at = start - jnp.where(first, other, same)
            t, b = lax.div(at, PIECE), lax.div(lax.rem(at, PIECE), BR)

            def send_when(cond, b0, size, start):
                whole = lax.rem(b - b0, size) == size - 1

                @pl.when(jnp.logical_and(cond, whole))
                def _():
                    start(b - (size - 1), size)

            straight = jnp.logical_and(first, t == 0)
            send_when(jnp.logical_and(straight, home), G, UA_HOME, lambda b, n: c_a(b, n).start())
            send_when(jnp.logical_and(straight, away), 0, UA_AWAY, lambda b, n: c_a(b, n).start())
            send_when(jnp.logical_and(jnp.logical_and(first, t == 1), away), G, UG, lambda b, n: c_gy(b, n).start())
            send_when(jnp.logical_and(jnp.logical_and(jnp.logical_not(first), t == 1), away), 0, UD,
                      lambda b, n: c_dy(b).start())

        loop(G, 4 * NB, rest)

        def add_into(base, t, b, n, src):
            def step(c):
                at = rows_of(base + t * PIECE + b * BR + c * CH, CH)
                ybuf[at, :] = ybuf[at, :] + src[rows_of(b * BR + c * CH, CH), :]
            loop(0, n * BR // CH, step)

        @pl.when(away)
        def _away():
            @pl.when(k == 0)
            def _():
                for c in range(X0C):
                    x0_copy(mine, c).wait_send()

            @pl.when(jnp.logical_not(last))
            def _():
                signal(cr_x, mate)

            @pl.when(k == 0)
            def _():
                first_mass()
                s0_out.start()

            def forward(b, n):
                units(0, n, UA_AWAY, lambda i: c_a(b + i, UA_AWAY).wait())
                add_into(same, 0, b, n, ra)

            def forward_full(b, n, h):
                forward(b, n)
                c_fy(b, n).start()

            def forward_half(b, n, h):
                forward(b, n)
                c_fy(b, n, h).start()
            forward_units(forward_full)
            tail_units(0, forward_half)
            tail_units(1, lambda b, n, h: c_fy(b, n, h).start())

            @pl.when(jnp.logical_not(last))
            def _():
                signal(cr_ww, xn)

            for half in range(2):
                lead_units(half, lambda b, n, h: c_gy(b, n, h).wait_send())
            units(G, NB, UG, lambda b: c_gy(b, UG).wait_send())
            units(0, NB, UD, lambda b: c_dy(b).wait_send())

            @pl.when(k == 0)
            def _():
                v_out.wait_send()
                d_out.wait_send()
                s0_out.wait_send()

            @pl.when(jnp.logical_not(last))
            def _():
                for t in range(2):
                    forward_units(lambda b, n, h: c_x(t, b, n, h).wait_recv())
                    tail_units(0, lambda b, n, h: c_x(t, b, n, h).wait_recv())

        @pl.when(home)
        def _home():
            for half in range(2):
                lead_units(half, lambda b, n, h: c_gy(b, n, h).wait_recv())

            def arrived(b, n):
                @pl.when(b >= G)
                def _():
                    units(0, n, UG, lambda i: c_gy(b + i, UG).wait_recv())

            def forward_full(b, n, h):
                arrived(b, n)
                add_into(other, 1, b, n, rgy)
                c_fx(b, n).start()

            def forward_half(b, n, h):
                arrived(b, n)
                add_into(other, 1, b, n, rgy)
                c_fx(b, n, h).start()
            forward_units(forward_full)
            tail_units(0, forward_half)
            tail_units(1, lambda b, n, h: c_fx(b, n, h).start())

            @pl.when(jnp.logical_not(last))
            def _():
                signal(cr_gy, yn)

            @pl.when(k == 0)
            def _():
                first_mass()
                v_in.start()
                remote(d_hbm, dint.at[1 - row], ina_send.at[1], ina_recv.at[1], mate).wait_recv()
                spread(1 - row)
                remote(s0buf.at[1 - row], s0buf.at[1 - row], s0_s, s0_r, mate).wait_recv()
                s_publish(0, s0buf[0] + s0buf[1])
                for c in range(X0C):
                    x0_copy(mine, c).wait_send()
                remote(v_hbm, vbuf.at[far_piece], ina_send.at[0], ina_recv.at[0], mate).wait_recv()
                v_in.wait()

            @pl.when(k > 0)
            def _():
                for t in range(2):
                    forward_units(lambda b, n, h: c_x(t, b, n, h).wait_send())
                    for half in range(2):
                        tail_units(half, lambda b, n, h: c_x(t, b, n, h).wait_send())

            for off in range(1, 4):
                s_wait(par, off).wait_recv()
                s_copy(par, off).wait_send()
            total = (sbuf[par, 0] + sbuf[par, 1]) + (sbuf[par, 2] + sbuf[par, 3])
            mass = jnp.sum(total, axis=0, keepdims=True) / VERTS
            coef[...] = jnp.broadcast_to(DAMPING * mass + (1.0 - DAMPING), (8, VECS))

            @pl.when(jnp.logical_not(last))
            def _():
                pl.semaphore_wait(cr_x, 1)

            for half in range(2):
                lead_units(half, lambda b, n, h: c_a(b, n, h).wait())
            units(G, NB, UA_HOME, lambda b: c_a(b, UA_HOME).wait())
            units(0, NB, UD, lambda b: c_dy(b).wait_recv())
            acc = lax.fori_loop(
                0, E // UF, lambda u, acc: finish(u * UF, UF, None, last, acc), jnp.zeros((8, VECS), jnp.float32))
            sacc[...] = acc

            @pl.when(jnp.logical_not(last))
            def _():
                signal(cr_hh1, xn)
            finish_half(0, last)

        return carry

    lax.fori_loop(0, SWEEPS, sweep, 0)

    @pl.when(home)
    def _():
        finish_half(1, jnp.bool_(True))
    drain_forward()

    @pl.when(home)
    def _():
        def close(b, n, h):
            o_local(row, b, n, h).wait()
            o_remote(1 - row, b, n, h).wait_send()
        forward_units(close)
        for half in range(2):
            tail_units(half, close)

    @pl.when(away)
    def _():
        def close(b, n, h):
            o_remote(1 - row, b, n, h).wait_recv()
        forward_units(close)
        for half in range(2):
            tail_units(half, close)


def solution(mesh):
    dma = pltpu.SemaphoreType.DMA
    reg = pltpu.SemaphoreType.REGULAR

    def local_sweeps(mat_tile, x_piece, tele_piece, dang_piece):
        part = pltpu.VMEM((PIECE, VECS), jnp.float32)
        return pl.pallas_call(
            kernel,
            name="sweeps",
            out_shape=jax.ShapeDtypeStruct((PIECE, VECS), jnp.float32),
            in_specs=[pl.BlockSpec(memory_space=pl.ANY)] * 4,
            out_specs=pl.BlockSpec(memory_space=pl.ANY),
            scratch_shapes=[
                pltpu.VMEM((RING, BR, COLS), jnp.bfloat16),
                pltpu.VMEM((COLS, VECS), jnp.bfloat16),
                pltpu.VMEM((ROWS, VECS), jnp.float32),
                part, part, part, part, part,
                pltpu.VMEM((COLS, VECS), jnp.float32),
                pltpu.VMEM((COLS, 128), jnp.float32),
                pltpu.VMEM((2, PIECE // 128, 128), jnp.int32),
                pltpu.VMEM((2, 4, 8, VECS), jnp.float32),
                pltpu.VMEM((2, 8, VECS), jnp.float32),
                pltpu.VMEM((8, VECS), jnp.float32),
                pltpu.VMEM((8, VECS), jnp.float32),
                dma((RING,)), dma((X0C,)), dma((2,)), dma((2,)), dma((2,)), dma((X0C,)), dma((X0C,)),
                dma((2 * NB,)), dma((2 * NB,)), dma((2 * NB,)), dma((2 * NB,)), dma((NB,)), dma((NB,)),
                dma((2 * NB,)), dma((2 * NB,)), dma((2 * NB,)), dma((2 * NB,)),
                dma((4 * NB,)), dma((4 * NB,)), dma((2, 4)), dma((2, 4)), dma, dma,
                dma((2 * NB,)), dma((2 * NB,)), dma((2 * NB,)),
                reg, reg, reg, reg, reg, reg,
            ],
            compiler_params=pltpu.CompilerParams(
                collective_id=0, has_side_effects=True, vmem_limit_bytes=67_000_000),
            cost_estimate=pl.CostEstimate(
                flops=2 * ROWS * COLS * VECS * SWEEPS, bytes_accessed=2 * ROWS * COLS * SWEEPS, transcendentals=0),
        )(mat_tile, x_piece, tele_piece, dang_piece.reshape(PIECE // 128, 128))

    vec_spec = P(('col', 'row'), None)
    return jax.shard_map(local_sweeps, mesh=mesh,
                         in_specs=(P('row', 'col'), vec_spec, vec_spec, P(('col', 'row'))),
                         out_specs=vec_spec, check_vma=False)
```

```python
import jax
import jax.numpy as jnp
from jax import lax
from jax.experimental import pallas as pl
from jax.experimental.pallas import tpu as pltpu
from jax.sharding import PartitionSpec as P

SWEEPS = 8
DAMPING = 0.85
MESH = pl.DeviceIdType.MESH

VERTS = 24576
VECS = 256
HALF = 128
PIECE = 3072
ROWS = 12288
COLS = 6144
BR = 256
NB = PIECE // BR
G = 4
E = NB - G
CH = 32
LEAD = (1, 1)
TAIL = (1, 1)
UA_HOME = 1
UA_AWAY = 1
UG = 1
UD = 1
UF = 1
HOLD = 24
RING = 4
X0C = 6
X0R = PIECE // X0C


def kernel(a_hbm, x_hbm, v_hbm, d_hbm, out_hbm,
           abuf, xbf, ybuf, ra, rgy, rdy, rfx, rfy, vbuf, dbuf, dint, sbuf, s0buf, coef, sacc,
           a_sem, xin_sem, in_sem, ina_send, ina_recv, x0_s, x0_r,
           a_s, a_r, gy_s, gy_r, dy_s, dy_r, fx_s, fx_r, fy_s, fy_r,
           x_s, x_r, s_s, s_r, s0_s, s0_r, o_l, o_s, o_r,
           cr_hh1, cr_hh2, cr_hw, cr_gy, cr_ww, cr_x):
    col = lax.axis_index('col')
    row = lax.axis_index('row')
    cx, cy = lax.rem(col, 2), lax.div(col, 2)
    home = row == cy
    away = jnp.logical_not(home)
    xn = (cy * 2 + 1 - cx, row)
    yn = ((1 - cy) * 2 + cx, row)
    mate = (col, 1 - row)
    same = cx * COLS
    other = (1 - cx) * COLS

    barrier = pltpu.get_barrier_semaphore()
    for off in range(4):
        for r in range(2):
            if off == 0 and r == 1:
                continue
            dev = (lax.rem(col + off, 4), row if r == 0 and off else 1 - row)
            pl.semaphore_signal(barrier, inc=1, device_id=dev, device_id_type=MESH)

    def signal(sem, dev):
        pl.semaphore_signal(sem, inc=1, device_id=dev, device_id_type=MESH)

    def rows_of(start, size):
        return pl.ds(pl.multiple_of(start, size), size)

    def blk(b, n):
        return pl.ds(pl.multiple_of(b * BR, BR), n * BR)

    def cols(h):
        return pl.ds(0, VECS) if h is None else pl.ds(h * HALF, HALF)

    def slot_of(b, h):
        return b if h != 1 else NB + b

    def remote(src, dst, send, recv, dev):
        return pltpu.make_async_remote_copy(
            src_ref=src, dst_ref=dst, send_sem=send, recv_sem=recv, device_id=dev, device_id_type=MESH)

    def y_rows(base, t, b, n):
        return pl.ds(pl.multiple_of(base + t * PIECE + b * BR, BR), n * BR)

    def flow(base, t, b, n, h, dst, send, recv, dev):
        i = slot_of(b, h)
        return remote(ybuf.at[y_rows(base, t, b, n), cols(h)], dst.at[blk(b, n), cols(h)], send.at[i], recv.at[i], dev)

    def c_a(b, n, h=None):
        return flow(other, 0, b, n, h, ra, a_s, a_r, xn)

    def c_gy(b, n, h=None):
        return flow(other, 1, b, n, h, rgy, gy_s, gy_r, yn)

    def c_dy(b):
        return flow(same, 1, b, UD, None, rdy, dy_s, dy_r, yn)

    def c_fx(b, n, h=None):
        return flow(other, 1, b, n, h, rfx, fx_s, fx_r, xn)

    def c_fy(b, n, h=None):
        return flow(same, 0, b, n, h, rfy, fy_s, fy_r, yn)

    def c_x(t, b, n, h=None):
        at = pl.ds(pl.multiple_of(t * PIECE + b * BR, BR), n * BR)
        i = t * 2 * NB + slot_of(b, h)
        return remote(xbf.at[at, cols(h)], xbf.at[at, cols(h)], x_s.at[i], x_r.at[i], mate)

    def block_of(n):
        m = n - G
        pair = m < 2 * E
        t0 = jnp.where(pair, lax.rem(m, 2), 1)
        b0 = jnp.where(pair, jnp.where(t0 == 0, G, 0) + lax.div(m, 2), m - E)
        b0 = jnp.where(m < 0, n, b0)
        t0 = jnp.where(jnp.logical_xor(home, jnp.logical_or(m < 0, t0 == 0)), 1, 0)
        m = n - 2 * NB
        first = n < 2 * NB
        t = jnp.where(first, t0, 1 - lax.div(m, NB))
        b = jnp.where(first, b0, lax.rem(m, NB))
        return jnp.where(first, other, same) + t * PIECE + b * BR

    def a_copy(n):
        slot = lax.rem(n, RING)
        return pltpu.make_async_copy(a_hbm.at[rows_of(block_of(n), BR)], abuf.at[slot], a_sem.at[slot])

    def loop(lo, hi, body):
        def step(i, c):
            body(i)
            return c
        lax.fori_loop(lo, hi, step, 0)

    def units(lo, hi, n, body):
        loop(0, (hi - lo) // n, lambda u: body(lo + u * n))

    def lead_units(h, body):
        units(0, G, LEAD[h], lambda b: body(b, LEAD[h], h))

    def tail_units(h, body):
        units(E, NB, TAIL[h], lambda b: body(b, TAIL[h], h))

    def forward_units(body):
        units(0, E, UF, lambda b: body(b, UF, None))

    mine = row * PIECE
    far = (1 - row) * PIECE
    piece = rows_of(mine, PIECE)
    far_piece = rows_of(far, PIECE)

    def x_in(c):
        return pltpu.make_async_copy(x_hbm.at[rows_of(c * X0R, X0R)], vbuf.at[rows_of(mine + c * X0R, X0R)], xin_sem.at[c])

    def x0_copy(base, c):
        at = rows_of(base + c * X0R, X0R)
        return remote(xbf.at[at], xbf.at[at], x0_s.at[c], x0_r.at[c], mate)

    for c in range(X0C):
        x_in(c).start()
    d_in = pltpu.make_async_copy(d_hbm, dint.at[row], in_sem.at[0])
    v_in = pltpu.make_async_copy(v_hbm, vbuf.at[piece], in_sem.at[1])
    v_out = remote(v_hbm, vbuf.at[piece], ina_send.at[0], ina_recv.at[0], mate)
    d_out = remote(d_hbm, dint.at[row], ina_send.at[1], ina_recv.at[1], mate)
    s0_out = remote(s0buf.at[row], s0buf.at[row], s0_s, s0_r, mate)

    for c in range(X0C):
        x_in(c).wait()

        def convert(i, c=c):
            at = rows_of(mine + c * X0R + i * CH, CH)
            xbf[at, :] = vbuf[at, :].astype(jnp.bfloat16)
        loop(0, X0R // CH, convert)
        if c == 0:
            pl.semaphore_wait(barrier, 7)
        x0_copy(mine, c).start()
        if c < RING:
            a_copy(jnp.int32(c)).start()
    d_in.start()

    @pl.when(away)
    def _():
        d_out.start()
        v_out.start()

    for c in range(X0C):
        x0_copy(far, c).wait_recv()

    def s_copy(par, off):
        dst_col = lax.rem(col + off, 4)
        return remote(sbuf.at[par, col], sbuf.at[par, col], s_s.at[par, off], s_r.at[par, col],
                      (dst_col, lax.div(dst_col, 2)))

    def s_wait(par, off):
        src_col = lax.rem(col + off, 4)
        return remote(sbuf.at[par, src_col], sbuf.at[par, src_col], s_s.at[par, off], s_r.at[par, src_col],
                      (src_col, lax.div(src_col, 2)))

    def s_publish(par, value):
        sbuf[par, col] = value
        for off in range(1, 4):
            s_copy(par, off).start()

    def spread(r):
        def group(g):
            flags = dint[r, pl.ds(g, 1), :].astype(jnp.float32)
            dbuf[rows_of(r * PIECE + g * 128, 128), :] = jnp.broadcast_to(flags, (128, 128)).T
        loop(0, PIECE // 128, group)

    def first_mass():
        d_in.wait()
        spread(row)

        def add(c, acc):
            at = rows_of(mine + c * CH, CH)
            d = dbuf[at, :]
            w = vbuf[at, :] * jnp.concatenate([d, d], axis=1)
            return acc + jnp.sum(w.reshape(CH // 8, 8, VECS), axis=0)
        s0buf[row] = lax.fori_loop(0, PIECE // CH, add, jnp.zeros((8, VECS), jnp.float32))

    def update(t, b, n, h, one, two, acc):
        def step(c, acc):
            at = rows_of(same + t * PIECE + b * BR + c * CH, CH)
            own = rows_of(t * PIECE + b * BR + c * CH, CH)
            there = rows_of(b * BR + c * CH, CH)
            y = (ybuf[at, cols(h)] + one[there, cols(h)]) + two[there, cols(h)]
            cf = jnp.concatenate([coef[:, cols(h)]] * (CH // 8), axis=0)
            x = DAMPING * y + cf * vbuf[own, cols(h)]
            xbf[own, cols(h)] = x.astype(jnp.bfloat16)
            ybuf[at, cols(h)] = x
            d = dbuf[own, :]
            if h is None:
                d = jnp.concatenate([d, d], axis=1)
            return acc + jnp.sum((x * d).reshape(CH // 8, 8, d.shape[1]), axis=0)
        return lax.fori_loop(0, n * BR // CH, step, acc)

    def o_local(t, b, n, h):
        return pltpu.make_async_copy(
            ybuf.at[y_rows(same, t, b, n), cols(h)], out_hbm.at[blk(b, n), cols(h)], o_l.at[slot_of(b, h)])

    def o_remote(t, b, n, h):
        i = slot_of(b, h)
        return remote(ybuf.at[y_rows(same, t, b, n), cols(h)], out_hbm.at[blk(b, n), cols(h)], o_s.at[i], o_r.at[i], mate)

    def emit(t, b, n, h, last):
        @pl.when(jnp.logical_not(last))
        def _():
            c_x(t, b, n, h).start()

        @pl.when(jnp.logical_and(last, row == t))
        def _():
            o_local(t, b, n, h).start()

        @pl.when(jnp.logical_and(last, row != t))
        def _():
            o_remote(t, b, n, h).start()

    def finish(b, n, h, last, acc):
        c_fy(b, n, h).wait_recv()
        acc = update(0, b, n, h, ra, rfy, acc)
        emit(0, b, n, h, last)
        c_fx(b, n, h).wait_recv()
        acc = update(1, b, n, h, rdy, rfx, acc)
        emit(1, b, n, h, last)
        return acc

    def finish_half(h, last):
        n = TAIL[h]
        part = lax.fori_loop(
            0, G // n, lambda u, acc: finish(E + u * n, n, h, last, acc), jnp.zeros((8, HALF), jnp.float32))
        sacc[:, cols(h)] = sacc[:, cols(h)] + part

    def drain_forward():
        @pl.when(home)
        def _():
            forward_units(lambda b, n, h: c_fx(b, n, h).wait_send())
            for half in range(2):
                tail_units(half, lambda b, n, h: c_fx(b, n, h).wait_send())

        @pl.when(away)
        def _():
            forward_units(lambda b, n, h: c_fy(b, n, h).wait_send())
            for half in range(2):
                tail_units(half, lambda b, n, h: c_fy(b, n, h).wait_send())

    def sweep(k, carry):
        last = k == SWEEPS - 1
        par = lax.rem(k, 2)

        def multiply(n, h):
            start = block_of(n)
            ybuf[rows_of(start, BR), cols(h)] = jnp.dot(
                abuf[lax.rem(n, RING)], xbf[:, cols(h)], preferred_element_type=jnp.float32)

        def fetch(n):
            @pl.when(jnp.logical_not(jnp.logical_and(last, n >= 4 * NB)))
            def _():
                a_copy(lax.rem(n, 4 * NB)).start()

        @pl.when(k > 0)
        def _():
            @pl.when(home)
            def _():
                pl.semaphore_wait(cr_hh1, 1)

            @pl.when(away)
            def _():
                pl.semaphore_wait(cr_gy, 1)

        def lead(h):
            def one(n):
                if h == 0:
                    a_copy(n).wait()
                multiply(n, h)
                if h == 1:
                    fetch(n + RING)
                size = LEAD[h]
                whole = lax.rem(n, size) == size - 1
                b = n - (size - 1)

                @pl.when(jnp.logical_and(whole, home))
                def _():
                    c_a(b, size, h).start()

                @pl.when(jnp.logical_and(whole, away))
                def _():
                    c_gy(b, size, h).start()
            loop(0, G, one)

        lead(0)

        @pl.when(k > 0)
        def _():
            @pl.when(home)
            def _():
                finish_half(1, jnp.bool_(False))
                s_publish(par, sacc[...])
                signal(cr_hh2, xn)
                signal(cr_hw, yn)

            @pl.when(away)
            def _():
                for t in range(2):
                    tail_units(1, lambda b, n, h: c_x(t, b, n, h).wait_recv())

        lead(1)

        @pl.when(k > 0)
        def _():
            drain_forward()

            @pl.when(home)
            def _():
                pl.semaphore_wait(cr_hh2, 1)

            @pl.when(away)
            def _():
                pl.semaphore_wait(cr_ww, 1)
                pl.semaphore_wait(cr_hw, 1)

        def rest(n):
            a_copy(n).wait()
            multiply(n, None)
            fetch(n + RING)
            start = block_of(n)
            first = n < 2 * NB
            at = start - jnp.where(first, other, same)
            t, b = lax.div(at, PIECE), lax.div(lax.rem(at, PIECE), BR)

            def send_when(cond, b0, size, start):
                whole = lax.rem(b - b0, size) == size - 1

                @pl.when(jnp.logical_and(cond, whole))
                def _():
                    start(b - (size - 1), size)

            straight = jnp.logical_and(first, t == 0)
            held = n - HOLD + G
            send_when(jnp.logical_and(straight, away), 0, UA_AWAY, lambda b, n: c_a(b, n).start())

            @pl.when(jnp.logical_and(jnp.logical_and(held >= G, held < NB), home))
            def _():
                c_a(held, 1).start()
            send_when(jnp.logical_and(jnp.logical_and(first, t == 1), away), G, UG, lambda b, n: c_gy(b, n).start())
            send_when(jnp.logical_and(jnp.logical_and(jnp.logical_not(first), t == 1), away), 0, UD,
                      lambda b, n: c_dy(b).start())

        loop(G, 4 * NB, rest)

        def add_into(base, t, b, n, src):
            def step(c):
                at = rows_of(base + t * PIECE + b * BR + c * CH, CH)
                ybuf[at, :] = ybuf[at, :] + src[rows_of(b * BR + c * CH, CH), :]
            loop(0, n * BR // CH, step)

        @pl.when(away)
        def _away():
            @pl.when(k == 0)
            def _():
                for c in range(X0C):
                    x0_copy(mine, c).wait_send()

            @pl.when(jnp.logical_not(last))
            def _():
                signal(cr_x, mate)

            @pl.when(k == 0)
            def _():
                first_mass()
                s0_out.start()

            def forward(b, n):
                units(0, n, UA_AWAY, lambda i: c_a(b + i, UA_AWAY).wait())
                add_into(same, 0, b, n, ra)

            def forward_full(b, n, h):
                forward(b, n)
                c_fy(b, n).start()

            def forward_half(b, n, h):
                forward(b, n)
                c_fy(b, n, h).start()
            forward_units(forward_full)
            tail_units(0, forward_half)
            tail_units(1, lambda b, n, h: c_fy(b, n, h).start())

            @pl.when(jnp.logical_not(last))
            def _():
                signal(cr_ww, xn)

            for half in range(2):
                lead_units(half, lambda b, n, h: c_gy(b, n, h).wait_send())
            units(G, NB, UG, lambda b: c_gy(b, UG).wait_send())
            units(0, NB, UD, lambda b: c_dy(b).wait_send())

            @pl.when(k == 0)
            def _():
                v_out.wait_send()
                d_out.wait_send()
                s0_out.wait_send()

            @pl.when(jnp.logical_not(last))
            def _():
                for t in range(2):
                    forward_units(lambda b, n, h: c_x(t, b, n, h).wait_recv())
                    tail_units(0, lambda b, n, h: c_x(t, b, n, h).wait_recv())

        @pl.when(home)
        def _home():
            for half in range(2):
                lead_units(half, lambda b, n, h: c_gy(b, n, h).wait_recv())

            def arrived(b, n):
                @pl.when(b >= G)
                def _():
                    units(0, n, UG, lambda i: c_gy(b + i, UG).wait_recv())

            def forward_full(b, n, h):
                arrived(b, n)
                add_into(other, 1, b, n, rgy)
                c_fx(b, n).start()

            def forward_half(b, n, h):
                arrived(b, n)
                add_into(other, 1, b, n, rgy)
                c_fx(b, n, h).start()
            forward_units(forward_full)
            tail_units(0, forward_half)
            tail_units(1, lambda b, n, h: c_fx(b, n, h).start())

            @pl.when(jnp.logical_not(last))
            def _():
                signal(cr_gy, yn)

            @pl.when(k == 0)
            def _():
                first_mass()
                v_in.start()
                remote(d_hbm, dint.at[1 - row], ina_send.at[1], ina_recv.at[1], mate).wait_recv()
                spread(1 - row)
                remote(s0buf.at[1 - row], s0buf.at[1 - row], s0_s, s0_r, mate).wait_recv()
                s_publish(0, s0buf[0] + s0buf[1])
                for c in range(X0C):
                    x0_copy(mine, c).wait_send()
                remote(v_hbm, vbuf.at[far_piece], ina_send.at[0], ina_recv.at[0], mate).wait_recv()
                v_in.wait()

            @pl.when(k > 0)
            def _():
                for t in range(2):
                    forward_units(lambda b, n, h: c_x(t, b, n, h).wait_send())
                    for half in range(2):
                        tail_units(half, lambda b, n, h: c_x(t, b, n, h).wait_send())

            for off in range(1, 4):
                s_wait(par, off).wait_recv()
                s_copy(par, off).wait_send()
            total = (sbuf[par, 0] + sbuf[par, 1]) + (sbuf[par, 2] + sbuf[par, 3])
            mass = jnp.sum(total, axis=0, keepdims=True) / VERTS
            coef[...] = jnp.broadcast_to(DAMPING * mass + (1.0 - DAMPING), (8, VECS))

            @pl.when(jnp.logical_not(last))
            def _():
                pl.semaphore_wait(cr_x, 1)

            for half in range(2):
                lead_units(half, lambda b, n, h: c_a(b, n, h).wait())
            units(G, NB, UA_HOME, lambda b: c_a(b, UA_HOME).wait())
            units(0, NB, UD, lambda b: c_dy(b).wait_recv())
            acc = lax.fori_loop(
                0, E // UF, lambda u, acc: finish(u * UF, UF, None, last, acc), jnp.zeros((8, VECS), jnp.float32))
            sacc[...] = acc

            @pl.when(jnp.logical_not(last))
            def _():
                signal(cr_hh1, xn)
            finish_half(0, last)

        return carry

    lax.fori_loop(0, SWEEPS, sweep, 0)

    @pl.when(home)
    def _():
        finish_half(1, jnp.bool_(True))
    drain_forward()

    @pl.when(home)
    def _():
        def close(b, n, h):
            o_local(row, b, n, h).wait()
            o_remote(1 - row, b, n, h).wait_send()
        forward_units(close)
        for half in range(2):
            tail_units(half, close)

    @pl.when(away)
    def _():
        def close(b, n, h):
            o_remote(1 - row, b, n, h).wait_recv()
        forward_units(close)
        for half in range(2):
            tail_units(half, close)


def solution(mesh):
    dma = pltpu.SemaphoreType.DMA
    reg = pltpu.SemaphoreType.REGULAR

    def local_sweeps(mat_tile, x_piece, tele_piece, dang_piece):
        part = pltpu.VMEM((PIECE, VECS), jnp.float32)
        return pl.pallas_call(
            kernel,
            name="sweeps",
            out_shape=jax.ShapeDtypeStruct((PIECE, VECS), jnp.float32),
            in_specs=[pl.BlockSpec(memory_space=pl.ANY)] * 4,
            out_specs=pl.BlockSpec(memory_space=pl.ANY),
            scratch_shapes=[
                pltpu.VMEM((RING, BR, COLS), jnp.bfloat16),
                pltpu.VMEM((COLS, VECS), jnp.bfloat16),
                pltpu.VMEM((ROWS, VECS), jnp.float32),
                part, part, part, part, part,
                pltpu.VMEM((COLS, VECS), jnp.float32),
                pltpu.VMEM((COLS, 128), jnp.float32),
                pltpu.VMEM((2, PIECE // 128, 128), jnp.int32),
                pltpu.VMEM((2, 4, 8, VECS), jnp.float32),
                pltpu.VMEM((2, 8, VECS), jnp.float32),
                pltpu.VMEM((8, VECS), jnp.float32),
                pltpu.VMEM((8, VECS), jnp.float32),
                dma((RING,)), dma((X0C,)), dma((2,)), dma((2,)), dma((2,)), dma((X0C,)), dma((X0C,)),
                dma((2 * NB,)), dma((2 * NB,)), dma((2 * NB,)), dma((2 * NB,)), dma((NB,)), dma((NB,)),
                dma((2 * NB,)), dma((2 * NB,)), dma((2 * NB,)), dma((2 * NB,)),
                dma((4 * NB,)), dma((4 * NB,)), dma((2, 4)), dma((2, 4)), dma, dma,
                dma((2 * NB,)), dma((2 * NB,)), dma((2 * NB,)),
                reg, reg, reg, reg, reg, reg,
            ],
            compiler_params=pltpu.CompilerParams(
                collective_id=0, has_side_effects=True, vmem_limit_bytes=67_000_000),
            cost_estimate=pl.CostEstimate(
                flops=2 * ROWS * COLS * VECS * SWEEPS, bytes_accessed=2 * ROWS * COLS * SWEEPS, transcendentals=0),
        )(mat_tile, x_piece, tele_piece, dang_piece.reshape(PIECE // 128, 128))

    vec_spec = P(('col', 'row'), None)
    return jax.shard_map(local_sweeps, mesh=mesh,
                         in_specs=(P('row', 'col'), vec_spec, vec_spec, P(('col', 'row'))),
                         out_specs=vec_spec, check_vma=False)
```

```python
import jax
import jax.numpy as jnp
from jax import lax
from jax.experimental import pallas as pl
from jax.experimental.pallas import tpu as pltpu
from jax.sharding import PartitionSpec as P

SWEEPS = 8
DAMPING = 0.85
MESH = pl.DeviceIdType.MESH

VERTS = 24576
VECS = 256
HALF = 128
PIECE = 3072
ROWS = 12288
COLS = 6144
BR = 256
NB = PIECE // BR
G = 4
E = NB - G
CH = 32
LEAD = (1, 1)
TAIL = (1, 1)
UA_HOME = 1
UA_AWAY = 1
UG = 1
UD = 1
UF = 1
HOLD = 16
RING = 4
X0C = 6
X0R = PIECE // X0C


def kernel(a_hbm, x_hbm, v_hbm, d_hbm, out_hbm,
           abuf, xbf, ybuf, ra, rgy, rdy, rfx, rfy, vbuf, dbuf, dint, sbuf, s0buf, coef, sacc,
           a_sem, xin_sem, in_sem, ina_send, ina_recv, x0_s, x0_r,
           a_s, a_r, gy_s, gy_r, dy_s, dy_r, fx_s, fx_r, fy_s, fy_r,
           x_s, x_r, s_s, s_r, s0_s, s0_r, o_l, o_s, o_r,
           cr_hh1, cr_hh2, cr_hw, cr_gy, cr_ww, cr_x):
    col = lax.axis_index('col')
    row = lax.axis_index('row')
    cx, cy = lax.rem(col, 2), lax.div(col, 2)
    home = row == cy
    away = jnp.logical_not(home)
    xn = (cy * 2 + 1 - cx, row)
    yn = ((1 - cy) * 2 + cx, row)
    mate = (col, 1 - row)
    same = cx * COLS
    other = (1 - cx) * COLS

    barrier = pltpu.get_barrier_semaphore()
    for off in range(4):
        for r in range(2):
            if off == 0 and r == 1:
                continue
            dev = (lax.rem(col + off, 4), row if r == 0 and off else 1 - row)
            pl.semaphore_signal(barrier, inc=1, device_id=dev, device_id_type=MESH)

    def signal(sem, dev):
        pl.semaphore_signal(sem, inc=1, device_id=dev, device_id_type=MESH)

    def rows_of(start, size):
        return pl.ds(pl.multiple_of(start, size), size)

    def blk(b, n):
        return pl.ds(pl.multiple_of(b * BR, BR), n * BR)

    def cols(h):
        return pl.ds(0, VECS) if h is None else pl.ds(h * HALF, HALF)

    def slot_of(b, h):
        return b if h != 1 else NB + b

    def remote(src, dst, send, recv, dev):
        return pltpu.make_async_remote_copy(
            src_ref=src, dst_ref=dst, send_sem=send, recv_sem=recv, device_id=dev, device_id_type=MESH)

    def y_rows(base, t, b, n):
        return pl.ds(pl.multiple_of(base + t * PIECE + b * BR, BR), n * BR)

    def flow(base, t, b, n, h, dst, send, recv, dev):
        i = slot_of(b, h)
        return remote(ybuf.at[y_rows(base, t, b, n), cols(h)], dst.at[blk(b, n), cols(h)], send.at[i], recv.at[i], dev)

    def c_a(b, n, h=None):
        return flow(other, 0, b, n, h, ra, a_s, a_r, xn)

    def c_gy(b, n, h=None):
        return flow(other, 1, b, n, h, rgy, gy_s, gy_r, yn)

    def c_dy(b):
        return flow(same, 1, b, UD, None, rdy, dy_s, dy_r, yn)

    def c_fx(b, n, h=None):
        return flow(other, 1, b, n, h, rfx, fx_s, fx_r, xn)

    def c_fy(b, n, h=None):
        return flow(same, 0, b, n, h, rfy, fy_s, fy_r, yn)

    def c_x(t, b, n, h=None):
        at = pl.ds(pl.multiple_of(t * PIECE + b * BR, BR), n * BR)
        i = t * 2 * NB + slot_of(b, h)
        return remote(xbf.at[at, cols(h)], xbf.at[at, cols(h)], x_s.at[i], x_r.at[i], mate)

    def block_of(n):
        m = n - G
        pair = m < 2 * E
        t0 = jnp.where(pair, lax.rem(m, 2), 1)
        b0 = jnp.where(pair, jnp.where(t0 == 0, G, 0) + lax.div(m, 2), m - E)
        b0 = jnp.where(m < 0, n, b0)
        t0 = jnp.where(jnp.logical_xor(home, jnp.logical_or(m < 0, t0 == 0)), 1, 0)
        m = n - 2 * NB
        first = n < 2 * NB
        t = jnp.where(first, t0, 1 - lax.div(m, NB))
        b = jnp.where(first, b0, lax.rem(m, NB))
        return jnp.where(first, other, same) + t * PIECE + b * BR

    def a_copy(n):
        slot = lax.rem(n, RING)
        return pltpu.make_async_copy(a_hbm.at[rows_of(block_of(n), BR)], abuf.at[slot], a_sem.at[slot])

    def loop(lo, hi, body):
        def step(i, c):
            body(i)
            return c
        lax.fori_loop(lo, hi, step, 0)

    def units(lo, hi, n, body):
        loop(0, (hi - lo) // n, lambda u: body(lo + u * n))

    def lead_units(h, body):
        units(0, G, LEAD[h], lambda b: body(b, LEAD[h], h))

    def tail_units(h, body):
        units(E, NB, TAIL[h], lambda b: body(b, TAIL[h], h))

    def forward_units(body):
        units(0, E, UF, lambda b: body(b, UF, None))

    mine = row * PIECE
    far = (1 - row) * PIECE
    piece = rows_of(mine, PIECE)
    far_piece = rows_of(far, PIECE)

    def x_in(c):
        return pltpu.make_async_copy(x_hbm.at[rows_of(c * X0R, X0R)], vbuf.at[rows_of(mine + c * X0R, X0R)], xin_sem.at[c])

    def x0_copy(base, c):
        at = rows_of(base + c * X0R, X0R)
        return remote(xbf.at[at], xbf.at[at], x0_s.at[c], x0_r.at[c], mate)

    for c in range(X0C):
        x_in(c).start()
    d_in = pltpu.make_async_copy(d_hbm, dint.at[row], in_sem.at[0])
    v_in = pltpu.make_async_copy(v_hbm, vbuf.at[piece], in_sem.at[1])
    v_out = remote(v_hbm, vbuf.at[piece], ina_send.at[0], ina_recv.at[0], mate)
    d_out = remote(d_hbm, dint.at[row], ina_send.at[1], ina_recv.at[1], mate)
    s0_out = remote(s0buf.at[row], s0buf.at[row], s0_s, s0_r, mate)

    for c in range(X0C):
        x_in(c).wait()

        def convert(i, c=c):
            at = rows_of(mine + c * X0R + i * CH, CH)
            xbf[at, :] = vbuf[at, :].astype(jnp.bfloat16)
        loop(0, X0R // CH, convert)
        if c == 0:
            pl.semaphore_wait(barrier, 7)
        x0_copy(mine, c).start()
        if c < RING:
            a_copy(jnp.int32(c)).start()
    d_in.start()

    @pl.when(away)
    def _():
        d_out.start()
        v_out.start()

    for c in range(X0C):
        x0_copy(far, c).wait_recv()

    def s_copy(par, off):
        dst_col = lax.rem(col + off, 4)
        return remote(sbuf.at[par, col], sbuf.at[par, col], s_s.at[par, off], s_r.at[par, col],
                      (dst_col, lax.div(dst_col, 2)))

    def s_wait(par, off):
        src_col = lax.rem(col + off, 4)
        return remote(sbuf.at[par, src_col], sbuf.at[par, src_col], s_s.at[par, off], s_r.at[par, src_col],
                      (src_col, lax.div(src_col, 2)))

    def s_publish(par, value):
        sbuf[par, col] = value
        for off in range(1, 4):
            s_copy(par, off).start()

    def spread(r):
        def group(g):
            flags = dint[r, pl.ds(g, 1), :].astype(jnp.float32)
            dbuf[rows_of(r * PIECE + g * 128, 128), :] = jnp.broadcast_to(flags, (128, 128)).T
        loop(0, PIECE // 128, group)

    def first_mass():
        d_in.wait()
        spread(row)

        def add(c, acc):
            at = rows_of(mine + c * CH, CH)
            d = dbuf[at, :]
            w = vbuf[at, :] * jnp.concatenate([d, d], axis=1)
            return acc + jnp.sum(w.reshape(CH // 8, 8, VECS), axis=0)
        s0buf[row] = lax.fori_loop(0, PIECE // CH, add, jnp.zeros((8, VECS), jnp.float32))

    def update(t, b, n, h, one, two, acc):
        def step(c, acc):
            at = rows_of(same + t * PIECE + b * BR + c * CH, CH)
            own = rows_of(t * PIECE + b * BR + c * CH, CH)
            there = rows_of(b * BR + c * CH, CH)
            y = (ybuf[at, cols(h)] + one[there, cols(h)]) + two[there, cols(h)]
            cf = jnp.concatenate([coef[:, cols(h)]] * (CH // 8), axis=0)
            x = DAMPING * y + cf * vbuf[own, cols(h)]
            xbf[own, cols(h)] = x.astype(jnp.bfloat16)
            ybuf[at, cols(h)] = x
            d = dbuf[own, :]
            if h is None:
                d = jnp.concatenate([d, d], axis=1)
            return acc + jnp.sum((x * d).reshape(CH // 8, 8, d.shape[1]), axis=0)
        return lax.fori_loop(0, n * BR // CH, step, acc)

    def o_local(t, b, n, h):
        return pltpu.make_async_copy(
            ybuf.at[y_rows(same, t, b, n), cols(h)], out_hbm.at[blk(b, n), cols(h)], o_l.at[slot_of(b, h)])

    def o_remote(t, b, n, h):
        i = slot_of(b, h)
        return remote(ybuf.at[y_rows(same, t, b, n), cols(h)], out_hbm.at[blk(b, n), cols(h)], o_s.at[i], o_r.at[i], mate)

    def emit(t, b, n, h, last):
        @pl.when(jnp.logical_not(last))
        def _():
            c_x(t, b, n, h).start()

        @pl.when(jnp.logical_and(last, row == t))
        def _():
            o_local(t, b, n, h).start()

        @pl.when(jnp.logical_and(last, row != t))
        def _():
            o_remote(t, b, n, h).start()

    def finish(b, n, h, last, acc):
        c_fy(b, n, h).wait_recv()
        acc = update(0, b, n, h, ra, rfy, acc)
        emit(0, b, n, h, last)
        c_fx(b, n, h).wait_recv()
        acc = update(1, b, n, h, rdy, rfx, acc)
        emit(1, b, n, h, last)
        return acc

    def finish_half(h, last):
        n = TAIL[h]
        part = lax.fori_loop(
            0, G // n, lambda u, acc: finish(E + u * n, n, h, last, acc), jnp.zeros((8, HALF), jnp.float32))
        sacc[:, cols(h)] = sacc[:, cols(h)] + part

    def drain_forward():
        @pl.when(home)
        def _():
            forward_units(lambda b, n, h: c_fx(b, n, h).wait_send())
            for half in range(2):
                tail_units(half, lambda b, n, h: c_fx(b, n, h).wait_send())

        @pl.when(away)
        def _():
            forward_units(lambda b, n, h: c_fy(b, n, h).wait_send())
            for half in range(2):
                tail_units(half, lambda b, n, h: c_fy(b, n, h).wait_send())

    def sweep(k, carry):
        last = k == SWEEPS - 1
        par = lax.rem(k, 2)

        def multiply(n, h):
            start = block_of(n)
            ybuf[rows_of(start, BR), cols(h)] = jnp.dot(
                abuf[lax.rem(n, RING)], xbf[:, cols(h)], preferred_element_type=jnp.float32)

        def fetch(n):
            @pl.when(jnp.logical_not(jnp.logical_and(last, n >= 4 * NB)))
            def _():
                a_copy(lax.rem(n, 4 * NB)).start()

        @pl.when(k > 0)
        def _():
            @pl.when(home)
            def _():
                pl.semaphore_wait(cr_hh1, 1)

            @pl.when(away)
            def _():
                pl.semaphore_wait(cr_gy, 1)

        def lead(h):
            def one(n):
                if h == 0:
                    a_copy(n).wait()
                multiply(n, h)
                if h == 1:
                    fetch(n + RING)
                size = LEAD[h]
                whole = lax.rem(n, size) == size - 1
                b = n - (size - 1)

                @pl.when(jnp.logical_and(whole, home))
                def _():
                    c_a(b, size, h).start()

                @pl.when(jnp.logical_and(whole, away))
                def _():
                    c_gy(b, size, h).start()
            loop(0, G, one)

        lead(0)

        @pl.when(k > 0)
        def _():
            @pl.when(home)
            def _():
                finish_half(1, jnp.bool_(False))
                s_publish(par, sacc[...])
                signal(cr_hh2, xn)
                signal(cr_hw, yn)

            @pl.when(away)
            def _():
                for t in range(2):
                    tail_units(1, lambda b, n, h: c_x(t, b, n, h).wait_recv())

        lead(1)

        @pl.when(k > 0)
        def _():
            drain_forward()

            @pl.when(home)
            def _():
                pl.semaphore_wait(cr_hh2, 1)

            @pl.when(away)
            def _():
                pl.semaphore_wait(cr_ww, 1)
                pl.semaphore_wait(cr_hw, 1)

        def rest(n):
            a_copy(n).wait()
            multiply(n, None)
            fetch(n + RING)
            start = block_of(n)
            first = n < 2 * NB
            at = start - jnp.where(first, other, same)
            t, b = lax.div(at, PIECE), lax.div(lax.rem(at, PIECE), BR)

            def send_when(cond, b0, size, start):
                whole = lax.rem(b - b0, size) == size - 1

                @pl.when(jnp.logical_and(cond, whole))
                def _():
                    start(b - (size - 1), size)

            straight = jnp.logical_and(first, t == 0)
            held = n - HOLD + G
            send_when(jnp.logical_and(straight, away), 0, UA_AWAY, lambda b, n: c_a(b, n).start())

            @pl.when(jnp.logical_and(jnp.logical_and(held >= G, held < NB), home))
            def _():
                c_a(held, 1).start()
            send_when(jnp.logical_and(jnp.logical_and(first, t == 1), away), G, UG, lambda b, n: c_gy(b, n).start())
            send_when(jnp.logical_and(jnp.logical_and(jnp.logical_not(first), t == 1), away), 0, UD,
                      lambda b, n: c_dy(b).start())

        loop(G, 2 * NB, rest)

        @pl.when(home)
        def _():
            for half in range(2):
                lead_units(half, lambda b, n, h: c_gy(b, n, h).wait_recv())

        def add_into(base, t, b, n, src):
            def step(c):
                at = rows_of(base + t * PIECE + b * BR + c * CH, CH)
                ybuf[at, :] = ybuf[at, :] + src[rows_of(b * BR + c * CH, CH), :]
            loop(0, n * BR // CH, step)

        def forward_home(b):
            @pl.when(b >= G)
            def _():
                c_gy(b, 1).wait_recv()
            add_into(other, 1, b, 1, rgy)

            @pl.when(b < E)
            def _():
                c_fx(b, 1).start()

            @pl.when(b >= E)
            def _():
                c_fx(b, 1, 0).start()

        def forward_away(b):
            c_a(b, 1).wait()
            add_into(same, 0, b, 1, ra)

            @pl.when(b < E)
            def _():
                c_fy(b, 1).start()

            @pl.when(b >= E)
            def _():
                c_fy(b, 1, 0).start()

        def third(n):
            rest(n)

            @pl.when(home)
            def _():
                forward_home(n - 2 * NB)

        def fourth(n):
            rest(n)

            @pl.when(away)
            def _():
                forward_away(n - 3 * NB)

        loop(2 * NB, 3 * NB, third)

        @pl.when(home)
        def _():
            tail_units(1, lambda b, n, h: c_fx(b, n, h).start())

        loop(3 * NB, 4 * NB, fourth)

        @pl.when(away)
        def _away():
            tail_units(1, lambda b, n, h: c_fy(b, n, h).start())

            @pl.when(k == 0)
            def _():
                for c in range(X0C):
                    x0_copy(mine, c).wait_send()

            @pl.when(jnp.logical_not(last))
            def _():
                signal(cr_x, mate)

            @pl.when(k == 0)
            def _():
                first_mass()
                s0_out.start()

            @pl.when(jnp.logical_not(last))
            def _():
                signal(cr_ww, xn)

            for half in range(2):
                lead_units(half, lambda b, n, h: c_gy(b, n, h).wait_send())
            units(G, NB, UG, lambda b: c_gy(b, UG).wait_send())
            units(0, NB, UD, lambda b: c_dy(b).wait_send())

            @pl.when(k == 0)
            def _():
                v_out.wait_send()
                d_out.wait_send()
                s0_out.wait_send()

            @pl.when(jnp.logical_not(last))
            def _():
                for t in range(2):
                    forward_units(lambda b, n, h: c_x(t, b, n, h).wait_recv())
                    tail_units(0, lambda b, n, h: c_x(t, b, n, h).wait_recv())

        @pl.when(home)
        def _home():
            @pl.when(jnp.logical_not(last))
            def _():
                signal(cr_gy, yn)

            @pl.when(k == 0)
            def _():
                first_mass()
                v_in.start()
                remote(d_hbm, dint.at[1 - row], ina_send.at[1], ina_recv.at[1], mate).wait_recv()
                spread(1 - row)
                remote(s0buf.at[1 - row], s0buf.at[1 - row], s0_s, s0_r, mate).wait_recv()
                s_publish(0, s0buf[0] + s0buf[1])
                for c in range(X0C):
                    x0_copy(mine, c).wait_send()
                remote(v_hbm, vbuf.at[far_piece], ina_send.at[0], ina_recv.at[0], mate).wait_recv()
                v_in.wait()

            @pl.when(k > 0)
            def _():
                for t in range(2):
                    forward_units(lambda b, n, h: c_x(t, b, n, h).wait_send())
                    for half in range(2):
                        tail_units(half, lambda b, n, h: c_x(t, b, n, h).wait_send())

            for off in range(1, 4):
                s_wait(par, off).wait_recv()
                s_copy(par, off).wait_send()
            total = (sbuf[par, 0] + sbuf[par, 1]) + (sbuf[par, 2] + sbuf[par, 3])
            mass = jnp.sum(total, axis=0, keepdims=True) / VERTS
            coef[...] = jnp.broadcast_to(DAMPING * mass + (1.0 - DAMPING), (8, VECS))

            @pl.when(jnp.logical_not(last))
            def _():
                pl.semaphore_wait(cr_x, 1)

            for half in range(2):
                lead_units(half, lambda b, n, h: c_a(b, n, h).wait())
            units(G, NB, UA_HOME, lambda b: c_a(b, UA_HOME).wait())
            units(0, NB, UD, lambda b: c_dy(b).wait_recv())
            acc = lax.fori_loop(
                0, E // UF, lambda u, acc: finish(u * UF, UF, None, last, acc), jnp.zeros((8, VECS), jnp.float32))
            sacc[...] = acc

            @pl.when(jnp.logical_not(last))
            def _():
                signal(cr_hh1, xn)
            finish_half(0, last)

        return carry

    lax.fori_loop(0, SWEEPS, sweep, 0)

    @pl.when(home)
    def _():
        finish_half(1, jnp.bool_(True))
    drain_forward()

    @pl.when(home)
    def _():
        def close(b, n, h):
            o_local(row, b, n, h).wait()
            o_remote(1 - row, b, n, h).wait_send()
        forward_units(close)
        for half in range(2):
            tail_units(half, close)

    @pl.when(away)
    def _():
        def close(b, n, h):
            o_remote(1 - row, b, n, h).wait_recv()
        forward_units(close)
        for half in range(2):
            tail_units(half, close)


def solution(mesh):
    dma = pltpu.SemaphoreType.DMA
    reg = pltpu.SemaphoreType.REGULAR

    def local_sweeps(mat_tile, x_piece, tele_piece, dang_piece):
        part = pltpu.VMEM((PIECE, VECS), jnp.float32)
        return pl.pallas_call(
            kernel,
            name="sweeps",
            out_shape=jax.ShapeDtypeStruct((PIECE, VECS), jnp.float32),
            in_specs=[pl.BlockSpec(memory_space=pl.ANY)] * 4,
            out_specs=pl.BlockSpec(memory_space=pl.ANY),
            scratch_shapes=[
                pltpu.VMEM((RING, BR, COLS), jnp.bfloat16),
                pltpu.VMEM((COLS, VECS), jnp.bfloat16),
                pltpu.VMEM((ROWS, VECS), jnp.float32),
                part, part, part, part, part,
                pltpu.VMEM((COLS, VECS), jnp.float32),
                pltpu.VMEM((COLS, 128), jnp.float32),
                pltpu.VMEM((2, PIECE // 128, 128), jnp.int32),
                pltpu.VMEM((2, 4, 8, VECS), jnp.float32),
                pltpu.VMEM((2, 8, VECS), jnp.float32),
                pltpu.VMEM((8, VECS), jnp.float32),
                pltpu.VMEM((8, VECS), jnp.float32),
                dma((RING,)), dma((X0C,)), dma((2,)), dma((2,)), dma((2,)), dma((X0C,)), dma((X0C,)),
                dma((2 * NB,)), dma((2 * NB,)), dma((2 * NB,)), dma((2 * NB,)), dma((NB,)), dma((NB,)),
                dma((2 * NB,)), dma((2 * NB,)), dma((2 * NB,)), dma((2 * NB,)),
                dma((4 * NB,)), dma((4 * NB,)), dma((2, 4)), dma((2, 4)), dma, dma,
                dma((2 * NB,)), dma((2 * NB,)), dma((2 * NB,)),
                reg, reg, reg, reg, reg, reg,
            ],
            compiler_params=pltpu.CompilerParams(
                collective_id=0, has_side_effects=True, vmem_limit_bytes=67_000_000),
            cost_estimate=pl.CostEstimate(
                flops=2 * ROWS * COLS * VECS * SWEEPS, bytes_accessed=2 * ROWS * COLS * SWEEPS, transcendentals=0),
        )(mat_tile, x_piece, tele_piece, dang_piece.reshape(PIECE // 128, 128))

    vec_spec = P(('col', 'row'), None)
    return jax.shard_map(local_sweeps, mesh=mesh,
                         in_specs=(P('row', 'col'), vec_spec, vec_spec, P(('col', 'row'))),
                         out_specs=vec_spec, check_vma=False)
```

```python
import jax
import jax.numpy as jnp
from jax import lax
from jax.experimental import pallas as pl
from jax.experimental.pallas import tpu as pltpu
from jax.sharding import PartitionSpec as P

SWEEPS = 8
DAMPING = 0.85
MESH = pl.DeviceIdType.MESH

VERTS = 24576
VECS = 256
HALF = 128
PIECE = 3072
ROWS = 12288
COLS = 6144
BR = 256
NB = PIECE // BR
G = 6
E = NB - G
CH = 32
LEAD = (1, 1)
TAIL = (1, 1)
UA_HOME = 1
UA_AWAY = 1
UG = 1
UD = 1
UF = 1
HOLD = 16
RING = 6
X0C = 6
X0R = PIECE // X0C


def kernel(a_hbm, x_hbm, v_hbm, d_hbm, out_hbm,
           abuf, xbf, ybuf, ra, rgy, rdy, rfx, rfy, vbuf, dbuf, dint, sbuf, s0buf, coef, sacc,
           a_sem, xin_sem, in_sem, ina_send, ina_recv, x0_s, x0_r,
           a_s, a_r, gy_s, gy_r, dy_s, dy_r, fx_s, fx_r, fy_s, fy_r,
           x_s, x_r, s_s, s_r, s0_s, s0_r, o_l, o_s, o_r,
           cr_hh1, cr_hh2, cr_hw, cr_gy, cr_ww, cr_x):
    col = lax.axis_index('col')
    row = lax.axis_index('row')
    cx, cy = lax.rem(col, 2), lax.div(col, 2)
    home = row == cy
    away = jnp.logical_not(home)
    xn = (cy * 2 + 1 - cx, row)
    yn = ((1 - cy) * 2 + cx, row)
    mate = (col, 1 - row)
    same = cx * COLS
    other = (1 - cx) * COLS

    barrier = pltpu.get_barrier_semaphore()
    for off in range(4):
        for r in range(2):
            if off == 0 and r == 1:
                continue
            dev = (lax.rem(col + off, 4), row if r == 0 and off else 1 - row)
            pl.semaphore_signal(barrier, inc=1, device_id=dev, device_id_type=MESH)

    def signal(sem, dev):
        pl.semaphore_signal(sem, inc=1, device_id=dev, device_id_type=MESH)

    def rows_of(start, size):
        return pl.ds(pl.multiple_of(start, size), size)

    def blk(b, n):
        return pl.ds(pl.multiple_of(b * BR, BR), n * BR)

    def cols(h):
        return pl.ds(0, VECS) if h is None else pl.ds(h * HALF, HALF)

    def slot_of(b, h):
        return b if h != 1 else NB + b

    def remote(src, dst, send, recv, dev):
        return pltpu.make_async_remote_copy(
            src_ref=src, dst_ref=dst, send_sem=send, recv_sem=recv, device_id=dev, device_id_type=MESH)

    def y_rows(base, t, b, n):
        return pl.ds(pl.multiple_of(base + t * PIECE + b * BR, BR), n * BR)

    def flow(base, t, b, n, h, dst, send, recv, dev):
        i = slot_of(b, h)
        return remote(ybuf.at[y_rows(base, t, b, n), cols(h)], dst.at[blk(b, n), cols(h)], send.at[i], recv.at[i], dev)

    def c_a(b, n, h=None):
        return flow(other, 0, b, n, h, ra, a_s, a_r, xn)

    def c_gy(b, n, h=None):
        return flow(other, 1, b, n, h, rgy, gy_s, gy_r, yn)

    def c_dy(b):
        return flow(same, 1, b, UD, None, rdy, dy_s, dy_r, yn)

    def c_fx(b, n, h=None):
        return flow(other, 1, b, n, h, rfx, fx_s, fx_r, xn)

    def c_fy(b, n, h=None):
        return flow(same, 0, b, n, h, rfy, fy_s, fy_r, yn)

    def c_x(t, b, n, h=None):
        at = pl.ds(pl.multiple_of(t * PIECE + b * BR, BR), n * BR)
        i = t * 2 * NB + slot_of(b, h)
        return remote(xbf.at[at, cols(h)], xbf.at[at, cols(h)], x_s.at[i], x_r.at[i], mate)

    def block_of(n):
        m = n - G
        pair = m < 2 * E
        t0 = jnp.where(pair, lax.rem(m, 2), 1)
        b0 = jnp.where(pair, jnp.where(t0 == 0, G, 0) + lax.div(m, 2), m - E)
        b0 = jnp.where(m < 0, n, b0)
        t0 = jnp.where(jnp.logical_xor(home, jnp.logical_or(m < 0, t0 == 0)), 1, 0)
        m = n - 2 * NB
        first = n < 2 * NB
        t = jnp.where(first, t0, 1 - lax.div(m, NB))
        b = jnp.where(first, b0, lax.rem(m, NB))
        return jnp.where(first, other, same) + t * PIECE + b * BR

    def a_copy(n):
        slot = lax.rem(n, RING)
        return pltpu.make_async_copy(a_hbm.at[rows_of(block_of(n), BR)], abuf.at[slot], a_sem.at[slot])

    def loop(lo, hi, body):
        def step(i, c):
            body(i)
            return c
        lax.fori_loop(lo, hi, step, 0)

    def units(lo, hi, n, body):
        loop(0, (hi - lo) // n, lambda u: body(lo + u * n))

    def lead_units(h, body):
        units(0, G, LEAD[h], lambda b: body(b, LEAD[h], h))

    def tail_units(h, body):
        units(E, NB, TAIL[h], lambda b: body(b, TAIL[h], h))

    def forward_units(body):
        units(0, E, UF, lambda b: body(b, UF, None))

    mine = row * PIECE
    far = (1 - row) * PIECE
    piece = rows_of(mine, PIECE)
    far_piece = rows_of(far, PIECE)

    def x_in(c):
        return pltpu.make_async_copy(x_hbm.at[rows_of(c * X0R, X0R)], vbuf.at[rows_of(mine + c * X0R, X0R)], xin_sem.at[c])

    def x0_copy(base, c):
        at = rows_of(base + c * X0R, X0R)
        return remote(xbf.at[at], xbf.at[at], x0_s.at[c], x0_r.at[c], mate)

    for c in range(X0C):
        x_in(c).start()
    d_in = pltpu.make_async_copy(d_hbm, dint.at[row], in_sem.at[0])
    v_in = pltpu.make_async_copy(v_hbm, vbuf.at[piece], in_sem.at[1])
    v_out = remote(v_hbm, vbuf.at[piece], ina_send.at[0], ina_recv.at[0], mate)
    d_out = remote(d_hbm, dint.at[row], ina_send.at[1], ina_recv.at[1], mate)
    s0_out = remote(s0buf.at[row], s0buf.at[row], s0_s, s0_r, mate)

    for c in range(X0C):
        x_in(c).wait()

        def convert(i, c=c):
            at = rows_of(mine + c * X0R + i * CH, CH)
            xbf[at, :] = vbuf[at, :].astype(jnp.bfloat16)
        loop(0, X0R // CH, convert)
        if c == 0:
            pl.semaphore_wait(barrier, 7)
        x0_copy(mine, c).start()
        if c < RING:
            a_copy(jnp.int32(c)).start()
    d_in.start()

    @pl.when(away)
    def _():
        d_out.start()
        v_out.start()

    for c in range(X0C):
        x0_copy(far, c).wait_recv()

    def s_copy(par, off):
        dst_col = lax.rem(col + off, 4)
        return remote(sbuf.at[par, col], sbuf.at[par, col], s_s.at[par, off], s_r.at[par, col],
                      (dst_col, lax.div(dst_col, 2)))

    def s_wait(par, off):
        src_col = lax.rem(col + off, 4)
        return remote(sbuf.at[par, src_col], sbuf.at[par, src_col], s_s.at[par, off], s_r.at[par, src_col],
                      (src_col, lax.div(src_col, 2)))

    def s_publish(par, value):
        sbuf[par, col] = value
        for off in range(1, 4):
            s_copy(par, off).start()

    def spread(r):
        def group(g):
            flags = dint[r, pl.ds(g, 1), :].astype(jnp.float32)
            dbuf[rows_of(r * PIECE + g * 128, 128), :] = jnp.broadcast_to(flags, (128, 128)).T
        loop(0, PIECE // 128, group)

    def first_mass():
        d_in.wait()
        spread(row)

        def add(c, acc):
            at = rows_of(mine + c * CH, CH)
            d = dbuf[at, :]
            w = vbuf[at, :] * jnp.concatenate([d, d], axis=1)
            return acc + jnp.sum(w.reshape(CH // 8, 8, VECS), axis=0)
        s0buf[row] = lax.fori_loop(0, PIECE // CH, add, jnp.zeros((8, VECS), jnp.float32))

    def update(t, b, n, h, one, two, acc):
        def step(c, acc):
            at = rows_of(same + t * PIECE + b * BR + c * CH, CH)
            own = rows_of(t * PIECE + b * BR + c * CH, CH)
            there = rows_of(b * BR + c * CH, CH)
            y = (ybuf[at, cols(h)] + one[there, cols(h)]) + two[there, cols(h)]
            cf = jnp.concatenate([coef[:, cols(h)]] * (CH // 8), axis=0)
            x = DAMPING * y + cf * vbuf[own, cols(h)]
            xbf[own, cols(h)] = x.astype(jnp.bfloat16)
            ybuf[at, cols(h)] = x
            d = dbuf[own, :]
            if h is None:
                d = jnp.concatenate([d, d], axis=1)
            return acc + jnp.sum((x * d).reshape(CH // 8, 8, d.shape[1]), axis=0)
        return lax.fori_loop(0, n * BR // CH, step, acc)

    def o_local(t, b, n, h):
        return pltpu.make_async_copy(
            ybuf.at[y_rows(same, t, b, n), cols(h)], out_hbm.at[blk(b, n), cols(h)], o_l.at[slot_of(b, h)])

    def o_remote(t, b, n, h):
        i = slot_of(b, h)
        return remote(ybuf.at[y_rows(same, t, b, n), cols(h)], out_hbm.at[blk(b, n), cols(h)], o_s.at[i], o_r.at[i], mate)

    def emit(t, b, n, h, last):
        @pl.when(jnp.logical_not(last))
        def _():
            c_x(t, b, n, h).start()

        @pl.when(jnp.logical_and(last, row == t))
        def _():
            o_local(t, b, n, h).start()

        @pl.when(jnp.logical_and(last, row != t))
        def _():
            o_remote(t, b, n, h).start()

    def finish(b, n, h, last, acc):
        c_fy(b, n, h).wait_recv()
        acc = update(0, b, n, h, ra, rfy, acc)
        emit(0, b, n, h, last)
        c_fx(b, n, h).wait_recv()
        acc = update(1, b, n, h, rdy, rfx, acc)
        emit(1, b, n, h, last)
        return acc

    def finish_half(h, last):
        n = TAIL[h]
        part = lax.fori_loop(
            0, G // n, lambda u, acc: finish(E + u * n, n, h, last, acc), jnp.zeros((8, HALF), jnp.float32))
        sacc[:, cols(h)] = sacc[:, cols(h)] + part

    def drain_forward():
        @pl.when(home)
        def _():
            forward_units(lambda b, n, h: c_fx(b, n, h).wait_send())
            for half in range(2):
                tail_units(half, lambda b, n, h: c_fx(b, n, h).wait_send())

        @pl.when(away)
        def _():
            forward_units(lambda b, n, h: c_fy(b, n, h).wait_send())
            for half in range(2):
                tail_units(half, lambda b, n, h: c_fy(b, n, h).wait_send())

    def sweep(k, carry):
        last = k == SWEEPS - 1
        par = lax.rem(k, 2)

        def multiply(n, h):
            start = block_of(n)
            ybuf[rows_of(start, BR), cols(h)] = jnp.dot(
                abuf[lax.rem(n, RING)], xbf[:, cols(h)], preferred_element_type=jnp.float32)

        def fetch(n):
            @pl.when(jnp.logical_not(jnp.logical_and(last, n >= 4 * NB)))
            def _():
                a_copy(lax.rem(n, 4 * NB)).start()

        @pl.when(k > 0)
        def _():
            @pl.when(home)
            def _():
                pl.semaphore_wait(cr_hh1, 1)

            @pl.when(away)
            def _():
                pl.semaphore_wait(cr_gy, 1)

        def lead(h):
            def one(n):
                if h == 0:
                    a_copy(n).wait()
                multiply(n, h)
                if h == 1:
                    fetch(n + RING)
                size = LEAD[h]
                whole = lax.rem(n, size) == size - 1
                b = n - (size - 1)

                @pl.when(jnp.logical_and(whole, home))
                def _():
                    c_a(b, size, h).start()

                @pl.when(jnp.logical_and(whole, away))
                def _():
                    c_gy(b, size, h).start()
            loop(0, G, one)

        lead(0)

        @pl.when(k > 0)
        def _():
            @pl.when(home)
            def _():
                finish_half(1, jnp.bool_(False))
                s_publish(par, sacc[...])
                signal(cr_hh2, xn)
                signal(cr_hw, yn)

            @pl.when(away)
            def _():
                for t in range(2):
                    tail_units(1, lambda b, n, h: c_x(t, b, n, h).wait_recv())

        lead(1)

        @pl.when(k > 0)
        def _():
            drain_forward()

            @pl.when(home)
            def _():
                pl.semaphore_wait(cr_hh2, 1)

            @pl.when(away)
            def _():
                pl.semaphore_wait(cr_ww, 1)
                pl.semaphore_wait(cr_hw, 1)

        def rest(n):
            a_copy(n).wait()
            multiply(n, None)
            fetch(n + RING)
            start = block_of(n)
            first = n < 2 * NB
            at = start - jnp.where(first, other, same)
            t, b = lax.div(at, PIECE), lax.div(lax.rem(at, PIECE), BR)

            def send_when(cond, b0, size, start):
                whole = lax.rem(b - b0, size) == size - 1

                @pl.when(jnp.logical_and(cond, whole))
                def _():
                    start(b - (size - 1), size)

            straight = jnp.logical_and(first, t == 0)
            held = n - HOLD + G
            send_when(jnp.logical_and(straight, away), 0, UA_AWAY, lambda b, n: c_a(b, n).start())

            @pl.when(jnp.logical_and(jnp.logical_and(held >= G, held < NB), home))
            def _():
                c_a(held, 1).start()
            send_when(jnp.logical_and(jnp.logical_and(first, t == 1), away), G, UG, lambda b, n: c_gy(b, n).start())
            send_when(jnp.logical_and(jnp.logical_and(jnp.logical_not(first), t == 1), away), 0, UD,
                      lambda b, n: c_dy(b).start())

        loop(G, 2 * NB, rest)

        @pl.when(home)
        def _():
            for half in range(2):
                lead_units(half, lambda b, n, h: c_gy(b, n, h).wait_recv())

        def add_into(base, t, b, n, src):
            def step(c):
                at = rows_of(base + t * PIECE + b * BR + c * CH, CH)
                ybuf[at, :] = ybuf[at, :] + src[rows_of(b * BR + c * CH, CH), :]
            loop(0, n * BR // CH, step)

        def forward_home(b):
            @pl.when(b >= G)
            def _():
                c_gy(b, 1).wait_recv()
            add_into(other, 1, b, 1, rgy)

            @pl.when(b < E)
            def _():
                c_fx(b, 1).start()

            @pl.when(b >= E)
            def _():
                c_fx(b, 1, 0).start()

        def forward_away(b):
            c_a(b, 1).wait()
            add_into(same, 0, b, 1, ra)

            @pl.when(b < E)
            def _():
                c_fy(b, 1).start()

            @pl.when(b >= E)
            def _():
                c_fy(b, 1, 0).start()

        def third(n):
            rest(n)

            @pl.when(home)
            def _():
                forward_home(n - 2 * NB)

        def fourth(n):
            rest(n)

            @pl.when(away)
            def _():
                forward_away(n - 3 * NB)

        loop(2 * NB, 3 * NB, third)

        @pl.when(home)
        def _():
            tail_units(1, lambda b, n, h: c_fx(b, n, h).start())

        loop(3 * NB, 4 * NB, fourth)

        @pl.when(away)
        def _away():
            tail_units(1, lambda b, n, h: c_fy(b, n, h).start())

            @pl.when(k == 0)
            def _():
                for c in range(X0C):
                    x0_copy(mine, c).wait_send()

            @pl.when(jnp.logical_not(last))
            def _():
                signal(cr_x, mate)

            @pl.when(k == 0)
            def _():
                first_mass()
                s0_out.start()

            @pl.when(jnp.logical_not(last))
            def _():
                signal(cr_ww, xn)

            for half in range(2):
                lead_units(half, lambda b, n, h: c_gy(b, n, h).wait_send())
            units(G, NB, UG, lambda b: c_gy(b, UG).wait_send())
            units(0, NB, UD, lambda b: c_dy(b).wait_send())

            @pl.when(k == 0)
            def _():
                v_out.wait_send()
                d_out.wait_send()
                s0_out.wait_send()

            @pl.when(jnp.logical_not(last))
            def _():
                for t in range(2):
                    forward_units(lambda b, n, h: c_x(t, b, n, h).wait_recv())
                    tail_units(0, lambda b, n, h: c_x(t, b, n, h).wait_recv())

        @pl.when(home)
        def _home():
            @pl.when(jnp.logical_not(last))
            def _():
                signal(cr_gy, yn)

            @pl.when(k == 0)
            def _():
                first_mass()
                v_in.start()
                remote(d_hbm, dint.at[1 - row], ina_send.at[1], ina_recv.at[1], mate).wait_recv()
                spread(1 - row)
                remote(s0buf.at[1 - row], s0buf.at[1 - row], s0_s, s0_r, mate).wait_recv()
                s_publish(0, s0buf[0] + s0buf[1])
                for c in range(X0C):
                    x0_copy(mine, c).wait_send()
                remote(v_hbm, vbuf.at[far_piece], ina_send.at[0], ina_recv.at[0], mate).wait_recv()
                v_in.wait()

            @pl.when(k > 0)
            def _():
                for t in range(2):
                    forward_units(lambda b, n, h: c_x(t, b, n, h).wait_send())
                    for half in range(2):
                        tail_units(half, lambda b, n, h: c_x(t, b, n, h).wait_send())

            for off in range(1, 4):
                s_wait(par, off).wait_recv()
                s_copy(par, off).wait_send()
            total = (sbuf[par, 0] + sbuf[par, 1]) + (sbuf[par, 2] + sbuf[par, 3])
            mass = jnp.sum(total, axis=0, keepdims=True) / VERTS
            coef[...] = jnp.broadcast_to(DAMPING * mass + (1.0 - DAMPING), (8, VECS))

            @pl.when(jnp.logical_not(last))
            def _():
                pl.semaphore_wait(cr_x, 1)

            for half in range(2):
                lead_units(half, lambda b, n, h: c_a(b, n, h).wait())
            units(G, NB, UA_HOME, lambda b: c_a(b, UA_HOME).wait())
            units(0, NB, UD, lambda b: c_dy(b).wait_recv())
            acc = lax.fori_loop(
                0, E // UF, lambda u, acc: finish(u * UF, UF, None, last, acc), jnp.zeros((8, VECS), jnp.float32))
            sacc[...] = acc

            @pl.when(jnp.logical_not(last))
            def _():
                signal(cr_hh1, xn)
            finish_half(0, last)

        return carry

    lax.fori_loop(0, SWEEPS, sweep, 0)

    @pl.when(home)
    def _():
        finish_half(1, jnp.bool_(True))
    drain_forward()

    @pl.when(home)
    def _():
        def close(b, n, h):
            o_local(row, b, n, h).wait()
            o_remote(1 - row, b, n, h).wait_send()
        forward_units(close)
        for half in range(2):
            tail_units(half, close)

    @pl.when(away)
    def _():
        def close(b, n, h):
            o_remote(1 - row, b, n, h).wait_recv()
        forward_units(close)
        for half in range(2):
            tail_units(half, close)


def solution(mesh):
    dma = pltpu.SemaphoreType.DMA
    reg = pltpu.SemaphoreType.REGULAR

    def local_sweeps(mat_tile, x_piece, tele_piece, dang_piece):
        part = pltpu.VMEM((PIECE, VECS), jnp.float32)
        return pl.pallas_call(
            kernel,
            name="sweeps",
            out_shape=jax.ShapeDtypeStruct((PIECE, VECS), jnp.float32),
            in_specs=[pl.BlockSpec(memory_space=pl.ANY)] * 4,
            out_specs=pl.BlockSpec(memory_space=pl.ANY),
            scratch_shapes=[
                pltpu.VMEM((RING, BR, COLS), jnp.bfloat16),
                pltpu.VMEM((COLS, VECS), jnp.bfloat16),
                pltpu.VMEM((ROWS, VECS), jnp.float32),
                part, part, part, part, part,
                pltpu.VMEM((COLS, VECS), jnp.float32),
                pltpu.VMEM((COLS, 128), jnp.float32),
                pltpu.VMEM((2, PIECE // 128, 128), jnp.int32),
                pltpu.VMEM((2, 4, 8, VECS), jnp.float32),
                pltpu.VMEM((2, 8, VECS), jnp.float32),
                pltpu.VMEM((8, VECS), jnp.float32),
                pltpu.VMEM((8, VECS), jnp.float32),
                dma((RING,)), dma((X0C,)), dma((2,)), dma((2,)), dma((2,)), dma((X0C,)), dma((X0C,)),
                dma((2 * NB,)), dma((2 * NB,)), dma((2 * NB,)), dma((2 * NB,)), dma((NB,)), dma((NB,)),
                dma((2 * NB,)), dma((2 * NB,)), dma((2 * NB,)), dma((2 * NB,)),
                dma((4 * NB,)), dma((4 * NB,)), dma((2, 4)), dma((2, 4)), dma, dma,
                dma((2 * NB,)), dma((2 * NB,)), dma((2 * NB,)),
                reg, reg, reg, reg, reg, reg,
            ],
            compiler_params=pltpu.CompilerParams(
                collective_id=0, has_side_effects=True, vmem_limit_bytes=67_000_000),
            cost_estimate=pl.CostEstimate(
                flops=2 * ROWS * COLS * VECS * SWEEPS, bytes_accessed=2 * ROWS * COLS * SWEEPS, transcendentals=0),
        )(mat_tile, x_piece, tele_piece, dang_piece.reshape(PIECE // 128, 128))

    vec_spec = P(('col', 'row'), None)
    return jax.shard_map(local_sweeps, mesh=mesh,
                         in_specs=(P('row', 'col'), vec_spec, vec_spec, P(('col', 'row'))),
                         out_specs=vec_spec, check_vma=False)
```

```python
import jax
import jax.numpy as jnp
from jax import lax
from jax.experimental import pallas as pl
from jax.experimental.pallas import tpu as pltpu
from jax.sharding import PartitionSpec as P

SWEEPS = 8
DAMPING = 0.85
MESH = pl.DeviceIdType.MESH

VERTS = 24576
VECS = 256
HALF = 128
PIECE = 3072
ROWS = 12288
COLS = 6144
BR = 256
NB = PIECE // BR
G = 4
E = NB - G
CH = 32
LEAD = (1, 1)
TAIL = (1, 1)
UA_HOME = 1
UA_AWAY = 1
UG = 1
UD = 1
UF = 1
HOLD = 36
RING = 4
X0C = 6
X0R = PIECE // X0C


def kernel(a_hbm, x_hbm, v_hbm, d_hbm, out_hbm,
           abuf, xbf, ybuf, ra, rgy, rdy, rfx, rfy, vbuf, dbuf, dint, sbuf, s0buf, coef, sacc,
           a_sem, xin_sem, in_sem, ina_send, ina_recv, x0_s, x0_r,
           a_s, a_r, gy_s, gy_r, dy_s, dy_r, fx_s, fx_r, fy_s, fy_r,
           x_s, x_r, s_s, s_r, s0_s, s0_r, o_l, o_s, o_r,
           cr_hh1, cr_hh2, cr_hw, cr_gy, cr_ww, cr_x):
    col = lax.axis_index('col')
    row = lax.axis_index('row')
    cx, cy = lax.rem(col, 2), lax.div(col, 2)
    home = row == cy
    away = jnp.logical_not(home)
    xn = (cy * 2 + 1 - cx, row)
    yn = ((1 - cy) * 2 + cx, row)
    mate = (col, 1 - row)
    same = cx * COLS
    other = (1 - cx) * COLS

    barrier = pltpu.get_barrier_semaphore()
    for off in range(4):
        for r in range(2):
            if off == 0 and r == 1:
                continue
            dev = (lax.rem(col + off, 4), row if r == 0 and off else 1 - row)
            pl.semaphore_signal(barrier, inc=1, device_id=dev, device_id_type=MESH)

    def signal(sem, dev):
        pl.semaphore_signal(sem, inc=1, device_id=dev, device_id_type=MESH)

    def rows_of(start, size):
        return pl.ds(pl.multiple_of(start, size), size)

    def blk(b, n):
        return pl.ds(pl.multiple_of(b * BR, BR), n * BR)

    def cols(h):
        return pl.ds(0, VECS) if h is None else pl.ds(h * HALF, HALF)

    def slot_of(b, h):
        return b if h != 1 else NB + b

    def remote(src, dst, send, recv, dev):
        return pltpu.make_async_remote_copy(
            src_ref=src, dst_ref=dst, send_sem=send, recv_sem=recv, device_id=dev, device_id_type=MESH)

    def y_rows(base, t, b, n):
        return pl.ds(pl.multiple_of(base + t * PIECE + b * BR, BR), n * BR)

    def flow(base, t, b, n, h, dst, send, recv, dev):
        i = slot_of(b, h)
        return remote(ybuf.at[y_rows(base, t, b, n), cols(h)], dst.at[blk(b, n), cols(h)], send.at[i], recv.at[i], dev)

    def c_a(b, n, h=None):
        return flow(other, 0, b, n, h, ra, a_s, a_r, xn)

    def c_gy(b, n, h=None):
        return flow(other, 1, b, n, h, rgy, gy_s, gy_r, yn)

    def c_dy(b):
        return flow(same, 1, b, UD, None, rdy, dy_s, dy_r, yn)

    def c_fx(b, n, h=None):
        return flow(other, 1, b, n, h, rfx, fx_s, fx_r, xn)

    def c_fy(b, n, h=None):
        return flow(same, 0, b, n, h, rfy, fy_s, fy_r, yn)

    def c_x(t, b, n, h=None):
        at = pl.ds(pl.multiple_of(t * PIECE + b * BR, BR), n * BR)
        i = t * 2 * NB + slot_of(b, h)
        return remote(xbf.at[at, cols(h)], xbf.at[at, cols(h)], x_s.at[i], x_r.at[i], mate)

    def block_of(n):
        m = n - G
        pair = m < 2 * E
        t0 = jnp.where(pair, lax.rem(m, 2), 1)
        b0 = jnp.where(pair, jnp.where(t0 == 0, G, 0) + lax.div(m, 2), m - E)
        b0 = jnp.where(m < 0, n, b0)
        t0 = jnp.where(jnp.logical_xor(home, jnp.logical_or(m < 0, t0 == 0)), 1, 0)
        m = n - 2 * NB
        first = n < 2 * NB
        t = jnp.where(first, t0, 1 - lax.div(m, NB))
        b = jnp.where(first, b0, lax.rem(m, NB))
        return jnp.where(first, other, same) + t * PIECE + b * BR

    def a_copy(n):
        slot = lax.rem(n, RING)
        return pltpu.make_async_copy(a_hbm.at[rows_of(block_of(n), BR)], abuf.at[slot], a_sem.at[slot])

    def loop(lo, hi, body):
        def step(i, c):
            body(i)
            return c
        lax.fori_loop(lo, hi, step, 0)

    def units(lo, hi, n, body):
        loop(0, (hi - lo) // n, lambda u: body(lo + u * n))

    def lead_units(h, body):
        units(0, G, LEAD[h], lambda b: body(b, LEAD[h], h))

    def tail_units(h, body):
        units(E, NB, TAIL[h], lambda b: body(b, TAIL[h], h))

    def forward_units(body):
        units(0, E, UF, lambda b: body(b, UF, None))

    mine = row * PIECE
    far = (1 - row) * PIECE
    piece = rows_of(mine, PIECE)
    far_piece = rows_of(far, PIECE)

    def x_in(c):
        return pltpu.make_async_copy(x_hbm.at[rows_of(c * X0R, X0R)], vbuf.at[rows_of(mine + c * X0R, X0R)], xin_sem.at[c])

    def x0_copy(base, c):
        at = rows_of(base + c * X0R, X0R)
        return remote(xbf.at[at], xbf.at[at], x0_s.at[c], x0_r.at[c], mate)

    for c in range(X0C):
        x_in(c).start()
    d_in = pltpu.make_async_copy(d_hbm, dint.at[row], in_sem.at[0])
    v_in = pltpu.make_async_copy(v_hbm, vbuf.at[piece], in_sem.at[1])
    v_out = remote(v_hbm, vbuf.at[piece], ina_send.at[0], ina_recv.at[0], mate)
    d_out = remote(d_hbm, dint.at[row], ina_send.at[1], ina_recv.at[1], mate)
    s0_out = remote(s0buf.at[row], s0buf.at[row], s0_s, s0_r, mate)

    for c in range(X0C):
        x_in(c).wait()

        def convert(i, c=c):
            at = rows_of(mine + c * X0R + i * CH, CH)
            xbf[at, :] = vbuf[at, :].astype(jnp.bfloat16)
        loop(0, X0R // CH, convert)
        if c == 0:
            pl.semaphore_wait(barrier, 7)
        x0_copy(mine, c).start()
        if c < RING:
            a_copy(jnp.int32(c)).start()
    d_in.start()

    @pl.when(away)
    def _():
        d_out.start()
        v_out.start()

    for c in range(X0C):
        x0_copy(far, c).wait_recv()

    def s_copy(par, off):
        dst_col = lax.rem(col + off, 4)
        return remote(sbuf.at[par, col], sbuf.at[par, col], s_s.at[par, off], s_r.at[par, col],
                      (dst_col, lax.div(dst_col, 2)))

    def s_wait(par, off):
        src_col = lax.rem(col + off, 4)
        return remote(sbuf.at[par, src_col], sbuf.at[par, src_col], s_s.at[par, off], s_r.at[par, src_col],
                      (src_col, lax.div(src_col, 2)))

    def s_publish(par, value):
        sbuf[par, col] = value
        for off in range(1, 4):
            s_copy(par, off).start()

    def spread(r):
        def group(g):
            flags = dint[r, pl.ds(g, 1), :].astype(jnp.float32)
            dbuf[rows_of(r * PIECE + g * 128, 128), :] = jnp.broadcast_to(flags, (128, 128)).T
        loop(0, PIECE // 128, group)

    def first_mass():
        d_in.wait()
        spread(row)

        def add(c, acc):
            at = rows_of(mine + c * CH, CH)
            d = dbuf[at, :]
            w = vbuf[at, :] * jnp.concatenate([d, d], axis=1)
            return acc + jnp.sum(w.reshape(CH // 8, 8, VECS), axis=0)
        s0buf[row] = lax.fori_loop(0, PIECE // CH, add, jnp.zeros((8, VECS), jnp.float32))

    def update(t, b, n, h, one, two, acc):
        def step(c, acc):
            at = rows_of(same + t * PIECE + b * BR + c * CH, CH)
            own = rows_of(t * PIECE + b * BR + c * CH, CH)
            there = rows_of(b * BR + c * CH, CH)
            y = (ybuf[at, cols(h)] + one[there, cols(h)]) + two[there, cols(h)]
            cf = jnp.concatenate([coef[:, cols(h)]] * (CH // 8), axis=0)
            x = DAMPING * y + cf * vbuf[own, cols(h)]
            xbf[own, cols(h)] = x.astype(jnp.bfloat16)
            ybuf[at, cols(h)] = x
            d = dbuf[own, :]
            if h is None:
                d = jnp.concatenate([d, d], axis=1)
            return acc + jnp.sum((x * d).reshape(CH // 8, 8, d.shape[1]), axis=0)
        return lax.fori_loop(0, n * BR // CH, step, acc)

    def o_local(t, b, n, h):
        return pltpu.make_async_copy(
            ybuf.at[y_rows(same, t, b, n), cols(h)], out_hbm.at[blk(b, n), cols(h)], o_l.at[slot_of(b, h)])

    def o_remote(t, b, n, h):
        i = slot_of(b, h)
        return remote(ybuf.at[y_rows(same, t, b, n), cols(h)], out_hbm.at[blk(b, n), cols(h)], o_s.at[i], o_r.at[i], mate)

    def emit(t, b, n, h, last):
        @pl.when(jnp.logical_not(last))
        def _():
            c_x(t, b, n, h).start()

        @pl.when(jnp.logical_and(last, row == t))
        def _():
            o_local(t, b, n, h).start()

        @pl.when(jnp.logical_and(last, row != t))
        def _():
            o_remote(t, b, n, h).start()

    def finish(b, n, h, last, acc):
        c_fy(b, n, h).wait_recv()
        acc = update(0, b, n, h, ra, rfy, acc)
        emit(0, b, n, h, last)
        c_fx(b, n, h).wait_recv()
        acc = update(1, b, n, h, rdy, rfx, acc)
        emit(1, b, n, h, last)
        return acc

    def finish_half(h, last):
        n = TAIL[h]
        part = lax.fori_loop(
            0, G // n, lambda u, acc: finish(E + u * n, n, h, last, acc), jnp.zeros((8, HALF), jnp.float32))
        sacc[:, cols(h)] = sacc[:, cols(h)] + part

    def drain_forward():
        @pl.when(home)
        def _():
            forward_units(lambda b, n, h: c_fx(b, n, h).wait_send())
            for half in range(2):
                tail_units(half, lambda b, n, h: c_fx(b, n, h).wait_send())

        @pl.when(away)
        def _():
            forward_units(lambda b, n, h: c_fy(b, n, h).wait_send())
            for half in range(2):
                tail_units(half, lambda b, n, h: c_fy(b, n, h).wait_send())

    def sweep(k, carry):
        last = k == SWEEPS - 1
        par = lax.rem(k, 2)

        def multiply(n, h):
            start = block_of(n)
            ybuf[rows_of(start, BR), cols(h)] = jnp.dot(
                abuf[lax.rem(n, RING)], xbf[:, cols(h)], preferred_element_type=jnp.float32)

        def fetch(n):
            @pl.when(jnp.logical_not(jnp.logical_and(last, n >= 4 * NB)))
            def _():
                a_copy(lax.rem(n, 4 * NB)).start()

        @pl.when(k > 0)
        def _():
            @pl.when(home)
            def _():
                pl.semaphore_wait(cr_hh1, 1)

            @pl.when(away)
            def _():
                pl.semaphore_wait(cr_gy, 1)

        def lead(h):
            def one(n):
                if h == 0:
                    a_copy(n).wait()
                multiply(n, h)
                if h == 1:
                    fetch(n + RING)
                size = LEAD[h]
                whole = lax.rem(n, size) == size - 1
                b = n - (size - 1)

                @pl.when(jnp.logical_and(whole, home))
                def _():
                    c_a(b, size, h).start()

                @pl.when(jnp.logical_and(whole, away))
                def _():
                    c_gy(b, size, h).start()
            loop(0, G, one)

        lead(0)

        @pl.when(k > 0)
        def _():
            @pl.when(home)
            def _():
                finish_half(1, jnp.bool_(False))
                s_publish(par, sacc[...])
                signal(cr_hh2, xn)
                signal(cr_hw, yn)

            @pl.when(away)
            def _():
                for t in range(2):
                    tail_units(1, lambda b, n, h: c_x(t, b, n, h).wait_recv())

        lead(1)

        @pl.when(k > 0)
        def _():
            drain_forward()

            @pl.when(home)
            def _():
                pl.semaphore_wait(cr_hh2, 1)

            @pl.when(away)
            def _():
                pl.semaphore_wait(cr_ww, 1)
                pl.semaphore_wait(cr_hw, 1)

        def rest(n):
            a_copy(n).wait()
            multiply(n, None)
            fetch(n + RING)
            start = block_of(n)
            first = n < 2 * NB
            at = start - jnp.where(first, other, same)
            t, b = lax.div(at, PIECE), lax.div(lax.rem(at, PIECE), BR)

            def send_when(cond, b0, size, start):
                whole = lax.rem(b - b0, size) == size - 1

                @pl.when(jnp.logical_and(cond, whole))
                def _():
                    start(b - (size - 1), size)

            straight = jnp.logical_and(first, t == 0)
            held = n - HOLD + G
            send_when(jnp.logical_and(straight, away), 0, UA_AWAY, lambda b, n: c_a(b, n).start())

            @pl.when(jnp.logical_and(jnp.logical_and(held >= G, held < NB), home))
            def _():
                c_a(held, 1).start()
            send_when(jnp.logical_and(jnp.logical_and(first, t == 1), away), G, UG, lambda b, n: c_gy(b, n).start())
            send_when(jnp.logical_and(jnp.logical_and(jnp.logical_not(first), t == 1), away), 0, UD,
                      lambda b, n: c_dy(b).start())

        loop(G, 4 * NB, rest)

        def add_into(base, t, b, n, src):
            def step(c):
                at = rows_of(base + t * PIECE + b * BR + c * CH, CH)
                ybuf[at, :] = ybuf[at, :] + src[rows_of(b * BR + c * CH, CH), :]
            loop(0, n * BR // CH, step)

        @pl.when(away)
        def _away():
            @pl.when(k == 0)
            def _():
                for c in range(X0C):
                    x0_copy(mine, c).wait_send()

            @pl.when(jnp.logical_not(last))
            def _():
                signal(cr_x, mate)

            @pl.when(k == 0)
            def _():
                first_mass()
                s0_out.start()

            def forward(b, n):
                units(0, n, UA_AWAY, lambda i: c_a(b + i, UA_AWAY).wait())
                add_into(same, 0, b, n, ra)

            def forward_full(b, n, h):
                forward(b, n)
                c_fy(b, n).start()

            def forward_half(b, n, h):
                forward(b, n)
                c_fy(b, n, h).start()
            forward_units(forward_full)
            tail_units(0, forward_half)
            tail_units(1, lambda b, n, h: c_fy(b, n, h).start())

            @pl.when(jnp.logical_not(last))
            def _():
                signal(cr_ww, xn)

            for half in range(2):
                lead_units(half, lambda b, n, h: c_gy(b, n, h).wait_send())
            units(G, NB, UG, lambda b: c_gy(b, UG).wait_send())
            units(0, NB, UD, lambda b: c_dy(b).wait_send())

            @pl.when(k == 0)
            def _():
                v_out.wait_send()
                d_out.wait_send()
                s0_out.wait_send()

            @pl.when(jnp.logical_not(last))
            def _():
                for t in range(2):
                    forward_units(lambda b, n, h: c_x(t, b, n, h).wait_recv())
                    tail_units(0, lambda b, n, h: c_x(t, b, n, h).wait_recv())

        @pl.when(home)
        def _home():
            for half in range(2):
                lead_units(half, lambda b, n, h: c_gy(b, n, h).wait_recv())

            def arrived(b, n):
                @pl.when(b >= G)
                def _():
                    units(0, n, UG, lambda i: c_gy(b + i, UG).wait_recv())

            def forward_full(b, n, h):
                arrived(b, n)
                add_into(other, 1, b, n, rgy)
                c_fx(b, n).start()

            def forward_half(b, n, h):
                arrived(b, n)
                add_into(other, 1, b, n, rgy)
                c_fx(b, n, h).start()
            forward_units(forward_full)
            tail_units(0, forward_half)
            tail_units(1, lambda b, n, h: c_fx(b, n, h).start())

            @pl.when(jnp.logical_not(last))
            def _():
                signal(cr_gy, yn)

            @pl.when(k == 0)
            def _():
                first_mass()
                v_in.start()
                remote(d_hbm, dint.at[1 - row], ina_send.at[1], ina_recv.at[1], mate).wait_recv()
                spread(1 - row)
                remote(s0buf.at[1 - row], s0buf.at[1 - row], s0_s, s0_r, mate).wait_recv()
                s_publish(0, s0buf[0] + s0buf[1])
                for c in range(X0C):
                    x0_copy(mine, c).wait_send()
                remote(v_hbm, vbuf.at[far_piece], ina_send.at[0], ina_recv.at[0], mate).wait_recv()
                v_in.wait()

            @pl.when(k > 0)
            def _():
                for t in range(2):
                    forward_units(lambda b, n, h: c_x(t, b, n, h).wait_send())
                    for half in range(2):
                        tail_units(half, lambda b, n, h: c_x(t, b, n, h).wait_send())

            for off in range(1, 4):
                s_wait(par, off).wait_recv()
                s_copy(par, off).wait_send()
            total = (sbuf[par, 0] + sbuf[par, 1]) + (sbuf[par, 2] + sbuf[par, 3])
            mass = jnp.sum(total, axis=0, keepdims=True) / VERTS
            coef[...] = jnp.broadcast_to(DAMPING * mass + (1.0 - DAMPING), (8, VECS))

            @pl.when(jnp.logical_not(last))
            def _():
                pl.semaphore_wait(cr_x, 1)

            for half in range(2):
                lead_units(half, lambda b, n, h: c_a(b, n, h).wait())
            units(G, NB, UA_HOME, lambda b: c_a(b, UA_HOME).wait())
            units(0, NB, UD, lambda b: c_dy(b).wait_recv())
            acc = lax.fori_loop(
                0, E // UF, lambda u, acc: finish(u * UF, UF, None, last, acc), jnp.zeros((8, VECS), jnp.float32))
            sacc[...] = acc

            @pl.when(jnp.logical_not(last))
            def _():
                signal(cr_hh1, xn)
            finish_half(0, last)

        return carry

    lax.fori_loop(0, SWEEPS, sweep, 0)

    @pl.when(home)
    def _():
        finish_half(1, jnp.bool_(True))
    drain_forward()

    @pl.when(home)
    def _():
        def close(b, n, h):
            o_local(row, b, n, h).wait()
            o_remote(1 - row, b, n, h).wait_send()
        forward_units(close)
        for half in range(2):
            tail_units(half, close)

    @pl.when(away)
    def _():
        def close(b, n, h):
            o_remote(1 - row, b, n, h).wait_recv()
        forward_units(close)
        for half in range(2):
            tail_units(half, close)


def solution(mesh):
    dma = pltpu.SemaphoreType.DMA
    reg = pltpu.SemaphoreType.REGULAR

    def local_sweeps(mat_tile, x_piece, tele_piece, dang_piece):
        part = pltpu.VMEM((PIECE, VECS), jnp.float32)
        return pl.pallas_call(
            kernel,
            name="sweeps",
            out_shape=jax.ShapeDtypeStruct((PIECE, VECS), jnp.float32),
            in_specs=[pl.BlockSpec(memory_space=pl.ANY)] * 4,
            out_specs=pl.BlockSpec(memory_space=pl.ANY),
            scratch_shapes=[
                pltpu.VMEM((RING, BR, COLS), jnp.bfloat16),
                pltpu.VMEM((COLS, VECS), jnp.bfloat16),
                pltpu.VMEM((ROWS, VECS), jnp.float32),
                part, part, part, part, part,
                pltpu.VMEM((COLS, VECS), jnp.float32),
                pltpu.VMEM((COLS, 128), jnp.float32),
                pltpu.VMEM((2, PIECE // 128, 128), jnp.int32),
                pltpu.VMEM((2, 4, 8, VECS), jnp.float32),
                pltpu.VMEM((2, 8, VECS), jnp.float32),
                pltpu.VMEM((8, VECS), jnp.float32),
                pltpu.VMEM((8, VECS), jnp.float32),
                dma((RING,)), dma((X0C,)), dma((2,)), dma((2,)), dma((2,)), dma((X0C,)), dma((X0C,)),
                dma((2 * NB,)), dma((2 * NB,)), dma((2 * NB,)), dma((2 * NB,)), dma((NB,)), dma((NB,)),
                dma((2 * NB,)), dma((2 * NB,)), dma((2 * NB,)), dma((2 * NB,)),
                dma((4 * NB,)), dma((4 * NB,)), dma((2, 4)), dma((2, 4)), dma, dma,
                dma((2 * NB,)), dma((2 * NB,)), dma((2 * NB,)),
                reg, reg, reg, reg, reg, reg,
            ],
            compiler_params=pltpu.CompilerParams(
                collective_id=0, has_side_effects=True, vmem_limit_bytes=67_000_000),
            cost_estimate=pl.CostEstimate(
                flops=2 * ROWS * COLS * VECS * SWEEPS, bytes_accessed=2 * ROWS * COLS * SWEEPS, transcendentals=0),
        )(mat_tile, x_piece, tele_piece, dang_piece.reshape(PIECE // 128, 128))

    vec_spec = P(('col', 'row'), None)
    return jax.shard_map(local_sweeps, mesh=mesh,
                         in_specs=(P('row', 'col'), vec_spec, vec_spec, P(('col', 'row'))),
                         out_specs=vec_spec, check_vma=False)
```

```python
import jax
import jax.numpy as jnp
from jax import lax
from jax.experimental import pallas as pl
from jax.experimental.pallas import tpu as pltpu
from jax.sharding import PartitionSpec as P

SWEEPS = 8
DAMPING = 0.85
MESH = pl.DeviceIdType.MESH

VERTS = 24576
VECS = 256
HALF = 128
PIECE = 3072
ROWS = 12288
COLS = 6144
BR = 256
NB = PIECE // BR
G = 4
E = NB - G
CH = 32
LEAD = (1, 1)
TAIL = (1, 1)
UA_HOME = 1
UA_AWAY = 4
UG = 1
UD = 1
UF = 1
HOLD = 16
RING = 4
X0C = 6
X0R = PIECE // X0C


def kernel(a_hbm, x_hbm, v_hbm, d_hbm, out_hbm,
           abuf, xbf, ybuf, ra, rgy, rdy, rfx, rfy, vbuf, dbuf, dint, sbuf, s0buf, coef, sacc,
           a_sem, xin_sem, in_sem, ina_send, ina_recv, x0_s, x0_r,
           a_s, a_r, gy_s, gy_r, dy_s, dy_r, fx_s, fx_r, fy_s, fy_r,
           x_s, x_r, s_s, s_r, s0_s, s0_r, o_l, o_s, o_r,
           cr_hh1, cr_hh2, cr_hw, cr_gy, cr_ww, cr_x):
    col = lax.axis_index('col')
    row = lax.axis_index('row')
    cx, cy = lax.rem(col, 2), lax.div(col, 2)
    home = row == cy
    away = jnp.logical_not(home)
    xn = (cy * 2 + 1 - cx, row)
    yn = ((1 - cy) * 2 + cx, row)
    mate = (col, 1 - row)
    same = cx * COLS
    other = (1 - cx) * COLS

    barrier = pltpu.get_barrier_semaphore()
    for off in range(4):
        for r in range(2):
            if off == 0 and r == 1:
                continue
            dev = (lax.rem(col + off, 4), row if r == 0 and off else 1 - row)
            pl.semaphore_signal(barrier, inc=1, device_id=dev, device_id_type=MESH)

    def signal(sem, dev):
        pl.semaphore_signal(sem, inc=1, device_id=dev, device_id_type=MESH)

    def rows_of(start, size):
        return pl.ds(pl.multiple_of(start, size), size)

    def blk(b, n):
        return pl.ds(pl.multiple_of(b * BR, BR), n * BR)

    def cols(h):
        return pl.ds(0, VECS) if h is None else pl.ds(h * HALF, HALF)

    def slot_of(b, h):
        return b if h != 1 else NB + b

    def remote(src, dst, send, recv, dev):
        return pltpu.make_async_remote_copy(
            src_ref=src, dst_ref=dst, send_sem=send, recv_sem=recv, device_id=dev, device_id_type=MESH)

    def y_rows(base, t, b, n):
        return pl.ds(pl.multiple_of(base + t * PIECE + b * BR, BR), n * BR)

    def flow(base, t, b, n, h, dst, send, recv, dev):
        i = slot_of(b, h)
        return remote(ybuf.at[y_rows(base, t, b, n), cols(h)], dst.at[blk(b, n), cols(h)], send.at[i], recv.at[i], dev)

    def c_a(b, n, h=None):
        return flow(other, 0, b, n, h, ra, a_s, a_r, xn)

    def c_gy(b, n, h=None):
        return flow(other, 1, b, n, h, rgy, gy_s, gy_r, yn)

    def c_dy(b):
        return flow(same, 1, b, UD, None, rdy, dy_s, dy_r, yn)

    def c_fx(b, n, h=None):
        return flow(other, 1, b, n, h, rfx, fx_s, fx_r, xn)

    def c_fy(b, n, h=None):
        return flow(same, 0, b, n, h, rfy, fy_s, fy_r, yn)

    def c_x(t, b, n, h=None):
        at = pl.ds(pl.multiple_of(t * PIECE + b * BR, BR), n * BR)
        i = t * 2 * NB + slot_of(b, h)
        return remote(xbf.at[at, cols(h)], xbf.at[at, cols(h)], x_s.at[i], x_r.at[i], mate)

    def block_of(n):
        m = n - G
        pair = m < 2 * E
        t0 = jnp.where(pair, lax.rem(m, 2), 1)
        b0 = jnp.where(pair, jnp.where(t0 == 0, G, 0) + lax.div(m, 2), m - E)
        b0 = jnp.where(m < 0, n, b0)
        t0 = jnp.where(jnp.logical_xor(home, jnp.logical_or(m < 0, t0 == 0)), 1, 0)
        m = n - 2 * NB
        first = n < 2 * NB
        t = jnp.where(first, t0, 1 - lax.div(m, NB))
        b = jnp.where(first, b0, lax.rem(m, NB))
        return jnp.where(first, other, same) + t * PIECE + b * BR

    def a_copy(n):
        slot = lax.rem(n, RING)
        return pltpu.make_async_copy(a_hbm.at[rows_of(block_of(n), BR)], abuf.at[slot], a_sem.at[slot])

    def loop(lo, hi, body):
        def step(i, c):
            body(i)
            return c
        lax.fori_loop(lo, hi, step, 0)

    def units(lo, hi, n, body):
        loop(0, (hi - lo) // n, lambda u: body(lo + u * n))

    def lead_units(h, body):
        units(0, G, LEAD[h], lambda b: body(b, LEAD[h], h))

    def tail_units(h, body):
        units(E, NB, TAIL[h], lambda b: body(b, TAIL[h], h))

    def forward_units(body):
        units(0, E, UF, lambda b: body(b, UF, None))

    mine = row * PIECE
    far = (1 - row) * PIECE
    piece = rows_of(mine, PIECE)
    far_piece = rows_of(far, PIECE)

    def x_in(c):
        return pltpu.make_async_copy(x_hbm.at[rows_of(c * X0R, X0R)], vbuf.at[rows_of(mine + c * X0R, X0R)], xin_sem.at[c])

    def x0_copy(base, c):
        at = rows_of(base + c * X0R, X0R)
        return remote(xbf.at[at], xbf.at[at], x0_s.at[c], x0_r.at[c], mate)

    for c in range(X0C):
        x_in(c).start()
    d_in = pltpu.make_async_copy(d_hbm, dint.at[row], in_sem.at[0])
    v_in = pltpu.make_async_copy(v_hbm, vbuf.at[piece], in_sem.at[1])
    v_out = remote(v_hbm, vbuf.at[piece], ina_send.at[0], ina_recv.at[0], mate)
    d_out = remote(d_hbm, dint.at[row], ina_send.at[1], ina_recv.at[1], mate)
    s0_out = remote(s0buf.at[row], s0buf.at[row], s0_s, s0_r, mate)

    for c in range(X0C):
        x_in(c).wait()

        def convert(i, c=c):
            at = rows_of(mine + c * X0R + i * CH, CH)
            xbf[at, :] = vbuf[at, :].astype(jnp.bfloat16)
        loop(0, X0R // CH, convert)
        if c == 0:
            pl.semaphore_wait(barrier, 7)
        x0_copy(mine, c).start()
        if c < RING:
            a_copy(jnp.int32(c)).start()
    d_in.start()

    @pl.when(away)
    def _():
        d_out.start()
        v_out.start()

    for c in range(X0C):
        x0_copy(far, c).wait_recv()

    def s_copy(par, off):
        dst_col = lax.rem(col + off, 4)
        return remote(sbuf.at[par, col], sbuf.at[par, col], s_s.at[par, off], s_r.at[par, col],
                      (dst_col, lax.div(dst_col, 2)))

    def s_wait(par, off):
        src_col = lax.rem(col + off, 4)
        return remote(sbuf.at[par, src_col], sbuf.at[par, src_col], s_s.at[par, off], s_r.at[par, src_col],
                      (src_col, lax.div(src_col, 2)))

    def s_publish(par, value):
        sbuf[par, col] = value
        for off in range(1, 4):
            s_copy(par, off).start()

    def spread(r):
        def group(g):
            flags = dint[r, pl.ds(g, 1), :].astype(jnp.float32)
            dbuf[rows_of(r * PIECE + g * 128, 128), :] = jnp.broadcast_to(flags, (128, 128)).T
        loop(0, PIECE // 128, group)

    def first_mass():
        d_in.wait()
        spread(row)

        def add(c, acc):
            at = rows_of(mine + c * CH, CH)
            d = dbuf[at, :]
            w = vbuf[at, :] * jnp.concatenate([d, d], axis=1)
            return acc + jnp.sum(w.reshape(CH // 8, 8, VECS), axis=0)
        s0buf[row] = lax.fori_loop(0, PIECE // CH, add, jnp.zeros((8, VECS), jnp.float32))

    def update(t, b, n, h, one, two, acc):
        def step(c, acc):
            at = rows_of(same + t * PIECE + b * BR + c * CH, CH)
            own = rows_of(t * PIECE + b * BR + c * CH, CH)
            there = rows_of(b * BR + c * CH, CH)
            y = (ybuf[at, cols(h)] + one[there, cols(h)]) + two[there, cols(h)]
            cf = jnp.concatenate([coef[:, cols(h)]] * (CH // 8), axis=0)
            x = DAMPING * y + cf * vbuf[own, cols(h)]
            xbf[own, cols(h)] = x.astype(jnp.bfloat16)
            ybuf[at, cols(h)] = x
            d = dbuf[own, :]
            if h is None:
                d = jnp.concatenate([d, d], axis=1)
            return acc + jnp.sum((x * d).reshape(CH // 8, 8, d.shape[1]), axis=0)
        return lax.fori_loop(0, n * BR // CH, step, acc)

    def o_local(t, b, n, h):
        return pltpu.make_async_copy(
            ybuf.at[y_rows(same, t, b, n), cols(h)], out_hbm.at[blk(b, n), cols(h)], o_l.at[slot_of(b, h)])

    def o_remote(t, b, n, h):
        i = slot_of(b, h)
        return remote(ybuf.at[y_rows(same, t, b, n), cols(h)], out_hbm.at[blk(b, n), cols(h)], o_s.at[i], o_r.at[i], mate)

    def emit(t, b, n, h, last):
        @pl.when(jnp.logical_not(last))
        def _():
            c_x(t, b, n, h).start()

        @pl.when(jnp.logical_and(last, row == t))
        def _():
            o_local(t, b, n, h).start()

        @pl.when(jnp.logical_and(last, row != t))
        def _():
            o_remote(t, b, n, h).start()

    def finish(b, n, h, last, acc):
        c_fy(b, n, h).wait_recv()
        acc = update(0, b, n, h, ra, rfy, acc)
        emit(0, b, n, h, last)
        c_fx(b, n, h).wait_recv()
        acc = update(1, b, n, h, rdy, rfx, acc)
        emit(1, b, n, h, last)
        return acc

    def finish_half(h, last):
        n = TAIL[h]
        part = lax.fori_loop(
            0, G // n, lambda u, acc: finish(E + u * n, n, h, last, acc), jnp.zeros((8, HALF), jnp.float32))
        sacc[:, cols(h)] = sacc[:, cols(h)] + part

    def drain_forward():
        @pl.when(home)
        def _():
            forward_units(lambda b, n, h: c_fx(b, n, h).wait_send())
            for half in range(2):
                tail_units(half, lambda b, n, h: c_fx(b, n, h).wait_send())

        @pl.when(away)
        def _():
            forward_units(lambda b, n, h: c_fy(b, n, h).wait_send())
            for half in range(2):
                tail_units(half, lambda b, n, h: c_fy(b, n, h).wait_send())

    def sweep(k, carry):
        last = k == SWEEPS - 1
        par = lax.rem(k, 2)

        def multiply(n, h):
            start = block_of(n)
            ybuf[rows_of(start, BR), cols(h)] = jnp.dot(
                abuf[lax.rem(n, RING)], xbf[:, cols(h)], preferred_element_type=jnp.float32)

        def fetch(n):
            @pl.when(jnp.logical_not(jnp.logical_and(last, n >= 4 * NB)))
            def _():
                a_copy(lax.rem(n, 4 * NB)).start()

        @pl.when(k > 0)
        def _():
            @pl.when(home)
            def _():
                pl.semaphore_wait(cr_hh1, 1)

            @pl.when(away)
            def _():
                pl.semaphore_wait(cr_gy, 1)

        def lead(h):
            def one(n):
                if h == 0:
                    a_copy(n).wait()
                multiply(n, h)
                if h == 1:
                    fetch(n + RING)
                size = LEAD[h]
                whole = lax.rem(n, size) == size - 1
                b = n - (size - 1)

                @pl.when(jnp.logical_and(whole, home))
                def _():
                    c_a(b, size, h).start()

                @pl.when(jnp.logical_and(whole, away))
                def _():
                    c_gy(b, size, h).start()
            loop(0, G, one)

        lead(0)

        @pl.when(k > 0)
        def _():
            @pl.when(home)
            def _():
                finish_half(1, jnp.bool_(False))
                s_publish(par, sacc[...])
                signal(cr_hh2, xn)
                signal(cr_hw, yn)

            @pl.when(away)
            def _():
                for t in range(2):
                    tail_units(1, lambda b, n, h: c_x(t, b, n, h).wait_recv())

        lead(1)

        @pl.when(k > 0)
        def _():
            drain_forward()

            @pl.when(home)
            def _():
                pl.semaphore_wait(cr_hh2, 1)

            @pl.when(away)
            def _():
                pl.semaphore_wait(cr_ww, 1)
                pl.semaphore_wait(cr_hw, 1)

        def rest(n):
            a_copy(n).wait()
            multiply(n, None)
            fetch(n + RING)
            start = block_of(n)
            first = n < 2 * NB
            at = start - jnp.where(first, other, same)
            t, b = lax.div(at, PIECE), lax.div(lax.rem(at, PIECE), BR)

            def send_when(cond, b0, size, start):
                whole = lax.rem(b - b0, size) == size - 1

                @pl.when(jnp.logical_and(cond, whole))
                def _():
                    start(b - (size - 1), size)

            straight = jnp.logical_and(first, t == 0)
            held = n - HOLD + G
            send_when(jnp.logical_and(straight, away), 0, UA_AWAY, lambda b, n: c_a(b, n).start())

            @pl.when(jnp.logical_and(jnp.logical_and(held >= G, held < NB), home))
            def _():
                c_a(held, 1).start()
            send_when(jnp.logical_and(jnp.logical_and(first, t == 1), away), G, UG, lambda b, n: c_gy(b, n).start())
            send_when(jnp.logical_and(jnp.logical_and(jnp.logical_not(first), t == 1), away), 0, UD,
                      lambda b, n: c_dy(b).start())

        loop(G, 2 * NB, rest)

        @pl.when(home)
        def _():
            for half in range(2):
                lead_units(half, lambda b, n, h: c_gy(b, n, h).wait_recv())

        def add_into(base, t, b, n, src):
            def step(c):
                at = rows_of(base + t * PIECE + b * BR + c * CH, CH)
                ybuf[at, :] = ybuf[at, :] + src[rows_of(b * BR + c * CH, CH), :]
            loop(0, n * BR // CH, step)

        def forward_home(b):
            @pl.when(b >= G)
            def _():
                c_gy(b, 1).wait_recv()
            add_into(other, 1, b, 1, rgy)

            @pl.when(b < E)
            def _():
                c_fx(b, 1).start()

            @pl.when(b >= E)
            def _():
                c_fx(b, 1, 0).start()

        def forward_away(b):
            @pl.when(lax.rem(b, UA_AWAY) == 0)
            def _():
                c_a(b, UA_AWAY).wait()
            add_into(same, 0, b, 1, ra)

            @pl.when(b < E)
            def _():
                c_fy(b, 1).start()

            @pl.when(b >= E)
            def _():
                c_fy(b, 1, 0).start()

        def third(n):
            rest(n)

            @pl.when(home)
            def _():
                forward_home(n - 2 * NB)

        def fourth(n):
            rest(n)

            @pl.when(away)
            def _():
                forward_away(n - 3 * NB)

        loop(2 * NB, 3 * NB, third)

        @pl.when(home)
        def _():
            tail_units(1, lambda b, n, h: c_fx(b, n, h).start())

        loop(3 * NB, 4 * NB, fourth)

        @pl.when(away)
        def _away():
            tail_units(1, lambda b, n, h: c_fy(b, n, h).start())

            @pl.when(k == 0)
            def _():
                for c in range(X0C):
                    x0_copy(mine, c).wait_send()

            @pl.when(jnp.logical_not(last))
            def _():
                signal(cr_x, mate)

            @pl.when(k == 0)
            def _():
                first_mass()
                s0_out.start()

            @pl.when(jnp.logical_not(last))
            def _():
                signal(cr_ww, xn)

            for half in range(2):
                lead_units(half, lambda b, n, h: c_gy(b, n, h).wait_send())
            units(G, NB, UG, lambda b: c_gy(b, UG).wait_send())
            units(0, NB, UD, lambda b: c_dy(b).wait_send())

            @pl.when(k == 0)
            def _():
                v_out.wait_send()
                d_out.wait_send()
                s0_out.wait_send()

            @pl.when(jnp.logical_not(last))
            def _():
                for t in range(2):
                    forward_units(lambda b, n, h: c_x(t, b, n, h).wait_recv())
                    tail_units(0, lambda b, n, h: c_x(t, b, n, h).wait_recv())

        @pl.when(home)
        def _home():
            @pl.when(jnp.logical_not(last))
            def _():
                signal(cr_gy, yn)

            @pl.when(k == 0)
            def _():
                first_mass()
                v_in.start()
                remote(d_hbm, dint.at[1 - row], ina_send.at[1], ina_recv.at[1], mate).wait_recv()
                spread(1 - row)
                remote(s0buf.at[1 - row], s0buf.at[1 - row], s0_s, s0_r, mate).wait_recv()
                s_publish(0, s0buf[0] + s0buf[1])
                for c in range(X0C):
                    x0_copy(mine, c).wait_send()
                remote(v_hbm, vbuf.at[far_piece], ina_send.at[0], ina_recv.at[0], mate).wait_recv()
                v_in.wait()

            @pl.when(k > 0)
            def _():
                for t in range(2):
                    forward_units(lambda b, n, h: c_x(t, b, n, h).wait_send())
                    for half in range(2):
                        tail_units(half, lambda b, n, h: c_x(t, b, n, h).wait_send())

            for off in range(1, 4):
                s_wait(par, off).wait_recv()
                s_copy(par, off).wait_send()
            total = (sbuf[par, 0] + sbuf[par, 1]) + (sbuf[par, 2] + sbuf[par, 3])
            mass = jnp.sum(total, axis=0, keepdims=True) / VERTS
            coef[...] = jnp.broadcast_to(DAMPING * mass + (1.0 - DAMPING), (8, VECS))

            @pl.when(jnp.logical_not(last))
            def _():
                pl.semaphore_wait(cr_x, 1)

            for half in range(2):
                lead_units(half, lambda b, n, h: c_a(b, n, h).wait())
            units(G, NB, UA_HOME, lambda b: c_a(b, UA_HOME).wait())
            units(0, NB, UD, lambda b: c_dy(b).wait_recv())
            acc = lax.fori_loop(
                0, E // UF, lambda u, acc: finish(u * UF, UF, None, last, acc), jnp.zeros((8, VECS), jnp.float32))
            sacc[...] = acc

            @pl.when(jnp.logical_not(last))
            def _():
                signal(cr_hh1, xn)
            finish_half(0, last)

        return carry

    lax.fori_loop(0, SWEEPS, sweep, 0)

    @pl.when(home)
    def _():
        finish_half(1, jnp.bool_(True))
    drain_forward()

    @pl.when(home)
    def _():
        def close(b, n, h):
            o_local(row, b, n, h).wait()
            o_remote(1 - row, b, n, h).wait_send()
        forward_units(close)
        for half in range(2):
            tail_units(half, close)

    @pl.when(away)
    def _():
        def close(b, n, h):
            o_remote(1 - row, b, n, h).wait_recv()
        forward_units(close)
        for half in range(2):
            tail_units(half, close)


def solution(mesh):
    dma = pltpu.SemaphoreType.DMA
    reg = pltpu.SemaphoreType.REGULAR

    def local_sweeps(mat_tile, x_piece, tele_piece, dang_piece):
        part = pltpu.VMEM((PIECE, VECS), jnp.float32)
        return pl.pallas_call(
            kernel,
            name="sweeps",
            out_shape=jax.ShapeDtypeStruct((PIECE, VECS), jnp.float32),
            in_specs=[pl.BlockSpec(memory_space=pl.ANY)] * 4,
            out_specs=pl.BlockSpec(memory_space=pl.ANY),
            scratch_shapes=[
                pltpu.VMEM((RING, BR, COLS), jnp.bfloat16),
                pltpu.VMEM((COLS, VECS), jnp.bfloat16),
                pltpu.VMEM((ROWS, VECS), jnp.float32),
                part, part, part, part, part,
                pltpu.VMEM((COLS, VECS), jnp.float32),
                pltpu.VMEM((COLS, 128), jnp.float32),
                pltpu.VMEM((2, PIECE // 128, 128), jnp.int32),
                pltpu.VMEM((2, 4, 8, VECS), jnp.float32),
                pltpu.VMEM((2, 8, VECS), jnp.float32),
                pltpu.VMEM((8, VECS), jnp.float32),
                pltpu.VMEM((8, VECS), jnp.float32),
                dma((RING,)), dma((X0C,)), dma((2,)), dma((2,)), dma((2,)), dma((X0C,)), dma((X0C,)),
                dma((2 * NB,)), dma((2 * NB,)), dma((2 * NB,)), dma((2 * NB,)), dma((NB,)), dma((NB,)),
                dma((2 * NB,)), dma((2 * NB,)), dma((2 * NB,)), dma((2 * NB,)),
                dma((4 * NB,)), dma((4 * NB,)), dma((2, 4)), dma((2, 4)), dma, dma,
                dma((2 * NB,)), dma((2 * NB,)), dma((2 * NB,)),
                reg, reg, reg, reg, reg, reg,
            ],
            compiler_params=pltpu.CompilerParams(
                collective_id=0, has_side_effects=True, vmem_limit_bytes=67_000_000),
            cost_estimate=pl.CostEstimate(
                flops=2 * ROWS * COLS * VECS * SWEEPS, bytes_accessed=2 * ROWS * COLS * SWEEPS, transcendentals=0),
        )(mat_tile, x_piece, tele_piece, dang_piece.reshape(PIECE // 128, 128))

    vec_spec = P(('col', 'row'), None)
    return jax.shard_map(local_sweeps, mesh=mesh,
                         in_specs=(P('row', 'col'), vec_spec, vec_spec, P(('col', 'row'))),
                         out_specs=vec_spec, check_vma=False)
```

```python
import jax
import jax.numpy as jnp
from jax import lax
from jax.experimental import pallas as pl
from jax.experimental.pallas import tpu as pltpu
from jax.sharding import PartitionSpec as P

SWEEPS = 8
DAMPING = 0.85
MESH = pl.DeviceIdType.MESH

VERTS = 24576
VECS = 256
HALF = 128
PIECE = 3072
ROWS = 12288
COLS = 6144
BR = 256
NB = PIECE // BR
G = 4
E = NB - G
CH = 32
LEAD = (1, 1)
TAIL = (1, 1)
UA_HOME = 1
UA_AWAY = 1
UG = 1
UD = 1
UF = 1
RING = 4
X0C = 6
X0R = PIECE // X0C


def kernel(a_hbm, x_hbm, v_hbm, d_hbm, out_hbm,
           abuf, xbf, ybuf, ra, rgy, rdy, rfx, rfy, vbuf, dbuf, dint, sbuf, s0buf, coef, sacc,
           a_sem, xin_sem, in_sem, ina_send, ina_recv, x0_s, x0_r,
           a_s, a_r, gy_s, gy_r, dy_s, dy_r, fx_s, fx_r, fy_s, fy_r,
           x_s, x_r, s_s, s_r, s0_s, s0_r, o_l, o_s, o_r,
           cr_hh1, cr_hh2, cr_hw, cr_gy, cr_ww, cr_x):
    col = lax.axis_index('col')
    row = lax.axis_index('row')
    cx, cy = lax.rem(col, 2), lax.div(col, 2)
    home = row == cy
    away = jnp.logical_not(home)
    xn = (cy * 2 + 1 - cx, row)
    yn = ((1 - cy) * 2 + cx, row)
    mate = (col, 1 - row)
    same = cx * COLS
    other = (1 - cx) * COLS

    barrier = pltpu.get_barrier_semaphore()
    for off in range(4):
        for r in range(2):
            if off == 0 and r == 1:
                continue
            dev = (lax.rem(col + off, 4), row if r == 0 and off else 1 - row)
            pl.semaphore_signal(barrier, inc=1, device_id=dev, device_id_type=MESH)

    def signal(sem, dev):
        pl.semaphore_signal(sem, inc=1, device_id=dev, device_id_type=MESH)

    def rows_of(start, size):
        return pl.ds(pl.multiple_of(start, size), size)

    def blk(b, n):
        return pl.ds(pl.multiple_of(b * BR, BR), n * BR)

    def cols(h):
        return pl.ds(0, VECS) if h is None else pl.ds(h * HALF, HALF)

    def slot_of(b, h):
        return b if h != 1 else NB + b

    def remote(src, dst, send, recv, dev):
        return pltpu.make_async_remote_copy(
            src_ref=src, dst_ref=dst, send_sem=send, recv_sem=recv, device_id=dev, device_id_type=MESH)

    def y_rows(base, t, b, n):
        return pl.ds(pl.multiple_of(base + t * PIECE + b * BR, BR), n * BR)

    def flow(base, t, b, n, h, dst, send, recv, dev):
        i = slot_of(b, h)
        return remote(ybuf.at[y_rows(base, t, b, n), cols(h)], dst.at[blk(b, n), cols(h)], send.at[i], recv.at[i], dev)

    def c_a(b, n, h=None):
        return flow(other, 0, b, n, h, ra, a_s, a_r, xn)

    def c_gy(b, n, h=None):
        return flow(other, 1, b, n, h, rgy, gy_s, gy_r, yn)

    def c_dy(b):
        return flow(same, 1, b, UD, None, rdy, dy_s, dy_r, yn)

    def c_fx(b, n, h=None):
        return flow(other, 1, b, n, h, rfx, fx_s, fx_r, xn)

    def c_fy(b, n, h=None):
        return flow(same, 0, b, n, h, rfy, fy_s, fy_r, yn)

    def c_x(t, b, n, h=None):
        at = pl.ds(pl.multiple_of(t * PIECE + b * BR, BR), n * BR)
        i = t * 2 * NB + slot_of(b, h)
        return remote(xbf.at[at, cols(h)], xbf.at[at, cols(h)], x_s.at[i], x_r.at[i], mate)

    def block_of(n):
        m = n - G
        pair = m < 2 * E
        t0 = jnp.where(pair, lax.rem(m, 2), 1)
        b0 = jnp.where(pair, jnp.where(t0 == 0, G, 0) + lax.div(m, 2), m - E)
        b0 = jnp.where(m < 0, n, b0)
        t0 = jnp.where(jnp.logical_xor(home, jnp.logical_or(m < 0, t0 == 0)), 1, 0)
        m = n - 2 * NB
        first = n < 2 * NB
        t = jnp.where(first, t0, 1 - lax.div(m, NB))
        b = jnp.where(first, b0, lax.rem(m, NB))
        return jnp.where(first, other, same) + t * PIECE + b * BR

    def a_copy(n):
        slot = lax.rem(n, RING)
        return pltpu.make_async_copy(a_hbm.at[rows_of(block_of(n), BR)], abuf.at[slot], a_sem.at[slot])

    def loop(lo, hi, body):
        def step(i, c):
            body(i)
            return c
        lax.fori_loop(lo, hi, step, 0)

    def units(lo, hi, n, body):
        loop(0, (hi - lo) // n, lambda u: body(lo + u * n))

    def lead_units(h, body):
        units(0, G, LEAD[h], lambda b: body(b, LEAD[h], h))

    def tail_units(h, body):
        units(E, NB, TAIL[h], lambda b: body(b, TAIL[h], h))

    def forward_units(body):
        units(0, E, UF, lambda b: body(b, UF, None))

    mine = row * PIECE
    far = (1 - row) * PIECE
    piece = rows_of(mine, PIECE)
    far_piece = rows_of(far, PIECE)

    def x_in(c):
        return pltpu.make_async_copy(x_hbm.at[rows_of(c * X0R, X0R)], vbuf.at[rows_of(mine + c * X0R, X0R)], xin_sem.at[c])

    def x0_copy(base, c):
        at = rows_of(base + c * X0R, X0R)
        return remote(xbf.at[at], xbf.at[at], x0_s.at[c], x0_r.at[c], mate)

    for c in range(X0C):
        x_in(c).start()
    d_in = pltpu.make_async_copy(d_hbm, dint.at[row], in_sem.at[0])
    v_in = pltpu.make_async_copy(v_hbm, vbuf.at[piece], in_sem.at[1])
    v_out = remote(v_hbm, vbuf.at[piece], ina_send.at[0], ina_recv.at[0], mate)
    d_out = remote(d_hbm, dint.at[row], ina_send.at[1], ina_recv.at[1], mate)
    s0_out = remote(s0buf.at[row], s0buf.at[row], s0_s, s0_r, mate)

    for c in range(X0C):
        x_in(c).wait()

        def convert(i, c=c):
            at = rows_of(mine + c * X0R + i * CH, CH)
            xbf[at, :] = vbuf[at, :].astype(jnp.bfloat16)
        loop(0, X0R // CH, convert)
        if c == 0:
            pl.semaphore_wait(barrier, 7)
        x0_copy(mine, c).start()
        if c < RING:
            a_copy(jnp.int32(c)).start()
    d_in.start()

    @pl.when(away)
    def _():
        d_out.start()
        v_out.start()

    for c in range(X0C):
        x0_copy(far, c).wait_recv()

    def s_copy(par, off):
        dst_col = lax.rem(col + off, 4)
        return remote(sbuf.at[par, col, pl.ds(0, 1)], sbuf.at[par, col, pl.ds(0, 1)], s_s.at[par, off], s_r.at[par, col],
                      (dst_col, lax.div(dst_col, 2)))

    def s_wait(par, off):
        src_col = lax.rem(col + off, 4)
        return remote(sbuf.at[par, src_col, pl.ds(0, 1)], sbuf.at[par, src_col, pl.ds(0, 1)], s_s.at[par, off],
                      s_r.at[par, src_col],
                      (src_col, lax.div(src_col, 2)))

    def s_publish(par, value):
        sbuf[par, col, 0:1, :] = jnp.sum(value, axis=0, keepdims=True)
        for off in range(1, 4):
            s_copy(par, off).start()

    def spread(r):
        def group(g):
            flags = dint[r, pl.ds(g, 1), :].astype(jnp.float32)
            dbuf[rows_of(r * PIECE + g * 128, 128), :] = jnp.broadcast_to(flags, (128, 128)).T
        loop(0, PIECE // 128, group)

    def first_mass():
        d_in.wait()
        spread(row)

        def add(c, acc):
            at = rows_of(mine + c * CH, CH)
            d = dbuf[at, :]
            w = vbuf[at, :] * jnp.concatenate([d, d], axis=1)
            return acc + jnp.sum(w.reshape(CH // 8, 8, VECS), axis=0)
        s0buf[row] = lax.fori_loop(0, PIECE // CH, add, jnp.zeros((8, VECS), jnp.float32))

    def update(t, b, n, h, one, two, acc):
        def step(c, acc):
            at = rows_of(same + t * PIECE + b * BR + c * CH, CH)
            own = rows_of(t * PIECE + b * BR + c * CH, CH)
            there = rows_of(b * BR + c * CH, CH)
            y = (ybuf[at, cols(h)] + one[there, cols(h)]) + two[there, cols(h)]
            cf = jnp.concatenate([coef[:, cols(h)]] * (CH // 8), axis=0)
            x = DAMPING * y + cf * vbuf[own, cols(h)]
            xbf[own, cols(h)] = x.astype(jnp.bfloat16)
            ybuf[at, cols(h)] = x
            d = dbuf[own, :]
            if h is None:
                d = jnp.concatenate([d, d], axis=1)
            return acc + jnp.sum((x * d).reshape(CH // 8, 8, d.shape[1]), axis=0)
        return lax.fori_loop(0, n * BR // CH, step, acc)

    def o_local(t, b, n, h):
        return pltpu.make_async_copy(
            ybuf.at[y_rows(same, t, b, n), cols(h)], out_hbm.at[blk(b, n), cols(h)], o_l.at[slot_of(b, h)])

    def o_remote(t, b, n, h):
        i = slot_of(b, h)
        return remote(ybuf.at[y_rows(same, t, b, n), cols(h)], out_hbm.at[blk(b, n), cols(h)], o_s.at[i], o_r.at[i], mate)

    def emit(t, b, n, h, last):
        @pl.when(jnp.logical_not(last))
        def _():
            c_x(t, b, n, h).start()

        @pl.when(jnp.logical_and(last, row == t))
        def _():
            o_local(t, b, n, h).start()

        @pl.when(jnp.logical_and(last, row != t))
        def _():
            o_remote(t, b, n, h).start()

    def finish(b, n, h, last, acc):
        c_fy(b, n, h).wait_recv()
        acc = update(0, b, n, h, ra, rfy, acc)
        emit(0, b, n, h, last)
        c_fx(b, n, h).wait_recv()
        acc = update(1, b, n, h, rdy, rfx, acc)
        emit(1, b, n, h, last)
        return acc

    def finish_half(h, last):
        n = TAIL[h]
        part = lax.fori_loop(
            0, G // n, lambda u, acc: finish(E + u * n, n, h, last, acc), jnp.zeros((8, HALF), jnp.float32))
        sacc[:, cols(h)] = sacc[:, cols(h)] + part

    def drain_forward(keep):
        @pl.when(home)
        def _():
            forward_units(lambda b, n, h: c_fx(b, n, h).wait_send())
            for half in range(2):
                loop(NB - 1 if half and keep else E, NB, lambda b: c_fx(b, 1, half).wait_send())

        @pl.when(away)
        def _():
            forward_units(lambda b, n, h: c_fy(b, n, h).wait_send())
            for half in range(2):
                loop(NB - 1 if half and keep else E, NB, lambda b: c_fy(b, 1, half).wait_send())

    def sweep(k, carry):
        last = k == SWEEPS - 1
        par = lax.rem(k, 2)

        def multiply(n, h):
            start = block_of(n)
            ybuf[rows_of(start, BR), cols(h)] = jnp.dot(
                abuf[lax.rem(n, RING)], xbf[:, cols(h)], preferred_element_type=jnp.float32)

        def fetch(n):
            @pl.when(jnp.logical_not(jnp.logical_and(last, n >= 4 * NB)))
            def _():
                a_copy(lax.rem(n, 4 * NB)).start()

        @pl.when(k > 0)
        def _():
            @pl.when(home)
            def _():
                pl.semaphore_wait(cr_hh1, 1)

            @pl.when(away)
            def _():
                pl.semaphore_wait(cr_gy, 1)

        def lead(h):
            def one(n):
                if h == 0:
                    a_copy(n).wait()
                multiply(n, h)
                if h == 1:
                    fetch(n + RING)
                size = LEAD[h]
                ready = n >= (1 if h == 0 else 0)

                @pl.when(jnp.logical_and(home, ready))
                def _():
                    if h == 0:
                        @pl.when(n == 1)
                        def _():
                            @pl.when(k > 0)
                            def _():
                                loop(E, NB - 1, lambda b: c_fx(b, 1, 1).wait_send())
                            c_a(0, 1, h).start()
                    c_a(n, 1, h).start()

                @pl.when(jnp.logical_and(away, ready))
                def _():
                    if h == 0:
                        @pl.when(n == 1)
                        def _():
                            @pl.when(k > 0)
                            def _():
                                loop(E, NB - 1, lambda b: c_fy(b, 1, 1).wait_send())
                            c_gy(0, 1, h).start()
                    c_gy(n, 1, h).start()
            loop(0, G, one)

        lead(0)

        @pl.when(k > 0)
        def _():
            @pl.when(home)
            def _():
                finish_half(1, jnp.bool_(False))
                s_publish(par, sacc[...])
                signal(cr_hh2, xn)
                signal(cr_hw, yn)

            @pl.when(away)
            def _():
                for t in range(2):
                    tail_units(1, lambda b, n, h: c_x(t, b, n, h).wait_recv())

        lead(1)

        @pl.when(k > 0)
        def _():
            drain_forward(True)

            @pl.when(home)
            def _():
                pl.semaphore_wait(cr_hh2, 1)

            @pl.when(away)
            def _():
                pl.semaphore_wait(cr_ww, 1)
                pl.semaphore_wait(cr_hw, 1)

        def rest(n):
            a_copy(n).wait()
            multiply(n, None)
            fetch(n + RING)
            start = block_of(n)
            first = n < 2 * NB
            at = start - jnp.where(first, other, same)
            t, b = lax.div(at, PIECE), lax.div(lax.rem(at, PIECE), BR)

            def send_when(cond, b0, size, start):
                whole = lax.rem(b - b0, size) == size - 1

                @pl.when(jnp.logical_and(cond, whole))
                def _():
                    start(b - (size - 1), size)

            straight = jnp.logical_and(first, t == 0)
            send_when(straight, 0, 1, lambda b, n: c_a(b, n).start())
            send_when(jnp.logical_and(jnp.logical_and(first, t == 1), away), G, UG, lambda b, n: c_gy(b, n).start())
            send_when(jnp.logical_and(jnp.logical_and(jnp.logical_not(first), t == 1), away), 0, UD,
                      lambda b, n: c_dy(b).start())

        loop(G, 2 * NB, rest)

        @pl.when(home)
        def _():
            for half in range(2):
                lead_units(half, lambda b, n, h: c_gy(b, n, h).wait_recv())

        def add_into(base, t, b, n, src):
            def step(c):
                at = rows_of(base + t * PIECE + b * BR + c * CH, CH)
                ybuf[at, :] = ybuf[at, :] + src[rows_of(b * BR + c * CH, CH), :]
            loop(0, n * BR // CH, step)

        def forward_home(b):
            @pl.when(b >= G)
            def _():
                c_gy(b, 1).wait_recv()
            add_into(other, 1, b, 1, rgy)

            @pl.when(b < E)
            def _():
                c_fx(b, 1).start()

            @pl.when(b >= E)
            def _():
                c_fx(b, 1, 0).start()

        def forward_away(b):
            c_a(b, 1).wait()
            add_into(same, 0, b, 1, ra)

            @pl.when(b < E)
            def _():
                c_fy(b, 1).start()

            @pl.when(b >= E)
            def _():
                c_fy(b, 1, 0).start()

        def third(n):
            rest(n)

            @pl.when(home)
            def _():
                forward_home(n - 2 * NB)

        def fourth(n):
            rest(n)

            @pl.when(away)
            def _():
                forward_away(n - 3 * NB)

        loop(2 * NB, 3 * NB, third)

        @pl.when(home)
        def _():
            tail_units(1, lambda b, n, h: c_fx(b, n, h).start())

        loop(3 * NB, 4 * NB, fourth)

        @pl.when(away)
        def _away():
            tail_units(1, lambda b, n, h: c_fy(b, n, h).start())

            @pl.when(k == 0)
            def _():
                for c in range(X0C):
                    x0_copy(mine, c).wait_send()

            @pl.when(jnp.logical_not(last))
            def _():
                signal(cr_x, mate)

            @pl.when(k == 0)
            def _():
                first_mass()
                s0_out.start()

            @pl.when(jnp.logical_not(last))
            def _():
                signal(cr_ww, xn)

            for half in range(2):
                lead_units(half, lambda b, n, h: c_gy(b, n, h).wait_send())
            units(G, NB, UG, lambda b: c_gy(b, UG).wait_send())
            units(0, NB, UD, lambda b: c_dy(b).wait_send())

            @pl.when(k == 0)
            def _():
                v_out.wait_send()
                d_out.wait_send()
                s0_out.wait_send()

            @pl.when(jnp.logical_not(last))
            def _():
                for t in range(2):
                    forward_units(lambda b, n, h: c_x(t, b, n, h).wait_recv())
                    tail_units(0, lambda b, n, h: c_x(t, b, n, h).wait_recv())

        @pl.when(home)
        def _home():
            @pl.when(jnp.logical_not(last))
            def _():
                signal(cr_gy, yn)

            @pl.when(k == 0)
            def _():
                first_mass()
                v_in.start()
                remote(d_hbm, dint.at[1 - row], ina_send.at[1], ina_recv.at[1], mate).wait_recv()
                spread(1 - row)
                remote(s0buf.at[1 - row], s0buf.at[1 - row], s0_s, s0_r, mate).wait_recv()
                s_publish(0, s0buf[0] + s0buf[1])
                for c in range(X0C):
                    x0_copy(mine, c).wait_send()
                remote(v_hbm, vbuf.at[far_piece], ina_send.at[0], ina_recv.at[0], mate).wait_recv()
                v_in.wait()

            @pl.when(k > 0)
            def _():
                for t in range(2):
                    forward_units(lambda b, n, h: c_x(t, b, n, h).wait_send())
                    for half in range(2):
                        tail_units(half, lambda b, n, h: c_x(t, b, n, h).wait_send())

            for off in range(1, 4):
                s_wait(par, off).wait_recv()
                s_copy(par, off).wait_send()
            part = [sbuf[par, c, 0:1, :] for c in range(4)]
            mass = ((part[0] + part[1]) + (part[2] + part[3])) / VERTS
            coef[...] = jnp.broadcast_to(DAMPING * mass + (1.0 - DAMPING), (8, VECS))

            @pl.when(jnp.logical_not(last))
            def _():
                pl.semaphore_wait(cr_x, 1)

            for half in range(2):
                lead_units(half, lambda b, n, h: c_a(b, n, h).wait())
            units(G, NB, UA_HOME, lambda b: c_a(b, UA_HOME).wait())
            units(0, NB, UD, lambda b: c_dy(b).wait_recv())
            acc = lax.fori_loop(
                0, E // UF, lambda u, acc: finish(u * UF, UF, None, last, acc), jnp.zeros((8, VECS), jnp.float32))
            sacc[...] = acc

            @pl.when(jnp.logical_not(last))
            def _():
                signal(cr_hh1, xn)
            finish_half(0, last)

        return carry

    lax.fori_loop(0, SWEEPS, sweep, 0)

    @pl.when(home)
    def _():
        finish_half(1, jnp.bool_(True))
    drain_forward(False)

    @pl.when(home)
    def _():
        def close(b, n, h):
            o_local(row, b, n, h).wait()
            o_remote(1 - row, b, n, h).wait_send()
        forward_units(close)
        for half in range(2):
            tail_units(half, close)

    @pl.when(away)
    def _():
        def close(b, n, h):
            o_remote(1 - row, b, n, h).wait_recv()
        forward_units(close)
        for half in range(2):
            tail_units(half, close)


def solution(mesh):
    dma = pltpu.SemaphoreType.DMA
    reg = pltpu.SemaphoreType.REGULAR

    def local_sweeps(mat_tile, x_piece, tele_piece, dang_piece):
        part = pltpu.VMEM((PIECE, VECS), jnp.float32)
        return pl.pallas_call(
            kernel,
            name="sweeps",
            out_shape=jax.ShapeDtypeStruct((PIECE, VECS), jnp.float32),
            in_specs=[pl.BlockSpec(memory_space=pl.ANY)] * 4,
            out_specs=pl.BlockSpec(memory_space=pl.ANY),
            scratch_shapes=[
                pltpu.VMEM((RING, BR, COLS), jnp.bfloat16),
                pltpu.VMEM((COLS, VECS), jnp.bfloat16),
                pltpu.VMEM((ROWS, VECS), jnp.float32),
                part, part, part, part, part,
                pltpu.VMEM((COLS, VECS), jnp.float32),
                pltpu.VMEM((COLS, 128), jnp.float32),
                pltpu.VMEM((2, PIECE // 128, 128), jnp.int32),
                pltpu.VMEM((2, 4, 8, VECS), jnp.float32),
                pltpu.VMEM((2, 8, VECS), jnp.float32),
                pltpu.VMEM((8, VECS), jnp.float32),
                pltpu.VMEM((8, VECS), jnp.float32),
                dma((RING,)), dma((X0C,)), dma((2,)), dma((2,)), dma((2,)), dma((X0C,)), dma((X0C,)),
                dma((2 * NB,)), dma((2 * NB,)), dma((2 * NB,)), dma((2 * NB,)), dma((NB,)), dma((NB,)),
                dma((2 * NB,)), dma((2 * NB,)), dma((2 * NB,)), dma((2 * NB,)),
                dma((4 * NB,)), dma((4 * NB,)), dma((2, 4)), dma((2, 4)), dma, dma,
                dma((2 * NB,)), dma((2 * NB,)), dma((2 * NB,)),
                reg, reg, reg, reg, reg, reg,
            ],
            compiler_params=pltpu.CompilerParams(
                collective_id=0, has_side_effects=True, vmem_limit_bytes=67_000_000),
            cost_estimate=pl.CostEstimate(
                flops=2 * ROWS * COLS * VECS * SWEEPS, bytes_accessed=2 * ROWS * COLS * SWEEPS, transcendentals=0),
        )(mat_tile, x_piece, tele_piece, dang_piece.reshape(PIECE // 128, 128))

    vec_spec = P(('col', 'row'), None)
    return jax.shard_map(local_sweeps, mesh=mesh,
                         in_specs=(P('row', 'col'), vec_spec, vec_spec, P(('col', 'row'))),
                         out_specs=vec_spec, check_vma=False)
```

```python
import jax
import jax.numpy as jnp
from jax import lax
from jax.experimental import pallas as pl
from jax.experimental.pallas import tpu as pltpu
from jax.sharding import PartitionSpec as P

SWEEPS = 8
DAMPING = 0.85
MESH = pl.DeviceIdType.MESH

VERTS = 24576
VECS = 256
HALF = 128
PIECE = 3072
ROWS = 12288
COLS = 6144
BR = 256
NB = PIECE // BR
G = 4
E = NB - G
CH = 32
RING = 4
X0C = 6
X0R = PIECE // X0C


def kernel(a_hbm, x_hbm, v_hbm, d_hbm, out_hbm,
           abuf, xbf, ybuf, ra, rgy, rdy, rfx, rfy, vbuf, dbuf, dint, sbuf, s0buf, coef, sacc,
           a_sem, xin_sem, in_sem, ina_s, ina_r, x0_s, x0_r,
           a_s, a_r, gy_s, gy_r, dy_s, dy_r, fx_s, fx_r, fy_s, fy_r,
           x_s, x_r, s_s, s_r, s0_s, s0_r, o_l, o_s, o_r,
           cr_hh1, cr_hh2, cr_hw, cr_gy, cr_ww, cr_x):
    col = lax.axis_index('col')
    row = lax.axis_index('row')
    cx, cy = lax.rem(col, 2), lax.div(col, 2)
    home = row == cy
    away = jnp.logical_not(home)
    xn = (cy * 2 + 1 - cx, row)
    yn = ((1 - cy) * 2 + cx, row)
    mate = (col, 1 - row)
    same = cx * COLS
    other = (1 - cx) * COLS
    mine = row * PIECE
    far = (1 - row) * PIECE

    def rows_of(start, size):
        return pl.ds(pl.multiple_of(start, size), size)

    def blocks(start, b, n):
        return pl.ds(pl.multiple_of(start + b * BR, BR), n * BR)

    def cols(h):
        return pl.ds(0, VECS) if h is None else pl.ds(h * HALF, HALF)

    def remote(src, dst, send, recv, dev):
        return pltpu.make_async_remote_copy(
            src_ref=src, dst_ref=dst, send_sem=send, recv_sem=recv, device_id=dev, device_id_type=MESH)

    def loop(lo, hi, body):
        def step(i, c):
            body(i)
            return c
        lax.fori_loop(lo, hi, step, 0)

    def signal(sem, dev):
        pl.semaphore_signal(sem, inc=1, device_id=dev, device_id_type=MESH)

    def x_in(c):
        return pltpu.make_async_copy(x_hbm.at[rows_of(c * X0R, X0R)], vbuf.at[rows_of(mine + c * X0R, X0R)], xin_sem.at[c])

    for c in range(X0C):
        x_in(c).start()

    barrier = pltpu.get_barrier_semaphore()
    for off in range(4):
        for r in range(2):
            if off == 0 and r == 1:
                continue
            signal(barrier, (lax.rem(col + off, 4), row if r == 0 and off else 1 - row))

    def flow(start, b, n, h, dst, send, recv, dev, late):
        i = b if h != 1 else NB + b - (E if late else 0)
        return remote(ybuf.at[blocks(start, b, n), cols(h)], dst.at[blocks(0, b, n), cols(h)], send, recv.at[i], dev)

    def c_a(b, h=None, n=1):
        return flow(other, b, n, h, ra, a_s, a_r, xn, False)

    def c_gy(b, h=None, n=1):
        return flow(other + PIECE, b, n, h, rgy, gy_s, gy_r, yn, False)

    def c_dy(b, n=1):
        return remote(ybuf.at[blocks(same + PIECE, b, n)], rdy.at[blocks(0, b, n)], dy_s, dy_r, yn)

    def c_fx(b, h=None, n=1):
        return flow(other + PIECE, b, n, h, rfx, fx_s, fx_r, xn, True)

    def c_fy(b, h=None, n=1):
        return flow(same, b, n, h, rfy, fy_s, fy_r, yn, True)

    def c_x(t, b, h=None):
        at = blocks(t * PIECE, b, 1)
        return remote(xbf.at[at, cols(h)], xbf.at[at, cols(h)], x_s, x_r.at[1 if h == 1 else 0], mate)

    def x_bytes(rows, i):
        return remote(xbf.at[pl.ds(0, rows)], xbf.at[pl.ds(0, rows)], x_s, x_r.at[i], mate)

    def block_of(n):
        m = n - G
        pair = m < 2 * E
        t0 = jnp.where(pair, lax.rem(m, 2), 1)
        b0 = jnp.where(pair, jnp.where(t0 == 0, G, 0) + lax.div(m, 2), m - E)
        b0 = jnp.where(m < 0, n, b0)
        t0 = jnp.where(jnp.logical_xor(home, jnp.logical_or(m < 0, t0 == 0)), 1, 0)
        m = n - 2 * NB
        first = n < 2 * NB
        t = jnp.where(first, t0, 1 - lax.div(m, NB))
        b = jnp.where(first, b0, lax.rem(m, NB))
        return jnp.where(first, other, same) + t * PIECE + b * BR

    def a_copy(n):
        slot = lax.rem(n, RING)
        return pltpu.make_async_copy(a_hbm.at[rows_of(block_of(n), BR)], abuf.at[slot], a_sem.at[slot])

    d_in = pltpu.make_async_copy(d_hbm, dint.at[row], in_sem.at[0])
    v_in = pltpu.make_async_copy(v_hbm, vbuf.at[rows_of(mine, PIECE)], in_sem.at[1])
    v_out = remote(v_hbm, vbuf.at[rows_of(mine, PIECE)], ina_s.at[0], ina_r.at[0], mate)
    d_out = remote(d_hbm, dint.at[row], ina_s.at[1], ina_r.at[1], mate)
    s0_out = remote(s0buf.at[row], s0buf.at[row], s0_s, s0_r, mate)

    def x0_copy(start, c, n=1):
        at = pl.ds(pl.multiple_of(start + c * X0R, X0R), n * X0R)
        return remote(xbf.at[at], xbf.at[at], x0_s, x0_r, mate)

    for c in range(X0C):
        x_in(c).wait()

        def convert(i, c=c):
            at = rows_of(mine + c * X0R + i * CH, CH)
            xbf[at, :] = vbuf[at, :].astype(jnp.bfloat16)
        loop(0, X0R // CH, convert)
        if c == 0:
            pl.semaphore_wait(barrier, 7)
        x0_copy(mine, c).start()
        if c < RING:
            a_copy(jnp.int32(c)).start()
    d_in.start()

    @pl.when(away)
    def _():
        d_out.start()
        v_out.start()

    x0_copy(far, 0, X0C).wait_recv()

    def s_copy(par, off):
        dst_col = lax.rem(col + off, 4)
        return remote(sbuf.at[par, col], sbuf.at[par, col], s_s.at[par], s_r.at[par], (dst_col, lax.div(dst_col, 2)))

    def s_bytes(par):
        return remote(sbuf.at[par, pl.ds(0, 3)], sbuf.at[par, pl.ds(0, 3)], s_s.at[par], s_r.at[par], mate)

    def s_publish(par, value):
        sbuf[par, col] = jnp.sum(value, axis=0, keepdims=True)
        for off in range(1, 4):
            s_copy(par, off).start()

    def spread(r):
        def group(g):
            flags = dint[r, pl.ds(g, 1), :].astype(jnp.float32)
            dbuf[rows_of(r * PIECE + g * 128, 128), :] = jnp.broadcast_to(flags, (128, 128)).T.astype(jnp.bfloat16)
        loop(0, PIECE // 128, group)

    def flags(start, h):
        d = dbuf[rows_of(start, CH), :].astype(jnp.float32)
        return d if h is not None else jnp.concatenate([d, d], axis=1)

    def fold(w):
        return jnp.sum(w.reshape(CH // 8, 8, w.shape[1]), axis=0)

    def first_mass():
        d_in.wait()
        spread(row)

        def add(c, acc):
            at = mine + c * CH
            return acc + fold(vbuf[rows_of(at, CH), :] * flags(at, None))
        s0buf[row] = lax.fori_loop(0, PIECE // CH, add, jnp.zeros((8, VECS), jnp.float32))

    def update(t, b, h, one, two, acc):
        def step(c, acc):
            at = rows_of(same + t * PIECE + b * BR + c * CH, CH)
            own = rows_of(t * PIECE + b * BR + c * CH, CH)
            there = rows_of(b * BR + c * CH, CH)
            y = (ybuf[at, cols(h)] + one[there, cols(h)]) + two[there, cols(h)]
            cf = jnp.concatenate([coef[:, cols(h)]] * (CH // 8), axis=0)
            x = DAMPING * y + cf * vbuf[own, cols(h)]
            xbf[own, cols(h)] = x.astype(jnp.bfloat16)
            ybuf[at, cols(h)] = x
            return acc + fold(x * flags(t * PIECE + b * BR + c * CH, h))
        return lax.fori_loop(0, BR // CH, step, acc)

    def o_local(t, b, h=None, n=1):
        return pltpu.make_async_copy(
            ybuf.at[blocks(same + t * PIECE, b, n), cols(h)], out_hbm.at[blocks(0, b, n), cols(h)], o_l)

    def o_remote(t, b, h=None, n=1):
        return remote(ybuf.at[blocks(same + t * PIECE, b, n), cols(h)], out_hbm.at[blocks(0, b, n), cols(h)], o_s, o_r, mate)

    def emit(t, b, h, last):
        @pl.when(jnp.logical_not(last))
        def _():
            c_x(t, b, h).start()

        @pl.when(jnp.logical_and(last, row == t))
        def _():
            o_local(t, b, h).start()

        @pl.when(jnp.logical_and(last, row != t))
        def _():
            o_remote(t, b, h).start()

    def finish(b, h, last, acc):
        c_fy(b, h).wait_recv()
        acc = update(0, b, h, ra, rfy, acc)
        emit(0, b, h, last)
        c_fx(b, h).wait_recv()
        acc = update(1, b, h, rdy, rfx, acc)
        emit(1, b, h, last)
        return acc

    def finish_half(h, last):
        part = lax.fori_loop(E, NB, lambda b, acc: finish(b, h, last, acc), jnp.zeros((8, HALF), jnp.float32))
        sacc[:, cols(h)] = sacc[:, cols(h)] + part

    def drain_forward():
        @pl.when(home)
        def _():
            c_fx(0, n=NB).wait_send()

        @pl.when(away)
        def _():
            c_fy(0, n=NB).wait_send()

    def sweep(k, carry):
        last = k == SWEEPS - 1
        more = jnp.logical_not(last)
        par = lax.rem(k, 2)

        def multiply(n, h):
            start = block_of(n)
            ybuf[rows_of(start, BR), cols(h)] = jnp.dot(
                abuf[lax.rem(n, RING)], xbf[:, cols(h)], preferred_element_type=jnp.float32)

        def fetch(n):
            @pl.when(jnp.logical_not(jnp.logical_and(last, n >= 4 * NB)))
            def _():
                a_copy(lax.rem(n, 4 * NB)).start()

        @pl.when(k > 0)
        def _():
            @pl.when(home)
            def _():
                pl.semaphore_wait(cr_hh1, 1)

            @pl.when(away)
            def _():
                pl.semaphore_wait(cr_gy, 1)

        def lead(h):
            def one(n):
                if h == 0:
                    a_copy(n).wait()
                multiply(n, h)
                if h == 1:
                    fetch(n + RING)

                @pl.when(home)
                def _():
                    c_a(n, h).start()

                @pl.when(away)
                def _():
                    c_gy(n, h).start()
            loop(0, G, one)

        lead(0)

        @pl.when(k > 0)
        def _():
            @pl.when(home)
            def _():
                finish_half(1, jnp.bool_(False))
                s_publish(par, sacc[...])
                signal(cr_hh2, xn)
                signal(cr_hw, yn)

            @pl.when(away)
            def _():
                x_bytes(G * BR, 1).wait_recv()

        lead(1)

        @pl.when(k > 0)
        def _():
            drain_forward()

            @pl.when(home)
            def _():
                pl.semaphore_wait(cr_hh2, 1)

            @pl.when(away)
            def _():
                pl.semaphore_wait(cr_ww, 1)
                pl.semaphore_wait(cr_hw, 1)

        def step(n):
            a_copy(n).wait()
            multiply(n, None)
            fetch(n + RING)
            at = block_of(n) - jnp.where(n < 2 * NB, other, same)
            return lax.div(at, PIECE), lax.div(lax.rem(at, PIECE), BR)

        def part_one(n):
            t, b = step(n)

            @pl.when(t == 0)
            def _():
                c_a(b).start()

            @pl.when(jnp.logical_and(t == 1, away))
            def _():
                c_gy(b).start()
        loop(G, 2 * NB, part_one)

        @pl.when(k == 0)
        def _():
            first_mass()

            @pl.when(away)
            def _():
                s0_out.start()

            @pl.when(home)
            def _():
                v_in.start()
                remote(d_hbm, dint.at[1 - row], ina_s.at[1], ina_r.at[1], mate).wait_recv()
                remote(s0buf.at[1 - row], s0buf.at[1 - row], s0_s, s0_r, mate).wait_recv()
                s_publish(0, s0buf[0] + s0buf[1])

        def add_into(start, b, src):
            def add(c):
                at = rows_of(start + b * BR + c * CH, CH)
                ybuf[at, :] = ybuf[at, :] + src[rows_of(b * BR + c * CH, CH), :]
            loop(0, BR // CH, add)

        def send_on(copy, b):
            @pl.when(b < E)
            def _():
                copy(b).start()

            @pl.when(b >= E)
            def _():
                copy(b, 0).start()

        def part_two(n):
            b = n - 2 * NB
            step(n)

            @pl.when(away)
            def _():
                c_dy(b).start()

            @pl.when(home)
            def _():
                @pl.when(b < G)
                def _():
                    c_gy(b, 0).wait_recv()
                    c_gy(b, 1).wait_recv()

                @pl.when(b >= G)
                def _():
                    c_gy(b).wait_recv()
                add_into(other + PIECE, b, rgy)
                send_on(c_fx, b)
        loop(2 * NB, 3 * NB, part_two)

        @pl.when(home)
        def _():
            loop(E, NB, lambda b: c_fx(b, 1).start())

        def part_three(n):
            b = n - 3 * NB
            step(n)

            @pl.when(away)
            def _():
                c_a(b).wait_recv()
                add_into(same, b, ra)
                send_on(c_fy, b)
        loop(3 * NB, 4 * NB, part_three)

        @pl.when(away)
        def _away():
            loop(E, NB, lambda b: c_fy(b, 1).start())

            @pl.when(k == 0)
            def _():
                x0_copy(mine, 0, X0C).wait_send()
                v_out.wait_send()
                d_out.wait_send()
                s0_out.wait_send()

            @pl.when(more)
            def _():
                signal(cr_x, mate)
                signal(cr_ww, xn)
            c_a(0, n=NB).wait_send()
            c_gy(0, n=NB).wait_send()
            c_dy(0, NB).wait_send()

            @pl.when(more)
            def _():
                x_bytes(2 * PIECE - G * BR, 0).wait_recv()

        @pl.when(home)
        def _home():
            @pl.when(more)
            def _():
                signal(cr_gy, yn)

            @pl.when(k == 0)
            def _():
                spread(1 - row)
                x0_copy(mine, 0, X0C).wait_send()
                remote(v_hbm, vbuf.at[rows_of(far, PIECE)], ina_s.at[0], ina_r.at[0], mate).wait_recv()
                v_in.wait()

            @pl.when(k > 0)
            def _():
                x_bytes(2 * PIECE, 0).wait_send()

            s_bytes(par).wait_recv()
            s_bytes(par).wait_send()
            mass = ((sbuf[par, 0] + sbuf[par, 1]) + (sbuf[par, 2] + sbuf[par, 3])) / VERTS
            coef[...] = jnp.broadcast_to(DAMPING * mass + (1.0 - DAMPING), (8, VECS))

            @pl.when(more)
            def _():
                pl.semaphore_wait(cr_x, 1)

            c_a(0, n=NB).wait_send()
            for h in range(2):
                loop(0, G, lambda b: c_a(b, h).wait_recv())
            loop(G, NB, lambda b: c_a(b).wait_recv())
            c_dy(0, NB).wait_recv()
            sacc[...] = lax.fori_loop(0, E, lambda b, acc: finish(b, None, last, acc), jnp.zeros((8, VECS), jnp.float32))

            @pl.when(more)
            def _():
                signal(cr_hh1, xn)
            finish_half(0, last)

        return carry

    lax.fori_loop(0, SWEEPS, sweep, 0)

    @pl.when(home)
    def _():
        finish_half(1, jnp.bool_(True))
    drain_forward()

    @pl.when(home)
    def _():
        o_local(row, 0, n=NB).wait()
        o_remote(1 - row, 0, n=NB).wait_send()

    @pl.when(away)
    def _():
        o_remote(1 - row, 0, n=NB).wait_recv()


def solution(mesh):
    dma = pltpu.SemaphoreType.DMA
    reg = pltpu.SemaphoreType.REGULAR

    def local_sweeps(mat_tile, x_piece, tele_piece, dang_piece):
        part = pltpu.VMEM((PIECE, VECS), jnp.float32)
        return pl.pallas_call(
            kernel,
            name="sweeps",
            out_shape=jax.ShapeDtypeStruct((PIECE, VECS), jnp.float32),
            in_specs=[pl.BlockSpec(memory_space=pl.ANY)] * 4,
            out_specs=pl.BlockSpec(memory_space=pl.ANY),
            scratch_shapes=[
                pltpu.VMEM((RING, BR, COLS), jnp.bfloat16),
                pltpu.VMEM((COLS, VECS), jnp.bfloat16),
                pltpu.VMEM((ROWS, VECS), jnp.float32),
                part, part, part, part, part,
                pltpu.VMEM((COLS, VECS), jnp.float32),
                pltpu.VMEM((COLS, 128), jnp.bfloat16),
                pltpu.VMEM((2, PIECE // 128, 128), jnp.int32),
                pltpu.VMEM((2, 4, 1, VECS), jnp.float32),
                pltpu.VMEM((2, 8, VECS), jnp.float32),
                pltpu.VMEM((8, VECS), jnp.float32),
                pltpu.VMEM((8, VECS), jnp.float32),
                dma((RING,)), dma((X0C,)), dma((2,)), dma((2,)), dma((2,)), dma, dma,
                dma, dma((NB + G,)), dma, dma((NB + G,)), dma, dma, dma, dma((NB + G,)), dma, dma((NB + G,)),
                dma, dma((2,)), dma((2,)), dma((2,)), dma, dma, dma, dma, dma,
                reg, reg, reg, reg, reg, reg,
            ],
            compiler_params=pltpu.CompilerParams(
                collective_id=0, has_side_effects=True, vmem_limit_bytes=67_000_000),
            cost_estimate=pl.CostEstimate(
                flops=2 * ROWS * COLS * VECS * SWEEPS, bytes_accessed=2 * ROWS * COLS * SWEEPS, transcendentals=0),
        )(mat_tile, x_piece, tele_piece, dang_piece.reshape(PIECE // 128, 128))

    vec_spec = P(('col', 'row'), None)
    return jax.shard_map(local_sweeps, mesh=mesh,
                         in_specs=(P('row', 'col'), vec_spec, vec_spec, P(('col', 'row'))),
                         out_specs=vec_spec, check_vma=False)
```

```python
import jax
import jax.numpy as jnp
from jax import lax
from jax.experimental import pallas as pl
from jax.experimental.pallas import tpu as pltpu
from jax.sharding import PartitionSpec as P

SWEEPS = 8
DAMPING = 0.85
MESH = pl.DeviceIdType.MESH

VERTS = 24576
VECS = 256
HALF = 128
PIECE = 3072
ROWS = 12288
COLS = 6144
BR = 256
NB = PIECE // BR
G = 4
E = NB - G
CH = 32
RING = 4
X0C = 6
X0R = PIECE // X0C


def kernel(a_hbm, x_hbm, v_hbm, d_hbm, out,
           abuf, xbf, ybuf, ra, rgy, rdy, rfx, rfy, vbuf, dbuf, dint, sbuf, s0buf, coef, sacc,
           a_sem, xin_sem, in_sem, ina_s, ina_r, x0_s, x0_r,
           a_s, a_r, gy_s, gy_r, dy_s, dy_r, fx_s, fx_r, fy_s, fy_r,
           x_s, x_r, s_s, s_r, s0_s, s0_r, o_s, o_r,
           cr_hh1, cr_hh2, cr_hw, cr_gy, cr_ww, cr_x):
    col = lax.axis_index('col')
    row = lax.axis_index('row')
    cx, cy = lax.rem(col, 2), lax.div(col, 2)
    home = row == cy
    away = jnp.logical_not(home)
    xn = (cy * 2 + 1 - cx, row)
    yn = ((1 - cy) * 2 + cx, row)
    mate = (col, 1 - row)
    same = cx * COLS
    other = (1 - cx) * COLS
    mine = row * PIECE
    far = (1 - row) * PIECE

    def rows_of(start, size):
        return pl.ds(pl.multiple_of(start, size), size)

    def blocks(start, b, n):
        return pl.ds(pl.multiple_of(start + b * BR, BR), n * BR)

    def cols(h):
        return pl.ds(0, VECS) if h is None else pl.ds(h * HALF, HALF)

    def remote(src, dst, send, recv, dev):
        return pltpu.make_async_remote_copy(
            src_ref=src, dst_ref=dst, send_sem=send, recv_sem=recv, device_id=dev, device_id_type=MESH)

    def loop(lo, hi, body):
        def step(i, c):
            body(i)
            return c
        lax.fori_loop(lo, hi, step, 0)

    def signal(sem, dev):
        pl.semaphore_signal(sem, inc=1, device_id=dev, device_id_type=MESH)

    def x_in(c):
        return pltpu.make_async_copy(x_hbm.at[rows_of(c * X0R, X0R)], vbuf.at[rows_of(mine + c * X0R, X0R)], xin_sem.at[c])

    for c in range(X0C):
        x_in(c).start()

    barrier = pltpu.get_barrier_semaphore()
    for off in range(4):
        for r in range(2):
            if off == 0 and r == 1:
                continue
            signal(barrier, (lax.rem(col + off, 4), row if r == 0 and off else 1 - row))

    def flow(start, b, n, h, dst, send, recv, dev, late):
        i = b if h != 1 else NB + b - (E if late else 0)
        return remote(ybuf.at[blocks(start, b, n), cols(h)], dst.at[blocks(0, b, n), cols(h)], send, recv.at[i], dev)

    def c_a(b, h=None, n=1):
        return flow(other, b, n, h, ra, a_s, a_r, xn, False)

    def c_gy(b, h=None, n=1):
        return flow(other + PIECE, b, n, h, rgy, gy_s, gy_r, yn, False)

    def c_dy(b, n=1):
        return remote(ybuf.at[blocks(same + PIECE, b, n)], rdy.at[blocks(0, b, n)], dy_s, dy_r, yn)

    def c_fx(b, h=None, n=1):
        return flow(other + PIECE, b, n, h, rfx, fx_s, fx_r, xn, True)

    def c_fy(b, h=None, n=1):
        return flow(same, b, n, h, rfy, fy_s, fy_r, yn, True)

    def c_x(t, b, h=None):
        at = blocks(t * PIECE, b, 1)
        return remote(xbf.at[at, cols(h)], xbf.at[at, cols(h)], x_s, x_r.at[1 if h == 1 else 0], mate)

    def x_bytes(rows, i):
        return remote(xbf.at[pl.ds(0, rows)], xbf.at[pl.ds(0, rows)], x_s, x_r.at[i], mate)

    def block_of(n):
        m = n - G
        pair = m < 2 * E
        t0 = jnp.where(pair, lax.rem(m, 2), 1)
        b0 = jnp.where(pair, jnp.where(t0 == 0, G, 0) + lax.div(m, 2), m - E)
        b0 = jnp.where(m < 0, n, b0)
        t0 = jnp.where(jnp.logical_xor(home, jnp.logical_or(m < 0, t0 == 0)), 1, 0)
        m = n - 2 * NB
        first = n < 2 * NB
        t = jnp.where(first, t0, 1 - lax.div(m, NB))
        b = jnp.where(first, b0, lax.rem(m, NB))
        return jnp.where(first, other, same) + t * PIECE + b * BR

    def a_copy(n):
        slot = lax.rem(n, RING)
        return pltpu.make_async_copy(a_hbm.at[rows_of(block_of(n), BR)], abuf.at[slot], a_sem.at[slot])

    d_in = pltpu.make_async_copy(d_hbm, dint.at[row], in_sem.at[0])
    v_in = pltpu.make_async_copy(v_hbm, vbuf.at[rows_of(mine, PIECE)], in_sem.at[1])
    v_out = remote(v_hbm, vbuf.at[rows_of(mine, PIECE)], ina_s.at[0], ina_r.at[0], mate)
    d_out = remote(d_hbm, dint.at[row], ina_s.at[1], ina_r.at[1], mate)
    s0_out = remote(s0buf.at[row], s0buf.at[row], s0_s, s0_r, mate)

    def x0_copy(start, c, n=1):
        at = pl.ds(pl.multiple_of(start + c * X0R, X0R), n * X0R)
        return remote(xbf.at[at], xbf.at[at], x0_s, x0_r, mate)

    for c in range(X0C):
        x_in(c).wait()

        def convert(i, c=c):
            at = rows_of(mine + c * X0R + i * CH, CH)
            xbf[at, :] = vbuf[at, :].astype(jnp.bfloat16)
        loop(0, X0R // CH, convert)
        if c == 0:
            pl.semaphore_wait(barrier, 7)
        x0_copy(mine, c).start()
        if c < RING:
            a_copy(jnp.int32(c)).start()
    d_in.start()

    @pl.when(away)
    def _():
        d_out.start()
        v_out.start()

    x0_copy(far, 0, X0C).wait_recv()

    def s_copy(par, off):
        dst_col = lax.rem(col + off, 4)
        return remote(sbuf.at[par, col], sbuf.at[par, col], s_s.at[par], s_r.at[par], (dst_col, lax.div(dst_col, 2)))

    def s_bytes(par):
        return remote(sbuf.at[par, pl.ds(0, 3)], sbuf.at[par, pl.ds(0, 3)], s_s.at[par], s_r.at[par], mate)

    def s_publish(par, value):
        sbuf[par, col] = jnp.sum(value, axis=0, keepdims=True)
        for off in range(1, 4):
            s_copy(par, off).start()

    def spread(r):
        def group(g):
            flags = dint[r, pl.ds(g, 1), :].astype(jnp.float32)
            dbuf[rows_of(r * PIECE + g * 128, 128), :] = jnp.broadcast_to(flags, (128, 128)).T.astype(jnp.bfloat16)
        loop(0, PIECE // 128, group)

    def flags(start, h):
        d = dbuf[rows_of(start, CH), :].astype(jnp.float32)
        return d if h is not None else jnp.concatenate([d, d], axis=1)

    def fold(w):
        return jnp.sum(w.reshape(CH // 8, 8, w.shape[1]), axis=0)

    def first_mass():
        d_in.wait()
        spread(row)

        def add(c, acc):
            at = mine + c * CH
            return acc + fold(vbuf[rows_of(at, CH), :] * flags(at, None))
        s0buf[row] = lax.fori_loop(0, PIECE // CH, add, jnp.zeros((8, VECS), jnp.float32))

    def update(t, b, h, one, two, acc):
        def step(c, acc):
            at = rows_of(same + t * PIECE + b * BR + c * CH, CH)
            own = rows_of(t * PIECE + b * BR + c * CH, CH)
            there = rows_of(b * BR + c * CH, CH)
            y = (ybuf[at, cols(h)] + one[there, cols(h)]) + two[there, cols(h)]
            cf = jnp.concatenate([coef[:, cols(h)]] * (CH // 8), axis=0)
            x = DAMPING * y + cf * vbuf[own, cols(h)]
            xbf[own, cols(h)] = x.astype(jnp.bfloat16)
            ybuf[at, cols(h)] = x
            return acc + fold(x * flags(t * PIECE + b * BR + c * CH, h))
        return lax.fori_loop(0, BR // CH, step, acc)

    def keep(t, b, h):
        def step(c):
            there = rows_of(b * BR + c * CH, CH)
            out[there, cols(h)] = ybuf[rows_of(same + t * PIECE + b * BR + c * CH, CH), cols(h)]
        loop(0, BR // CH, step)

    def o_remote(t, b, h=None, n=1):
        return remote(ybuf.at[blocks(same + t * PIECE, b, n), cols(h)], out.at[blocks(0, b, n), cols(h)], o_s, o_r, mate)

    def emit(t, b, h, last):
        @pl.when(jnp.logical_not(last))
        def _():
            c_x(t, b, h).start()

        @pl.when(jnp.logical_and(last, row == t))
        def _():
            keep(t, b, h)

        @pl.when(jnp.logical_and(last, row != t))
        def _():
            o_remote(t, b, h).start()

    def finish(b, h, last, acc):
        c_fy(b, h).wait_recv()
        acc = update(0, b, h, ra, rfy, acc)
        emit(0, b, h, last)
        c_fx(b, h).wait_recv()
        acc = update(1, b, h, rdy, rfx, acc)
        emit(1, b, h, last)
        return acc

    def finish_half(h, last):
        part = lax.fori_loop(E, NB, lambda b, acc: finish(b, h, last, acc), jnp.zeros((8, HALF), jnp.float32))
        sacc[:, cols(h)] = sacc[:, cols(h)] + part

    def drain_forward():
        @pl.when(home)
        def _():
            c_fx(0, n=NB).wait_send()

        @pl.when(away)
        def _():
            c_fy(0, n=NB).wait_send()

    def sweep(k, carry):
        last = k == SWEEPS - 1
        more = jnp.logical_not(last)
        par = lax.rem(k, 2)

        def multiply(n, h):
            start = block_of(n)
            ybuf[rows_of(start, BR), cols(h)] = jnp.dot(
                abuf[lax.rem(n, RING)], xbf[:, cols(h)], preferred_element_type=jnp.float32)

        def fetch(n):
            @pl.when(jnp.logical_not(jnp.logical_and(last, n >= 4 * NB)))
            def _():
                a_copy(lax.rem(n, 4 * NB)).start()

        @pl.when(k > 0)
        def _():
            @pl.when(home)
            def _():
                pl.semaphore_wait(cr_hh1, 1)

            @pl.when(away)
            def _():
                pl.semaphore_wait(cr_gy, 1)

        def lead(h):
            def one(n):
                if h == 0:
                    a_copy(n).wait()
                multiply(n, h)
                if h == 1:
                    fetch(n + RING)

                @pl.when(home)
                def _():
                    c_a(n, h).start()

                @pl.when(away)
                def _():
                    c_gy(n, h).start()
            loop(0, G, one)

        lead(0)

        @pl.when(k > 0)
        def _():
            @pl.when(home)
            def _():
                finish_half(1, jnp.bool_(False))
                s_publish(par, sacc[...])
                signal(cr_hh2, xn)
                signal(cr_hw, yn)

            @pl.when(away)
            def _():
                x_bytes(G * BR, 1).wait_recv()

        lead(1)

        @pl.when(k > 0)
        def _():
            drain_forward()

            @pl.when(home)
            def _():
                pl.semaphore_wait(cr_hh2, 1)

            @pl.when(away)
            def _():
                pl.semaphore_wait(cr_ww, 1)
                pl.semaphore_wait(cr_hw, 1)

        def step(n):
            a_copy(n).wait()
            multiply(n, None)
            fetch(n + RING)
            at = block_of(n) - jnp.where(n < 2 * NB, other, same)
            return lax.div(at, PIECE), lax.div(lax.rem(at, PIECE), BR)

        def part_one(n):
            t, b = step(n)

            @pl.when(t == 0)
            def _():
                c_a(b).start()

            @pl.when(jnp.logical_and(t == 1, away))
            def _():
                c_gy(b).start()
        loop(G, 2 * NB, part_one)

        @pl.when(k == 0)
        def _():
            first_mass()

            @pl.when(away)
            def _():
                s0_out.start()

            @pl.when(home)
            def _():
                v_in.start()
                remote(d_hbm, dint.at[1 - row], ina_s.at[1], ina_r.at[1], mate).wait_recv()
                remote(s0buf.at[1 - row], s0buf.at[1 - row], s0_s, s0_r, mate).wait_recv()
                s_publish(0, s0buf[0] + s0buf[1])

        def add_into(start, b, src):
            def add(c):
                at = rows_of(start + b * BR + c * CH, CH)
                ybuf[at, :] = ybuf[at, :] + src[rows_of(b * BR + c * CH, CH), :]
            loop(0, BR // CH, add)

        def send_on(copy, b):
            @pl.when(b < E)
            def _():
                copy(b).start()

            @pl.when(b >= E)
            def _():
                copy(b, 0).start()

        def part_two(n):
            b = n - 2 * NB
            step(n)

            @pl.when(away)
            def _():
                c_dy(b).start()

            @pl.when(home)
            def _():
                @pl.when(b < G)
                def _():
                    c_gy(b, 0).wait_recv()
                    c_gy(b, 1).wait_recv()

                @pl.when(b >= G)
                def _():
                    c_gy(b).wait_recv()
                add_into(other + PIECE, b, rgy)
                send_on(c_fx, b)
        loop(2 * NB, 3 * NB, part_two)

        @pl.when(home)
        def _():
            loop(E, NB, lambda b: c_fx(b, 1).start())

        def part_three(n):
            b = n - 3 * NB
            step(n)

            @pl.when(away)
            def _():
                c_a(b).wait_recv()
                add_into(same, b, ra)
                send_on(c_fy, b)
        loop(3 * NB, 4 * NB, part_three)

        @pl.when(away)
        def _away():
            loop(E, NB, lambda b: c_fy(b, 1).start())

            @pl.when(k == 0)
            def _():
                x0_copy(mine, 0, X0C).wait_send()
                v_out.wait_send()
                d_out.wait_send()
                s0_out.wait_send()

            @pl.when(more)
            def _():
                signal(cr_x, mate)
                signal(cr_ww, xn)
            c_a(0, n=NB).wait_send()
            c_gy(0, n=NB).wait_send()
            c_dy(0, NB).wait_send()

            @pl.when(more)
            def _():
                x_bytes(2 * PIECE - G * BR, 0).wait_recv()

        @pl.when(home)
        def _home():
            @pl.when(more)
            def _():
                signal(cr_gy, yn)

            @pl.when(k == 0)
            def _():
                spread(1 - row)
                x0_copy(mine, 0, X0C).wait_send()
                remote(v_hbm, vbuf.at[rows_of(far, PIECE)], ina_s.at[0], ina_r.at[0], mate).wait_recv()
                v_in.wait()

            @pl.when(k > 0)
            def _():
                x_bytes(2 * PIECE, 0).wait_send()

            s_bytes(par).wait_recv()
            s_bytes(par).wait_send()
            mass = ((sbuf[par, 0] + sbuf[par, 1]) + (sbuf[par, 2] + sbuf[par, 3])) / VERTS
            coef[...] = jnp.broadcast_to(DAMPING * mass + (1.0 - DAMPING), (8, VECS))

            @pl.when(more)
            def _():
                pl.semaphore_wait(cr_x, 1)

            c_a(0, n=NB).wait_send()
            for h in range(2):
                loop(0, G, lambda b: c_a(b, h).wait_recv())
            loop(G, NB, lambda b: c_a(b).wait_recv())
            c_dy(0, NB).wait_recv()
            sacc[...] = lax.fori_loop(0, E, lambda b, acc: finish(b, None, last, acc), jnp.zeros((8, VECS), jnp.float32))

            @pl.when(more)
            def _():
                signal(cr_hh1, xn)
            finish_half(0, last)

        return carry

    lax.fori_loop(0, SWEEPS, sweep, 0)

    @pl.when(home)
    def _():
        finish_half(1, jnp.bool_(True))
    drain_forward()

    @pl.when(home)
    def _():
        o_remote(1 - row, 0, n=NB).wait_send()

    @pl.when(away)
    def _():
        o_remote(1 - row, 0, n=NB).wait_recv()


def solution(mesh):
    dma = pltpu.SemaphoreType.DMA
    reg = pltpu.SemaphoreType.REGULAR

    def in_hbm(a):
        return pltpu.with_memory_space_constraint(a, pltpu.HBM)

    def local_sweeps(mat_tile, x_piece, tele_piece, dang_piece):
        part = pltpu.VMEM((PIECE, VECS), jnp.float32)
        return pl.pallas_call(
            kernel,
            name="sweeps",
            out_shape=jax.ShapeDtypeStruct((PIECE, VECS), jnp.float32),
            in_specs=[pl.BlockSpec(memory_space=pltpu.HBM)] * 4,
            out_specs=pl.BlockSpec(memory_space=pltpu.VMEM),
            scratch_shapes=[
                pltpu.VMEM((RING, BR, COLS), jnp.bfloat16),
                pltpu.VMEM((COLS, VECS), jnp.bfloat16),
                pltpu.VMEM((ROWS, VECS), jnp.float32),
                part, part, part, part, part,
                pltpu.VMEM((COLS, VECS), jnp.float32),
                pltpu.VMEM((COLS, 128), jnp.bfloat16),
                pltpu.VMEM((2, PIECE // 128, 128), jnp.int32),
                pltpu.VMEM((2, 4, 1, VECS), jnp.float32),
                pltpu.VMEM((2, 8, VECS), jnp.float32),
                pltpu.VMEM((8, VECS), jnp.float32),
                pltpu.VMEM((8, VECS), jnp.float32),
                dma((RING,)), dma((X0C,)), dma((2,)), dma((2,)), dma((2,)), dma, dma,
                dma, dma((NB + G,)), dma, dma((NB + G,)), dma, dma, dma, dma((NB + G,)), dma, dma((NB + G,)),
                dma, dma((2,)), dma((2,)), dma((2,)), dma, dma, dma, dma,
                reg, reg, reg, reg, reg, reg,
            ],
            compiler_params=pltpu.CompilerParams(
                collective_id=0, has_side_effects=True, vmem_limit_bytes=53_300_000),
            cost_estimate=pl.CostEstimate(
                flops=2 * ROWS * COLS * VECS * SWEEPS, bytes_accessed=2 * ROWS * COLS * SWEEPS, transcendentals=0),
        )(mat_tile, x_piece, tele_piece, in_hbm(dang_piece.reshape(PIECE // 128, 128)))

    vec_spec = P(('col', 'row'), None)
    return jax.shard_map(local_sweeps, mesh=mesh,
                         in_specs=(P('row', 'col'), vec_spec, vec_spec, P(('col', 'row'))),
                         out_specs=vec_spec, check_vma=False)
```

```python
import jax
import jax.numpy as jnp
from jax import lax
from jax.experimental import pallas as pl
from jax.experimental.pallas import tpu as pltpu
from jax.sharding import PartitionSpec as P

SWEEPS = 8
DAMPING = 0.85
MESH = pl.DeviceIdType.MESH

VERTS = 24576
VECS = 256
HALF = 128
PIECE = 3072
ROWS = 12288
COLS = 6144
BR = 256
NB = PIECE // BR
G = 4
E = NB - G
CH = 32
RING = 4
X0C = 4
X0R = PIECE // X0C


def kernel(a_hbm, x_hbm, v_hbm, d_hbm, out,
           abuf, xbf, ybuf, ra, rgy, rdy, rfx, rfy, vbuf, dbuf, dint, sbuf, s0buf, coef, sacc,
           a_sem, in_sem, x0_s, x0_r,
           a_s, a_r, gy_s, gy_r, dy_s, dy_r, fx_s, fx_r, fy_s, fy_r,
           x_s, x_r, s_s, s_r, o_s, o_r, cr_0, cr_1, cr_2):
    col = lax.axis_index('col')
    row = lax.axis_index('row')
    cx, cy = lax.rem(col, 2), lax.div(col, 2)
    home = row == cy
    away = jnp.logical_not(home)
    xn = (cy * 2 + 1 - cx, row)
    yn = ((1 - cy) * 2 + cx, row)
    mate = (col, 1 - row)
    same = cx * COLS
    other = (1 - cx) * COLS
    mine = row * PIECE
    far = (1 - row) * PIECE

    def rows_of(start, size):
        return pl.ds(pl.multiple_of(start, size), size)

    def blocks(start, b, n):
        return pl.ds(pl.multiple_of(start + b * BR, BR), n * BR)

    def cols(h):
        return pl.ds(0, VECS) if h is None else pl.ds(h * HALF, HALF)

    def remote(src, dst, send, recv, dev):
        return pltpu.make_async_remote_copy(
            src_ref=src, dst_ref=dst, send_sem=send, recv_sem=recv, device_id=dev, device_id_type=MESH)

    def loop(lo, hi, body):
        def step(i, c):
            body(i)
            return c
        lax.fori_loop(lo, hi, step, 0)

    def signal(sem, dev):
        pl.semaphore_signal(sem, inc=1, device_id=dev, device_id_type=MESH)

    def x_in(c):
        return pltpu.make_async_copy(x_hbm.at[rows_of(c * X0R, X0R)], vbuf.at[rows_of(mine + c * X0R, X0R)], in_sem.at[c])

    for c in range(X0C):
        x_in(c).start()

    barrier = pltpu.get_barrier_semaphore()
    for off in range(4):
        for r in range(2):
            if off == 0 and r == 1:
                continue
            signal(barrier, (lax.rem(col + off, 4), row if r == 0 and off else 1 - row))

    def flow(start, b, n, h, dst, send, recv, i, dev):
        return remote(ybuf.at[blocks(start, b, n), cols(h)], dst.at[blocks(0, b, n), cols(h)], send, recv.at[i], dev)

    def c_a(b, h=None, n=1):
        return flow(other, b, n, h, ra, a_s, a_r, lax.div(b, G), xn)

    def c_gy(b, h=None, n=1):
        return flow(other + PIECE, b, n, h, rgy, gy_s, gy_r, lax.div(b, G), yn)

    def c_dy(b, n=1):
        return remote(ybuf.at[blocks(same + PIECE, b, n)], rdy.at[blocks(0, b, n)], dy_s, dy_r, yn)

    def late(b, h):
        return lax.div(b, G) if h is None else E // G + 2 * h + jnp.where(b == NB - 1, 1, 0)

    def c_fx(b, h=None, n=1):
        return flow(other + PIECE, b, n, h, rfx, fx_s, fx_r, late(b, h), xn)

    def c_fy(b, h=None, n=1):
        return flow(same, b, n, h, rfy, fy_s, fy_r, late(b, h), yn)

    def arrived(copy, b, h):
        if h is None:
            @pl.when(lax.rem(b, G) == 0)
            def _():
                copy(b, n=G).wait_recv()
        else:
            @pl.when(b == E)
            def _():
                copy(b, h, n=G - 1).wait_recv()

            @pl.when(b == NB - 1)
            def _():
                copy(b, h).wait_recv()

    def c_x(t, b, h=None):
        at = blocks(t * PIECE, b, 1)
        return remote(xbf.at[at, cols(h)], xbf.at[at, cols(h)], x_s, x_r.at[1 if h == 1 else 0], mate)

    def x_bytes(rows, i):
        return remote(xbf.at[pl.ds(0, rows)], xbf.at[pl.ds(0, rows)], x_s, x_r.at[i], mate)

    def block_of(n):
        m = n - G
        pair = m < 2 * E
        t0 = jnp.where(pair, lax.rem(m, 2), 1)
        b0 = jnp.where(pair, jnp.where(t0 == 0, G, 0) + lax.div(m, 2), m - E)
        b0 = jnp.where(m < 0, n, b0)
        t0 = jnp.where(jnp.logical_xor(home, jnp.logical_or(m < 0, t0 == 0)), 1, 0)
        m = n - 2 * NB
        first = n < 2 * NB
        t = jnp.where(first, t0, 1 - lax.div(m, NB))
        b = jnp.where(first, b0, lax.rem(m, NB))
        return jnp.where(first, other, same) + t * PIECE + b * BR

    def a_copy(n):
        slot = lax.rem(n, RING)
        return pltpu.make_async_copy(a_hbm.at[rows_of(block_of(n), BR)], abuf.at[slot], a_sem.at[slot])

    d_in = pltpu.make_async_copy(d_hbm, dint.at[row], in_sem.at[0])
    v_in = pltpu.make_async_copy(v_hbm, vbuf.at[rows_of(mine, PIECE)], in_sem.at[1])

    def v_copy(r):
        return remote(v_hbm, vbuf.at[rows_of(r * PIECE, PIECE)], fx_s, x_r.at[0], mate)

    def d_copy(r):
        return remote(d_hbm, dint.at[r], x_s, x_r.at[1], mate)

    def s0_copy(r):
        return remote(s0buf.at[r], s0buf.at[r], o_s, o_r, mate)

    def x0_copy(start, c, n=1):
        at = pl.ds(pl.multiple_of(start + c * X0R, X0R), n * X0R)
        return remote(xbf.at[at], xbf.at[at], x0_s, x0_r, mate)

    for c in range(X0C):
        x_in(c).wait()

        def convert(i, c=c):
            at = rows_of(mine + c * X0R + i * CH, CH)
            xbf[at, :] = vbuf[at, :].astype(jnp.bfloat16)
        loop(0, X0R // CH, convert)
        if c == 0:
            pl.semaphore_wait(barrier, 7)
        x0_copy(mine, c).start()
        if c < RING:
            a_copy(jnp.int32(c)).start()
    d_in.start()

    @pl.when(away)
    def _():
        d_copy(row).start()
        v_copy(row).start()

    def half_product(n, start):
        at = rows_of(start, PIECE)
        return jnp.dot(abuf[lax.rem(n, RING), :, at], xbf[at, :], preferred_element_type=jnp.float32)

    def first_own(n):
        a_copy(n).wait()
        ybuf[rows_of(block_of(n), BR), :] = half_product(n, mine)
    loop(0, G, first_own)
    x0_copy(far, 0, X0C).wait_recv()

    def first_far(n):
        at = rows_of(block_of(n), BR)
        ybuf[at, :] = ybuf[at, :] + half_product(n, far)
        a_copy(n + RING).start()
        for h in range(2):
            @pl.when(home)
            def _():
                c_a(n, h).start()

            @pl.when(away)
            def _():
                c_gy(n, h).start()
    loop(0, G, first_far)

    def s_copy(par, off):
        dst_col = lax.rem(col + off, 4)
        return remote(sbuf.at[par, col], sbuf.at[par, col], s_s, s_r.at[par], (dst_col, lax.div(dst_col, 2)))

    def s_bytes(par):
        return remote(sbuf.at[par, pl.ds(0, 3)], sbuf.at[par, pl.ds(0, 3)], s_s, s_r.at[par], mate)

    def s_publish(par, value):
        sbuf[par, col] = jnp.sum(value, axis=0, keepdims=True)
        for off in range(1, 4):
            s_copy(par, off).start()

    def spread(r):
        def group(g):
            flags = dint[r, pl.ds(g, 1), :].astype(jnp.float32)
            dbuf[rows_of(r * PIECE + g * 128, 128), :] = jnp.broadcast_to(flags, (128, 128)).T.astype(jnp.bfloat16)
        loop(0, PIECE // 128, group)

    def flags(start, h):
        d = dbuf[rows_of(start, CH), :].astype(jnp.float32)
        return d if h is not None else jnp.concatenate([d, d], axis=1)

    def fold(w):
        return jnp.sum(w.reshape(CH // 8, 8, w.shape[1]), axis=0)

    def first_mass():
        d_in.wait()
        spread(row)

        def add(c, acc):
            at = mine + c * CH
            return acc + fold(vbuf[rows_of(at, CH), :] * flags(at, None))
        s0buf[row] = lax.fori_loop(0, PIECE // CH, add, jnp.zeros((8, VECS), jnp.float32))

    def update(t, b, h, one, two, acc):
        def step(c, acc):
            at = rows_of(same + t * PIECE + b * BR + c * CH, CH)
            own = rows_of(t * PIECE + b * BR + c * CH, CH)
            there = rows_of(b * BR + c * CH, CH)
            y = (ybuf[at, cols(h)] + one[there, cols(h)]) + two[there, cols(h)]
            cf = jnp.concatenate([coef[:, cols(h)]] * (CH // 8), axis=0)
            x = DAMPING * y + cf * vbuf[own, cols(h)]
            xbf[own, cols(h)] = x.astype(jnp.bfloat16)
            ybuf[at, cols(h)] = x
            return acc + fold(x * flags(t * PIECE + b * BR + c * CH, h))
        return lax.fori_loop(0, BR // CH, step, acc)

    def keep(t, b, h):
        def step(c):
            there = rows_of(b * BR + c * CH, CH)
            out[there, cols(h)] = ybuf[rows_of(same + t * PIECE + b * BR + c * CH, CH), cols(h)]
        loop(0, BR // CH, step)

    def o_remote(t, b, h=None, n=1):
        return remote(ybuf.at[blocks(same + t * PIECE, b, n), cols(h)], out.at[blocks(0, b, n), cols(h)], o_s, o_r, mate)

    def emit(t, b, h, last):
        @pl.when(jnp.logical_not(last))
        def _():
            c_x(t, b, h).start()

        @pl.when(jnp.logical_and(last, row == t))
        def _():
            keep(t, b, h)

        @pl.when(jnp.logical_and(last, row != t))
        def _():
            o_remote(t, b, h).start()

    def finish(b, h, last, acc):
        arrived(c_fy, b, h)
        acc = update(0, b, h, ra, rfy, acc)
        emit(0, b, h, last)
        arrived(c_fx, b, h)
        acc = update(1, b, h, rdy, rfx, acc)
        emit(1, b, h, last)
        return acc

    def finish_half(h, last):
        part = lax.fori_loop(E, NB, lambda b, acc: finish(b, h, last, acc), jnp.zeros((8, HALF), jnp.float32))
        sacc[:, cols(h)] = sacc[:, cols(h)] + part

    def drain_forward():
        @pl.when(home)
        def _():
            c_fx(0, n=NB).wait_send()

        @pl.when(away)
        def _():
            c_fy(0, n=NB).wait_send()

    def sweep(k, carry):
        last = k == SWEEPS - 1
        more = jnp.logical_not(last)
        par = lax.rem(k, 2)

        def multiply(n, h):
            start = block_of(n)
            ybuf[rows_of(start, BR), cols(h)] = jnp.dot(
                abuf[lax.rem(n, RING)], xbf[:, cols(h)], preferred_element_type=jnp.float32)

        def fetch(n):
            @pl.when(jnp.logical_not(jnp.logical_and(last, n >= 4 * NB)))
            def _():
                a_copy(lax.rem(n, 4 * NB)).start()

        def lead(h):
            def one(n):
                if h == 0:
                    a_copy(n).wait()
                multiply(n, h)
                if h == 1:
                    fetch(n + RING)

                @pl.when(home)
                def _():
                    c_a(n, h).start()

                @pl.when(away)
                def _():
                    c_gy(n, h).start()
            loop(0, G, one)

        @pl.when(k > 0)
        def _head():
            pl.semaphore_wait(cr_0, 1)
            lead(0)

            @pl.when(home)
            def _():
                finish_half(1, jnp.bool_(False))
                s_publish(par, sacc[...])
                signal(cr_1, xn)
                signal(cr_1, yn)

            @pl.when(away)
            def _():
                x_bytes(G * BR, 1).wait_recv()

            lead(1)
            drain_forward()
            pl.semaphore_wait(cr_1, 1)

            @pl.when(away)
            def _():
                pl.semaphore_wait(cr_2, 1)

        def step(n):
            a_copy(n).wait()
            multiply(n, None)
            fetch(n + RING)
            at = block_of(n) - jnp.where(n < 2 * NB, other, same)
            return lax.div(at, PIECE), lax.div(lax.rem(at, PIECE), BR)

        def part_one(n):
            t, b = step(n)

            @pl.when(t == 0)
            def _():
                c_a(b).start()

            @pl.when(jnp.logical_and(t == 1, away))
            def _():
                c_gy(b).start()
        loop(G, 2 * NB, part_one)

        @pl.when(k == 0)
        def _():
            first_mass()

            @pl.when(away)
            def _():
                s0_copy(row).start()

            @pl.when(home)
            def _():
                v_in.start()
                d_copy(1 - row).wait_recv()
                s0_copy(1 - row).wait_recv()
                s_publish(0, s0buf[0] + s0buf[1])

        def add_into(start, b, src):
            def add(c):
                at = rows_of(start + b * BR + c * CH, CH)
                ybuf[at, :] = ybuf[at, :] + src[rows_of(b * BR + c * CH, CH), :]
            loop(0, BR // CH, add)

        def send_on(copy, b):
            @pl.when(b < E)
            def _():
                copy(b).start()

            @pl.when(b >= E)
            def _():
                copy(b, 0).start()

        def part_two(n):
            b = n - 2 * NB
            step(n)

            @pl.when(away)
            def _():
                c_dy(b).start()

            @pl.when(home)
            def _():
                @pl.when(lax.rem(b, G) == 0)
                def _():
                    c_gy(b, n=G).wait_recv()
                add_into(other + PIECE, b, rgy)
                send_on(c_fx, b)
        loop(2 * NB, 3 * NB, part_two)

        @pl.when(home)
        def _():
            loop(E, NB, lambda b: c_fx(b, 1).start())

        def part_three(n):
            b = n - 3 * NB
            step(n)

            @pl.when(away)
            def _():
                @pl.when(lax.rem(b, G) == 0)
                def _():
                    c_a(b, n=G).wait_recv()
                add_into(same, b, ra)
                send_on(c_fy, b)
        loop(3 * NB, 4 * NB, part_three)

        @pl.when(away)
        def _away():
            loop(E, NB, lambda b: c_fy(b, 1).start())

            @pl.when(k == 0)
            def _():
                x0_copy(mine, 0, X0C).wait_send()
                v_copy(row).wait_send()
                d_copy(row).wait_send()
                s0_copy(row).wait_send()

            @pl.when(more)
            def _():
                signal(cr_2, mate)
                signal(cr_2, xn)
            c_a(0, n=NB).wait_send()
            c_gy(0, n=NB).wait_send()
            c_dy(0, NB).wait_send()

            @pl.when(more)
            def _():
                x_bytes(2 * PIECE - G * BR, 0).wait_recv()

        @pl.when(home)
        def _home():
            @pl.when(more)
            def _():
                signal(cr_0, yn)

            @pl.when(k == 0)
            def _():
                spread(1 - row)
                x0_copy(mine, 0, X0C).wait_send()
                v_copy(1 - row).wait_recv()
                v_in.wait()

            @pl.when(k > 0)
            def _():
                x_bytes(2 * PIECE, 0).wait_send()

            s_bytes(par).wait_recv()
            s_bytes(par).wait_send()
            mass = ((sbuf[par, 0] + sbuf[par, 1]) + (sbuf[par, 2] + sbuf[par, 3])) / VERTS
            coef[...] = jnp.broadcast_to(DAMPING * mass + (1.0 - DAMPING), (8, VECS))

            @pl.when(more)
            def _():
                pl.semaphore_wait(cr_2, 1)

            c_a(0, n=NB).wait_send()
            for b in range(0, NB, G):
                c_a(b, n=G).wait_recv()
            c_dy(0, NB).wait_recv()
            sacc[...] = lax.fori_loop(0, E, lambda b, acc: finish(b, None, last, acc), jnp.zeros((8, VECS), jnp.float32))

            @pl.when(more)
            def _():
                signal(cr_0, xn)
            finish_half(0, last)

        return carry

    lax.fori_loop(0, SWEEPS, sweep, 0)

    @pl.when(home)
    def _():
        finish_half(1, jnp.bool_(True))
    drain_forward()

    @pl.when(home)
    def _():
        o_remote(1 - row, 0, n=NB).wait_send()

    @pl.when(away)
    def _():
        o_remote(1 - row, 0, n=NB).wait_recv()


def solution(mesh):
    dma = pltpu.SemaphoreType.DMA
    reg = pltpu.SemaphoreType.REGULAR

    def in_hbm(a):
        return pltpu.with_memory_space_constraint(a, pltpu.HBM)

    def local_sweeps(mat_tile, x_piece, tele_piece, dang_piece):
        part = pltpu.VMEM((PIECE, VECS), jnp.float32)
        return pl.pallas_call(
            kernel,
            name="sweeps",
            out_shape=jax.ShapeDtypeStruct((PIECE, VECS), jnp.float32),
            in_specs=[pl.BlockSpec(memory_space=pltpu.HBM)] * 4,
            out_specs=pl.BlockSpec(memory_space=pltpu.VMEM),
            scratch_shapes=[
                pltpu.VMEM((RING, BR, COLS), jnp.bfloat16),
                pltpu.VMEM((COLS, VECS), jnp.bfloat16),
                pltpu.VMEM((ROWS, VECS), jnp.float32),
                part, part, part, part, part,
                pltpu.VMEM((COLS, VECS), jnp.float32),
                pltpu.VMEM((COLS, 128), jnp.bfloat16),
                pltpu.VMEM((2, PIECE // 128, 128), jnp.int32),
                pltpu.VMEM((2, 4, 1, VECS), jnp.float32),
                pltpu.VMEM((2, 8, VECS), jnp.float32),
                pltpu.VMEM((8, VECS), jnp.float32),
                pltpu.VMEM((8, VECS), jnp.float32),
                dma((RING,)), dma((X0C,)), dma, dma,
                dma, dma((NB // G,)), dma, dma((NB // G,)), dma, dma, dma, dma((E // G + 4,)), dma, dma((E // G + 4,)),
                dma, dma((2,)), dma, dma((2,)), dma, dma, reg, reg, reg,
            ],
            compiler_params=pltpu.CompilerParams(
                collective_id=0, has_side_effects=True, vmem_limit_bytes=53_300_000),
            cost_estimate=pl.CostEstimate(
                flops=2 * ROWS * COLS * VECS * SWEEPS, bytes_accessed=2 * ROWS * COLS * SWEEPS, transcendentals=0),
        )(mat_tile, x_piece, tele_piece, in_hbm(dang_piece.reshape(PIECE // 128, 128)))

    vec_spec = P(('col', 'row'), None)
    return jax.shard_map(local_sweeps, mesh=mesh,
                         in_specs=(P('row', 'col'), vec_spec, vec_spec, P(('col', 'row'))),
                         out_specs=vec_spec, check_vma=False)
```

```python
import jax
import jax.numpy as jnp
from jax import lax
from jax.experimental import pallas as pl
from jax.experimental.pallas import tpu as pltpu
from jax.sharding import PartitionSpec as P

SWEEPS = 8
DAMPING = 0.85
MESH = pl.DeviceIdType.MESH

VERTS = 24576
VECS = 256
HALF = 128
PIECE = 3072
ROWS = 12288
COLS = 6144
BR = 256
NB = PIECE // BR
G = 4
E = NB - G
CH = 32
RING = 4
X0C = 4
X0R = PIECE // X0C
EARLY = 2


def kernel(a_hbm, x_hbm, v_hbm, d_hbm, out,
           abuf, xbf, ybuf, ra, rgy, rdy, rfx, rfy, vbuf, dbuf, dint, sbuf, s0buf, coef, sacc,
           a_sem, in_sem, x0_s, x0_r,
           a_s, a_r, gy_s, gy_r, dy_s, dy_r, fx_s, fx_r, fy_s, fy_r,
           x_s, x_r, s_s, s_r, o_s, o_r, cr_0, cr_1, cr_2):
    col = lax.axis_index('col')
    row = lax.axis_index('row')
    cx, cy = lax.rem(col, 2), lax.div(col, 2)
    home = row == cy
    away = jnp.logical_not(home)
    xn = (cy * 2 + 1 - cx, row)
    yn = ((1 - cy) * 2 + cx, row)
    mate = (col, 1 - row)
    same = cx * COLS
    other = (1 - cx) * COLS
    mine = row * PIECE
    far = (1 - row) * PIECE

    def rows_of(start, size):
        return pl.ds(pl.multiple_of(start, size), size)

    def blocks(start, b, n):
        return pl.ds(pl.multiple_of(start + b * BR, BR), n * BR)

    def cols(h):
        return pl.ds(0, VECS) if h is None else pl.ds(h * HALF, HALF)

    def remote(src, dst, send, recv, dev):
        return pltpu.make_async_remote_copy(
            src_ref=src, dst_ref=dst, send_sem=send, recv_sem=recv, device_id=dev, device_id_type=MESH)

    def loop(lo, hi, body):
        def step(i, c):
            body(i)
            return c
        lax.fori_loop(lo, hi, step, 0)

    def signal(sem, dev):
        pl.semaphore_signal(sem, inc=1, device_id=dev, device_id_type=MESH)

    def x_in(c):
        return pltpu.make_async_copy(x_hbm.at[rows_of(c * X0R, X0R)], vbuf.at[rows_of(mine + c * X0R, X0R)], in_sem.at[c])

    for c in range(X0C):
        x_in(c).start()

    barrier = pltpu.get_barrier_semaphore()
    for off in range(4):
        for r in range(2):
            if off == 0 and r == 1:
                continue
            signal(barrier, (lax.rem(col + off, 4), row if r == 0 and off else 1 - row))

    def flow(start, b, n, h, dst, send, recv, i, dev):
        return remote(ybuf.at[blocks(start, b, n), cols(h)], dst.at[blocks(0, b, n), cols(h)], send, recv.at[i], dev)

    def c_a(b, h=None, n=1):
        return flow(other, b, n, h, ra, a_s, a_r, lax.div(b, G), xn)

    def c_gy(b, h=None, n=1):
        return flow(other + PIECE, b, n, h, rgy, gy_s, gy_r, lax.div(b, G), yn)

    def c_dy(b, n=1):
        return remote(ybuf.at[blocks(same + PIECE, b, n)], rdy.at[blocks(0, b, n)], dy_s, dy_r, yn)

    def late(b, h):
        return lax.div(b, G) if h is None else E // G + 2 * h + jnp.where(b == NB - 1, 1, 0)

    def c_fx(b, h=None, n=1):
        return flow(other + PIECE, b, n, h, rfx, fx_s, fx_r, late(b, h), xn)

    def c_fy(b, h=None, n=1):
        return flow(same, b, n, h, rfy, fy_s, fy_r, late(b, h), yn)

    def arrived(copy, b, h):
        if h is None:
            @pl.when(lax.rem(b, G) == 0)
            def _():
                copy(b, n=G).wait_recv()
        else:
            @pl.when(b == E)
            def _():
                copy(b, h, n=G - 1).wait_recv()

            @pl.when(b == NB - 1)
            def _():
                copy(b, h).wait_recv()

    def c_x(t, b, h=None):
        at = blocks(t * PIECE, b, 1)
        return remote(xbf.at[at, cols(h)], xbf.at[at, cols(h)], x_s, x_r.at[1 if h == 1 else 0], mate)

    def x_bytes(rows, i):
        return remote(xbf.at[pl.ds(0, rows)], xbf.at[pl.ds(0, rows)], x_s, x_r.at[i], mate)

    def block_of(n):
        m = n - G
        pair = m < 2 * E
        t0 = jnp.where(pair, lax.rem(m, 2), 1)
        b0 = jnp.where(pair, jnp.where(t0 == 0, G, 0) + lax.div(m, 2), m - E)
        b0 = jnp.where(m < 0, n, b0)
        t0 = jnp.where(jnp.logical_xor(home, jnp.logical_or(m < 0, t0 == 0)), 1, 0)
        m = n - 2 * NB
        first = n < 2 * NB
        t = jnp.where(first, t0, 1 - lax.div(m, NB))
        b = jnp.where(first, b0, lax.rem(m, NB))
        return jnp.where(first, other, same) + t * PIECE + b * BR

    def a_copy(n):
        slot = lax.rem(n, RING)
        return pltpu.make_async_copy(a_hbm.at[rows_of(block_of(n), BR)], abuf.at[slot], a_sem.at[slot])

    d_in = pltpu.make_async_copy(d_hbm, dint.at[row], in_sem.at[0])
    v_in = pltpu.make_async_copy(v_hbm, vbuf.at[rows_of(mine, PIECE)], in_sem.at[1])

    def v_copy(r):
        return remote(v_hbm, vbuf.at[rows_of(r * PIECE, PIECE)], fx_s, x_r.at[0], mate)

    def d_copy(r):
        return remote(d_hbm, dint.at[r], x_s, x_r.at[1], mate)

    def s0_copy(r):
        return remote(s0buf.at[r], s0buf.at[r], o_s, o_r, mate)

    def x0_copy(start, c, n=1):
        at = pl.ds(pl.multiple_of(start + c * X0R, X0R), n * X0R)
        return remote(xbf.at[at], xbf.at[at], x0_s, x0_r, mate)

    for c in range(X0C):
        x_in(c).wait()

        def convert(i, c=c):
            at = rows_of(mine + c * X0R + i * CH, CH)
            xbf[at, :] = vbuf[at, :].astype(jnp.bfloat16)
        loop(0, X0R // CH, convert)
        if c == 0:
            pl.semaphore_wait(barrier, 7)
        x0_copy(mine, c).start()
        if c < RING:
            a_copy(jnp.int32(c)).start()
    d_in.start()

    @pl.when(away)
    def _():
        d_copy(row).start()
        v_copy(row).start()

    def half_product(n, start):
        at = rows_of(start, PIECE)
        return jnp.dot(abuf[lax.rem(n, RING), :, at], xbf[at, :], preferred_element_type=jnp.float32)

    def first_own(n):
        a_copy(n).wait()
        ybuf[rows_of(block_of(n), BR), :] = half_product(n, mine)
    loop(0, EARLY, first_own)
    x0_copy(far, 0, X0C).wait_recv()

    def first_send(n):
        a_copy(n + RING).start()
        for h in range(2):
            @pl.when(home)
            def _():
                c_a(n, h).start()

            @pl.when(away)
            def _():
                c_gy(n, h).start()

    def first_far(n):
        at = rows_of(block_of(n), BR)
        ybuf[at, :] = ybuf[at, :] + half_product(n, far)
        first_send(n)
    loop(0, EARLY, first_far)

    def first_whole(n):
        a_copy(n).wait()
        ybuf[rows_of(block_of(n), BR), :] = jnp.dot(
            abuf[lax.rem(n, RING)], xbf[...], preferred_element_type=jnp.float32)
        first_send(n)
    loop(EARLY, G, first_whole)

    def s_copy(par, off):
        dst_col = lax.rem(col + off, 4)
        return remote(sbuf.at[par, col], sbuf.at[par, col], s_s, s_r.at[par], (dst_col, lax.div(dst_col, 2)))

    def s_bytes(par):
        return remote(sbuf.at[par, pl.ds(0, 3)], sbuf.at[par, pl.ds(0, 3)], s_s, s_r.at[par], mate)

    def s_publish(par, value):
        sbuf[par, col] = jnp.sum(value, axis=0, keepdims=True)
        for off in range(1, 4):
            s_copy(par, off).start()

    def spread(r):
        def group(g):
            flags = dint[r, pl.ds(g, 1), :].astype(jnp.float32)
            dbuf[rows_of(r * PIECE + g * 128, 128), :] = jnp.broadcast_to(flags, (128, 128)).T.astype(jnp.bfloat16)
        loop(0, PIECE // 128, group)

    def flags(start, h):
        d = dbuf[rows_of(start, CH), :].astype(jnp.float32)
        return d if h is not None else jnp.concatenate([d, d], axis=1)

    def fold(w):
        return jnp.sum(w.reshape(CH // 8, 8, w.shape[1]), axis=0)

    def first_mass():
        d_in.wait()
        spread(row)

        def add(c, acc):
            at = mine + c * CH
            return acc + fold(vbuf[rows_of(at, CH), :] * flags(at, None))
        s0buf[row] = lax.fori_loop(0, PIECE // CH, add, jnp.zeros((8, VECS), jnp.float32))

    def update(t, b, h, one, two, acc):
        def step(c, acc):
            at = rows_of(same + t * PIECE + b * BR + c * CH, CH)
            own = rows_of(t * PIECE + b * BR + c * CH, CH)
            there = rows_of(b * BR + c * CH, CH)
            y = (ybuf[at, cols(h)] + one[there, cols(h)]) + two[there, cols(h)]
            cf = jnp.concatenate([coef[:, cols(h)]] * (CH // 8), axis=0)
            x = DAMPING * y + cf * vbuf[own, cols(h)]
            xbf[own, cols(h)] = x.astype(jnp.bfloat16)
            ybuf[at, cols(h)] = x
            return acc + fold(x * flags(t * PIECE + b * BR + c * CH, h))
        return lax.fori_loop(0, BR // CH, step, acc)

    def keep(t, b, h):
        def step(c):
            there = rows_of(b * BR + c * CH, CH)
            out[there, cols(h)] = ybuf[rows_of(same + t * PIECE + b * BR + c * CH, CH), cols(h)]
        loop(0, BR // CH, step)

    def o_remote(t, b, h=None, n=1):
        return remote(ybuf.at[blocks(same + t * PIECE, b, n), cols(h)], out.at[blocks(0, b, n), cols(h)], o_s, o_r, mate)

    def emit(t, b, h, last):
        @pl.when(jnp.logical_not(last))
        def _():
            c_x(t, b, h).start()

        @pl.when(jnp.logical_and(last, row == t))
        def _():
            keep(t, b, h)

        @pl.when(jnp.logical_and(last, row != t))
        def _():
            o_remote(t, b, h).start()

    def finish(b, h, last, acc):
        arrived(c_fy, b, h)
        acc = update(0, b, h, ra, rfy, acc)
        emit(0, b, h, last)
        arrived(c_fx, b, h)
        acc = update(1, b, h, rdy, rfx, acc)
        emit(1, b, h, last)
        return acc

    def finish_half(h, last):
        part = lax.fori_loop(E, NB, lambda b, acc: finish(b, h, last, acc), jnp.zeros((8, HALF), jnp.float32))
        sacc[:, cols(h)] = sacc[:, cols(h)] + part

    def drain_forward():
        @pl.when(home)
        def _():
            c_fx(0, n=NB).wait_send()

        @pl.when(away)
        def _():
            c_fy(0, n=NB).wait_send()

    def sweep(k, carry):
        last = k == SWEEPS - 1
        more = jnp.logical_not(last)
        par = lax.rem(k, 2)

        def multiply(n, h):
            start = block_of(n)
            ybuf[rows_of(start, BR), cols(h)] = jnp.dot(
                abuf[lax.rem(n, RING)], xbf[:, cols(h)], preferred_element_type=jnp.float32)

        def fetch(n):
            @pl.when(jnp.logical_not(jnp.logical_and(last, n >= 4 * NB)))
            def _():
                a_copy(lax.rem(n, 4 * NB)).start()

        def lead(h):
            def one(n):
                if h == 0:
                    a_copy(n).wait()
                multiply(n, h)
                if h == 1:
                    fetch(n + RING)

                @pl.when(home)
                def _():
                    c_a(n, h).start()

                @pl.when(away)
                def _():
                    c_gy(n, h).start()
            loop(0, G, one)

        @pl.when(k > 0)
        def _head():
            pl.semaphore_wait(cr_0, 1)
            lead(0)

            @pl.when(home)
            def _():
                finish_half(1, jnp.bool_(False))
                s_publish(par, sacc[...])
                signal(cr_1, xn)
                signal(cr_1, yn)

            @pl.when(away)
            def _():
                x_bytes(G * BR, 1).wait_recv()

            lead(1)
            drain_forward()
            pl.semaphore_wait(cr_1, 1)

            @pl.when(away)
            def _():
                pl.semaphore_wait(cr_2, 1)

        def step(n):
            a_copy(n).wait()
            multiply(n, None)
            fetch(n + RING)
            at = block_of(n) - jnp.where(n < 2 * NB, other, same)
            return lax.div(at, PIECE), lax.div(lax.rem(at, PIECE), BR)

        def part_one(n):
            t, b = step(n)

            @pl.when(t == 0)
            def _():
                c_a(b).start()

            @pl.when(jnp.logical_and(t == 1, away))
            def _():
                c_gy(b).start()
        loop(G, 2 * NB, part_one)

        @pl.when(k == 0)
        def _():
            first_mass()

            @pl.when(away)
            def _():
                s0_copy(row).start()

            @pl.when(home)
            def _():
                v_in.start()
                d_copy(1 - row).wait_recv()
                s0_copy(1 - row).wait_recv()
                s_publish(0, s0buf[0] + s0buf[1])

        def add_into(start, b, src):
            def add(c):
                at = rows_of(start + b * BR + c * CH, CH)
                ybuf[at, :] = ybuf[at, :] + src[rows_of(b * BR + c * CH, CH), :]
            loop(0, BR // CH, add)

        def send_on(copy, b):
            @pl.when(b < E)
            def _():
                copy(b).start()

            @pl.when(b >= E)
            def _():
                copy(b, 0).start()

        def part_two(n):
            b = n - 2 * NB
            step(n)

            @pl.when(away)
            def _():
                c_dy(b).start()

            @pl.when(home)
            def _():
                @pl.when(lax.rem(b, G) == 0)
                def _():
                    c_gy(b, n=G).wait_recv()
                add_into(other + PIECE, b, rgy)
                send_on(c_fx, b)
        loop(2 * NB, 3 * NB, part_two)

        @pl.when(home)
        def _():
            loop(E, NB, lambda b: c_fx(b, 1).start())

        def part_three(n):
            b = n - 3 * NB
            step(n)

            @pl.when(away)
            def _():
                @pl.when(lax.rem(b, G) == 0)
                def _():
                    c_a(b, n=G).wait_recv()
                add_into(same, b, ra)
                send_on(c_fy, b)
        loop(3 * NB, 4 * NB, part_three)

        @pl.when(away)
        def _away():
            loop(E, NB, lambda b: c_fy(b, 1).start())

            @pl.when(k == 0)
            def _():
                x0_copy(mine, 0, X0C).wait_send()
                v_copy(row).wait_send()
                d_copy(row).wait_send()
                s0_copy(row).wait_send()

            @pl.when(more)
            def _():
                signal(cr_2, mate)
                signal(cr_2, xn)
            c_a(0, n=NB).wait_send()
            c_gy(0, n=NB).wait_send()
            c_dy(0, NB).wait_send()

            @pl.when(more)
            def _():
                x_bytes(2 * PIECE - G * BR, 0).wait_recv()

        @pl.when(home)
        def _home():
            @pl.when(more)
            def _():
                signal(cr_0, yn)

            @pl.when(k == 0)
            def _():
                spread(1 - row)
                x0_copy(mine, 0, X0C).wait_send()
                v_copy(1 - row).wait_recv()
                v_in.wait()

            @pl.when(k > 0)
            def _():
                x_bytes(2 * PIECE, 0).wait_send()

            s_bytes(par).wait_recv()
            s_bytes(par).wait_send()
            mass = ((sbuf[par, 0] + sbuf[par, 1]) + (sbuf[par, 2] + sbuf[par, 3])) / VERTS
            coef[...] = jnp.broadcast_to(DAMPING * mass + (1.0 - DAMPING), (8, VECS))

            @pl.when(more)
            def _():
                pl.semaphore_wait(cr_2, 1)

            c_a(0, n=NB).wait_send()
            for b in range(0, NB, G):
                c_a(b, n=G).wait_recv()
            c_dy(0, NB).wait_recv()
            sacc[...] = lax.fori_loop(0, E, lambda b, acc: finish(b, None, last, acc), jnp.zeros((8, VECS), jnp.float32))

            @pl.when(more)
            def _():
                signal(cr_0, xn)
            finish_half(0, last)

        return carry

    lax.fori_loop(0, SWEEPS, sweep, 0)

    @pl.when(home)
    def _():
        finish_half(1, jnp.bool_(True))
    drain_forward()

    @pl.when(home)
    def _():
        o_remote(1 - row, 0, n=NB).wait_send()

    @pl.when(away)
    def _():
        o_remote(1 - row, 0, n=NB).wait_recv()


def solution(mesh):
    dma = pltpu.SemaphoreType.DMA
    reg = pltpu.SemaphoreType.REGULAR

    def in_hbm(a):
        return pltpu.with_memory_space_constraint(a, pltpu.HBM)

    def local_sweeps(mat_tile, x_piece, tele_piece, dang_piece):
        part = pltpu.VMEM((PIECE, VECS), jnp.float32)
        return pl.pallas_call(
            kernel,
            name="sweeps",
            out_shape=jax.ShapeDtypeStruct((PIECE, VECS), jnp.float32),
            in_specs=[pl.BlockSpec(memory_space=pltpu.HBM)] * 4,
            out_specs=pl.BlockSpec(memory_space=pltpu.VMEM),
            scratch_shapes=[
                pltpu.VMEM((RING, BR, COLS), jnp.bfloat16),
                pltpu.VMEM((COLS, VECS), jnp.bfloat16),
                pltpu.VMEM((ROWS, VECS), jnp.float32),
                part, part, part, part, part,
                pltpu.VMEM((COLS, VECS), jnp.float32),
                pltpu.VMEM((COLS, 128), jnp.bfloat16),
                pltpu.VMEM((2, PIECE // 128, 128), jnp.int32),
                pltpu.VMEM((2, 4, 1, VECS), jnp.float32),
                pltpu.VMEM((2, 8, VECS), jnp.float32),
                pltpu.VMEM((8, VECS), jnp.float32),
                pltpu.VMEM((8, VECS), jnp.float32),
                dma((RING,)), dma((X0C,)), dma, dma,
                dma, dma((NB // G,)), dma, dma((NB // G,)), dma, dma, dma, dma((E // G + 4,)), dma, dma((E // G + 4,)),
                dma, dma((2,)), dma, dma((2,)), dma, dma, reg, reg, reg,
            ],
            compiler_params=pltpu.CompilerParams(
                collective_id=0, has_side_effects=True, vmem_limit_bytes=53_300_000),
            cost_estimate=pl.CostEstimate(
                flops=2 * ROWS * COLS * VECS * SWEEPS, bytes_accessed=2 * ROWS * COLS * SWEEPS, transcendentals=0),
        )(mat_tile, x_piece, tele_piece, in_hbm(dang_piece.reshape(PIECE // 128, 128)))

    vec_spec = P(('col', 'row'), None)
    return jax.shard_map(local_sweeps, mesh=mesh,
                         in_specs=(P('row', 'col'), vec_spec, vec_spec, P(('col', 'row'))),
                         out_specs=vec_spec, check_vma=False)
```

```python
import jax
import jax.numpy as jnp
from jax import lax
from jax.experimental import pallas as pl
from jax.experimental.pallas import tpu as pltpu
from jax.sharding import PartitionSpec as P

SWEEPS = 8
DAMPING = 0.85
MESH = pl.DeviceIdType.MESH

VERTS = 24576
VECS = 256
HALF = 128
PIECE = 3072
ROWS = 12288
COLS = 6144
BR = 256
NB = PIECE // BR
G = 4
E = NB - G
CH = 32
RING = 4
X0C = 4
X0R = PIECE // X0C


def kernel(a_hbm, x_hbm, v_hbm, d_hbm, out,
           abuf, xbf, ybuf, ra, rgy, rdy, rfx, rfy, vbuf, dbuf, dint, sbuf, s0buf, coef, sacc,
           a_sem, in_sem, x0_s, x0_r,
           a_s, a_r, gy_s, gy_r, dy_s, dy_r, fx_s, fx_r, fy_s, fy_r,
           x_s, x_r, s_s, s_r, o_s, o_r, cr_0, cr_1, cr_2):
    col = lax.axis_index('col')
    row = lax.axis_index('row')
    cx, cy = lax.rem(col, 2), lax.div(col, 2)
    home = row == cy
    away = jnp.logical_not(home)
    xn = (cy * 2 + 1 - cx, row)
    yn = ((1 - cy) * 2 + cx, row)
    mate = (col, 1 - row)
    same = cx * COLS
    other = (1 - cx) * COLS
    mine = row * PIECE
    far = (1 - row) * PIECE

    def rows_of(start, size):
        return pl.ds(pl.multiple_of(start, size), size)

    def blocks(start, b, n):
        return pl.ds(pl.multiple_of(start + b * BR, BR), n * BR)

    def cols(h):
        return pl.ds(0, VECS) if h is None else pl.ds(h * HALF, HALF)

    def remote(src, dst, send, recv, dev):
        return pltpu.make_async_remote_copy(
            src_ref=src, dst_ref=dst, send_sem=send, recv_sem=recv, device_id=dev, device_id_type=MESH)

    def loop(lo, hi, body):
        def step(i, c):
            body(i)
            return c
        lax.fori_loop(lo, hi, step, 0)

    def signal(sem, dev):
        pl.semaphore_signal(sem, inc=1, device_id=dev, device_id_type=MESH)

    def x_in(c):
        return pltpu.make_async_copy(x_hbm.at[rows_of(c * X0R, X0R)], vbuf.at[rows_of(mine + c * X0R, X0R)], in_sem.at[c])

    for c in range(X0C):
        x_in(c).start()

    barrier = pltpu.get_barrier_semaphore()
    for off in range(4):
        for r in range(2):
            if off == 0 and r == 1:
                continue
            signal(barrier, (lax.rem(col + off, 4), row if r == 0 and off else 1 - row))

    def flow(start, b, n, h, dst, send, recv, i, dev):
        return remote(ybuf.at[blocks(start, b, n), cols(h)], dst.at[blocks(0, b, n), cols(h)], send, recv.at[i], dev)

    def c_a(b, h=None, n=1):
        return flow(other, b, n, h, ra, a_s, a_r, lax.div(b, G), xn)

    def c_gy(b, h=None, n=1):
        return flow(other + PIECE, b, n, h, rgy, gy_s, gy_r, lax.div(b, G), yn)

    def c_dy(b, n=1):
        return remote(ybuf.at[blocks(same + PIECE, b, n)], rdy.at[blocks(0, b, n)], dy_s, dy_r, yn)

    def late(b, h):
        return lax.div(b, G) if h is None else E // G + 2 * h + jnp.where(b == NB - 1, 1, 0)

    def c_fx(b, h=None, n=1):
        return flow(other + PIECE, b, n, h, rfx, fx_s, fx_r, late(b, h), xn)

    def c_fy(b, h=None, n=1):
        return flow(same, b, n, h, rfy, fy_s, fy_r, late(b, h), yn)

    def arrived(copy, b, h):
        if h is None:
            @pl.when(lax.rem(b, G) == 0)
            def _():
                copy(b, n=G).wait_recv()
        else:
            @pl.when(b == E)
            def _():
                copy(b, h, n=G - 1).wait_recv()

            @pl.when(b == NB - 1)
            def _():
                copy(b, h).wait_recv()

    def c_x(t, b, h=None):
        at = blocks(t * PIECE, b, 1)
        return remote(xbf.at[at, cols(h)], xbf.at[at, cols(h)], x_s, x_r.at[1 if h == 1 else 0], mate)

    def x_bytes(rows, i):
        return remote(xbf.at[pl.ds(0, rows)], xbf.at[pl.ds(0, rows)], x_s, x_r.at[i], mate)

    def block_of(n):
        m = n - G
        pair = m < 2 * E
        t0 = jnp.where(pair, lax.rem(m, 2), 1)
        b0 = jnp.where(pair, jnp.where(t0 == 0, G, 0) + lax.div(m, 2), m - E)
        b0 = jnp.where(m < 0, n, b0)
        t0 = jnp.where(jnp.logical_xor(home, jnp.logical_or(m < 0, t0 == 0)), 1, 0)
        m = n - 2 * NB
        first = n < 2 * NB
        t = jnp.where(first, t0, 1 - lax.div(m, NB))
        b = jnp.where(first, b0, lax.rem(m, NB))
        return jnp.where(first, other, same) + t * PIECE + b * BR

    def a_copy(n):
        slot = lax.rem(n, RING)
        return pltpu.make_async_copy(a_hbm.at[rows_of(block_of(n), BR)], abuf.at[slot], a_sem.at[slot])

    d_in = pltpu.make_async_copy(d_hbm, dint.at[row], in_sem.at[0])
    v_in = pltpu.make_async_copy(v_hbm, vbuf.at[rows_of(mine, PIECE)], in_sem.at[1])

    def v_copy(r):
        return remote(v_hbm, vbuf.at[rows_of(r * PIECE, PIECE)], fx_s, x_r.at[0], mate)

    def d_copy(r):
        return remote(d_hbm, dint.at[r], x_s, x_r.at[1], mate)

    def s0_copy(r):
        return remote(s0buf.at[r], s0buf.at[r], o_s, o_r, mate)

    def x0_copy(start, c, h, n=1):
        at = pl.ds(pl.multiple_of(start + c * X0R, X0R), n * X0R)
        return remote(xbf.at[at, cols(h)], xbf.at[at, cols(h)], x0_s, x0_r.at[1 if h == 1 else 0], mate)

    for c in range(X0C):
        x_in(c).wait()

        def convert(i, c=c):
            at = rows_of(mine + c * X0R + i * CH, CH)
            xbf[at, :] = vbuf[at, :].astype(jnp.bfloat16)
        loop(0, X0R // CH, convert)
        if c == 0:
            pl.semaphore_wait(barrier, 7)
        x0_copy(mine, c, 0).start()
        if c < RING:
            a_copy(jnp.int32(c)).start()
    for c in range(X0C):
        x0_copy(mine, c, 1).start()
    d_in.start()

    @pl.when(away)
    def _():
        d_copy(row).start()
        v_copy(row).start()

    def s_copy(par, off):
        dst_col = lax.rem(col + off, 4)
        return remote(sbuf.at[par, col], sbuf.at[par, col], s_s, s_r.at[par], (dst_col, lax.div(dst_col, 2)))

    def s_bytes(par):
        return remote(sbuf.at[par, pl.ds(0, 3)], sbuf.at[par, pl.ds(0, 3)], s_s, s_r.at[par], mate)

    def s_publish(par, value):
        sbuf[par, col] = jnp.sum(value, axis=0, keepdims=True)
        for off in range(1, 4):
            s_copy(par, off).start()

    def spread(r):
        def group(g):
            flags = dint[r, pl.ds(g, 1), :].astype(jnp.float32)
            dbuf[rows_of(r * PIECE + g * 128, 128), :] = jnp.broadcast_to(flags, (128, 128)).T.astype(jnp.bfloat16)
        loop(0, PIECE // 128, group)

    def flags(start, h):
        d = dbuf[rows_of(start, CH), :].astype(jnp.float32)
        return d if h is not None else jnp.concatenate([d, d], axis=1)

    def fold(w):
        return jnp.sum(w.reshape(CH // 8, 8, w.shape[1]), axis=0)

    def first_mass():
        d_in.wait()
        spread(row)

        def add(c, acc):
            at = mine + c * CH
            return acc + fold(vbuf[rows_of(at, CH), :] * flags(at, None))
        s0buf[row] = lax.fori_loop(0, PIECE // CH, add, jnp.zeros((8, VECS), jnp.float32))

    def update(t, b, h, one, two, acc):
        def step(c, acc):
            at = rows_of(same + t * PIECE + b * BR + c * CH, CH)
            own = rows_of(t * PIECE + b * BR + c * CH, CH)
            there = rows_of(b * BR + c * CH, CH)
            y = (ybuf[at, cols(h)] + one[there, cols(h)]) + two[there, cols(h)]
            cf = jnp.concatenate([coef[:, cols(h)]] * (CH // 8), axis=0)
            x = DAMPING * y + cf * vbuf[own, cols(h)]
            xbf[own, cols(h)] = x.astype(jnp.bfloat16)
            ybuf[at, cols(h)] = x
            return acc + fold(x * flags(t * PIECE + b * BR + c * CH, h))
        return lax.fori_loop(0, BR // CH, step, acc)

    def keep(t, b, h):
        def step(c):
            there = rows_of(b * BR + c * CH, CH)
            out[there, cols(h)] = ybuf[rows_of(same + t * PIECE + b * BR + c * CH, CH), cols(h)]
        loop(0, BR // CH, step)

    def o_remote(t, b, h=None, n=1):
        return remote(ybuf.at[blocks(same + t * PIECE, b, n), cols(h)], out.at[blocks(0, b, n), cols(h)], o_s, o_r, mate)

    def emit(t, b, h, last):
        @pl.when(jnp.logical_not(last))
        def _():
            c_x(t, b, h).start()

        @pl.when(jnp.logical_and(last, row == t))
        def _():
            keep(t, b, h)

        @pl.when(jnp.logical_and(last, row != t))
        def _():
            o_remote(t, b, h).start()

    def finish(b, h, last, acc):
        arrived(c_fy, b, h)
        acc = update(0, b, h, ra, rfy, acc)
        emit(0, b, h, last)
        arrived(c_fx, b, h)
        acc = update(1, b, h, rdy, rfx, acc)
        emit(1, b, h, last)
        return acc

    def finish_half(h, last):
        part = lax.fori_loop(E, NB, lambda b, acc: finish(b, h, last, acc), jnp.zeros((8, HALF), jnp.float32))
        sacc[:, cols(h)] = sacc[:, cols(h)] + part

    def drain_forward():
        @pl.when(home)
        def _():
            c_fx(0, n=NB).wait_send()

        @pl.when(away)
        def _():
            c_fy(0, n=NB).wait_send()

    def sweep(k, carry):
        last = k == SWEEPS - 1
        more = jnp.logical_not(last)
        par = lax.rem(k, 2)

        def multiply(n, h):
            start = block_of(n)
            ybuf[rows_of(start, BR), cols(h)] = jnp.dot(
                abuf[lax.rem(n, RING)], xbf[:, cols(h)], preferred_element_type=jnp.float32)

        def fetch(n):
            @pl.when(jnp.logical_not(jnp.logical_and(last, n >= 4 * NB)))
            def _():
                a_copy(lax.rem(n, 4 * NB)).start()

        def lead(h):
            def one(n):
                if h == 0:
                    a_copy(n).wait()
                multiply(n, h)
                if h == 1:
                    fetch(n + RING)

                @pl.when(home)
                def _():
                    c_a(n, h).start()

                @pl.when(away)
                def _():
                    c_gy(n, h).start()
            loop(0, G, one)

        @pl.when(k == 0)
        def _():
            x0_copy(far, 0, 0, X0C).wait_recv()

        @pl.when(k > 0)
        def _():
            pl.semaphore_wait(cr_0, 1)
        lead(0)

        @pl.when(k == 0)
        def _():
            x0_copy(far, 0, 1, X0C).wait_recv()

        @pl.when(jnp.logical_and(k > 0, home))
        def _():
            finish_half(1, jnp.bool_(False))
            s_publish(par, sacc[...])
            signal(cr_1, xn)
            signal(cr_1, yn)

        @pl.when(jnp.logical_and(k > 0, away))
        def _():
            x_bytes(G * BR, 1).wait_recv()
        lead(1)

        @pl.when(k > 0)
        def _():
            drain_forward()
            pl.semaphore_wait(cr_1, 1)

            @pl.when(away)
            def _():
                pl.semaphore_wait(cr_2, 1)

        def step(n):
            a_copy(n).wait()
            multiply(n, None)
            fetch(n + RING)
            at = block_of(n) - jnp.where(n < 2 * NB, other, same)
            return lax.div(at, PIECE), lax.div(lax.rem(at, PIECE), BR)

        def part_one(n):
            t, b = step(n)

            @pl.when(t == 0)
            def _():
                c_a(b).start()

            @pl.when(jnp.logical_and(t == 1, away))
            def _():
                c_gy(b).start()
        loop(G, 2 * NB, part_one)

        @pl.when(k == 0)
        def _():
            first_mass()

            @pl.when(away)
            def _():
                s0_copy(row).start()

            @pl.when(home)
            def _():
                v_in.start()
                d_copy(1 - row).wait_recv()
                s0_copy(1 - row).wait_recv()
                s_publish(0, s0buf[0] + s0buf[1])

        def add_into(start, b, src):
            def add(c):
                at = rows_of(start + b * BR + c * CH, CH)
                ybuf[at, :] = ybuf[at, :] + src[rows_of(b * BR + c * CH, CH), :]
            loop(0, BR // CH, add)

        def send_on(copy, b):
            @pl.when(b < E)
            def _():
                copy(b).start()

            @pl.when(b >= E)
            def _():
                copy(b, 0).start()

        def part_two(n):
            b = n - 2 * NB
            step(n)

            @pl.when(away)
            def _():
                c_dy(b).start()

            @pl.when(home)
            def _():
                @pl.when(lax.rem(b, G) == 0)
                def _():
                    c_gy(b, n=G).wait_recv()
                add_into(other + PIECE, b, rgy)
                send_on(c_fx, b)
        loop(2 * NB, 3 * NB, part_two)

        @pl.when(home)
        def _():
            loop(E, NB, lambda b: c_fx(b, 1).start())

        def part_three(n):
            b = n - 3 * NB
            step(n)

            @pl.when(away)
            def _():
                @pl.when(lax.rem(b, G) == 0)
                def _():
                    c_a(b, n=G).wait_recv()
                add_into(same, b, ra)
                send_on(c_fy, b)
        loop(3 * NB, 4 * NB, part_three)

        @pl.when(away)
        def _away():
            loop(E, NB, lambda b: c_fy(b, 1).start())

            @pl.when(k == 0)
            def _():
                x0_copy(mine, 0, None, X0C).wait_send()
                v_copy(row).wait_send()
                d_copy(row).wait_send()
                s0_copy(row).wait_send()

            @pl.when(more)
            def _():
                signal(cr_2, mate)
                signal(cr_2, xn)
            c_a(0, n=NB).wait_send()
            c_gy(0, n=NB).wait_send()
            c_dy(0, NB).wait_send()

            @pl.when(more)
            def _():
                x_bytes(2 * PIECE - G * BR, 0).wait_recv()

        @pl.when(home)
        def _home():
            @pl.when(more)
            def _():
                signal(cr_0, yn)

            @pl.when(k == 0)
            def _():
                spread(1 - row)
                x0_copy(mine, 0, None, X0C).wait_send()
                v_copy(1 - row).wait_recv()
                v_in.wait()

            @pl.when(k > 0)
            def _():
                x_bytes(2 * PIECE, 0).wait_send()

            s_bytes(par).wait_recv()
            s_bytes(par).wait_send()
            mass = ((sbuf[par, 0] + sbuf[par, 1]) + (sbuf[par, 2] + sbuf[par, 3])) / VERTS
            coef[...] = jnp.broadcast_to(DAMPING * mass + (1.0 - DAMPING), (8, VECS))

            @pl.when(more)
            def _():
                pl.semaphore_wait(cr_2, 1)

            c_a(0, n=NB).wait_send()
            for b in range(0, NB, G):
                c_a(b, n=G).wait_recv()
            c_dy(0, NB).wait_recv()
            sacc[...] = lax.fori_loop(0, E, lambda b, acc: finish(b, None, last, acc), jnp.zeros((8, VECS), jnp.float32))

            @pl.when(more)
            def _():
                signal(cr_0, xn)
            finish_half(0, last)

        return carry

    lax.fori_loop(0, SWEEPS, sweep, 0)

    @pl.when(home)
    def _():
        finish_half(1, jnp.bool_(True))
    drain_forward()

    @pl.when(home)
    def _():
        o_remote(1 - row, 0, n=NB).wait_send()

    @pl.when(away)
    def _():
        o_remote(1 - row, 0, n=NB).wait_recv()


def solution(mesh):
    dma = pltpu.SemaphoreType.DMA
    reg = pltpu.SemaphoreType.REGULAR

    def in_hbm(a):
        return pltpu.with_memory_space_constraint(a, pltpu.HBM)

    def local_sweeps(mat_tile, x_piece, tele_piece, dang_piece):
        part = pltpu.VMEM((PIECE, VECS), jnp.float32)
        return pl.pallas_call(
            kernel,
            name="sweeps",
            out_shape=jax.ShapeDtypeStruct((PIECE, VECS), jnp.float32),
            in_specs=[pl.BlockSpec(memory_space=pltpu.HBM)] * 4,
            out_specs=pl.BlockSpec(memory_space=pltpu.VMEM),
            scratch_shapes=[
                pltpu.VMEM((RING, BR, COLS), jnp.bfloat16),
                pltpu.VMEM((COLS, VECS), jnp.bfloat16),
                pltpu.VMEM((ROWS, VECS), jnp.float32),
                part, part, part, part, part,
                pltpu.VMEM((COLS, VECS), jnp.float32),
                pltpu.VMEM((COLS, 128), jnp.bfloat16),
                pltpu.VMEM((2, PIECE // 128, 128), jnp.int32),
                pltpu.VMEM((2, 4, 1, VECS), jnp.float32),
                pltpu.VMEM((2, 8, VECS), jnp.float32),
                pltpu.VMEM((8, VECS), jnp.float32),
                pltpu.VMEM((8, VECS), jnp.float32),
                dma((RING,)), dma((X0C,)), dma, dma((2,)),
                dma, dma((NB // G,)), dma, dma((NB // G,)), dma, dma, dma, dma((E // G + 4,)), dma, dma((E // G + 4,)),
                dma, dma((2,)), dma, dma((2,)), dma, dma, reg, reg, reg,
            ],
            compiler_params=pltpu.CompilerParams(
                collective_id=0, has_side_effects=True, vmem_limit_bytes=53_300_000),
            cost_estimate=pl.CostEstimate(
                flops=2 * ROWS * COLS * VECS * SWEEPS, bytes_accessed=2 * ROWS * COLS * SWEEPS, transcendentals=0),
        )(mat_tile, x_piece, tele_piece, in_hbm(dang_piece.reshape(PIECE // 128, 128)))

    vec_spec = P(('col', 'row'), None)
    return jax.shard_map(local_sweeps, mesh=mesh,
                         in_specs=(P('row', 'col'), vec_spec, vec_spec, P(('col', 'row'))),
                         out_specs=vec_spec, check_vma=False)
```

```python
import jax
import jax.numpy as jnp
from jax import lax
from jax.experimental import pallas as pl
from jax.experimental.pallas import tpu as pltpu
from jax.sharding import PartitionSpec as P

SWEEPS = 8
DAMPING = 0.85
MESH = pl.DeviceIdType.MESH

VERTS = 24576
VECS = 256
HALF = 128
PIECE = 3072
ROWS = 12288
COLS = 6144
BR = 256
NB = PIECE // BR
G = 4
E = NB - G
CH = 32
RING = 4
X0C = 4
X0R = PIECE // X0C


def kernel(a_hbm, x_hbm, v_hbm, d_hbm, out,
           abuf, xbf, ybuf, ra, rgy, rdy, rfx, rfy, vbuf, dbuf, dint, sbuf, s0buf, coef, sacc,
           a_sem, in_sem, x0_s, x0_r,
           a_s, a_r, gy_s, gy_r, dy_s, dy_r, fx_s, fx_r, fy_s, fy_r,
           x_s, x_r, s_s, s_r, o_s, o_r, held_r, cr_0, cr_1, cr_2):
    col = lax.axis_index('col')
    row = lax.axis_index('row')
    cx, cy = lax.rem(col, 2), lax.div(col, 2)
    home = row == cy
    away = jnp.logical_not(home)
    xn = (cy * 2 + 1 - cx, row)
    yn = ((1 - cy) * 2 + cx, row)
    mate = (col, 1 - row)
    same = cx * COLS
    other = (1 - cx) * COLS
    mine = row * PIECE
    far = (1 - row) * PIECE

    def rows_of(start, size):
        return pl.ds(pl.multiple_of(start, size), size)

    def blocks(start, b, n):
        return pl.ds(pl.multiple_of(start + b * BR, BR), n * BR)

    def cols(h):
        return pl.ds(0, VECS) if h is None else pl.ds(h * HALF, HALF)

    def remote(src, dst, send, recv, dev):
        return pltpu.make_async_remote_copy(
            src_ref=src, dst_ref=dst, send_sem=send, recv_sem=recv, device_id=dev, device_id_type=MESH)

    def loop(lo, hi, body):
        def step(i, c):
            body(i)
            return c
        lax.fori_loop(lo, hi, step, 0)

    def signal(sem, dev):
        pl.semaphore_signal(sem, inc=1, device_id=dev, device_id_type=MESH)

    def x_in(c):
        return pltpu.make_async_copy(x_hbm.at[rows_of(c * X0R, X0R)], vbuf.at[rows_of(mine + c * X0R, X0R)], in_sem.at[c])

    for c in range(X0C):
        x_in(c).start()

    barrier = pltpu.get_barrier_semaphore()
    for off in range(4):
        for r in range(2):
            if off == 0 and r == 1:
                continue
            signal(barrier, (lax.rem(col + off, 4), row if r == 0 and off else 1 - row))

    def flow(start, b, n, h, dst, send, recv, i, dev):
        return remote(ybuf.at[blocks(start, b, n), cols(h)], dst.at[blocks(0, b, n), cols(h)], send, recv.at[i], dev)

    def c_a(b, h=None, n=1):
        return flow(other, b, n, h, ra, a_s, a_r, lax.div(b, G), xn)

    def c_gy(b, h=None, n=1):
        return flow(other + PIECE, b, n, h, rgy, gy_s, gy_r, lax.div(b, G), yn)

    def c_dy(b, n=1):
        return remote(ybuf.at[blocks(same + PIECE, b, n)], rdy.at[blocks(0, b, n)], dy_s, dy_r, yn)

    def held_a():
        return remote(ybuf.at[blocks(other, NB - 1, 1)], ra.at[blocks(0, NB - 1, 1)], a_s, held_r, xn)

    def held_dy():
        return remote(ybuf.at[blocks(same + PIECE, NB - 1, 1)], rdy.at[blocks(0, NB - 1, 1)], dy_s, held_r, yn)

    def late(b, h):
        return lax.div(b, G) if h is None else E // G + 2 * h + jnp.where(b == NB - 1, 1, 0)

    def c_fx(b, h=None, n=1):
        return flow(other + PIECE, b, n, h, rfx, fx_s, fx_r, late(b, h), xn)

    def c_fy(b, h=None, n=1):
        return flow(same, b, n, h, rfy, fy_s, fy_r, late(b, h), yn)

    def arrived(copy, b, h):
        if h is None:
            @pl.when(lax.rem(b, G) == 0)
            def _():
                copy(b, n=G).wait_recv()
        else:
            @pl.when(b == E)
            def _():
                copy(b, h, n=G - 1).wait_recv()

            @pl.when(b == NB - 1)
            def _():
                copy(b, h).wait_recv()

    def c_x(t, b, h=None):
        at = blocks(t * PIECE, b, 1)
        return remote(xbf.at[at, cols(h)], xbf.at[at, cols(h)], x_s, x_r.at[1 if h == 1 else 0], mate)

    def x_bytes(rows, i):
        return remote(xbf.at[pl.ds(0, rows)], xbf.at[pl.ds(0, rows)], x_s, x_r.at[i], mate)

    def block_of(n):
        m = n - G
        pair = m < 2 * E
        t0 = jnp.where(pair, lax.rem(m, 2), 1)
        b0 = jnp.where(pair, jnp.where(t0 == 0, G, 0) + lax.div(m, 2), m - E)
        b0 = jnp.where(m < 0, n, b0)
        t0 = jnp.where(jnp.logical_xor(home, jnp.logical_or(m < 0, t0 == 0)), 1, 0)
        m = n - 2 * NB
        first = n < 2 * NB
        t = jnp.where(first, t0, 1 - lax.div(m, NB))
        b = jnp.where(first, b0, lax.rem(m, NB))
        return jnp.where(first, other, same) + t * PIECE + b * BR

    def a_copy(n):
        slot = lax.rem(n, RING)
        return pltpu.make_async_copy(a_hbm.at[rows_of(block_of(n), BR)], abuf.at[slot], a_sem.at[slot])

    d_in = pltpu.make_async_copy(d_hbm, dint.at[row], in_sem.at[0])
    v_in = pltpu.make_async_copy(v_hbm, vbuf.at[rows_of(mine, PIECE)], in_sem.at[1])

    def v_copy(r):
        return remote(v_hbm, vbuf.at[rows_of(r * PIECE, PIECE)], fx_s, x_r.at[0], mate)

    def d_copy(r):
        return remote(d_hbm, dint.at[r], x_s, x_r.at[1], mate)

    def s0_copy(r):
        return remote(s0buf.at[r], s0buf.at[r], o_s, o_r, mate)

    def x0_copy(start, c, h, n=1):
        at = pl.ds(pl.multiple_of(start + c * X0R, X0R), n * X0R)
        return remote(xbf.at[at, cols(h)], xbf.at[at, cols(h)], x0_s, x0_r.at[1 if h == 1 else 0], mate)

    for c in range(X0C):
        x_in(c).wait()

        def convert(i, c=c):
            at = rows_of(mine + c * X0R + i * CH, CH)
            xbf[at, :] = vbuf[at, :].astype(jnp.bfloat16)
        loop(0, X0R // CH, convert)
        if c == 0:
            pl.semaphore_wait(barrier, 7)
        x0_copy(mine, c, 0).start()
        if c < RING:
            a_copy(jnp.int32(c)).start()
    for c in range(X0C):
        x0_copy(mine, c, 1).start()
    d_in.start()

    @pl.when(away)
    def _():
        d_copy(row).start()
        v_copy(row).start()

    def s_copy(par, off):
        dst_col = lax.rem(col + off, 4)
        return remote(sbuf.at[par, col], sbuf.at[par, col], s_s, s_r.at[par], (dst_col, lax.div(dst_col, 2)))

    def s_bytes(par):
        return remote(sbuf.at[par, pl.ds(0, 3)], sbuf.at[par, pl.ds(0, 3)], s_s, s_r.at[par], mate)

    def s_publish(par, value):
        sbuf[par, col] = jnp.sum(value, axis=0, keepdims=True)
        for off in range(1, 4):
            s_copy(par, off).start()

    def spread(r):
        def group(g):
            flags = dint[r, pl.ds(g, 1), :].astype(jnp.float32)
            dbuf[rows_of(r * PIECE + g * 128, 128), :] = jnp.broadcast_to(flags, (128, 128)).T.astype(jnp.bfloat16)
        loop(0, PIECE // 128, group)

    def flags(start, h):
        d = dbuf[rows_of(start, CH), :].astype(jnp.float32)
        return d if h is not None else jnp.concatenate([d, d], axis=1)

    def fold(w):
        return jnp.sum(w.reshape(CH // 8, 8, w.shape[1]), axis=0)

    def first_mass():
        d_in.wait()
        spread(row)

        def add(c, acc):
            at = mine + c * CH
            return acc + fold(vbuf[rows_of(at, CH), :] * flags(at, None))
        s0buf[row] = lax.fori_loop(0, PIECE // CH, add, jnp.zeros((8, VECS), jnp.float32))

    def update(t, b, h, one, two, acc):
        def step(c, acc):
            at = rows_of(same + t * PIECE + b * BR + c * CH, CH)
            own = rows_of(t * PIECE + b * BR + c * CH, CH)
            there = rows_of(b * BR + c * CH, CH)
            y = (ybuf[at, cols(h)] + one[there, cols(h)]) + two[there, cols(h)]
            cf = jnp.concatenate([coef[:, cols(h)]] * (CH // 8), axis=0)
            x = DAMPING * y + cf * vbuf[own, cols(h)]
            xbf[own, cols(h)] = x.astype(jnp.bfloat16)
            ybuf[at, cols(h)] = x
            return acc + fold(x * flags(t * PIECE + b * BR + c * CH, h))
        return lax.fori_loop(0, BR // CH, step, acc)

    def keep(t, b, h):
        def step(c):
            there = rows_of(b * BR + c * CH, CH)
            out[there, cols(h)] = ybuf[rows_of(same + t * PIECE + b * BR + c * CH, CH), cols(h)]
        loop(0, BR // CH, step)

    def o_remote(t, b, h=None, n=1):
        return remote(ybuf.at[blocks(same + t * PIECE, b, n), cols(h)], out.at[blocks(0, b, n), cols(h)], o_s, o_r, mate)

    def emit(t, b, h, last):
        @pl.when(jnp.logical_not(last))
        def _():
            c_x(t, b, h).start()

        @pl.when(jnp.logical_and(last, row == t))
        def _():
            keep(t, b, h)

        @pl.when(jnp.logical_and(last, row != t))
        def _():
            o_remote(t, b, h).start()

    def finish(b, h, last, acc):
        arrived(c_fy, b, h)
        acc = update(0, b, h, ra, rfy, acc)
        emit(0, b, h, last)
        arrived(c_fx, b, h)
        acc = update(1, b, h, rdy, rfx, acc)
        emit(1, b, h, last)
        return acc

    def finish_half(h, last):
        part = lax.fori_loop(E, NB, lambda b, acc: finish(b, h, last, acc), jnp.zeros((8, HALF), jnp.float32))
        sacc[:, cols(h)] = sacc[:, cols(h)] + part

    def finish_last():
        def piece(t, b, h):
            arrived(c_fy if t == 0 else c_fx, b, h)
            result(t, b, h)

        def result(t, b, h):
            update(t, b, h, ra if t == 0 else rdy, rfy if t == 0 else rfx, jnp.zeros((8, HALF), jnp.float32))
            emit(t, b, h, jnp.bool_(True))

        for kept in range(2):
            @pl.when(row == kept)
            def _():
                end = jnp.int32(NB - 1)
                for h in range(2):
                    def both(b):
                        piece(1 - kept, b, h)
                        piece(kept, b, h)
                    loop(E, NB - 1, both)
                    piece(1 - kept, end, h)
                for h in range(2):
                    arrived(c_fy if kept == 0 else c_fx, end, h)
                (held_a() if kept == 0 else held_dy()).wait_recv()
                for h in range(2):
                    result(kept, end, h)

    def drain_forward():
        @pl.when(home)
        def _():
            c_fx(0, n=NB).wait_send()

        @pl.when(away)
        def _():
            c_fy(0, n=NB).wait_send()

    def sweep(k, carry):
        last = k == SWEEPS - 1
        more = jnp.logical_not(last)
        par = lax.rem(k, 2)
        hold_a = jnp.logical_and(jnp.logical_and(last, home), row == 0)
        hold_dy = jnp.logical_and(last, row == 1)

        def multiply(n, h):
            start = block_of(n)
            ybuf[rows_of(start, BR), cols(h)] = jnp.dot(
                abuf[lax.rem(n, RING)], xbf[:, cols(h)], preferred_element_type=jnp.float32)

        def fetch(n):
            @pl.when(jnp.logical_not(jnp.logical_and(last, n >= 4 * NB)))
            def _():
                a_copy(lax.rem(n, 4 * NB)).start()

        def lead(h):
            def one(n):
                if h == 0:
                    a_copy(n).wait()
                multiply(n, h)
                if h == 1:
                    fetch(n + RING)

                @pl.when(home)
                def _():
                    c_a(n, h).start()

                @pl.when(away)
                def _():
                    c_gy(n, h).start()
            loop(0, G, one)

        @pl.when(k == 0)
        def _():
            x0_copy(far, 0, 0, X0C).wait_recv()

        @pl.when(k > 0)
        def _():
            pl.semaphore_wait(cr_0, 1)
        lead(0)

        @pl.when(k == 0)
        def _():
            x0_copy(far, 0, 1, X0C).wait_recv()

        @pl.when(jnp.logical_and(k > 0, home))
        def _():
            finish_half(1, jnp.bool_(False))
            s_publish(par, sacc[...])
            signal(cr_1, xn)
            signal(cr_1, yn)

        @pl.when(jnp.logical_and(k > 0, away))
        def _():
            x_bytes(G * BR, 1).wait_recv()
        lead(1)

        @pl.when(k > 0)
        def _():
            drain_forward()
            pl.semaphore_wait(cr_1, 1)

            @pl.when(away)
            def _():
                pl.semaphore_wait(cr_2, 1)

        def step(n):
            a_copy(n).wait()
            multiply(n, None)
            fetch(n + RING)
            at = block_of(n) - jnp.where(n < 2 * NB, other, same)
            return lax.div(at, PIECE), lax.div(lax.rem(at, PIECE), BR)

        def part_one(n):
            t, b = step(n)

            @pl.when(jnp.logical_and(t == 0, jnp.logical_not(jnp.logical_and(hold_a, b == NB - 1))))
            def _():
                c_a(b).start()

            @pl.when(jnp.logical_and(t == 1, away))
            def _():
                c_gy(b).start()
        loop(G, 2 * NB, part_one)

        @pl.when(k == 0)
        def _():
            first_mass()

            @pl.when(away)
            def _():
                s0_copy(row).start()

            @pl.when(home)
            def _():
                v_in.start()
                d_copy(1 - row).wait_recv()
                s0_copy(1 - row).wait_recv()
                s_publish(0, s0buf[0] + s0buf[1])

        def add_into(start, b, src):
            def add(c):
                at = rows_of(start + b * BR + c * CH, CH)
                ybuf[at, :] = ybuf[at, :] + src[rows_of(b * BR + c * CH, CH), :]
            loop(0, BR // CH, add)

        def send_on(copy, b):
            @pl.when(b < E)
            def _():
                copy(b).start()

            @pl.when(b >= E)
            def _():
                copy(b, 0).start()

        def part_two(n):
            b = n - 2 * NB
            step(n)

            @pl.when(jnp.logical_and(away, jnp.logical_not(jnp.logical_and(hold_dy, b == NB - 1))))
            def _():
                c_dy(b).start()

            @pl.when(home)
            def _():
                @pl.when(lax.rem(b, G) == 0)
                def _():
                    c_gy(b, n=G).wait_recv()
                add_into(other + PIECE, b, rgy)
                send_on(c_fx, b)
        loop(2 * NB, 3 * NB, part_two)

        @pl.when(home)
        def _():
            loop(E, NB, lambda b: c_fx(b, 1).start())

            @pl.when(hold_a)
            def _():
                held_a().start()

        def part_three(n):
            b = n - 3 * NB
            step(n)

            @pl.when(away)
            def _():
                @pl.when(lax.rem(b, G) == 0)
                def _():
                    c_a(b, n=G).wait_recv()
                add_into(same, b, ra)
                send_on(c_fy, b)
        loop(3 * NB, 4 * NB, part_three)

        @pl.when(away)
        def _away():
            loop(E, NB, lambda b: c_fy(b, 1).start())

            @pl.when(hold_dy)
            def _():
                held_dy().start()

            @pl.when(k == 0)
            def _():
                x0_copy(mine, 0, None, X0C).wait_send()
                v_copy(row).wait_send()
                d_copy(row).wait_send()
                s0_copy(row).wait_send()

            @pl.when(more)
            def _():
                signal(cr_2, mate)
                signal(cr_2, xn)
            c_a(0, n=NB).wait_send()
            c_gy(0, n=NB).wait_send()
            c_dy(0, NB).wait_send()

            @pl.when(more)
            def _():
                x_bytes(2 * PIECE - G * BR, 0).wait_recv()

        @pl.when(home)
        def _home():
            @pl.when(more)
            def _():
                signal(cr_0, yn)

            @pl.when(k == 0)
            def _():
                spread(1 - row)
                x0_copy(mine, 0, None, X0C).wait_send()
                v_copy(1 - row).wait_recv()
                v_in.wait()

            @pl.when(k > 0)
            def _():
                x_bytes(2 * PIECE, 0).wait_send()

            s_bytes(par).wait_recv()
            s_bytes(par).wait_send()
            mass = ((sbuf[par, 0] + sbuf[par, 1]) + (sbuf[par, 2] + sbuf[par, 3])) / VERTS
            coef[...] = jnp.broadcast_to(DAMPING * mass + (1.0 - DAMPING), (8, VECS))

            @pl.when(more)
            def _():
                pl.semaphore_wait(cr_2, 1)

            @pl.when(more)
            def _():
                c_a(0, n=NB).wait_send()
            for b in range(0, E, G):
                c_a(b, n=G).wait_recv()

            @pl.when(hold_a)
            def _():
                c_a(E, n=G - 1).wait_recv()

            @pl.when(jnp.logical_not(hold_a))
            def _():
                c_a(E, n=G).wait_recv()

            @pl.when(hold_dy)
            def _():
                c_dy(0, NB - 1).wait_recv()

            @pl.when(jnp.logical_not(hold_dy))
            def _():
                c_dy(0, NB).wait_recv()
            sacc[...] = lax.fori_loop(0, E, lambda b, acc: finish(b, None, last, acc), jnp.zeros((8, VECS), jnp.float32))

            @pl.when(more)
            def _():
                signal(cr_0, xn)
                finish_half(0, jnp.bool_(False))

            @pl.when(last)
            def _():
                finish_last()

        return carry

    lax.fori_loop(0, SWEEPS, sweep, 0)

    drain_forward()

    @pl.when(home)
    def _():
        c_a(0, n=NB).wait_send()
        o_remote(1 - row, 0, n=NB).wait_send()

    @pl.when(away)
    def _():
        o_remote(1 - row, 0, n=NB).wait_recv()


def solution(mesh):
    dma = pltpu.SemaphoreType.DMA
    reg = pltpu.SemaphoreType.REGULAR

    def in_hbm(a):
        return pltpu.with_memory_space_constraint(a, pltpu.HBM)

    def local_sweeps(mat_tile, x_piece, tele_piece, dang_piece):
        part = pltpu.VMEM((PIECE, VECS), jnp.float32)
        return pl.pallas_call(
            kernel,
            name="sweeps",
            out_shape=jax.ShapeDtypeStruct((PIECE, VECS), jnp.float32),
            in_specs=[pl.BlockSpec(memory_space=pltpu.HBM)] * 4,
            out_specs=pl.BlockSpec(memory_space=pltpu.VMEM),
            scratch_shapes=[
                pltpu.VMEM((RING, BR, COLS), jnp.bfloat16),
                pltpu.VMEM((COLS, VECS), jnp.bfloat16),
                pltpu.VMEM((ROWS, VECS), jnp.float32),
                part, part, part, part, part,
                pltpu.VMEM((COLS, VECS), jnp.float32),
                pltpu.VMEM((COLS, 128), jnp.bfloat16),
                pltpu.VMEM((2, PIECE // 128, 128), jnp.int32),
                pltpu.VMEM((2, 4, 1, VECS), jnp.float32),
                pltpu.VMEM((2, 8, VECS), jnp.float32),
                pltpu.VMEM((8, VECS), jnp.float32),
                pltpu.VMEM((8, VECS), jnp.float32),
                dma((RING,)), dma((X0C,)), dma, dma((2,)),
                dma, dma((NB // G,)), dma, dma((NB // G,)), dma, dma, dma, dma((E // G + 4,)), dma, dma((E // G + 4,)),
                dma, dma((2,)), dma, dma((2,)), dma, dma, dma, reg, reg, reg,
            ],
            compiler_params=pltpu.CompilerParams(
                collective_id=0, has_side_effects=True, vmem_limit_bytes=53_300_000),
            cost_estimate=pl.CostEstimate(
                flops=2 * ROWS * COLS * VECS * SWEEPS, bytes_accessed=2 * ROWS * COLS * SWEEPS, transcendentals=0),
        )(mat_tile, x_piece, tele_piece, in_hbm(dang_piece.reshape(PIECE // 128, 128)))

    vec_spec = P(('col', 'row'), None)
    return jax.shard_map(local_sweeps, mesh=mesh,
                         in_specs=(P('row', 'col'), vec_spec, vec_spec, P(('col', 'row'))),
                         out_specs=vec_spec, check_vma=False)
```

```python
import jax
import jax.numpy as jnp
from jax import lax
from jax.experimental import pallas as pl
from jax.experimental.pallas import tpu as pltpu
from jax.sharding import PartitionSpec as P

SWEEPS = 8
DAMPING = 0.85
MESH = pl.DeviceIdType.MESH

VERTS = 24576
VECS = 256
HALF = 128
PIECE = 3072
ROWS = 12288
COLS = 6144
BR = 256
NB = PIECE // BR
G = 4
E = NB - G
CH = 32
RING = 4
X0C = 3
X0R = PIECE // X0C


def kernel(a_hbm, x_hbm, v_hbm, d_hbm, out,
           abuf, xbf, ybuf, ra, rgy, rdy, rfx, rfy, vbuf, dbuf, dint, sbuf, s0buf, coef, sacc,
           a_sem, in_sem, x0_s, x0_r,
           a_s, a_r, gy_s, gy_r, dy_s, dy_r, fx_s, fx_r, fy_s, fy_r,
           x_s, x_r, s_s, s_r, o_s, o_r, held_r, cr_0, cr_1, cr_2):
    col = lax.axis_index('col')
    row = lax.axis_index('row')
    cx, cy = lax.rem(col, 2), lax.div(col, 2)
    home = row == cy
    away = jnp.logical_not(home)
    xn = (cy * 2 + 1 - cx, row)
    yn = ((1 - cy) * 2 + cx, row)
    mate = (col, 1 - row)
    same = cx * COLS
    other = (1 - cx) * COLS
    mine = row * PIECE
    far = (1 - row) * PIECE

    def rows_of(start, size):
        return pl.ds(pl.multiple_of(start, size), size)

    def blocks(start, b, n):
        return pl.ds(pl.multiple_of(start + b * BR, BR), n * BR)

    def cols(h):
        return pl.ds(0, VECS) if h is None else pl.ds(h * HALF, HALF)

    def remote(src, dst, send, recv, dev):
        return pltpu.make_async_remote_copy(
            src_ref=src, dst_ref=dst, send_sem=send, recv_sem=recv, device_id=dev, device_id_type=MESH)

    def loop(lo, hi, body):
        def step(i, c):
            body(i)
            return c
        lax.fori_loop(lo, hi, step, 0)

    def signal(sem, dev):
        pl.semaphore_signal(sem, inc=1, device_id=dev, device_id_type=MESH)

    def x_in(c, h):
        return pltpu.make_async_copy(x_hbm.at[rows_of(c * X0R, X0R), cols(h)], vbuf.at[rows_of(mine + c * X0R, X0R), cols(h)],
                                     in_sem.at[h * X0C + c])

    for c in range(X0C):
        x_in(c, 0).start()

    barrier = pltpu.get_barrier_semaphore()
    for off in range(4):
        for r in range(2):
            if off == 0 and r == 1:
                continue
            signal(barrier, (lax.rem(col + off, 4), row if r == 0 and off else 1 - row))

    def flow(start, b, n, h, dst, send, recv, i, dev):
        return remote(ybuf.at[blocks(start, b, n), cols(h)], dst.at[blocks(0, b, n), cols(h)], send, recv.at[i], dev)

    def c_a(b, h=None, n=1):
        return flow(other, b, n, h, ra, a_s, a_r, lax.div(b, G), xn)

    def c_gy(b, h=None, n=1):
        return flow(other + PIECE, b, n, h, rgy, gy_s, gy_r, lax.div(b, G), yn)

    def c_dy(b, n=1):
        return remote(ybuf.at[blocks(same + PIECE, b, n)], rdy.at[blocks(0, b, n)], dy_s, dy_r, yn)

    def held_a():
        return remote(ybuf.at[blocks(other, NB - 1, 1)], ra.at[blocks(0, NB - 1, 1)], a_s, held_r, xn)

    def held_dy():
        return remote(ybuf.at[blocks(same + PIECE, NB - 1, 1)], rdy.at[blocks(0, NB - 1, 1)], dy_s, held_r, yn)

    def late(b, h):
        return lax.div(b, G) if h is None else E // G + 2 * h + jnp.where(b == NB - 1, 1, 0)

    def c_fx(b, h=None, n=1):
        return flow(other + PIECE, b, n, h, rfx, fx_s, fx_r, late(b, h), xn)

    def c_fy(b, h=None, n=1):
        return flow(same, b, n, h, rfy, fy_s, fy_r, late(b, h), yn)

    def arrived(copy, b, h):
        if h is None:
            @pl.when(lax.rem(b, G) == 0)
            def _():
                copy(b, n=G).wait_recv()
        else:
            @pl.when(b == E)
            def _():
                copy(b, h, n=G - 1).wait_recv()

            @pl.when(b == NB - 1)
            def _():
                copy(b, h).wait_recv()

    def c_x(t, b, h=None):
        at = blocks(t * PIECE, b, 1)
        return remote(xbf.at[at, cols(h)], xbf.at[at, cols(h)], x_s, x_r.at[1 if h == 1 else 0], mate)

    def x_bytes(rows, i):
        return remote(xbf.at[pl.ds(0, rows)], xbf.at[pl.ds(0, rows)], x_s, x_r.at[i], mate)

    def block_of(n):
        m = n - G
        pair = m < 2 * E
        t0 = jnp.where(pair, lax.rem(m, 2), 1)
        b0 = jnp.where(pair, jnp.where(t0 == 0, G, 0) + lax.div(m, 2), m - E)
        b0 = jnp.where(m < 0, n, b0)
        t0 = jnp.where(jnp.logical_xor(home, jnp.logical_or(m < 0, t0 == 0)), 1, 0)
        m = n - 2 * NB
        first = n < 2 * NB
        t = jnp.where(first, t0, 1 - lax.div(m, NB))
        b = jnp.where(first, b0, lax.rem(m, NB))
        return jnp.where(first, other, same) + t * PIECE + b * BR

    def a_copy(n):
        slot = lax.rem(n, RING)
        return pltpu.make_async_copy(a_hbm.at[rows_of(block_of(n), BR)], abuf.at[slot], a_sem.at[slot])

    d_in = pltpu.make_async_copy(d_hbm, dint.at[row], in_sem.at[0])
    v_in = pltpu.make_async_copy(v_hbm, vbuf.at[rows_of(mine, PIECE)], in_sem.at[1])

    def v_copy(r):
        return remote(v_hbm, vbuf.at[rows_of(r * PIECE, PIECE)], fx_s, x_r.at[0], mate)

    def d_copy(r):
        return remote(d_hbm, dint.at[r], x_s, x_r.at[1], mate)

    def s0_copy(r):
        return remote(s0buf.at[r], s0buf.at[r], o_s, o_r, mate)

    def x0_copy(start, c, h, n=1):
        at = pl.ds(pl.multiple_of(start + c * X0R, X0R), n * X0R)
        return remote(xbf.at[at, cols(h)], xbf.at[at, cols(h)], x0_s, x0_r.at[1 if h == 1 else 0], mate)

    a_copy(jnp.int32(0)).start()
    for c in range(X0C):
        x_in(c, 1).start()
    for n in range(1, RING):
        a_copy(jnp.int32(n)).start()

    def take_x(h):
        for c in range(X0C):
            x_in(c, h).wait()

            def convert(i, c=c):
                at = rows_of(mine + c * X0R + i * CH, CH)
                xbf[at, cols(h)] = vbuf[at, cols(h)].astype(jnp.bfloat16)
            loop(0, X0R // CH, convert)
            if c == 0 and h == 0:
                pl.semaphore_wait(barrier, 7)
            x0_copy(mine, c, h).start()

    def half_product(start):
        at = rows_of(start, PIECE)
        return jnp.dot(abuf[0, :, at], xbf[at, cols(0)], preferred_element_type=jnp.float32)

    take_x(0)
    a_copy(jnp.int32(0)).wait()
    first = rows_of(block_of(jnp.int32(0)), BR)
    ybuf[first, cols(0)] = half_product(mine)
    take_x(1)
    x0_copy(far, 0, 0, X0C).wait_recv()
    ybuf[first, cols(0)] = ybuf[first, cols(0)] + half_product(far)

    @pl.when(home)
    def _():
        c_a(jnp.int32(0), 0).start()

    @pl.when(away)
    def _():
        c_gy(jnp.int32(0), 0).start()
    d_in.start()

    @pl.when(away)
    def _():
        d_copy(row).start()
        v_copy(row).start()

    def s_copy(par, off):
        dst_col = lax.rem(col + off, 4)
        return remote(sbuf.at[par, col], sbuf.at[par, col], s_s, s_r.at[par], (dst_col, lax.div(dst_col, 2)))

    def s_bytes(par):
        return remote(sbuf.at[par, pl.ds(0, 3)], sbuf.at[par, pl.ds(0, 3)], s_s, s_r.at[par], mate)

    def s_publish(par, value):
        sbuf[par, col] = jnp.sum(value, axis=0, keepdims=True)
        for off in range(1, 4):
            s_copy(par, off).start()

    def spread(r):
        def group(g):
            flags = dint[r, pl.ds(g, 1), :].astype(jnp.float32)
            dbuf[rows_of(r * PIECE + g * 128, 128), :] = jnp.broadcast_to(flags, (128, 128)).T.astype(jnp.bfloat16)
        loop(0, PIECE // 128, group)

    def flags(start, h):
        d = dbuf[rows_of(start, CH), :].astype(jnp.float32)
        return d if h is not None else jnp.concatenate([d, d], axis=1)

    def fold(w):
        return jnp.sum(w.reshape(CH // 8, 8, w.shape[1]), axis=0)

    def first_mass():
        d_in.wait()
        spread(row)

        def add(c, acc):
            at = mine + c * CH
            return acc + fold(vbuf[rows_of(at, CH), :] * flags(at, None))
        s0buf[row] = lax.fori_loop(0, PIECE // CH, add, jnp.zeros((8, VECS), jnp.float32))

    def new_x(at, own, there, h, one, two):
        y = (ybuf[rows_of(at, CH), cols(h)] + one[there, cols(h)]) + two[there, cols(h)]
        cf = jnp.concatenate([coef[:, cols(h)]] * (CH // 8), axis=0)
        return DAMPING * y + cf * vbuf[rows_of(own, CH), cols(h)]

    def update(t, b, h, one, two, acc):
        def step(c, acc):
            own = t * PIECE + b * BR + c * CH
            x = new_x(same + own, own, rows_of(b * BR + c * CH, CH), h, one, two)
            xbf[rows_of(own, CH), cols(h)] = x.astype(jnp.bfloat16)
            ybuf[rows_of(same + own, CH), cols(h)] = x
            return acc + fold(x * flags(own, h))
        return lax.fori_loop(0, BR // CH, step, acc)

    def keep(t, b, h):
        def step(c):
            there = rows_of(b * BR + c * CH, CH)
            out[there, cols(h)] = ybuf[rows_of(same + t * PIECE + b * BR + c * CH, CH), cols(h)]
        loop(0, BR // CH, step)

    def o_remote(t, b, h=None, n=1):
        return remote(ybuf.at[blocks(same + t * PIECE, b, n), cols(h)], out.at[blocks(0, b, n), cols(h)], o_s, o_r, mate)

    def emit(t, b, h, last):
        @pl.when(jnp.logical_not(last))
        def _():
            c_x(t, b, h).start()

        @pl.when(jnp.logical_and(last, row == t))
        def _():
            keep(t, b, h)

        @pl.when(jnp.logical_and(last, row != t))
        def _():
            o_remote(t, b, h).start()

    def finish(b, h, last, acc):
        arrived(c_fy, b, h)
        acc = update(0, b, h, ra, rfy, acc)
        emit(0, b, h, last)
        arrived(c_fx, b, h)
        acc = update(1, b, h, rdy, rfx, acc)
        emit(1, b, h, last)
        return acc

    def finish_half(h, last):
        part = lax.fori_loop(E, NB, lambda b, acc: finish(b, h, last, acc), jnp.zeros((8, HALF), jnp.float32))
        sacc[:, cols(h)] = sacc[:, cols(h)] + part

    def finish_last():
        def piece(t, b, h):
            arrived(c_fy if t == 0 else c_fx, b, h)
            result(t, b, h)

        def result(t, b, h):
            update(t, b, h, ra if t == 0 else rdy, rfy if t == 0 else rfx, jnp.zeros((8, HALF), jnp.float32))
            emit(t, b, h, jnp.bool_(True))

        for kept in range(2):
            @pl.when(row == kept)
            def _():
                end = jnp.int32(NB - 1)
                for h in range(2):
                    def both(b):
                        piece(1 - kept, b, h)
                        piece(kept, b, h)
                    loop(E, NB - 1, both)
                    piece(1 - kept, end, h)
                for h in range(2):
                    arrived(c_fy if kept == 0 else c_fx, end, h)
                (held_a() if kept == 0 else held_dy()).wait_recv()
                one, two = (ra, rfy) if kept == 0 else (rdy, rfx)

                def last_rows(c):
                    own = kept * PIECE + (NB - 1) * BR + c * CH
                    there = rows_of((NB - 1) * BR + c * CH, CH)
                    out[there, :] = new_x(same + own, own, there, None, one, two)
                loop(0, BR // CH, last_rows)

    def drain_forward():
        @pl.when(home)
        def _():
            c_fx(0, n=NB).wait_send()

        @pl.when(away)
        def _():
            c_fy(0, n=NB).wait_send()

    def sweep(k, carry):
        last = k == SWEEPS - 1
        more = jnp.logical_not(last)
        par = lax.rem(k, 2)
        hold_a = jnp.logical_and(jnp.logical_and(last, home), row == 0)
        hold_dy = jnp.logical_and(last, row == 1)

        def multiply(n, h):
            start = block_of(n)
            ybuf[rows_of(start, BR), cols(h)] = jnp.dot(
                abuf[lax.rem(n, RING)], xbf[:, cols(h)], preferred_element_type=jnp.float32)

        def fetch(n):
            @pl.when(jnp.logical_not(jnp.logical_and(last, n >= 4 * NB)))
            def _():
                a_copy(lax.rem(n, 4 * NB)).start()

        def lead(h):
            def block(n):
                if h == 0:
                    a_copy(n).wait()
                multiply(n, h)
                if h == 1:
                    fetch(n + RING)

                @pl.when(home)
                def _():
                    c_a(n, h).start()

                @pl.when(away)
                def _():
                    c_gy(n, h).start()

            def one(n):
                @pl.when(jnp.logical_or(k > 0, n > 0))
                def _():
                    block(n)
            loop(0, G, one if h == 0 else block)

        @pl.when(k > 0)
        def _():
            pl.semaphore_wait(cr_0, 1)
        lead(0)

        @pl.when(k == 0)
        def _():
            x0_copy(far, 0, 1, X0C).wait_recv()

        @pl.when(jnp.logical_and(k > 0, home))
        def _():
            finish_half(1, jnp.bool_(False))
            s_publish(par, sacc[...])
            signal(cr_1, xn)
            signal(cr_1, yn)

        @pl.when(jnp.logical_and(k > 0, away))
        def _():
            x_bytes(G * BR, 1).wait_recv()
        lead(1)

        @pl.when(k > 0)
        def _():
            drain_forward()
            pl.semaphore_wait(cr_1, 1)

            @pl.when(away)
            def _():
                pl.semaphore_wait(cr_2, 1)

        def step(n):
            a_copy(n).wait()
            multiply(n, None)
            fetch(n + RING)
            at = block_of(n) - jnp.where(n < 2 * NB, other, same)
            return lax.div(at, PIECE), lax.div(lax.rem(at, PIECE), BR)

        def part_one(n):
            t, b = step(n)

            @pl.when(jnp.logical_and(t == 0, jnp.logical_not(jnp.logical_and(hold_a, b == NB - 1))))
            def _():
                c_a(b).start()

            @pl.when(jnp.logical_and(t == 1, away))
            def _():
                c_gy(b).start()
        loop(G, 2 * NB, part_one)

        @pl.when(k == 0)
        def _():
            first_mass()

            @pl.when(away)
            def _():
                s0_copy(row).start()

            @pl.when(home)
            def _():
                v_in.start()
                d_copy(1 - row).wait_recv()
                s0_copy(1 - row).wait_recv()
                s_publish(0, s0buf[0] + s0buf[1])

        def add_into(start, b, src):
            def add(c):
                at = rows_of(start + b * BR + c * CH, CH)
                ybuf[at, :] = ybuf[at, :] + src[rows_of(b * BR + c * CH, CH), :]
            loop(0, BR // CH, add)

        def send_on(copy, b):
            @pl.when(b < E)
            def _():
                copy(b).start()

            @pl.when(b >= E)
            def _():
                copy(b, 0).start()

        def part_two(n):
            b = n - 2 * NB
            step(n)

            @pl.when(jnp.logical_and(away, jnp.logical_not(jnp.logical_and(hold_dy, b == NB - 1))))
            def _():
                c_dy(b).start()

            @pl.when(home)
            def _():
                @pl.when(lax.rem(b, G) == 0)
                def _():
                    c_gy(b, n=G).wait_recv()
                add_into(other + PIECE, b, rgy)
                send_on(c_fx, b)
        loop(2 * NB, 3 * NB, part_two)

        @pl.when(home)
        def _():
            loop(E, NB, lambda b: c_fx(b, 1).start())

            @pl.when(hold_a)
            def _():
                held_a().start()

        def part_three(n):
            b = n - 3 * NB
            step(n)

            @pl.when(away)
            def _():
                @pl.when(lax.rem(b, G) == 0)
                def _():
                    c_a(b, n=G).wait_recv()
                add_into(same, b, ra)
                send_on(c_fy, b)
        loop(3 * NB, 4 * NB, part_three)

        @pl.when(away)
        def _away():
            loop(E, NB, lambda b: c_fy(b, 1).start())

            @pl.when(hold_dy)
            def _():
                held_dy().start()

            @pl.when(k == 0)
            def _():
                x0_copy(mine, 0, None, X0C).wait_send()
                v_copy(row).wait_send()
                d_copy(row).wait_send()
                s0_copy(row).wait_send()

            @pl.when(more)
            def _():
                signal(cr_2, mate)
                signal(cr_2, xn)
            c_a(0, n=NB).wait_send()
            c_gy(0, n=NB).wait_send()
            c_dy(0, NB).wait_send()

            @pl.when(more)
            def _():
                x_bytes(2 * PIECE - G * BR, 0).wait_recv()

        @pl.when(home)
        def _home():
            @pl.when(more)
            def _():
                signal(cr_0, yn)

            @pl.when(k == 0)
            def _():
                spread(1 - row)
                x0_copy(mine, 0, None, X0C).wait_send()
                v_copy(1 - row).wait_recv()
                v_in.wait()

            @pl.when(k > 0)
            def _():
                x_bytes(2 * PIECE, 0).wait_send()

            s_bytes(par).wait_recv()
            s_bytes(par).wait_send()
            mass = ((sbuf[par, 0] + sbuf[par, 1]) + (sbuf[par, 2] + sbuf[par, 3])) / VERTS
            coef[...] = jnp.broadcast_to(DAMPING * mass + (1.0 - DAMPING), (8, VECS))

            @pl.when(more)
            def _():
                pl.semaphore_wait(cr_2, 1)

            @pl.when(more)
            def _():
                c_a(0, n=NB).wait_send()
            for b in range(0, E, G):
                c_a(b, n=G).wait_recv()

            @pl.when(hold_a)
            def _():
                c_a(E, n=G - 1).wait_recv()

            @pl.when(jnp.logical_not(hold_a))
            def _():
                c_a(E, n=G).wait_recv()

            @pl.when(hold_dy)
            def _():
                c_dy(0, NB - 1).wait_recv()

            @pl.when(jnp.logical_not(hold_dy))
            def _():
                c_dy(0, NB).wait_recv()
            sacc[...] = lax.fori_loop(0, E, lambda b, acc: finish(b, None, last, acc), jnp.zeros((8, VECS), jnp.float32))

            @pl.when(more)
            def _():
                signal(cr_0, xn)
                finish_half(0, jnp.bool_(False))

            @pl.when(last)
            def _():
                finish_last()

        return carry

    lax.fori_loop(0, SWEEPS, sweep, 0)

    drain_forward()

    @pl.when(home)
    def _():
        c_a(0, n=NB).wait_send()
        o_remote(1 - row, 0, n=NB).wait_send()

    @pl.when(away)
    def _():
        o_remote(1 - row, 0, n=NB).wait_recv()


def solution(mesh):
    dma = pltpu.SemaphoreType.DMA
    reg = pltpu.SemaphoreType.REGULAR

    def in_hbm(a):
        return pltpu.with_memory_space_constraint(a, pltpu.HBM)

    def local_sweeps(mat_tile, x_piece, tele_piece, dang_piece):
        part = pltpu.VMEM((PIECE, VECS), jnp.float32)
        return pl.pallas_call(
            kernel,
            name="sweeps",
            out_shape=jax.ShapeDtypeStruct((PIECE, VECS), jnp.float32),
            in_specs=[pl.BlockSpec(memory_space=pltpu.HBM)] * 4,
            out_specs=pl.BlockSpec(memory_space=pltpu.VMEM),
            scratch_shapes=[
                pltpu.VMEM((RING, BR, COLS), jnp.bfloat16),
                pltpu.VMEM((COLS, VECS), jnp.bfloat16),
                pltpu.VMEM((ROWS, VECS), jnp.float32),
                part, part, part, part, part,
                pltpu.VMEM((COLS, VECS), jnp.float32),
                pltpu.VMEM((COLS, 128), jnp.bfloat16),
                pltpu.VMEM((2, PIECE // 128, 128), jnp.int32),
                pltpu.VMEM((2, 4, 1, VECS), jnp.float32),
                pltpu.VMEM((2, 8, VECS), jnp.float32),
                pltpu.VMEM((8, VECS), jnp.float32),
                pltpu.VMEM((8, VECS), jnp.float32),
                dma((RING,)), dma((2 * X0C,)), dma, dma((2,)),
                dma, dma((NB // G,)), dma, dma((NB // G,)), dma, dma, dma, dma((E // G + 4,)), dma, dma((E // G + 4,)),
                dma, dma((2,)), dma, dma((2,)), dma, dma, dma, reg, reg, reg,
            ],
            compiler_params=pltpu.CompilerParams(
                collective_id=0, has_side_effects=True, vmem_limit_bytes=53_300_000),
            cost_estimate=pl.CostEstimate(
                flops=2 * ROWS * COLS * VECS * SWEEPS, bytes_accessed=2 * ROWS * COLS * SWEEPS, transcendentals=0),
        )(mat_tile, x_piece, tele_piece, in_hbm(dang_piece.reshape(PIECE // 128, 128)))

    vec_spec = P(('col', 'row'), None)
    return jax.shard_map(local_sweeps, mesh=mesh,
                         in_specs=(P('row', 'col'), vec_spec, vec_spec, P(('col', 'row'))),
                         out_specs=vec_spec, check_vma=False)
```

```python
import jax
import jax.numpy as jnp
from jax import lax
from jax.experimental import pallas as pl
from jax.experimental.pallas import tpu as pltpu
from jax.sharding import PartitionSpec as P

SWEEPS = 8
DAMPING = 0.85
MESH = pl.DeviceIdType.MESH

VERTS = 24576
VECS = 256
HALF = 128
PIECE = 3072
ROWS = 12288
COLS = 6144
BR = 256
NB = PIECE // BR
G = 4
E = NB - G
CH = 32
RING = 4
X0C = 3
X0R = PIECE // X0C


def kernel(a_hbm, x_hbm, v_hbm, d_hbm, out,
           abuf, xbf, ybuf, ra, rgy, rdy, rfx, rfy, vbuf, dbuf, dint, sbuf, s0buf, coef, sacc,
           a_sem, in_sem, x0_s, x0_r,
           a_s, a_r, gy_s, gy_r, dy_s, dy_r, fx_s, fx_r, fy_s, fy_r,
           x_s, x_r, s_s, s_r, o_s, o_r, held_r, cr_0, cr_1, cr_2):
    col = lax.axis_index('col')
    row = lax.axis_index('row')
    cx, cy = lax.rem(col, 2), lax.div(col, 2)
    home = row == cy
    away = jnp.logical_not(home)
    xn = (cy * 2 + 1 - cx, row)
    yn = ((1 - cy) * 2 + cx, row)
    mate = (col, 1 - row)
    same = cx * COLS
    other = (1 - cx) * COLS
    mine = row * PIECE
    far = (1 - row) * PIECE

    def rows_of(start, size):
        return pl.ds(pl.multiple_of(start, size), size)

    def blocks(start, b, n):
        return pl.ds(pl.multiple_of(start + b * BR, BR), n * BR)

    def cols(h):
        return pl.ds(0, VECS) if h is None else pl.ds(h * HALF, HALF)

    def remote(src, dst, send, recv, dev):
        return pltpu.make_async_remote_copy(
            src_ref=src, dst_ref=dst, send_sem=send, recv_sem=recv, device_id=dev, device_id_type=MESH)

    def loop(lo, hi, body):
        def step(i, c):
            body(i)
            return c
        lax.fori_loop(lo, hi, step, 0)

    def signal(sem, dev):
        pl.semaphore_signal(sem, inc=1, device_id=dev, device_id_type=MESH)

    def x_in(c, h):
        return pltpu.make_async_copy(x_hbm.at[rows_of(c * X0R, X0R), cols(h)], vbuf.at[rows_of(mine + c * X0R, X0R), cols(h)],
                                     in_sem.at[h * X0C + c])

    for c in range(X0C):
        x_in(c, 0).start()

    barrier = pltpu.get_barrier_semaphore()
    for off in range(4):
        for r in range(2):
            if off == 0 and r == 1:
                continue
            signal(barrier, (lax.rem(col + off, 4), row if r == 0 and off else 1 - row))

    def flow(start, b, n, h, dst, send, recv, i, dev):
        return remote(ybuf.at[blocks(start, b, n), cols(h)], dst.at[blocks(0, b, n), cols(h)], send, recv.at[i], dev)

    def c_a(b, h=None, n=1):
        return flow(other, b, n, h, ra, a_s, a_r, lax.div(b, G), xn)

    def c_gy(b, h=None, n=1):
        return flow(other + PIECE, b, n, h, rgy, gy_s, gy_r, lax.div(b, G), yn)

    def c_dy(b, n=1):
        return remote(ybuf.at[blocks(same + PIECE, b, n)], rdy.at[blocks(0, b, n)], dy_s, dy_r, yn)

    def held_a():
        return remote(ybuf.at[blocks(other, NB - 1, 1)], ra.at[blocks(0, NB - 1, 1)], a_s, held_r, xn)

    def held_dy():
        return remote(ybuf.at[blocks(same + PIECE, NB - 1, 1)], rdy.at[blocks(0, NB - 1, 1)], dy_s, held_r, yn)

    def late(b, h):
        return lax.div(b, G) if h is None else E // G + 2 * h + jnp.where(b == NB - 1, 1, 0)

    def c_fx(b, h=None, n=1):
        return flow(other + PIECE, b, n, h, rfx, fx_s, fx_r, late(b, h), xn)

    def c_fy(b, h=None, n=1):
        return flow(same, b, n, h, rfy, fy_s, fy_r, late(b, h), yn)

    def arrived(copy, b, h):
        if h is None:
            @pl.when(lax.rem(b, G) == 0)
            def _():
                copy(b, n=G).wait_recv()
        else:
            @pl.when(b == E)
            def _():
                copy(b, h, n=G - 1).wait_recv()

            @pl.when(b == NB - 1)
            def _():
                copy(b, h).wait_recv()

    def c_x(t, b, h=None):
        at = blocks(t * PIECE, b, 1)
        return remote(xbf.at[at, cols(h)], xbf.at[at, cols(h)], x_s, x_r.at[1 if h == 1 else 0], mate)

    def x_bytes(rows, i):
        return remote(xbf.at[pl.ds(0, rows)], xbf.at[pl.ds(0, rows)], x_s, x_r.at[i], mate)

    def block_of(n):
        m = n - G
        pair = m < 2 * E
        t0 = jnp.where(pair, lax.rem(m, 2), 1)
        b0 = jnp.where(pair, jnp.where(t0 == 0, G, 0) + lax.div(m, 2), m - E)
        b0 = jnp.where(m < 0, n, b0)
        t0 = jnp.where(jnp.logical_xor(home, jnp.logical_or(m < 0, t0 == 0)), 1, 0)
        m = n - 2 * NB
        first = n < 2 * NB
        t = jnp.where(first, t0, 1 - lax.div(m, NB))
        b = jnp.where(first, b0, lax.rem(m, NB))
        return jnp.where(first, other, same) + t * PIECE + b * BR

    def a_copy(n):
        slot = lax.rem(n, RING)
        return pltpu.make_async_copy(a_hbm.at[rows_of(block_of(n), BR)], abuf.at[slot], a_sem.at[slot])

    d_in = pltpu.make_async_copy(d_hbm, dint.at[row], in_sem.at[0])
    v_in = pltpu.make_async_copy(v_hbm, vbuf.at[rows_of(mine, PIECE)], in_sem.at[1])

    def v_copy(r):
        return remote(v_hbm, vbuf.at[rows_of(r * PIECE, PIECE)], fx_s, x_r.at[0], mate)

    def d_copy(r):
        return remote(d_hbm, dint.at[r], x_s, x_r.at[1], mate)

    def s0_copy(r):
        return remote(s0buf.at[r], s0buf.at[r], o_s, o_r, mate)

    def x0_copy(start, c, h, n=1):
        at = pl.ds(pl.multiple_of(start + c * X0R, X0R), n * X0R)
        return remote(xbf.at[at, cols(h)], xbf.at[at, cols(h)], x0_s, x0_r.at[1 if h == 1 else 0], mate)

    a_copy(jnp.int32(0)).start()
    for c in range(X0C):
        x_in(c, 1).start()
    for n in range(1, RING):
        a_copy(jnp.int32(n)).start()

    def take_x(h):
        for c in range(X0C):
            x_in(c, h).wait()

            def convert(i, c=c):
                at = rows_of(mine + c * X0R + i * CH, CH)
                xbf[at, cols(h)] = vbuf[at, cols(h)].astype(jnp.bfloat16)
            loop(0, X0R // CH, convert)
            if c == 0 and h == 0:
                pl.semaphore_wait(barrier, 7)
            x0_copy(mine, c, h).start()

    def half_product(start):
        at = rows_of(start, PIECE)
        return jnp.dot(abuf[0, :, at], xbf[at, cols(0)], preferred_element_type=jnp.float32)

    take_x(0)
    a_copy(jnp.int32(0)).wait()
    first = rows_of(block_of(jnp.int32(0)), BR)
    ybuf[first, cols(0)] = half_product(mine)
    x0_copy(far, 0, 0, X0C).wait_recv()
    ybuf[first, cols(0)] = ybuf[first, cols(0)] + half_product(far)

    @pl.when(home)
    def _():
        c_a(jnp.int32(0), 0).start()

    @pl.when(away)
    def _():
        c_gy(jnp.int32(0), 0).start()
    take_x(1)
    d_in.start()

    @pl.when(away)
    def _():
        d_copy(row).start()
        v_copy(row).start()

    def s_copy(par, off):
        dst_col = lax.rem(col + off, 4)
        return remote(sbuf.at[par, col], sbuf.at[par, col], s_s, s_r.at[par], (dst_col, lax.div(dst_col, 2)))

    def s_bytes(par):
        return remote(sbuf.at[par, pl.ds(0, 3)], sbuf.at[par, pl.ds(0, 3)], s_s, s_r.at[par], mate)

    def s_publish(par, value):
        sbuf[par, col] = jnp.sum(value, axis=0, keepdims=True)
        for off in range(1, 4):
            s_copy(par, off).start()

    def spread(r):
        def group(g):
            flags = dint[r, pl.ds(g, 1), :].astype(jnp.float32)
            dbuf[rows_of(r * PIECE + g * 128, 128), :] = jnp.broadcast_to(flags, (128, 128)).T.astype(jnp.bfloat16)
        loop(0, PIECE // 128, group)

    def flags(start, h):
        d = dbuf[rows_of(start, CH), :].astype(jnp.float32)
        return d if h is not None else jnp.concatenate([d, d], axis=1)

    def fold(w):
        return jnp.sum(w.reshape(CH // 8, 8, w.shape[1]), axis=0)

    def first_mass():
        d_in.wait()
        spread(row)

        def add(c, acc):
            at = mine + c * CH
            return acc + fold(vbuf[rows_of(at, CH), :] * flags(at, None))
        s0buf[row] = lax.fori_loop(0, PIECE // CH, add, jnp.zeros((8, VECS), jnp.float32))

    def new_x(at, own, there, h, one, two):
        y = (ybuf[rows_of(at, CH), cols(h)] + one[there, cols(h)]) + two[there, cols(h)]
        cf = jnp.concatenate([coef[:, cols(h)]] * (CH // 8), axis=0)
        return DAMPING * y + cf * vbuf[rows_of(own, CH), cols(h)]

    def update(t, b, h, one, two, acc):
        def step(c, acc):
            own = t * PIECE + b * BR + c * CH
            x = new_x(same + own, own, rows_of(b * BR + c * CH, CH), h, one, two)
            xbf[rows_of(own, CH), cols(h)] = x.astype(jnp.bfloat16)
            ybuf[rows_of(same + own, CH), cols(h)] = x
            return acc + fold(x * flags(own, h))
        return lax.fori_loop(0, BR // CH, step, acc)

    def keep(t, b, h):
        def step(c):
            there = rows_of(b * BR + c * CH, CH)
            out[there, cols(h)] = ybuf[rows_of(same + t * PIECE + b * BR + c * CH, CH), cols(h)]
        loop(0, BR // CH, step)

    def o_remote(t, b, h=None, n=1):
        return remote(ybuf.at[blocks(same + t * PIECE, b, n), cols(h)], out.at[blocks(0, b, n), cols(h)], o_s, o_r, mate)

    def emit(t, b, h, last):
        @pl.when(jnp.logical_not(last))
        def _():
            c_x(t, b, h).start()

        @pl.when(jnp.logical_and(last, row == t))
        def _():
            keep(t, b, h)

        @pl.when(jnp.logical_and(last, row != t))
        def _():
            o_remote(t, b, h).start()

    def finish(b, h, last, acc):
        arrived(c_fy, b, h)
        acc = update(0, b, h, ra, rfy, acc)
        emit(0, b, h, last)
        arrived(c_fx, b, h)
        acc = update(1, b, h, rdy, rfx, acc)
        emit(1, b, h, last)
        return acc

    def finish_half(h, last):
        part = lax.fori_loop(E, NB, lambda b, acc: finish(b, h, last, acc), jnp.zeros((8, HALF), jnp.float32))
        sacc[:, cols(h)] = sacc[:, cols(h)] + part

    def finish_last():
        def piece(t, b, h):
            arrived(c_fy if t == 0 else c_fx, b, h)
            result(t, b, h)

        def result(t, b, h):
            update(t, b, h, ra if t == 0 else rdy, rfy if t == 0 else rfx, jnp.zeros((8, HALF), jnp.float32))
            emit(t, b, h, jnp.bool_(True))

        for kept in range(2):
            @pl.when(row == kept)
            def _():
                end = jnp.int32(NB - 1)
                for h in range(2):
                    def both(b):
                        piece(1 - kept, b, h)
                        piece(kept, b, h)
                    loop(E, NB - 1, both)
                    piece(1 - kept, end, h)
                for h in range(2):
                    arrived(c_fy if kept == 0 else c_fx, end, h)
                (held_a() if kept == 0 else held_dy()).wait_recv()
                one, two = (ra, rfy) if kept == 0 else (rdy, rfx)

                def last_rows(c):
                    own = kept * PIECE + (NB - 1) * BR + c * CH
                    there = rows_of((NB - 1) * BR + c * CH, CH)
                    out[there, :] = new_x(same + own, own, there, None, one, two)
                loop(0, BR // CH, last_rows)

    def drain_forward():
        @pl.when(home)
        def _():
            c_fx(0, n=NB).wait_send()

        @pl.when(away)
        def _():
            c_fy(0, n=NB).wait_send()

    def sweep(k, carry):
        last = k == SWEEPS - 1
        more = jnp.logical_not(last)
        par = lax.rem(k, 2)
        hold_a = jnp.logical_and(jnp.logical_and(last, home), row == 0)
        hold_dy = jnp.logical_and(last, row == 1)

        def multiply(n, h):
            start = block_of(n)
            ybuf[rows_of(start, BR), cols(h)] = jnp.dot(
                abuf[lax.rem(n, RING)], xbf[:, cols(h)], preferred_element_type=jnp.float32)

        def fetch(n):
            @pl.when(jnp.logical_not(jnp.logical_and(last, n >= 4 * NB)))
            def _():
                a_copy(lax.rem(n, 4 * NB)).start()

        def lead(h):
            def block(n):
                if h == 0:
                    a_copy(n).wait()
                multiply(n, h)
                if h == 1:
                    fetch(n + RING)

                @pl.when(home)
                def _():
                    c_a(n, h).start()

                @pl.when(away)
                def _():
                    c_gy(n, h).start()

            def one(n):
                @pl.when(jnp.logical_or(k > 0, n > 0))
                def _():
                    block(n)
            loop(0, G, one if h == 0 else block)

        @pl.when(k > 0)
        def _():
            pl.semaphore_wait(cr_0, 1)
        lead(0)

        @pl.when(k == 0)
        def _():
            x0_copy(far, 0, 1, X0C).wait_recv()

        @pl.when(jnp.logical_and(k > 0, home))
        def _():
            finish_half(1, jnp.bool_(False))
            s_publish(par, sacc[...])
            signal(cr_1, xn)
            signal(cr_1, yn)

        @pl.when(jnp.logical_and(k > 0, away))
        def _():
            x_bytes(G * BR, 1).wait_recv()
        lead(1)

        @pl.when(k > 0)
        def _():
            drain_forward()
            pl.semaphore_wait(cr_1, 1)

            @pl.when(away)
            def _():
                pl.semaphore_wait(cr_2, 1)

        def step(n):
            a_copy(n).wait()
            multiply(n, None)
            fetch(n + RING)
            at = block_of(n) - jnp.where(n < 2 * NB, other, same)
            return lax.div(at, PIECE), lax.div(lax.rem(at, PIECE), BR)

        def part_one(n):
            t, b = step(n)

            @pl.when(jnp.logical_and(t == 0, jnp.logical_not(jnp.logical_and(hold_a, b == NB - 1))))
            def _():
                c_a(b).start()

            @pl.when(jnp.logical_and(t == 1, away))
            def _():
                c_gy(b).start()
        loop(G, 2 * NB, part_one)

        @pl.when(k == 0)
        def _():
            first_mass()

            @pl.when(away)
            def _():
                s0_copy(row).start()

            @pl.when(home)
            def _():
                v_in.start()
                d_copy(1 - row).wait_recv()
                s0_copy(1 - row).wait_recv()
                s_publish(0, s0buf[0] + s0buf[1])

        def add_into(start, b, src):
            def add(c):
                at = rows_of(start + b * BR + c * CH, CH)
                ybuf[at, :] = ybuf[at, :] + src[rows_of(b * BR + c * CH, CH), :]
            loop(0, BR // CH, add)

        def send_on(copy, b):
            @pl.when(b < E)
            def _():
                copy(b).start()

            @pl.when(b >= E)
            def _():
                copy(b, 0).start()

        def part_two(n):
            b = n - 2 * NB
            step(n)

            @pl.when(jnp.logical_and(away, jnp.logical_not(jnp.logical_and(hold_dy, b == NB - 1))))
            def _():
                c_dy(b).start()

            @pl.when(home)
            def _():
                @pl.when(lax.rem(b, G) == 0)
                def _():
                    c_gy(b, n=G).wait_recv()
                add_into(other + PIECE, b, rgy)
                send_on(c_fx, b)
        loop(2 * NB, 3 * NB, part_two)

        @pl.when(home)
        def _():
            loop(E, NB, lambda b: c_fx(b, 1).start())

            @pl.when(hold_a)
            def _():
                held_a().start()

        def part_three(n):
            b = n - 3 * NB
            step(n)

            @pl.when(away)
            def _():
                @pl.when(lax.rem(b, G) == 0)
                def _():
                    c_a(b, n=G).wait_recv()
                add_into(same, b, ra)
                send_on(c_fy, b)
        loop(3 * NB, 4 * NB, part_three)

        @pl.when(away)
        def _away():
            loop(E, NB, lambda b: c_fy(b, 1).start())

            @pl.when(hold_dy)
            def _():
                held_dy().start()

            @pl.when(k == 0)
            def _():
                x0_copy(mine, 0, None, X0C).wait_send()
                v_copy(row).wait_send()
                d_copy(row).wait_send()
                s0_copy(row).wait_send()

            @pl.when(more)
            def _():
                signal(cr_2, mate)
                signal(cr_2, xn)
            c_a(0, n=NB).wait_send()
            c_gy(0, n=NB).wait_send()
            c_dy(0, NB).wait_send()

            @pl.when(more)
            def _():
                x_bytes(2 * PIECE - G * BR, 0).wait_recv()

        @pl.when(home)
        def _home():
            @pl.when(more)
            def _():
                signal(cr_0, yn)

            @pl.when(k == 0)
            def _():
                spread(1 - row)
                x0_copy(mine, 0, None, X0C).wait_send()
                v_copy(1 - row).wait_recv()
                v_in.wait()

            @pl.when(k > 0)
            def _():
                x_bytes(2 * PIECE, 0).wait_send()

            s_bytes(par).wait_recv()
            s_bytes(par).wait_send()
            mass = ((sbuf[par, 0] + sbuf[par, 1]) + (sbuf[par, 2] + sbuf[par, 3])) / VERTS
            coef[...] = jnp.broadcast_to(DAMPING * mass + (1.0 - DAMPING), (8, VECS))

            @pl.when(more)
            def _():
                pl.semaphore_wait(cr_2, 1)

            @pl.when(more)
            def _():
                c_a(0, n=NB).wait_send()
            for b in range(0, E, G):
                c_a(b, n=G).wait_recv()

            @pl.when(hold_a)
            def _():
                c_a(E, n=G - 1).wait_recv()

            @pl.when(jnp.logical_not(hold_a))
            def _():
                c_a(E, n=G).wait_recv()

            @pl.when(hold_dy)
            def _():
                c_dy(0, NB - 1).wait_recv()

            @pl.when(jnp.logical_not(hold_dy))
            def _():
                c_dy(0, NB).wait_recv()
            sacc[...] = lax.fori_loop(0, E, lambda b, acc: finish(b, None, last, acc), jnp.zeros((8, VECS), jnp.float32))

            @pl.when(more)
            def _():
                signal(cr_0, xn)
                finish_half(0, jnp.bool_(False))

            @pl.when(last)
            def _():
                finish_last()

        return carry

    lax.fori_loop(0, SWEEPS, sweep, 0)

    drain_forward()

    @pl.when(home)
    def _():
        c_a(0, n=NB).wait_send()
        o_remote(1 - row, 0, n=NB).wait_send()

    @pl.when(away)
    def _():
        o_remote(1 - row, 0, n=NB).wait_recv()


def solution(mesh):
    dma = pltpu.SemaphoreType.DMA
    reg = pltpu.SemaphoreType.REGULAR

    def in_hbm(a):
        return pltpu.with_memory_space_constraint(a, pltpu.HBM)

    def local_sweeps(mat_tile, x_piece, tele_piece, dang_piece):
        part = pltpu.VMEM((PIECE, VECS), jnp.float32)
        return pl.pallas_call(
            kernel,
            name="sweeps",
            out_shape=jax.ShapeDtypeStruct((PIECE, VECS), jnp.float32),
            in_specs=[pl.BlockSpec(memory_space=pltpu.HBM)] * 4,
            out_specs=pl.BlockSpec(memory_space=pltpu.VMEM),
            scratch_shapes=[
                pltpu.VMEM((RING, BR, COLS), jnp.bfloat16),
                pltpu.VMEM((COLS, VECS), jnp.bfloat16),
                pltpu.VMEM((ROWS, VECS), jnp.float32),
                part, part, part, part, part,
                pltpu.VMEM((COLS, VECS), jnp.float32),
                pltpu.VMEM((COLS, 128), jnp.bfloat16),
                pltpu.VMEM((2, PIECE // 128, 128), jnp.int32),
                pltpu.VMEM((2, 4, 1, VECS), jnp.float32),
                pltpu.VMEM((2, 8, VECS), jnp.float32),
                pltpu.VMEM((8, VECS), jnp.float32),
                pltpu.VMEM((8, VECS), jnp.float32),
                dma((RING,)), dma((2 * X0C,)), dma, dma((2,)),
                dma, dma((NB // G,)), dma, dma((NB // G,)), dma, dma, dma, dma((E // G + 4,)), dma, dma((E // G + 4,)),
                dma, dma((2,)), dma, dma((2,)), dma, dma, dma, reg, reg, reg,
            ],
            compiler_params=pltpu.CompilerParams(
                collective_id=0, has_side_effects=True, vmem_limit_bytes=53_300_000),
            cost_estimate=pl.CostEstimate(
                flops=2 * ROWS * COLS * VECS * SWEEPS, bytes_accessed=2 * ROWS * COLS * SWEEPS, transcendentals=0),
        )(mat_tile, x_piece, tele_piece, in_hbm(dang_piece.reshape(PIECE // 128, 128)))

    vec_spec = P(('col', 'row'), None)
    return jax.shard_map(local_sweeps, mesh=mesh,
                         in_specs=(P('row', 'col'), vec_spec, vec_spec, P(('col', 'row'))),
                         out_specs=vec_spec, check_vma=False)
```

```python
import jax
import jax.numpy as jnp
from jax import lax
from jax.experimental import pallas as pl
from jax.experimental.pallas import tpu as pltpu
from jax.sharding import PartitionSpec as P

SWEEPS = 8
DAMPING = 0.85
MESH = pl.DeviceIdType.MESH

VERTS = 24576
VECS = 256
HALF = 128
PIECE = 3072
ROWS = 12288
COLS = 6144
BR = 256
NB = PIECE // BR
G = 4
E = NB - G
CH = 32
RING = 4
X0C = 4
X0R = PIECE // X0C


def kernel(a_hbm, x_hbm, v_hbm, d_hbm, out,
           abuf, xbf, ybuf, ra, rgy, rdy, rfx, rfy, vbuf, dbuf, dint, sbuf, s0buf, coef, sacc,
           a_sem, in_sem, x0_s, x0_r,
           a_s, a_r, gy_s, gy_r, dy_s, dy_r, fx_s, fx_r, fy_s, fy_r,
           x_s, x_r, s_s, s_r, o_s, o_r, held_r, cr_0, cr_1, cr_2):
    col = lax.axis_index('col')
    row = lax.axis_index('row')
    cx, cy = lax.rem(col, 2), lax.div(col, 2)
    home = row == cy
    away = jnp.logical_not(home)
    xn = (cy * 2 + 1 - cx, row)
    yn = ((1 - cy) * 2 + cx, row)
    mate = (col, 1 - row)
    same = cx * COLS
    other = (1 - cx) * COLS
    mine = row * PIECE
    far = (1 - row) * PIECE

    def rows_of(start, size):
        return pl.ds(pl.multiple_of(start, size), size)

    def blocks(start, b, n):
        return pl.ds(pl.multiple_of(start + b * BR, BR), n * BR)

    def cols(h):
        return pl.ds(0, VECS) if h is None else pl.ds(h * HALF, HALF)

    def remote(src, dst, send, recv, dev):
        return pltpu.make_async_remote_copy(
            src_ref=src, dst_ref=dst, send_sem=send, recv_sem=recv, device_id=dev, device_id_type=MESH)

    def loop(lo, hi, body):
        def step(i, c):
            body(i)
            return c
        lax.fori_loop(lo, hi, step, 0)

    def signal(sem, dev):
        pl.semaphore_signal(sem, inc=1, device_id=dev, device_id_type=MESH)

    def x_in(c):
        return pltpu.make_async_copy(x_hbm.at[rows_of(c * X0R, X0R)], vbuf.at[rows_of(mine + c * X0R, X0R)], in_sem.at[c])

    for c in range(X0C):
        x_in(c).start()

    barrier = pltpu.get_barrier_semaphore()
    for off in range(4):
        for r in range(2):
            if off == 0 and r == 1:
                continue
            signal(barrier, (lax.rem(col + off, 4), row if r == 0 and off else 1 - row))

    def flow(start, b, n, h, dst, send, recv, i, dev):
        return remote(ybuf.at[blocks(start, b, n), cols(h)], dst.at[blocks(0, b, n), cols(h)], send, recv.at[i], dev)

    def c_a(b, h=None, n=1):
        return flow(other, b, n, h, ra, a_s, a_r, lax.div(b, G), xn)

    def c_gy(b, h=None, n=1):
        return flow(other + PIECE, b, n, h, rgy, gy_s, gy_r, lax.div(b, G), yn)

    def c_dy(b, n=1):
        return remote(ybuf.at[blocks(same + PIECE, b, n)], rdy.at[blocks(0, b, n)], dy_s, dy_r, yn)

    def held_a():
        return remote(ybuf.at[blocks(other, NB - 1, 1)], ra.at[blocks(0, NB - 1, 1)], a_s, held_r, xn)

    def held_dy():
        return remote(ybuf.at[blocks(same + PIECE, NB - 1, 1)], rdy.at[blocks(0, NB - 1, 1)], dy_s, held_r, yn)

    def late(b, h):
        return lax.div(b, G) if h is None else E // G + 2 * h + jnp.where(b == NB - 1, 1, 0)

    def c_fx(b, h=None, n=1):
        return flow(other + PIECE, b, n, h, rfx, fx_s, fx_r, late(b, h), xn)

    def c_fy(b, h=None, n=1):
        return flow(same, b, n, h, rfy, fy_s, fy_r, late(b, h), yn)

    def arrived(copy, b, h):
        if h is None:
            @pl.when(lax.rem(b, G) == 0)
            def _():
                copy(b, n=G).wait_recv()
        else:
            @pl.when(b == E)
            def _():
                copy(b, h, n=G - 1).wait_recv()

            @pl.when(b == NB - 1)
            def _():
                copy(b, h).wait_recv()

    def c_x(t, b, h=None):
        at = blocks(t * PIECE, b, 1)
        return remote(xbf.at[at, cols(h)], xbf.at[at, cols(h)], x_s, x_r.at[1 if h == 1 else 0], mate)

    def x_bytes(rows, i):
        return remote(xbf.at[pl.ds(0, rows)], xbf.at[pl.ds(0, rows)], x_s, x_r.at[i], mate)

    def block_of(n):
        m = n - G
        pair = m < 2 * E
        t0 = jnp.where(pair, lax.rem(m, 2), 1)
        b0 = jnp.where(pair, jnp.where(t0 == 0, G, 0) + lax.div(m, 2), m - E)
        b0 = jnp.where(m < 0, n, b0)
        t0 = jnp.where(jnp.logical_xor(home, jnp.logical_or(m < 0, t0 == 0)), 1, 0)
        m = n - 2 * NB
        first = n < 2 * NB
        t = jnp.where(first, t0, 1 - lax.div(m, NB))
        b = jnp.where(first, b0, lax.rem(m, NB))
        return jnp.where(first, other, same) + t * PIECE + b * BR

    def a_copy(n):
        slot = lax.rem(n, RING)
        return pltpu.make_async_copy(a_hbm.at[rows_of(block_of(n), BR)], abuf.at[slot], a_sem.at[slot])

    d_in = pltpu.make_async_copy(d_hbm, dint.at[row], in_sem.at[0])
    v_in = pltpu.make_async_copy(v_hbm, vbuf.at[rows_of(mine, PIECE)], in_sem.at[1])

    def v_copy(r):
        return remote(v_hbm, vbuf.at[rows_of(r * PIECE, PIECE)], fx_s, x_r.at[0], mate)

    def d_copy(r):
        return remote(d_hbm, dint.at[r], x_s, x_r.at[1], mate)

    def s0_copy(r):
        return remote(s0buf.at[r], s0buf.at[r], o_s, o_r, mate)

    def x0_copy(start, c, h, n=1):
        at = pl.ds(pl.multiple_of(start + c * X0R, X0R), n * X0R)
        return remote(xbf.at[at, cols(h)], xbf.at[at, cols(h)], x0_s, x0_r.at[1 if h == 1 else 0], mate)

    for c in range(X0C):
        x_in(c).wait()

        def convert(i, c=c):
            at = rows_of(mine + c * X0R + i * CH, CH)
            xbf[at, :] = vbuf[at, :].astype(jnp.bfloat16)
        loop(0, X0R // CH, convert)
        if c == 0:
            pl.semaphore_wait(barrier, 7)
        x0_copy(mine, c, 0).start()
        if c < RING:
            a_copy(jnp.int32(c)).start()
    for c in range(X0C):
        x0_copy(mine, c, 1).start()
    d_in.start()

    @pl.when(away)
    def _():
        d_copy(row).start()
        v_copy(row).start()

    def s_copy(par, off):
        dst_col = lax.rem(col + off, 4)
        return remote(sbuf.at[par, col], sbuf.at[par, col], s_s, s_r.at[par], (dst_col, lax.div(dst_col, 2)))

    def s_bytes(par):
        return remote(sbuf.at[par, pl.ds(0, 3)], sbuf.at[par, pl.ds(0, 3)], s_s, s_r.at[par], mate)

    def s_publish(par, value):
        sbuf[par, col] = jnp.sum(value, axis=0, keepdims=True)
        for off in range(1, 4):
            s_copy(par, off).start()

    def spread(r):
        def group(g):
            flags = dint[r, pl.ds(g, 1), :].astype(jnp.float32)
            dbuf[rows_of(r * PIECE + g * 128, 128), :] = jnp.broadcast_to(flags, (128, 128)).T.astype(jnp.bfloat16)
        loop(0, PIECE // 128, group)

    def flags(start, h):
        d = dbuf[rows_of(start, CH), :].astype(jnp.float32)
        return d if h is not None else jnp.concatenate([d, d], axis=1)

    def fold(w):
        return jnp.sum(w.reshape(CH // 8, 8, w.shape[1]), axis=0)

    def first_mass():
        d_in.wait()
        spread(row)

        def add(c, acc):
            at = mine + c * CH
            return acc + fold(vbuf[rows_of(at, CH), :] * flags(at, None))
        s0buf[row] = lax.fori_loop(0, PIECE // CH, add, jnp.zeros((8, VECS), jnp.float32))

    def new_x(at, own, there, h, one, two):
        y = (ybuf[rows_of(at, CH), cols(h)] + one[there, cols(h)]) + two[there, cols(h)]
        cf = jnp.concatenate([coef[:, cols(h)]] * (CH // 8), axis=0)
        return DAMPING * y + cf * vbuf[rows_of(own, CH), cols(h)]

    def update(t, b, h, one, two, acc):
        def step(c, acc):
            own = t * PIECE + b * BR + c * CH
            x = new_x(same + own, own, rows_of(b * BR + c * CH, CH), h, one, two)
            xbf[rows_of(own, CH), cols(h)] = x.astype(jnp.bfloat16)
            ybuf[rows_of(same + own, CH), cols(h)] = x
            return acc + fold(x * flags(own, h))
        return lax.fori_loop(0, BR // CH, step, acc)

    def keep(t, b, h):
        def step(c):
            there = rows_of(b * BR + c * CH, CH)
            out[there, cols(h)] = ybuf[rows_of(same + t * PIECE + b * BR + c * CH, CH), cols(h)]
        loop(0, BR // CH, step)

    def o_remote(t, b, h=None, n=1):
        return remote(ybuf.at[blocks(same + t * PIECE, b, n), cols(h)], out.at[blocks(0, b, n), cols(h)], o_s, o_r, mate)

    def emit(t, b, h, last):
        @pl.when(jnp.logical_not(last))
        def _():
            c_x(t, b, h).start()

        @pl.when(jnp.logical_and(last, row == t))
        def _():
            keep(t, b, h)

        @pl.when(jnp.logical_and(last, row != t))
        def _():
            o_remote(t, b, h).start()

    def finish(b, h, last, acc):
        arrived(c_fy, b, h)
        acc = update(0, b, h, ra, rfy, acc)
        emit(0, b, h, last)
        arrived(c_fx, b, h)
        acc = update(1, b, h, rdy, rfx, acc)
        emit(1, b, h, last)
        return acc

    def finish_half(h, last):
        part = lax.fori_loop(E, NB, lambda b, acc: finish(b, h, last, acc), jnp.zeros((8, HALF), jnp.float32))
        sacc[:, cols(h)] = sacc[:, cols(h)] + part

    def finish_last():
        def piece(t, b, h):
            arrived(c_fy if t == 0 else c_fx, b, h)
            result(t, b, h)

        def result(t, b, h):
            update(t, b, h, ra if t == 0 else rdy, rfy if t == 0 else rfx, jnp.zeros((8, HALF), jnp.float32))
            emit(t, b, h, jnp.bool_(True))

        for kept in range(2):
            @pl.when(row == kept)
            def _():
                end = jnp.int32(NB - 1)
                for h in range(2):
                    def both(b):
                        piece(1 - kept, b, h)
                        piece(kept, b, h)
                    loop(E, NB - 1, both)
                    piece(1 - kept, end, h)
                for h in range(2):
                    arrived(c_fy if kept == 0 else c_fx, end, h)
                (held_a() if kept == 0 else held_dy()).wait_recv()
                one, two = (ra, rfy) if kept == 0 else (rdy, rfx)

                def last_rows(c):
                    own = kept * PIECE + (NB - 1) * BR + c * CH
                    there = rows_of((NB - 1) * BR + c * CH, CH)
                    out[there, :] = new_x(same + own, own, there, None, one, two)
                loop(0, BR // CH, last_rows)

    def drain_forward():
        @pl.when(home)
        def _():
            c_fx(0, n=NB).wait_send()

        @pl.when(away)
        def _():
            c_fy(0, n=NB).wait_send()

    def sweep(k, carry):
        last = k == SWEEPS - 1
        more = jnp.logical_not(last)
        par = lax.rem(k, 2)
        hold_a = jnp.logical_and(jnp.logical_and(last, home), row == 0)
        hold_dy = jnp.logical_and(last, row == 1)

        def multiply(n, h):
            start = block_of(n)
            ybuf[rows_of(start, BR), cols(h)] = jnp.dot(
                abuf[lax.rem(n, RING)], xbf[:, cols(h)], preferred_element_type=jnp.float32)

        def fetch(n):
            @pl.when(jnp.logical_not(jnp.logical_and(last, n >= 4 * NB)))
            def _():
                a_copy(lax.rem(n, 4 * NB)).start()

        def lead(h):
            def one(n):
                if h == 0:
                    a_copy(n).wait()
                multiply(n, h)
                if h == 1:
                    fetch(n + RING)

                @pl.when(home)
                def _():
                    c_a(n, h).start()

                @pl.when(away)
                def _():
                    c_gy(n, h).start()
            loop(0, G, one)

        @pl.when(k == 0)
        def _():
            x0_copy(far, 0, 0, X0C).wait_recv()

        @pl.when(k > 0)
        def _():
            pl.semaphore_wait(cr_0, 1)
        lead(0)

        @pl.when(k == 0)
        def _():
            x0_copy(far, 0, 1, X0C).wait_recv()

        @pl.when(jnp.logical_and(k > 0, home))
        def _():
            finish_half(1, jnp.bool_(False))
            s_publish(par, sacc[...])
            signal(cr_1, xn)
            signal(cr_1, yn)

        @pl.when(jnp.logical_and(k > 0, away))
        def _():
            x_bytes(G * BR, 1).wait_recv()
        lead(1)

        @pl.when(k > 0)
        def _():
            drain_forward()
            pl.semaphore_wait(cr_1, 1)

            @pl.when(away)
            def _():
                pl.semaphore_wait(cr_2, 1)

        def step(n):
            a_copy(n).wait()
            multiply(n, None)
            fetch(n + RING)
            at = block_of(n) - jnp.where(n < 2 * NB, other, same)
            return lax.div(at, PIECE), lax.div(lax.rem(at, PIECE), BR)

        def part_one(n):
            t, b = step(n)

            @pl.when(jnp.logical_and(t == 0, jnp.logical_not(jnp.logical_and(hold_a, b == NB - 1))))
            def _():
                c_a(b).start()

            @pl.when(jnp.logical_and(t == 1, away))
            def _():
                c_gy(b).start()
        loop(G, 2 * NB, part_one)

        @pl.when(k == 0)
        def _():
            first_mass()

            @pl.when(away)
            def _():
                s0_copy(row).start()

            @pl.when(home)
            def _():
                v_in.start()
                d_copy(1 - row).wait_recv()
                s0_copy(1 - row).wait_recv()
                s_publish(0, s0buf[0] + s0buf[1])

        def add_into(start, b, src):
            def add(c):
                at = rows_of(start + b * BR + c * CH, CH)
                ybuf[at, :] = ybuf[at, :] + src[rows_of(b * BR + c * CH, CH), :]
            loop(0, BR // CH, add)

        def send_on(copy, b):
            @pl.when(b < E)
            def _():
                copy(b).start()

            @pl.when(b >= E)
            def _():
                copy(b, 0).start()

        def part_two(n):
            b = n - 2 * NB
            step(n)

            @pl.when(jnp.logical_and(away, jnp.logical_not(jnp.logical_and(hold_dy, b == NB - 1))))
            def _():
                c_dy(b).start()

            @pl.when(home)
            def _():
                @pl.when(lax.rem(b, G) == 0)
                def _():
                    c_gy(b, n=G).wait_recv()
                add_into(other + PIECE, b, rgy)
                send_on(c_fx, b)
        loop(2 * NB, 3 * NB, part_two)

        @pl.when(home)
        def _():
            loop(E, NB, lambda b: c_fx(b, 1).start())

            @pl.when(hold_a)
            def _():
                held_a().start()

        def part_three(n):
            b = n - 3 * NB
            step(n)

            @pl.when(away)
            def _():
                @pl.when(lax.rem(b, G) == 0)
                def _():
                    c_a(b, n=G).wait_recv()
                add_into(same, b, ra)
                send_on(c_fy, b)
        loop(3 * NB, 4 * NB, part_three)

        @pl.when(away)
        def _away():
            loop(E, NB, lambda b: c_fy(b, 1).start())

            @pl.when(hold_dy)
            def _():
                held_dy().start()

            @pl.when(k == 0)
            def _():
                x0_copy(mine, 0, None, X0C).wait_send()
                v_copy(row).wait_send()
                d_copy(row).wait_send()
                s0_copy(row).wait_send()

            @pl.when(more)
            def _():
                signal(cr_2, mate)
                signal(cr_2, xn)
            c_a(0, n=NB).wait_send()
            c_gy(0, n=NB).wait_send()
            c_dy(0, NB).wait_send()

            @pl.when(more)
            def _():
                x_bytes(2 * PIECE - G * BR, 0).wait_recv()

        @pl.when(home)
        def _home():
            @pl.when(more)
            def _():
                signal(cr_0, yn)

            @pl.when(k == 0)
            def _():
                spread(1 - row)
                x0_copy(mine, 0, None, X0C).wait_send()
                v_copy(1 - row).wait_recv()
                v_in.wait()

            @pl.when(k > 0)
            def _():
                x_bytes(2 * PIECE, 0).wait_send()

            s_bytes(par).wait_recv()
            s_bytes(par).wait_send()
            mass = ((sbuf[par, 0] + sbuf[par, 1]) + (sbuf[par, 2] + sbuf[par, 3])) / VERTS
            coef[...] = jnp.broadcast_to(DAMPING * mass + (1.0 - DAMPING), (8, VECS))

            @pl.when(more)
            def _():
                pl.semaphore_wait(cr_2, 1)

            @pl.when(more)
            def _():
                c_a(0, n=NB).wait_send()
            for b in range(0, E, G):
                c_a(b, n=G).wait_recv()

            @pl.when(hold_a)
            def _():
                c_a(E, n=G - 1).wait_recv()

            @pl.when(jnp.logical_not(hold_a))
            def _():
                c_a(E, n=G).wait_recv()

            @pl.when(hold_dy)
            def _():
                c_dy(0, NB - 1).wait_recv()

            @pl.when(jnp.logical_not(hold_dy))
            def _():
                c_dy(0, NB).wait_recv()
            sacc[...] = lax.fori_loop(0, E, lambda b, acc: finish(b, None, last, acc), jnp.zeros((8, VECS), jnp.float32))

            @pl.when(more)
            def _():
                signal(cr_0, xn)
                finish_half(0, jnp.bool_(False))

            @pl.when(last)
            def _():
                finish_last()

        return carry

    lax.fori_loop(0, SWEEPS, sweep, 0)

    drain_forward()

    @pl.when(home)
    def _():
        c_a(0, n=NB).wait_send()
        o_remote(1 - row, 0, n=NB).wait_send()

    @pl.when(away)
    def _():
        o_remote(1 - row, 0, n=NB).wait_recv()


def solution(mesh):
    dma = pltpu.SemaphoreType.DMA
    reg = pltpu.SemaphoreType.REGULAR

    def in_hbm(a):
        return pltpu.with_memory_space_constraint(a, pltpu.HBM)

    def local_sweeps(mat_tile, x_piece, tele_piece, dang_piece):
        part = pltpu.VMEM((PIECE, VECS), jnp.float32)
        return pl.pallas_call(
            kernel,
            name="sweeps",
            out_shape=jax.ShapeDtypeStruct((PIECE, VECS), jnp.float32),
            in_specs=[pl.BlockSpec(memory_space=pltpu.HBM)] * 4,
            out_specs=pl.BlockSpec(memory_space=pltpu.VMEM),
            scratch_shapes=[
                pltpu.VMEM((RING, BR, COLS), jnp.bfloat16),
                pltpu.VMEM((COLS, VECS), jnp.bfloat16),
                pltpu.VMEM((ROWS, VECS), jnp.float32),
                part, part, part, part, part,
                pltpu.VMEM((COLS, VECS), jnp.float32),
                pltpu.VMEM((COLS, 128), jnp.bfloat16),
                pltpu.VMEM((2, PIECE // 128, 128), jnp.int32),
                pltpu.VMEM((2, 4, 1, VECS), jnp.float32),
                pltpu.VMEM((2, 8, VECS), jnp.float32),
                pltpu.VMEM((8, VECS), jnp.float32),
                pltpu.VMEM((8, VECS), jnp.float32),
                dma((RING,)), dma((X0C,)), dma, dma((2,)),
                dma, dma((NB // G,)), dma, dma((NB // G,)), dma, dma, dma, dma((E // G + 4,)), dma, dma((E // G + 4,)),
                dma, dma((2,)), dma, dma((2,)), dma, dma, dma, reg, reg, reg,
            ],
            compiler_params=pltpu.CompilerParams(
                collective_id=0, has_side_effects=True, vmem_limit_bytes=53_300_000),
            cost_estimate=pl.CostEstimate(
                flops=2 * ROWS * COLS * VECS * SWEEPS, bytes_accessed=2 * ROWS * COLS * SWEEPS, transcendentals=0),
        )(mat_tile, x_piece, tele_piece, in_hbm(dang_piece.reshape(PIECE // 128, 128)))

    vec_spec = P(('col', 'row'), None)
    return jax.shard_map(local_sweeps, mesh=mesh,
                         in_specs=(P('row', 'col'), vec_spec, vec_spec, P(('col', 'row'))),
                         out_specs=vec_spec, check_vma=False)
```

```python
import jax
import jax.numpy as jnp
from jax import lax
from jax.experimental import pallas as pl
from jax.experimental.pallas import tpu as pltpu
from jax.sharding import PartitionSpec as P

SWEEPS = 8
DAMPING = 0.85
MESH = pl.DeviceIdType.MESH

VERTS = 24576
VECS = 256
HALF = 128
PIECE = 3072
ROWS = 12288
COLS = 6144
BR = 256
NB = PIECE // BR
G = 4
E = NB - G
CH = 32
RING = 4
X0C = 3
X0R = PIECE // X0C


def kernel(a_hbm, x_hbm, v_hbm, d_hbm, out,
           abuf, xbf, ybuf, ra, rgy, rdy, rfx, rfy, vbuf, dbuf, dint, sbuf, s0buf, coef, sacc,
           a_sem, in_sem, x0_s, x0_r,
           a_s, a_r, gy_s, gy_r, dy_s, dy_r, fx_s, fx_r, fy_s, fy_r,
           x_s, x_r, s_s, s_r, o_s, o_r, held_r, cr_0, cr_1, cr_2):
    col = lax.axis_index('col')
    row = lax.axis_index('row')
    cx, cy = lax.rem(col, 2), lax.div(col, 2)
    home = row == cy
    away = jnp.logical_not(home)
    xn = (cy * 2 + 1 - cx, row)
    yn = ((1 - cy) * 2 + cx, row)
    mate = (col, 1 - row)
    same = cx * COLS
    other = (1 - cx) * COLS
    mine = row * PIECE
    far = (1 - row) * PIECE

    def rows_of(start, size):
        return pl.ds(pl.multiple_of(start, size), size)

    def blocks(start, b, n):
        return pl.ds(pl.multiple_of(start + b * BR, BR), n * BR)

    def cols(h):
        return pl.ds(0, VECS) if h is None else pl.ds(h * HALF, HALF)

    def remote(src, dst, send, recv, dev):
        return pltpu.make_async_remote_copy(
            src_ref=src, dst_ref=dst, send_sem=send, recv_sem=recv, device_id=dev, device_id_type=MESH)

    def loop(lo, hi, body):
        def step(i, c):
            body(i)
            return c
        lax.fori_loop(lo, hi, step, 0)

    def signal(sem, dev):
        pl.semaphore_signal(sem, inc=1, device_id=dev, device_id_type=MESH)

    def x_in(c, h):
        return pltpu.make_async_copy(x_hbm.at[rows_of(c * X0R, X0R), cols(h)], vbuf.at[rows_of(mine + c * X0R, X0R), cols(h)],
                                     in_sem.at[h * X0C + c])

    for c in range(X0C):
        x_in(c, 0).start()

    barrier = pltpu.get_barrier_semaphore()
    for off in range(4):
        for r in range(2):
            if off == 0 and r == 1:
                continue
            signal(barrier, (lax.rem(col + off, 4), row if r == 0 and off else 1 - row))

    def flow(start, b, n, h, dst, send, recv, i, dev):
        return remote(ybuf.at[blocks(start, b, n), cols(h)], dst.at[blocks(0, b, n), cols(h)], send, recv.at[i], dev)

    def c_a(b, h=None, n=1):
        return flow(other, b, n, h, ra, a_s, a_r, lax.div(b, G), xn)

    def c_gy(b, h=None, n=1):
        return flow(other + PIECE, b, n, h, rgy, gy_s, gy_r, lax.div(b, G), yn)

    def c_dy(b, n=1):
        return remote(ybuf.at[blocks(same + PIECE, b, n)], rdy.at[blocks(0, b, n)], dy_s, dy_r, yn)

    def held_a():
        return remote(ybuf.at[blocks(other, NB - 1, 1)], ra.at[blocks(0, NB - 1, 1)], a_s, held_r, xn)

    def held_dy():
        return remote(ybuf.at[blocks(same + PIECE, NB - 1, 1)], rdy.at[blocks(0, NB - 1, 1)], dy_s, held_r, yn)

    def late(b, h):
        return lax.div(b, G) if h is None else E // G + 2 * h + jnp.where(b == NB - 1, 1, 0)

    def c_fx(b, h=None, n=1):
        return flow(other + PIECE, b, n, h, rfx, fx_s, fx_r, late(b, h), xn)

    def c_fy(b, h=None, n=1):
        return flow(same, b, n, h, rfy, fy_s, fy_r, late(b, h), yn)

    def arrived(copy, b, h):
        if h is None:
            @pl.when(lax.rem(b, G) == 0)
            def _():
                copy(b, n=G).wait_recv()
        else:
            @pl.when(b == E)
            def _():
                copy(b, h, n=G - 1).wait_recv()

            @pl.when(b == NB - 1)
            def _():
                copy(b, h).wait_recv()

    def c_x(t, b, h=None):
        at = blocks(t * PIECE, b, 1)
        return remote(xbf.at[at, cols(h)], xbf.at[at, cols(h)], x_s, x_r.at[1 if h == 1 else 0], mate)

    def x_bytes(rows, i):
        return remote(xbf.at[pl.ds(0, rows)], xbf.at[pl.ds(0, rows)], x_s, x_r.at[i], mate)

    def block_of(n):
        m = n - G
        pair = m < 2 * E
        t0 = jnp.where(pair, lax.rem(m, 2), 1)
        b0 = jnp.where(pair, jnp.where(t0 == 0, G, 0) + lax.div(m, 2), m - E)
        b0 = jnp.where(m < 0, n, b0)
        t0 = jnp.where(jnp.logical_xor(home, jnp.logical_or(m < 0, t0 == 0)), 1, 0)
        m = n - 2 * NB
        first = n < 2 * NB
        t = jnp.where(first, t0, 1 - lax.div(m, NB))
        b = jnp.where(first, b0, lax.rem(m, NB))
        return jnp.where(first, other, same) + t * PIECE + b * BR

    def a_copy(n):
        slot = lax.rem(n, RING)
        return pltpu.make_async_copy(a_hbm.at[rows_of(block_of(n), BR)], abuf.at[slot], a_sem.at[slot])

    d_in = pltpu.make_async_copy(d_hbm, dint.at[row], in_sem.at[0])
    v_in = pltpu.make_async_copy(v_hbm, vbuf.at[rows_of(mine, PIECE)], in_sem.at[1])

    def v_copy(r):
        return remote(v_hbm, vbuf.at[rows_of(r * PIECE, PIECE)], fx_s, x_r.at[0], mate)

    def d_copy(r):
        return remote(d_hbm, dint.at[r], x_s, x_r.at[1], mate)

    def s0_copy(r):
        return remote(s0buf.at[r], s0buf.at[r], o_s, o_r, mate)

    def x0_copy(start, c, h, n=1):
        at = pl.ds(pl.multiple_of(start + c * X0R, X0R), n * X0R)
        return remote(xbf.at[at, cols(h)], xbf.at[at, cols(h)], x0_s, x0_r.at[1 if h == 1 else 0], mate)

    a_copy(jnp.int32(0)).start()
    for c in range(X0C):
        x_in(c, 1).start()
    for n in range(1, RING):
        a_copy(jnp.int32(n)).start()

    def take_x(h):
        for c in range(X0C):
            x_in(c, h).wait()

            def convert(i, c=c):
                at = rows_of(mine + c * X0R + i * CH, CH)
                xbf[at, cols(h)] = vbuf[at, cols(h)].astype(jnp.bfloat16)
            loop(0, X0R // CH, convert)
            if c == 0 and h == 0:
                pl.semaphore_wait(barrier, 7)
            x0_copy(mine, c, h).start()

    def half_product(start):
        at = rows_of(start, PIECE)
        return jnp.dot(abuf[0, :, at], xbf[at, cols(0)], preferred_element_type=jnp.float32)

    take_x(0)
    a_copy(jnp.int32(0)).wait()
    first = rows_of(block_of(jnp.int32(0)), BR)
    ybuf[first, cols(0)] = half_product(mine)
    x0_copy(far, 0, 0, X0C).wait_recv()
    ybuf[first, cols(0)] = ybuf[first, cols(0)] + half_product(far)

    @pl.when(home)
    def _():
        c_a(jnp.int32(0), 0).start()

    @pl.when(away)
    def _():
        c_gy(jnp.int32(0), 0).start()
    take_x(1)
    d_in.start()

    @pl.when(away)
    def _():
        d_copy(row).start()
        v_copy(row).start()

    def s_copy(par, off):
        dst_col = lax.rem(col + off, 4)
        return remote(sbuf.at[par, col], sbuf.at[par, col], s_s, s_r.at[par], (dst_col, lax.div(dst_col, 2)))

    def s_bytes(par):
        return remote(sbuf.at[par, pl.ds(0, 3)], sbuf.at[par, pl.ds(0, 3)], s_s, s_r.at[par], mate)

    def s_publish(par, value):
        sbuf[par, col] = jnp.sum(value, axis=0, keepdims=True)
        for off in range(1, 4):
            s_copy(par, off).start()

    def spread(r):
        def group(g):
            flags = dint[r, pl.ds(g, 1), :].astype(jnp.float32)
            dbuf[rows_of(r * PIECE + g * 128, 128), :] = jnp.broadcast_to(flags, (128, 128)).T.astype(jnp.bfloat16)
        loop(0, PIECE // 128, group)

    def flags(start, h):
        d = dbuf[rows_of(start, CH), :].astype(jnp.float32)
        return d if h is not None else jnp.concatenate([d, d], axis=1)

    def fold(w):
        return jnp.sum(w.reshape(CH // 8, 8, w.shape[1]), axis=0)

    def first_mass():
        d_in.wait()
        spread(row)

        def add(c, acc):
            at = mine + c * CH
            return acc + fold(vbuf[rows_of(at, CH), :] * flags(at, None))
        s0buf[row] = lax.fori_loop(0, PIECE // CH, add, jnp.zeros((8, VECS), jnp.float32))

    def new_x(at, own, there, h, one, two):
        y = (ybuf[rows_of(at, CH), cols(h)] + one[there, cols(h)]) + two[there, cols(h)]
        cf = jnp.concatenate([coef[:, cols(h)]] * (CH // 8), axis=0)
        return DAMPING * y + cf * vbuf[rows_of(own, CH), cols(h)]

    def update(t, b, h, one, two, acc):
        def step(c, acc):
            own = t * PIECE + b * BR + c * CH
            x = new_x(same + own, own, rows_of(b * BR + c * CH, CH), h, one, two)
            xbf[rows_of(own, CH), cols(h)] = x.astype(jnp.bfloat16)
            ybuf[rows_of(same + own, CH), cols(h)] = x
            return acc + fold(x * flags(own, h))
        return lax.fori_loop(0, BR // CH, step, acc)

    def keep(t, b, h):
        def step(c):
            there = rows_of(b * BR + c * CH, CH)
            out[there, cols(h)] = ybuf[rows_of(same + t * PIECE + b * BR + c * CH, CH), cols(h)]
        loop(0, BR // CH, step)

    def o_remote(t, b, h=None, n=1):
        return remote(ybuf.at[blocks(same + t * PIECE, b, n), cols(h)], out.at[blocks(0, b, n), cols(h)], o_s, o_r, mate)

    def emit(t, b, h, last):
        @pl.when(jnp.logical_not(last))
        def _():
            c_x(t, b, h).start()

        @pl.when(jnp.logical_and(last, row == t))
        def _():
            keep(t, b, h)

        @pl.when(jnp.logical_and(last, row != t))
        def _():
            o_remote(t, b, h).start()

    def finish(b, h, last, acc):
        arrived(c_fy, b, h)
        acc = update(0, b, h, ra, rfy, acc)
        emit(0, b, h, last)
        arrived(c_fx, b, h)
        acc = update(1, b, h, rdy, rfx, acc)
        emit(1, b, h, last)
        return acc

    def finish_half(h, last):
        part = lax.fori_loop(E, NB, lambda b, acc: finish(b, h, last, acc), jnp.zeros((8, HALF), jnp.float32))
        sacc[:, cols(h)] = sacc[:, cols(h)] + part

    def finish_last():
        def piece(t, b, h):
            arrived(c_fy if t == 0 else c_fx, b, h)
            result(t, b, h)

        def result(t, b, h):
            update(t, b, h, ra if t == 0 else rdy, rfy if t == 0 else rfx, jnp.zeros((8, HALF), jnp.float32))
            emit(t, b, h, jnp.bool_(True))

        for kept in range(2):
            @pl.when(row == kept)
            def _():
                end = jnp.int32(NB - 1)
                for h in range(2):
                    loop(E, NB, lambda b: piece(1 - kept, b, h))
                    loop(E, NB - 1, lambda b: piece(kept, b, h))
                for h in range(2):
                    arrived(c_fy if kept == 0 else c_fx, end, h)
                (held_a() if kept == 0 else held_dy()).wait_recv()
                one, two = (ra, rfy) if kept == 0 else (rdy, rfx)

                def last_rows(c):
                    own = kept * PIECE + (NB - 1) * BR + c * CH
                    there = rows_of((NB - 1) * BR + c * CH, CH)
                    out[there, :] = new_x(same + own, own, there, None, one, two)
                loop(0, BR // CH, last_rows)

    def drain_forward():
        @pl.when(home)
        def _():
            c_fx(0, n=NB).wait_send()

        @pl.when(away)
        def _():
            c_fy(0, n=NB).wait_send()

    def sweep(k, carry):
        last = k == SWEEPS - 1
        more = jnp.logical_not(last)
        par = lax.rem(k, 2)
        hold_a = jnp.logical_and(jnp.logical_and(last, home), row == 0)
        hold_dy = jnp.logical_and(last, row == 1)

        def multiply(n, h):
            start = block_of(n)
            ybuf[rows_of(start, BR), cols(h)] = jnp.dot(
                abuf[lax.rem(n, RING)], xbf[:, cols(h)], preferred_element_type=jnp.float32)

        def fetch(n):
            @pl.when(jnp.logical_not(jnp.logical_and(last, n >= 4 * NB)))
            def _():
                a_copy(lax.rem(n, 4 * NB)).start()

        def lead(h):
            def block(n):
                if h == 0:
                    a_copy(n).wait()
                multiply(n, h)
                if h == 1:
                    fetch(n + RING)

                @pl.when(home)
                def _():
                    c_a(n, h).start()

                @pl.when(away)
                def _():
                    c_gy(n, h).start()

            def one(n):
                @pl.when(jnp.logical_or(k > 0, n > 0))
                def _():
                    block(n)
            loop(0, G, one if h == 0 else block)

        @pl.when(k > 0)
        def _():
            pl.semaphore_wait(cr_0, 1)
        lead(0)

        @pl.when(k == 0)
        def _():
            x0_copy(far, 0, 1, X0C).wait_recv()

        @pl.when(jnp.logical_and(k > 0, home))
        def _():
            finish_half(1, jnp.bool_(False))
            s_publish(par, sacc[...])
            signal(cr_1, xn)
            signal(cr_1, yn)

        @pl.when(jnp.logical_and(k > 0, away))
        def _():
            x_bytes(G * BR, 1).wait_recv()
        lead(1)

        @pl.when(k > 0)
        def _():
            drain_forward()
            pl.semaphore_wait(cr_1, 1)

            @pl.when(away)
            def _():
                pl.semaphore_wait(cr_2, 1)

        def step(n):
            a_copy(n).wait()
            multiply(n, None)
            fetch(n + RING)
            at = block_of(n) - jnp.where(n < 2 * NB, other, same)
            return lax.div(at, PIECE), lax.div(lax.rem(at, PIECE), BR)

        def part_one(n):
            t, b = step(n)

            @pl.when(jnp.logical_and(t == 0, jnp.logical_not(jnp.logical_and(hold_a, b == NB - 1))))
            def _():
                c_a(b).start()

            @pl.when(jnp.logical_and(t == 1, away))
            def _():
                c_gy(b).start()
        loop(G, 2 * NB, part_one)

        @pl.when(k == 0)
        def _():
            first_mass()

            @pl.when(away)
            def _():
                s0_copy(row).start()

            @pl.when(home)
            def _():
                v_in.start()
                d_copy(1 - row).wait_recv()
                s0_copy(1 - row).wait_recv()
                s_publish(0, s0buf[0] + s0buf[1])

        def add_into(start, b, src):
            def add(c):
                at = rows_of(start + b * BR + c * CH, CH)
                ybuf[at, :] = ybuf[at, :] + src[rows_of(b * BR + c * CH, CH), :]
            loop(0, BR // CH, add)

        def send_on(copy, b):
            @pl.when(b < E)
            def _():
                copy(b).start()

            @pl.when(b >= E)
            def _():
                copy(b, 0).start()

        def part_two(n):
            b = n - 2 * NB
            step(n)

            @pl.when(jnp.logical_and(away, jnp.logical_not(jnp.logical_and(hold_dy, b == NB - 1))))
            def _():
                c_dy(b).start()

            @pl.when(home)
            def _():
                @pl.when(lax.rem(b, G) == 0)
                def _():
                    c_gy(b, n=G).wait_recv()
                add_into(other + PIECE, b, rgy)
                send_on(c_fx, b)
        loop(2 * NB, 3 * NB, part_two)

        @pl.when(home)
        def _():
            loop(E, NB, lambda b: c_fx(b, 1).start())

            @pl.when(hold_a)
            def _():
                held_a().start()

        def part_three(n):
            b = n - 3 * NB
            step(n)

            @pl.when(away)
            def _():
                @pl.when(lax.rem(b, G) == 0)
                def _():
                    c_a(b, n=G).wait_recv()
                add_into(same, b, ra)
                send_on(c_fy, b)
        loop(3 * NB, 4 * NB, part_three)

        @pl.when(away)
        def _away():
            loop(E, NB, lambda b: c_fy(b, 1).start())

            @pl.when(hold_dy)
            def _():
                held_dy().start()

            @pl.when(k == 0)
            def _():
                x0_copy(mine, 0, None, X0C).wait_send()
                v_copy(row).wait_send()
                d_copy(row).wait_send()
                s0_copy(row).wait_send()

            @pl.when(more)
            def _():
                signal(cr_2, mate)
                signal(cr_2, xn)
            c_a(0, n=NB).wait_send()
            c_gy(0, n=NB).wait_send()
            c_dy(0, NB).wait_send()

            @pl.when(more)
            def _():
                x_bytes(2 * PIECE - G * BR, 0).wait_recv()

        @pl.when(home)
        def _home():
            @pl.when(more)
            def _():
                signal(cr_0, yn)

            @pl.when(k == 0)
            def _():
                spread(1 - row)
                x0_copy(mine, 0, None, X0C).wait_send()
                v_copy(1 - row).wait_recv()
                v_in.wait()

            @pl.when(k > 0)
            def _():
                x_bytes(2 * PIECE, 0).wait_send()

            s_bytes(par).wait_recv()
            s_bytes(par).wait_send()
            mass = ((sbuf[par, 0] + sbuf[par, 1]) + (sbuf[par, 2] + sbuf[par, 3])) / VERTS
            coef[...] = jnp.broadcast_to(DAMPING * mass + (1.0 - DAMPING), (8, VECS))

            @pl.when(more)
            def _():
                pl.semaphore_wait(cr_2, 1)

            @pl.when(more)
            def _():
                c_a(0, n=NB).wait_send()
            for b in range(0, E, G):
                c_a(b, n=G).wait_recv()

            @pl.when(hold_a)
            def _():
                c_a(E, n=G - 1).wait_recv()

            @pl.when(jnp.logical_not(hold_a))
            def _():
                c_a(E, n=G).wait_recv()

            @pl.when(hold_dy)
            def _():
                c_dy(0, NB - 1).wait_recv()

            @pl.when(jnp.logical_not(hold_dy))
            def _():
                c_dy(0, NB).wait_recv()
            sacc[...] = lax.fori_loop(0, E, lambda b, acc: finish(b, None, last, acc), jnp.zeros((8, VECS), jnp.float32))

            @pl.when(more)
            def _():
                signal(cr_0, xn)
                finish_half(0, jnp.bool_(False))

            @pl.when(last)
            def _():
                finish_last()

        return carry

    lax.fori_loop(0, SWEEPS, sweep, 0)

    drain_forward()

    @pl.when(home)
    def _():
        c_a(0, n=NB).wait_send()
        o_remote(1 - row, 0, n=NB).wait_send()

    @pl.when(away)
    def _():
        o_remote(1 - row, 0, n=NB).wait_recv()


def solution(mesh):
    dma = pltpu.SemaphoreType.DMA
    reg = pltpu.SemaphoreType.REGULAR

    def in_hbm(a):
        return pltpu.with_memory_space_constraint(a, pltpu.HBM)

    def local_sweeps(mat_tile, x_piece, tele_piece, dang_piece):
        part = pltpu.VMEM((PIECE, VECS), jnp.float32)
        return pl.pallas_call(
            kernel,
            name="sweeps",
            out_shape=jax.ShapeDtypeStruct((PIECE, VECS), jnp.float32),
            in_specs=[pl.BlockSpec(memory_space=pltpu.HBM)] * 4,
            out_specs=pl.BlockSpec(memory_space=pltpu.VMEM),
            scratch_shapes=[
                pltpu.VMEM((RING, BR, COLS), jnp.bfloat16),
                pltpu.VMEM((COLS, VECS), jnp.bfloat16),
                pltpu.VMEM((ROWS, VECS), jnp.float32),
                part, part, part, part, part,
                pltpu.VMEM((COLS, VECS), jnp.float32),
                pltpu.VMEM((COLS, 128), jnp.bfloat16),
                pltpu.VMEM((2, PIECE // 128, 128), jnp.int32),
                pltpu.VMEM((2, 4, 1, VECS), jnp.float32),
                pltpu.VMEM((2, 8, VECS), jnp.float32),
                pltpu.VMEM((8, VECS), jnp.float32),
                pltpu.VMEM((8, VECS), jnp.float32),
                dma((RING,)), dma((2 * X0C,)), dma, dma((2,)),
                dma, dma((NB // G,)), dma, dma((NB // G,)), dma, dma, dma, dma((E // G + 4,)), dma, dma((E // G + 4,)),
                dma, dma((2,)), dma, dma((2,)), dma, dma, dma, reg, reg, reg,
            ],
            compiler_params=pltpu.CompilerParams(
                collective_id=0, has_side_effects=True, vmem_limit_bytes=53_300_000),
            cost_estimate=pl.CostEstimate(
                flops=2 * ROWS * COLS * VECS * SWEEPS, bytes_accessed=2 * ROWS * COLS * SWEEPS, transcendentals=0),
        )(mat_tile, x_piece, tele_piece, in_hbm(dang_piece.reshape(PIECE // 128, 128)))

    vec_spec = P(('col', 'row'), None)
    return jax.shard_map(local_sweeps, mesh=mesh,
                         in_specs=(P('row', 'col'), vec_spec, vec_spec, P(('col', 'row'))),
                         out_specs=vec_spec, check_vma=False)
```

```python
import jax
import jax.numpy as jnp
from jax import lax
from jax.experimental import pallas as pl
from jax.experimental.pallas import tpu as pltpu
from jax.sharding import PartitionSpec as P

SWEEPS = 8
DAMPING = 0.85
MESH = pl.DeviceIdType.MESH

VERTS = 24576
VECS = 256
HALF = 128
PIECE = 3072
ROWS = 12288
COLS = 6144
BR = 256
NB = PIECE // BR
G = 4
E = NB - G
CH = 32
RING = 4
X0C = 3
X0R = PIECE // X0C


def kernel(a_hbm, x_hbm, v_hbm, d_hbm, out,
           abuf, xbf, ybuf, ra, rgy, rdy, rfx, rfy, vbuf, dbuf, dint, sbuf, s0buf, coef, sacc,
           a_sem, in_sem, x0_s, x0_r,
           a_s, a_r, gy_s, gy_r, dy_s, dy_r, fx_s, fx_r, fy_s, fy_r,
           x_s, x_r, s_s, s_r, o_s, o_r, held_r, cr_0, cr_1, cr_2):
    col = lax.axis_index('col')
    row = lax.axis_index('row')
    cx, cy = lax.rem(col, 2), lax.div(col, 2)
    home = row == cy
    away = jnp.logical_not(home)
    xn = (cy * 2 + 1 - cx, row)
    yn = ((1 - cy) * 2 + cx, row)
    mate = (col, 1 - row)
    same = cx * COLS
    other = (1 - cx) * COLS
    mine = row * PIECE
    far = (1 - row) * PIECE

    def rows_of(start, size):
        return pl.ds(pl.multiple_of(start, size), size)

    def blocks(start, b, n):
        return pl.ds(pl.multiple_of(start + b * BR, BR), n * BR)

    def cols(h):
        return pl.ds(0, VECS) if h is None else pl.ds(h * HALF, HALF)

    def remote(src, dst, send, recv, dev):
        return pltpu.make_async_remote_copy(
            src_ref=src, dst_ref=dst, send_sem=send, recv_sem=recv, device_id=dev, device_id_type=MESH)

    def loop(lo, hi, body):
        def step(i, c):
            body(i)
            return c
        lax.fori_loop(lo, hi, step, 0)

    def signal(sem, dev):
        pl.semaphore_signal(sem, inc=1, device_id=dev, device_id_type=MESH)

    def x_in(c, h):
        return pltpu.make_async_copy(x_hbm.at[rows_of(c * X0R, X0R), cols(h)], vbuf.at[rows_of(mine + c * X0R, X0R), cols(h)],
                                     in_sem.at[h * X0C + c])

    for c in range(X0C):
        x_in(c, 0).start()

    barrier = pltpu.get_barrier_semaphore()
    for off in range(4):
        for r in range(2):
            if off == 0 and r == 1:
                continue
            signal(barrier, (lax.rem(col + off, 4), row if r == 0 and off else 1 - row))

    def flow(start, b, n, h, dst, send, recv, i, dev):
        return remote(ybuf.at[blocks(start, b, n), cols(h)], dst.at[blocks(0, b, n), cols(h)], send, recv.at[i], dev)

    def c_a(b, h=None, n=1):
        return flow(other, b, n, h, ra, a_s, a_r, lax.div(b, G), xn)

    def c_gy(b, h=None, n=1):
        return flow(other + PIECE, b, n, h, rgy, gy_s, gy_r, lax.div(b, G), yn)

    def c_dy(b, n=1):
        return remote(ybuf.at[blocks(same + PIECE, b, n)], rdy.at[blocks(0, b, n)], dy_s, dy_r, yn)

    def held_a():
        return remote(ybuf.at[blocks(other, NB - 1, 1)], ra.at[blocks(0, NB - 1, 1)], a_s, held_r, xn)

    def held_dy():
        return remote(ybuf.at[blocks(same + PIECE, NB - 1, 1)], rdy.at[blocks(0, NB - 1, 1)], dy_s, held_r, yn)

    def late(b, h):
        return lax.div(b, G) if h is None else E // G + 2 * h + jnp.where(b == NB - 1, 1, 0)

    def c_fx(b, h=None, n=1):
        return flow(other + PIECE, b, n, h, rfx, fx_s, fx_r, late(b, h), xn)

    def c_fy(b, h=None, n=1):
        return flow(same, b, n, h, rfy, fy_s, fy_r, late(b, h), yn)

    def arrived(copy, b, h):
        if h is None:
            @pl.when(lax.rem(b, G) == 0)
            def _():
                copy(b, n=G).wait_recv()
        else:
            @pl.when(b == E)
            def _():
                copy(b, h, n=G - 1).wait_recv()

            @pl.when(b == NB - 1)
            def _():
                copy(b, h).wait_recv()

    def c_x(t, b, h=None):
        at = blocks(t * PIECE, b, 1)
        return remote(xbf.at[at, cols(h)], xbf.at[at, cols(h)], x_s, x_r.at[1 if h == 1 else 0], mate)

    def x_bytes(rows, i):
        return remote(xbf.at[pl.ds(0, rows)], xbf.at[pl.ds(0, rows)], x_s, x_r.at[i], mate)

    def block_of(n):
        m = n - G
        pair = m < 2 * E
        t0 = jnp.where(pair, lax.rem(m, 2), 1)
        b0 = jnp.where(pair, jnp.where(t0 == 0, G, 0) + lax.div(m, 2), m - E)
        b0 = jnp.where(m < 0, n, b0)
        t0 = jnp.where(jnp.logical_xor(home, jnp.logical_or(m < 0, t0 == 0)), 1, 0)
        m = n - 2 * NB
        first = n < 2 * NB
        t = jnp.where(first, t0, 1 - lax.div(m, NB))
        b = jnp.where(first, b0, lax.rem(m, NB))
        return jnp.where(first, other, same) + t * PIECE + b * BR

    def a_copy(n):
        slot = lax.rem(n, RING)
        return pltpu.make_async_copy(a_hbm.at[rows_of(block_of(n), BR)], abuf.at[slot], a_sem.at[slot])

    d_in = pltpu.make_async_copy(d_hbm, dint.at[row], in_sem.at[0])
    v_in = pltpu.make_async_copy(v_hbm, vbuf.at[rows_of(mine, PIECE)], in_sem.at[1])

    def v_copy(r):
        return remote(v_hbm, vbuf.at[rows_of(r * PIECE, PIECE)], fx_s, x_r.at[0], mate)

    def d_copy(r):
        return remote(d_hbm, dint.at[r], x_s, x_r.at[1], mate)

    def s0_copy(r):
        return remote(s0buf.at[r], s0buf.at[r], o_s, o_r, mate)

    def x0_copy(start, c, h, n=1):
        at = pl.ds(pl.multiple_of(start + c * X0R, X0R), n * X0R)
        return remote(xbf.at[at, cols(h)], xbf.at[at, cols(h)], x0_s, x0_r.at[1 if h == 1 else 0], mate)

    a_copy(jnp.int32(0)).start()
    for c in range(X0C):
        x_in(c, 1).start()
    for n in range(1, RING):
        a_copy(jnp.int32(n)).start()

    def take_x(h):
        for c in range(X0C):
            x_in(c, h).wait()

            def convert(i, c=c):
                at = rows_of(mine + c * X0R + i * CH, CH)
                xbf[at, cols(h)] = vbuf[at, cols(h)].astype(jnp.bfloat16)
            loop(0, X0R // CH, convert)
            if c == 0 and h == 0:
                pl.semaphore_wait(barrier, 7)
            x0_copy(mine, c, h).start()

    def half_product(start):
        at = rows_of(start, PIECE)
        return jnp.dot(abuf[0, :, at], xbf[at, cols(0)], preferred_element_type=jnp.float32)

    take_x(0)
    a_copy(jnp.int32(0)).wait()
    first = rows_of(block_of(jnp.int32(0)), BR)
    ybuf[first, cols(0)] = half_product(mine)
    x0_copy(far, 0, 0, X0C).wait_recv()
    ybuf[first, cols(0)] = ybuf[first, cols(0)] + half_product(far)

    def send_lead(n, h):
        @pl.when(home)
        def _():
            c_a(n, h).start()

        @pl.when(away)
        def _():
            c_gy(n, h).start()

    send_lead(jnp.int32(0), 0)
    a_copy(jnp.int32(1)).wait()
    ybuf[rows_of(block_of(jnp.int32(1)), BR), cols(0)] = jnp.dot(
        abuf[1], xbf[:, cols(0)], preferred_element_type=jnp.float32)
    send_lead(jnp.int32(1), 0)
    take_x(1)
    d_in.start()

    @pl.when(away)
    def _():
        d_copy(row).start()
        v_copy(row).start()

    def s_copy(par, off):
        dst_col = lax.rem(col + off, 4)
        return remote(sbuf.at[par, col], sbuf.at[par, col], s_s, s_r.at[par], (dst_col, lax.div(dst_col, 2)))

    def s_bytes(par):
        return remote(sbuf.at[par, pl.ds(0, 3)], sbuf.at[par, pl.ds(0, 3)], s_s, s_r.at[par], mate)

    def s_publish(par, value):
        sbuf[par, col] = jnp.sum(value, axis=0, keepdims=True)
        for off in range(1, 4):
            s_copy(par, off).start()

    def spread(r):
        def group(g):
            flags = dint[r, pl.ds(g, 1), :].astype(jnp.float32)
            dbuf[rows_of(r * PIECE + g * 128, 128), :] = jnp.broadcast_to(flags, (128, 128)).T.astype(jnp.bfloat16)
        loop(0, PIECE // 128, group)

    def flags(start, h):
        d = dbuf[rows_of(start, CH), :].astype(jnp.float32)
        return d if h is not None else jnp.concatenate([d, d], axis=1)

    def fold(w):
        return jnp.sum(w.reshape(CH // 8, 8, w.shape[1]), axis=0)

    def first_mass():
        d_in.wait()
        spread(row)

        def add(c, acc):
            at = mine + c * CH
            return acc + fold(vbuf[rows_of(at, CH), :] * flags(at, None))
        s0buf[row] = lax.fori_loop(0, PIECE // CH, add, jnp.zeros((8, VECS), jnp.float32))

    def new_x(at, own, there, h, one, two):
        y = (ybuf[rows_of(at, CH), cols(h)] + one[there, cols(h)]) + two[there, cols(h)]
        cf = jnp.concatenate([coef[:, cols(h)]] * (CH // 8), axis=0)
        return DAMPING * y + cf * vbuf[rows_of(own, CH), cols(h)]

    def update(t, b, h, one, two, acc):
        def step(c, acc):
            own = t * PIECE + b * BR + c * CH
            x = new_x(same + own, own, rows_of(b * BR + c * CH, CH), h, one, two)
            xbf[rows_of(own, CH), cols(h)] = x.astype(jnp.bfloat16)
            ybuf[rows_of(same + own, CH), cols(h)] = x
            return acc + fold(x * flags(own, h))
        return lax.fori_loop(0, BR // CH, step, acc)

    def keep(t, b, h):
        def step(c):
            there = rows_of(b * BR + c * CH, CH)
            out[there, cols(h)] = ybuf[rows_of(same + t * PIECE + b * BR + c * CH, CH), cols(h)]
        loop(0, BR // CH, step)

    def o_remote(t, b, h=None, n=1):
        return remote(ybuf.at[blocks(same + t * PIECE, b, n), cols(h)], out.at[blocks(0, b, n), cols(h)], o_s, o_r, mate)

    def emit(t, b, h, last):
        @pl.when(jnp.logical_not(last))
        def _():
            c_x(t, b, h).start()

        @pl.when(jnp.logical_and(last, row == t))
        def _():
            keep(t, b, h)

        @pl.when(jnp.logical_and(last, row != t))
        def _():
            o_remote(t, b, h).start()

    def finish(b, h, last, acc):
        arrived(c_fy, b, h)
        acc = update(0, b, h, ra, rfy, acc)
        emit(0, b, h, last)
        arrived(c_fx, b, h)
        acc = update(1, b, h, rdy, rfx, acc)
        emit(1, b, h, last)
        return acc

    def finish_half(h, last):
        part = lax.fori_loop(E, NB, lambda b, acc: finish(b, h, last, acc), jnp.zeros((8, HALF), jnp.float32))
        sacc[:, cols(h)] = sacc[:, cols(h)] + part

    def finish_last():
        def piece(t, b, h):
            arrived(c_fy if t == 0 else c_fx, b, h)
            result(t, b, h)

        def result(t, b, h):
            update(t, b, h, ra if t == 0 else rdy, rfy if t == 0 else rfx, jnp.zeros((8, HALF), jnp.float32))
            emit(t, b, h, jnp.bool_(True))

        for kept in range(2):
            @pl.when(row == kept)
            def _():
                end = jnp.int32(NB - 1)
                for h in range(2):
                    loop(E, NB, lambda b: piece(1 - kept, b, h))
                    loop(E, NB - 1, lambda b: piece(kept, b, h))
                for h in range(2):
                    arrived(c_fy if kept == 0 else c_fx, end, h)
                (held_a() if kept == 0 else held_dy()).wait_recv()
                one, two = (ra, rfy) if kept == 0 else (rdy, rfx)

                def last_rows(c):
                    own = kept * PIECE + (NB - 1) * BR + c * CH
                    there = rows_of((NB - 1) * BR + c * CH, CH)
                    out[there, :] = new_x(same + own, own, there, None, one, two)
                loop(0, BR // CH, last_rows)

    def drain_forward():
        @pl.when(home)
        def _():
            c_fx(0, n=NB).wait_send()

        @pl.when(away)
        def _():
            c_fy(0, n=NB).wait_send()

    def sweep(k, carry):
        last = k == SWEEPS - 1
        more = jnp.logical_not(last)
        par = lax.rem(k, 2)
        hold_a = jnp.logical_and(jnp.logical_and(last, home), row == 0)
        hold_dy = jnp.logical_and(last, row == 1)

        def multiply(n, h):
            start = block_of(n)
            ybuf[rows_of(start, BR), cols(h)] = jnp.dot(
                abuf[lax.rem(n, RING)], xbf[:, cols(h)], preferred_element_type=jnp.float32)

        def fetch(n):
            @pl.when(jnp.logical_not(jnp.logical_and(last, n >= 4 * NB)))
            def _():
                a_copy(lax.rem(n, 4 * NB)).start()

        def lead(h):
            def block(n):
                if h == 0:
                    a_copy(n).wait()
                multiply(n, h)
                if h == 1:
                    fetch(n + RING)

                send_lead(n, h)

            def one(n):
                @pl.when(jnp.logical_or(k > 0, n > 1))
                def _():
                    block(n)
            loop(0, G, one if h == 0 else block)

        @pl.when(k > 0)
        def _():
            pl.semaphore_wait(cr_0, 1)
        lead(0)

        @pl.when(k == 0)
        def _():
            x0_copy(far, 0, 1, X0C).wait_recv()

        @pl.when(jnp.logical_and(k > 0, home))
        def _():
            finish_half(1, jnp.bool_(False))
            s_publish(par, sacc[...])
            signal(cr_1, xn)
            signal(cr_1, yn)

        @pl.when(jnp.logical_and(k > 0, away))
        def _():
            x_bytes(G * BR, 1).wait_recv()
        lead(1)

        @pl.when(k > 0)
        def _():
            drain_forward()
            pl.semaphore_wait(cr_1, 1)

            @pl.when(away)
            def _():
                pl.semaphore_wait(cr_2, 1)

        def step(n):
            a_copy(n).wait()
            multiply(n, None)
            fetch(n + RING)
            at = block_of(n) - jnp.where(n < 2 * NB, other, same)
            return lax.div(at, PIECE), lax.div(lax.rem(at, PIECE), BR)

        def part_one(n):
            t, b = step(n)

            @pl.when(jnp.logical_and(t == 0, jnp.logical_not(jnp.logical_and(hold_a, b == NB - 1))))
            def _():
                c_a(b).start()

            @pl.when(jnp.logical_and(t == 1, away))
            def _():
                c_gy(b).start()
        loop(G, 2 * NB, part_one)

        @pl.when(k == 0)
        def _():
            first_mass()

            @pl.when(away)
            def _():
                s0_copy(row).start()

            @pl.when(home)
            def _():
                v_in.start()
                d_copy(1 - row).wait_recv()
                s0_copy(1 - row).wait_recv()
                s_publish(0, s0buf[0] + s0buf[1])

        def add_into(start, b, src):
            def add(c):
                at = rows_of(start + b * BR + c * CH, CH)
                ybuf[at, :] = ybuf[at, :] + src[rows_of(b * BR + c * CH, CH), :]
            loop(0, BR // CH, add)

        def send_on(copy, b):
            @pl.when(b < E)
            def _():
                copy(b).start()

            @pl.when(b >= E)
            def _():
                copy(b, 0).start()

        def part_two(n):
            b = n - 2 * NB
            step(n)

            @pl.when(jnp.logical_and(away, jnp.logical_not(jnp.logical_and(hold_dy, b == NB - 1))))
            def _():
                c_dy(b).start()

            @pl.when(home)
            def _():
                @pl.when(lax.rem(b, G) == 0)
                def _():
                    c_gy(b, n=G).wait_recv()
                add_into(other + PIECE, b, rgy)
                send_on(c_fx, b)
        loop(2 * NB, 3 * NB, part_two)

        @pl.when(home)
        def _():
            loop(E, NB, lambda b: c_fx(b, 1).start())

            @pl.when(hold_a)
            def _():
                held_a().start()

        def part_three(n):
            b = n - 3 * NB
            step(n)

            @pl.when(away)
            def _():
                @pl.when(lax.rem(b, G) == 0)
                def _():
                    c_a(b, n=G).wait_recv()
                add_into(same, b, ra)
                send_on(c_fy, b)
        loop(3 * NB, 4 * NB, part_three)

        @pl.when(away)
        def _away():
            loop(E, NB, lambda b: c_fy(b, 1).start())

            @pl.when(hold_dy)
            def _():
                held_dy().start()

            @pl.when(k == 0)
            def _():
                x0_copy(mine, 0, None, X0C).wait_send()
                v_copy(row).wait_send()
                d_copy(row).wait_send()
                s0_copy(row).wait_send()

            @pl.when(more)
            def _():
                signal(cr_2, mate)
                signal(cr_2, xn)
            c_a(0, n=NB).wait_send()
            c_gy(0, n=NB).wait_send()
            c_dy(0, NB).wait_send()

            @pl.when(more)
            def _():
                x_bytes(2 * PIECE - G * BR, 0).wait_recv()

        @pl.when(home)
        def _home():
            @pl.when(more)
            def _():
                signal(cr_0, yn)

            @pl.when(k == 0)
            def _():
                spread(1 - row)
                x0_copy(mine, 0, None, X0C).wait_send()
                v_copy(1 - row).wait_recv()
                v_in.wait()

            @pl.when(k > 0)
            def _():
                x_bytes(2 * PIECE, 0).wait_send()

            s_bytes(par).wait_recv()
            s_bytes(par).wait_send()
            mass = ((sbuf[par, 0] + sbuf[par, 1]) + (sbuf[par, 2] + sbuf[par, 3])) / VERTS
            coef[...] = jnp.broadcast_to(DAMPING * mass + (1.0 - DAMPING), (8, VECS))

            @pl.when(more)
            def _():
                pl.semaphore_wait(cr_2, 1)

            @pl.when(more)
            def _():
                c_a(0, n=NB).wait_send()
            for b in range(0, E, G):
                c_a(b, n=G).wait_recv()

            @pl.when(hold_a)
            def _():
                c_a(E, n=G - 1).wait_recv()

            @pl.when(jnp.logical_not(hold_a))
            def _():
                c_a(E, n=G).wait_recv()

            @pl.when(hold_dy)
            def _():
                c_dy(0, NB - 1).wait_recv()

            @pl.when(jnp.logical_not(hold_dy))
            def _():
                c_dy(0, NB).wait_recv()
            sacc[...] = lax.fori_loop(0, E, lambda b, acc: finish(b, None, last, acc), jnp.zeros((8, VECS), jnp.float32))

            @pl.when(more)
            def _():
                signal(cr_0, xn)
                finish_half(0, jnp.bool_(False))

            @pl.when(last)
            def _():
                finish_last()

        return carry

    lax.fori_loop(0, SWEEPS, sweep, 0)

    drain_forward()

    @pl.when(home)
    def _():
        c_a(0, n=NB).wait_send()
        o_remote(1 - row, 0, n=NB).wait_send()

    @pl.when(away)
    def _():
        o_remote(1 - row, 0, n=NB).wait_recv()


def solution(mesh):
    dma = pltpu.SemaphoreType.DMA
    reg = pltpu.SemaphoreType.REGULAR

    def in_hbm(a):
        return pltpu.with_memory_space_constraint(a, pltpu.HBM)

    def local_sweeps(mat_tile, x_piece, tele_piece, dang_piece):
        part = pltpu.VMEM((PIECE, VECS), jnp.float32)
        return pl.pallas_call(
            kernel,
            name="sweeps",
            out_shape=jax.ShapeDtypeStruct((PIECE, VECS), jnp.float32),
            in_specs=[pl.BlockSpec(memory_space=pltpu.HBM)] * 4,
            out_specs=pl.BlockSpec(memory_space=pltpu.VMEM),
            scratch_shapes=[
                pltpu.VMEM((RING, BR, COLS), jnp.bfloat16),
                pltpu.VMEM((COLS, VECS), jnp.bfloat16),
                pltpu.VMEM((ROWS, VECS), jnp.float32),
                part, part, part, part, part,
                pltpu.VMEM((COLS, VECS), jnp.float32),
                pltpu.VMEM((COLS, 128), jnp.bfloat16),
                pltpu.VMEM((2, PIECE // 128, 128), jnp.int32),
                pltpu.VMEM((2, 4, 1, VECS), jnp.float32),
                pltpu.VMEM((2, 8, VECS), jnp.float32),
                pltpu.VMEM((8, VECS), jnp.float32),
                pltpu.VMEM((8, VECS), jnp.float32),
                dma((RING,)), dma((2 * X0C,)), dma, dma((2,)),
                dma, dma((NB // G,)), dma, dma((NB // G,)), dma, dma, dma, dma((E // G + 4,)), dma, dma((E // G + 4,)),
                dma, dma((2,)), dma, dma((2,)), dma, dma, dma, reg, reg, reg,
            ],
            compiler_params=pltpu.CompilerParams(
                collective_id=0, has_side_effects=True, vmem_limit_bytes=53_300_000),
            cost_estimate=pl.CostEstimate(
                flops=2 * ROWS * COLS * VECS * SWEEPS, bytes_accessed=2 * ROWS * COLS * SWEEPS, transcendentals=0),
        )(mat_tile, x_piece, tele_piece, in_hbm(dang_piece.reshape(PIECE // 128, 128)))

    vec_spec = P(('col', 'row'), None)
    return jax.shard_map(local_sweeps, mesh=mesh,
                         in_specs=(P('row', 'col'), vec_spec, vec_spec, P(('col', 'row'))),
                         out_specs=vec_spec, check_vma=False)
```

```python
import jax
import jax.numpy as jnp
from jax import lax
from jax.experimental import pallas as pl
from jax.experimental.pallas import tpu as pltpu
from jax.sharding import PartitionSpec as P

SWEEPS = 8
DAMPING = 0.85
MESH = pl.DeviceIdType.MESH

VERTS = 24576
VECS = 256
HALF = 128
PIECE = 3072
ROWS = 12288
COLS = 6144
BR = 256
NB = PIECE // BR
G = 4
E = NB - G
CH = 32
RING = 4
X0C = 3
X0R = PIECE // X0C


def kernel(a_hbm, x_hbm, v_hbm, d_hbm, out,
           abuf, xbf, ybuf, ra, rgy, rdy, rfx, rfy, vbuf, dbuf, dint, sbuf, s0buf, coef, sacc,
           a_sem, in_sem, x0_s, x0_r,
           a_s, a_r, gy_s, gy_r, dy_s, dy_r, fx_s, fx_r, fy_s, fy_r,
           x_s, x_r, s_s, s_r, o_s, o_r, held_r, cr_0, cr_1, cr_2):
    col = lax.axis_index('col')
    row = lax.axis_index('row')
    cx, cy = lax.rem(col, 2), lax.div(col, 2)
    home = row == cy
    away = jnp.logical_not(home)
    xn = (cy * 2 + 1 - cx, row)
    yn = ((1 - cy) * 2 + cx, row)
    mate = (col, 1 - row)
    same = cx * COLS
    other = (1 - cx) * COLS
    mine = row * PIECE
    far = (1 - row) * PIECE

    def rows_of(start, size):
        return pl.ds(pl.multiple_of(start, size), size)

    def blocks(start, b, n):
        return pl.ds(pl.multiple_of(start + b * BR, BR), n * BR)

    def cols(h):
        return pl.ds(0, VECS) if h is None else pl.ds(h * HALF, HALF)

    def remote(src, dst, send, recv, dev):
        return pltpu.make_async_remote_copy(
            src_ref=src, dst_ref=dst, send_sem=send, recv_sem=recv, device_id=dev, device_id_type=MESH)

    def loop(lo, hi, body):
        def step(i, c):
            body(i)
            return c
        lax.fori_loop(lo, hi, step, 0)

    def signal(sem, dev):
        pl.semaphore_signal(sem, inc=1, device_id=dev, device_id_type=MESH)

    def x_in(c, h):
        return pltpu.make_async_copy(x_hbm.at[rows_of(c * X0R, X0R), cols(h)], vbuf.at[rows_of(mine + c * X0R, X0R), cols(h)],
                                     in_sem.at[h * X0C + c])

    for c in range(X0C):
        x_in(c, 0).start()

    barrier = pltpu.get_barrier_semaphore()
    for off in range(4):
        for r in range(2):
            if off == 0 and r == 1:
                continue
            signal(barrier, (lax.rem(col + off, 4), row if r == 0 and off else 1 - row))

    def flow(start, b, n, h, dst, send, recv, i, dev):
        return remote(ybuf.at[blocks(start, b, n), cols(h)], dst.at[blocks(0, b, n), cols(h)], send, recv.at[i], dev)

    def c_a(b, h=None, n=1):
        return flow(other, b, n, h, ra, a_s, a_r, lax.div(b, G), xn)

    def c_gy(b, h=None, n=1):
        return flow(other + PIECE, b, n, h, rgy, gy_s, gy_r, lax.div(b, G), yn)

    def c_dy(b, n=1):
        return remote(ybuf.at[blocks(same + PIECE, b, n)], rdy.at[blocks(0, b, n)], dy_s, dy_r, yn)

    def held_a():
        return remote(ybuf.at[blocks(other, NB - 1, 1)], ra.at[blocks(0, NB - 1, 1)], a_s, held_r, xn)

    def held_dy():
        return remote(ybuf.at[blocks(same + PIECE, NB - 1, 1)], rdy.at[blocks(0, NB - 1, 1)], dy_s, held_r, yn)

    def late(b, h):
        return lax.div(b, G) if h is None else E // G + 2 * h + jnp.where(b == NB - 1, 1, 0)

    def c_fx(b, h=None, n=1):
        return flow(other + PIECE, b, n, h, rfx, fx_s, fx_r, late(b, h), xn)

    def c_fy(b, h=None, n=1):
        return flow(same, b, n, h, rfy, fy_s, fy_r, late(b, h), yn)

    def arrived(copy, b, h):
        if h is None:
            @pl.when(lax.rem(b, G) == 0)
            def _():
                copy(b, n=G).wait_recv()
        else:
            @pl.when(b == E)
            def _():
                copy(b, h, n=G - 1).wait_recv()

            @pl.when(b == NB - 1)
            def _():
                copy(b, h).wait_recv()

    def c_x(t, b, h=None):
        at = blocks(t * PIECE, b, 1)
        return remote(xbf.at[at, cols(h)], xbf.at[at, cols(h)], x_s, x_r.at[1 if h == 1 else 0], mate)

    def x_bytes(rows, i):
        return remote(xbf.at[pl.ds(0, rows)], xbf.at[pl.ds(0, rows)], x_s, x_r.at[i], mate)

    def block_of(n):
        m = n - G
        pair = m < 2 * E
        t0 = jnp.where(pair, lax.rem(m, 2), 1)
        b0 = jnp.where(pair, jnp.where(t0 == 0, G, 0) + lax.div(m, 2), m - E)
        b0 = jnp.where(m < 0, n, b0)
        t0 = jnp.where(jnp.logical_xor(home, jnp.logical_or(m < 0, t0 == 0)), 1, 0)
        m = n - 2 * NB
        first = n < 2 * NB
        t = jnp.where(first, t0, 1 - lax.div(m, NB))
        b = jnp.where(first, b0, lax.rem(m, NB))
        return jnp.where(first, other, same) + t * PIECE + b * BR

    def a_copy(n):
        slot = lax.rem(n, RING)
        return pltpu.make_async_copy(a_hbm.at[rows_of(block_of(n), BR)], abuf.at[slot], a_sem.at[slot])

    d_in = pltpu.make_async_copy(d_hbm, dint.at[row], in_sem.at[0])
    v_in = pltpu.make_async_copy(v_hbm, vbuf.at[rows_of(mine, PIECE)], in_sem.at[1])

    def v_copy(r):
        return remote(v_hbm, vbuf.at[rows_of(r * PIECE, PIECE)], fx_s, x_r.at[0], mate)

    def d_copy(r):
        return remote(d_hbm, dint.at[r], x_s, x_r.at[1], mate)

    def s0_copy(r):
        return remote(s0buf.at[r], s0buf.at[r], o_s, o_r, mate)

    def x0_copy(start, c, h, n=1):
        at = pl.ds(pl.multiple_of(start + c * X0R, X0R), n * X0R)
        return remote(xbf.at[at, cols(h)], xbf.at[at, cols(h)], x0_s, x0_r.at[1 if h == 1 else 0], mate)

    a_copy(jnp.int32(0)).start()
    for c in range(X0C):
        x_in(c, 1).start()
    for n in range(1, RING):
        a_copy(jnp.int32(n)).start()

    def take_x(h):
        for c in range(X0C):
            x_in(c, h).wait()

            def convert(i, c=c):
                at = rows_of(mine + c * X0R + i * HALF, HALF)
                xbf[at, cols(h)] = vbuf[at, cols(h)].astype(jnp.bfloat16)
            loop(0, X0R // HALF, convert)
            if c == 0 and h == 0:
                pl.semaphore_wait(barrier, 7)
            x0_copy(mine, c, h).start()

    def half_product(start):
        at = rows_of(start, PIECE)
        return jnp.dot(abuf[0, :, at], xbf[at, cols(0)], preferred_element_type=jnp.float32)

    take_x(0)
    a_copy(jnp.int32(0)).wait()
    first = rows_of(block_of(jnp.int32(0)), BR)
    ybuf[first, cols(0)] = half_product(mine)
    x0_copy(far, 0, 0, X0C).wait_recv()
    ybuf[first, cols(0)] = ybuf[first, cols(0)] + half_product(far)

    def send_lead(n, h):
        @pl.when(home)
        def _():
            c_a(n, h).start()

        @pl.when(away)
        def _():
            c_gy(n, h).start()

    send_lead(jnp.int32(0), 0)
    a_copy(jnp.int32(1)).wait()
    ybuf[rows_of(block_of(jnp.int32(1)), BR), cols(0)] = jnp.dot(
        abuf[1], xbf[:, cols(0)], preferred_element_type=jnp.float32)
    send_lead(jnp.int32(1), 0)
    take_x(1)
    d_in.start()

    @pl.when(away)
    def _():
        d_copy(row).start()
        v_copy(row).start()

    def s_copy(par, off):
        dst_col = lax.rem(col + off, 4)
        return remote(sbuf.at[par, col], sbuf.at[par, col], s_s, s_r.at[par], (dst_col, lax.div(dst_col, 2)))

    def s_bytes(par):
        return remote(sbuf.at[par, pl.ds(0, 3)], sbuf.at[par, pl.ds(0, 3)], s_s, s_r.at[par], mate)

    def s_publish(par, value):
        sbuf[par, col] = jnp.sum(value, axis=0, keepdims=True)
        for off in range(1, 4):
            s_copy(par, off).start()

    def spread(r):
        def group(g):
            flags = dint[r, pl.ds(g, 1), :].astype(jnp.float32)
            dbuf[rows_of(r * PIECE + g * 128, 128), :] = jnp.broadcast_to(flags, (128, 128)).T.astype(jnp.bfloat16)
        loop(0, PIECE // 128, group)

    def flags(start, h):
        d = dbuf[rows_of(start, CH), :].astype(jnp.float32)
        return d if h is not None else jnp.concatenate([d, d], axis=1)

    def fold(w):
        return jnp.sum(w.reshape(CH // 8, 8, w.shape[1]), axis=0)

    def first_mass():
        d_in.wait()
        spread(row)

        def add(c, acc):
            at = mine + c * CH
            return acc + fold(vbuf[rows_of(at, CH), :] * flags(at, None))
        s0buf[row] = lax.fori_loop(0, PIECE // CH, add, jnp.zeros((8, VECS), jnp.float32))

    def new_x(at, own, there, h, one, two):
        y = (ybuf[rows_of(at, CH), cols(h)] + one[there, cols(h)]) + two[there, cols(h)]
        cf = jnp.concatenate([coef[:, cols(h)]] * (CH // 8), axis=0)
        return DAMPING * y + cf * vbuf[rows_of(own, CH), cols(h)]

    def update(t, b, h, one, two, acc):
        def step(c, acc):
            own = t * PIECE + b * BR + c * CH
            x = new_x(same + own, own, rows_of(b * BR + c * CH, CH), h, one, two)
            xbf[rows_of(own, CH), cols(h)] = x.astype(jnp.bfloat16)
            ybuf[rows_of(same + own, CH), cols(h)] = x
            return acc + fold(x * flags(own, h))
        return lax.fori_loop(0, BR // CH, step, acc)

    def keep(t, b, h):
        def step(c):
            there = rows_of(b * BR + c * CH, CH)
            out[there, cols(h)] = ybuf[rows_of(same + t * PIECE + b * BR + c * CH, CH), cols(h)]
        loop(0, BR // CH, step)

    def o_remote(t, b, h=None, n=1):
        return remote(ybuf.at[blocks(same + t * PIECE, b, n), cols(h)], out.at[blocks(0, b, n), cols(h)], o_s, o_r, mate)

    def emit(t, b, h, last):
        @pl.when(jnp.logical_not(last))
        def _():
            c_x(t, b, h).start()

        @pl.when(jnp.logical_and(last, row == t))
        def _():
            keep(t, b, h)

        @pl.when(jnp.logical_and(last, row != t))
        def _():
            o_remote(t, b, h).start()

    def finish(b, h, last, acc):
        arrived(c_fy, b, h)
        acc = update(0, b, h, ra, rfy, acc)
        emit(0, b, h, last)
        arrived(c_fx, b, h)
        acc = update(1, b, h, rdy, rfx, acc)
        emit(1, b, h, last)
        return acc

    def finish_half(h, last):
        part = lax.fori_loop(E, NB, lambda b, acc: finish(b, h, last, acc), jnp.zeros((8, HALF), jnp.float32))
        sacc[:, cols(h)] = sacc[:, cols(h)] + part

    def finish_last():
        def piece(t, b, h):
            arrived(c_fy if t == 0 else c_fx, b, h)
            result(t, b, h)

        def result(t, b, h):
            update(t, b, h, ra if t == 0 else rdy, rfy if t == 0 else rfx, jnp.zeros((8, HALF), jnp.float32))
            emit(t, b, h, jnp.bool_(True))

        for kept in range(2):
            @pl.when(row == kept)
            def _():
                end = jnp.int32(NB - 1)
                for h in range(2):
                    loop(E, NB, lambda b: piece(1 - kept, b, h))
                    loop(E, NB - 1, lambda b: piece(kept, b, h))
                for h in range(2):
                    arrived(c_fy if kept == 0 else c_fx, end, h)
                (held_a() if kept == 0 else held_dy()).wait_recv()
                one, two = (ra, rfy) if kept == 0 else (rdy, rfx)

                def last_rows(c):
                    own = kept * PIECE + (NB - 1) * BR + c * CH
                    there = rows_of((NB - 1) * BR + c * CH, CH)
                    out[there, :] = new_x(same + own, own, there, None, one, two)
                loop(0, BR // CH, last_rows)

    def drain_forward():
        @pl.when(home)
        def _():
            c_fx(0, n=NB).wait_send()

        @pl.when(away)
        def _():
            c_fy(0, n=NB).wait_send()

    def sweep(k, carry):
        last = k == SWEEPS - 1
        more = jnp.logical_not(last)
        par = lax.rem(k, 2)
        hold_a = jnp.logical_and(jnp.logical_and(last, home), row == 0)
        hold_dy = jnp.logical_and(last, row == 1)

        def multiply(n, h):
            start = block_of(n)
            ybuf[rows_of(start, BR), cols(h)] = jnp.dot(
                abuf[lax.rem(n, RING)], xbf[:, cols(h)], preferred_element_type=jnp.float32)

        def fetch(n):
            @pl.when(jnp.logical_not(jnp.logical_and(last, n >= 4 * NB)))
            def _():
                a_copy(lax.rem(n, 4 * NB)).start()

        def lead(h):
            def block(n):
                if h == 0:
                    a_copy(n).wait()
                multiply(n, h)
                if h == 1:
                    fetch(n + RING)

                send_lead(n, h)

            def one(n):
                @pl.when(jnp.logical_or(k > 0, n > 1))
                def _():
                    block(n)
            loop(0, G, one if h == 0 else block)

        @pl.when(k > 0)
        def _():
            pl.semaphore_wait(cr_0, 1)
        lead(0)

        @pl.when(k == 0)
        def _():
            x0_copy(far, 0, 1, X0C).wait_recv()

        @pl.when(jnp.logical_and(k > 0, home))
        def _():
            finish_half(1, jnp.bool_(False))
            s_publish(par, sacc[...])
            signal(cr_1, xn)
            signal(cr_1, yn)

        @pl.when(jnp.logical_and(k > 0, away))
        def _():
            x_bytes(G * BR, 1).wait_recv()
        lead(1)

        @pl.when(k > 0)
        def _():
            drain_forward()
            pl.semaphore_wait(cr_1, 1)

            @pl.when(away)
            def _():
                pl.semaphore_wait(cr_2, 1)

        def step(n):
            a_copy(n).wait()
            multiply(n, None)
            fetch(n + RING)
            at = block_of(n) - jnp.where(n < 2 * NB, other, same)
            return lax.div(at, PIECE), lax.div(lax.rem(at, PIECE), BR)

        def part_one(n):
            t, b = step(n)

            @pl.when(jnp.logical_and(t == 0, jnp.logical_not(jnp.logical_and(hold_a, b == NB - 1))))
            def _():
                c_a(b).start()

            @pl.when(jnp.logical_and(t == 1, away))
            def _():
                c_gy(b).start()
        loop(G, 2 * NB, part_one)

        @pl.when(k == 0)
        def _():
            first_mass()

            @pl.when(away)
            def _():
                s0_copy(row).start()

            @pl.when(home)
            def _():
                v_in.start()
                d_copy(1 - row).wait_recv()
                s0_copy(1 - row).wait_recv()
                s_publish(0, s0buf[0] + s0buf[1])

        def add_into(start, b, src):
            def add(c):
                at = rows_of(start + b * BR + c * CH, CH)
                ybuf[at, :] = ybuf[at, :] + src[rows_of(b * BR + c * CH, CH), :]
            loop(0, BR // CH, add)

        def send_on(copy, b):
            @pl.when(b < E)
            def _():
                copy(b).start()

            @pl.when(b >= E)
            def _():
                copy(b, 0).start()

        def part_two(n):
            b = n - 2 * NB
            step(n)

            @pl.when(jnp.logical_and(away, jnp.logical_not(jnp.logical_and(hold_dy, b == NB - 1))))
            def _():
                c_dy(b).start()

            @pl.when(home)
            def _():
                @pl.when(lax.rem(b, G) == 0)
                def _():
                    c_gy(b, n=G).wait_recv()
                add_into(other + PIECE, b, rgy)
                send_on(c_fx, b)
        loop(2 * NB, 3 * NB, part_two)

        @pl.when(home)
        def _():
            loop(E, NB, lambda b: c_fx(b, 1).start())

            @pl.when(hold_a)
            def _():
                held_a().start()

        def part_three(n):
            b = n - 3 * NB
            step(n)

            @pl.when(away)
            def _():
                @pl.when(lax.rem(b, G) == 0)
                def _():
                    c_a(b, n=G).wait_recv()
                add_into(same, b, ra)
                send_on(c_fy, b)
        loop(3 * NB, 4 * NB, part_three)

        @pl.when(away)
        def _away():
            loop(E, NB, lambda b: c_fy(b, 1).start())

            @pl.when(hold_dy)
            def _():
                held_dy().start()

            @pl.when(k == 0)
            def _():
                x0_copy(mine, 0, None, X0C).wait_send()
                v_copy(row).wait_send()
                d_copy(row).wait_send()
                s0_copy(row).wait_send()

            @pl.when(more)
            def _():
                signal(cr_2, mate)
                signal(cr_2, xn)
            c_a(0, n=NB).wait_send()
            c_gy(0, n=NB).wait_send()
            c_dy(0, NB).wait_send()

            @pl.when(more)
            def _():
                x_bytes(2 * PIECE - G * BR, 0).wait_recv()

        @pl.when(home)
        def _home():
            @pl.when(more)
            def _():
                signal(cr_0, yn)

            @pl.when(k == 0)
            def _():
                spread(1 - row)
                x0_copy(mine, 0, None, X0C).wait_send()
                v_copy(1 - row).wait_recv()
                v_in.wait()

            @pl.when(k > 0)
            def _():
                x_bytes(2 * PIECE, 0).wait_send()

            s_bytes(par).wait_recv()
            s_bytes(par).wait_send()
            mass = ((sbuf[par, 0] + sbuf[par, 1]) + (sbuf[par, 2] + sbuf[par, 3])) / VERTS
            coef[...] = jnp.broadcast_to(DAMPING * mass + (1.0 - DAMPING), (8, VECS))

            @pl.when(more)
            def _():
                pl.semaphore_wait(cr_2, 1)

            @pl.when(more)
            def _():
                c_a(0, n=NB).wait_send()
            for b in range(0, E, G):
                c_a(b, n=G).wait_recv()

            @pl.when(hold_a)
            def _():
                c_a(E, n=G - 1).wait_recv()

            @pl.when(jnp.logical_not(hold_a))
            def _():
                c_a(E, n=G).wait_recv()

            @pl.when(hold_dy)
            def _():
                c_dy(0, NB - 1).wait_recv()

            @pl.when(jnp.logical_not(hold_dy))
            def _():
                c_dy(0, NB).wait_recv()
            sacc[...] = lax.fori_loop(0, E, lambda b, acc: finish(b, None, last, acc), jnp.zeros((8, VECS), jnp.float32))

            @pl.when(more)
            def _():
                signal(cr_0, xn)
                finish_half(0, jnp.bool_(False))

            @pl.when(last)
            def _():
                finish_last()

        return carry

    lax.fori_loop(0, SWEEPS, sweep, 0)

    drain_forward()

    @pl.when(home)
    def _():
        c_a(0, n=NB).wait_send()
        o_remote(1 - row, 0, n=NB).wait_send()

    @pl.when(away)
    def _():
        o_remote(1 - row, 0, n=NB).wait_recv()


def solution(mesh):
    dma = pltpu.SemaphoreType.DMA
    reg = pltpu.SemaphoreType.REGULAR

    def in_hbm(a):
        return pltpu.with_memory_space_constraint(a, pltpu.HBM)

    def local_sweeps(mat_tile, x_piece, tele_piece, dang_piece):
        part = pltpu.VMEM((PIECE, VECS), jnp.float32)
        return pl.pallas_call(
            kernel,
            name="sweeps",
            out_shape=jax.ShapeDtypeStruct((PIECE, VECS), jnp.float32),
            in_specs=[pl.BlockSpec(memory_space=pltpu.HBM)] * 4,
            out_specs=pl.BlockSpec(memory_space=pltpu.VMEM),
            scratch_shapes=[
                pltpu.VMEM((RING, BR, COLS), jnp.bfloat16),
                pltpu.VMEM((COLS, VECS), jnp.bfloat16),
                pltpu.VMEM((ROWS, VECS), jnp.float32),
                part, part, part, part, part,
                pltpu.VMEM((COLS, VECS), jnp.float32),
                pltpu.VMEM((COLS, 128), jnp.bfloat16),
                pltpu.VMEM((2, PIECE // 128, 128), jnp.int32),
                pltpu.VMEM((2, 4, 1, VECS), jnp.float32),
                pltpu.VMEM((2, 8, VECS), jnp.float32),
                pltpu.VMEM((8, VECS), jnp.float32),
                pltpu.VMEM((8, VECS), jnp.float32),
                dma((RING,)), dma((2 * X0C,)), dma, dma((2,)),
                dma, dma((NB // G,)), dma, dma((NB // G,)), dma, dma, dma, dma((E // G + 4,)), dma, dma((E // G + 4,)),
                dma, dma((2,)), dma, dma((2,)), dma, dma, dma, reg, reg, reg,
            ],
            compiler_params=pltpu.CompilerParams(
                collective_id=0, has_side_effects=True, vmem_limit_bytes=53_300_000),
            cost_estimate=pl.CostEstimate(
                flops=2 * ROWS * COLS * VECS * SWEEPS, bytes_accessed=2 * ROWS * COLS * SWEEPS, transcendentals=0),
        )(mat_tile, x_piece, tele_piece, in_hbm(dang_piece.reshape(PIECE // 128, 128)))

    vec_spec = P(('col', 'row'), None)
    return jax.shard_map(local_sweeps, mesh=mesh,
                         in_specs=(P('row', 'col'), vec_spec, vec_spec, P(('col', 'row'))),
                         out_specs=vec_spec, check_vma=False)
```
